8 devices in a mesh: inst: 1 (over z), qy: 2 (over y), qx: 4 (over x, core).
Axes of the slice: x: 2, y: 2, z: 1, core: 2. Of those that a mesh axis runs over, the one named last changes fastest.
Arguments:
- cost_diag: float32 [2097152], P(('inst', 'qx', 'qy'))
- gammas: float32 [8], replicated
- betas: float32 [8], replicated
Outputs:
- output 1: float32 [1], P('inst')
- output 2: float32 [2097152], P(('inst', 'qx', 'qy'))
- output 3: float32 [2097152], P(('inst', 'qx', 'qy'))
All inputs are finite; a program needn't handle non-finite values.
Results may differ from the reference program's by a relative error of at most 0.001.
Values sent between devices are 32-bit elements.
A program may use at most 1 GiB of HBM per device.

```python
import math
import jax
import jax.numpy as jnp
from jax import lax

STATE = 2097152
LAYERS = 8
DEGREE = 3

QUBITS = int(math.log2(STATE))
EDGES = DEGREE * QUBITS // 2


def setup_inputs(seed: int = 0, part: int = 0) -> dict:
    base_key = jax.random.key(seed)
    part_key = jax.random.fold_in(base_key, part)
    key_offset, key_weight = jax.random.split(part_key)
    first_node = jnp.arange(EDGES, dtype=jnp.int32) % QUBITS
    offsets = jax.random.randint(key_offset, (EDGES,), 1, QUBITS, dtype=jnp.int32)
    second_node = (first_node + offsets) % QUBITS
    weights = jax.random.uniform(key_weight, (EDGES,), jnp.float32, 0.5, 1.5) * (2.0 / math.sqrt(EDGES))
    basis_index = jnp.arange(STATE, dtype=jnp.int32)

    def add_edge(edge_id, cost_acc):
        cut_bit = ((basis_index >> first_node[edge_id]) ^ (basis_index >> second_node[edge_id])) & 1
        return cost_acc + weights[edge_id] * cut_bit.astype(jnp.float32)

    cost_diag = lax.fori_loop(0, EDGES, add_edge, jnp.zeros((STATE,), jnp.float32))
    key_gamma, key_beta = jax.random.split(jax.random.key(seed + 1))
    gammas = jax.random.uniform(key_gamma, (LAYERS,), jnp.float32, 0.3, 1.0)
    betas = jax.random.uniform(key_beta, (LAYERS,), jnp.float32, 0.4, 1.2)
    return {'cost_diag': cost_diag, 'gammas': gammas, 'betas': betas}


def apply_mixer(state_re, state_im, cos_half, sin_half):
    for qubit_id in range(QUBITS):
        view_shape = (STATE >> (qubit_id + 1), 2, 1 << qubit_id)
        view_re = state_re.reshape(view_shape)
        view_im = state_im.reshape(view_shape)
        flip_re = jnp.flip(view_re, axis=1)
        flip_im = jnp.flip(view_im, axis=1)
        state_re = (cos_half * view_re + sin_half * flip_im).reshape(STATE)
        state_im = (cos_half * view_im - sin_half * flip_re).reshape(STATE)
    return state_re, state_im


def reference(cost_diag, gammas, betas):
    def layer_step(scan_carry, angles):
        state_re, state_im = scan_carry
        layer_gamma, layer_beta = angles
        phase_angle = layer_gamma * cost_diag
        cos_phase = jnp.cos(phase_angle)
        sin_phase = jnp.sin(phase_angle)
        new_re = state_re * cos_phase + state_im * sin_phase
        new_im = state_im * cos_phase - state_re * sin_phase
        cos_half = jnp.cos(0.5 * layer_beta)
        sin_half = jnp.sin(0.5 * layer_beta)
        return apply_mixer(new_re, new_im, cos_half, sin_half), None

    init_state = (jnp.ones((STATE,), jnp.float32), jnp.zeros((STATE,), jnp.float32))
    final_state, layer_outs = lax.scan(layer_step, init_state, (gammas, betas))
    state_re, state_im = final_state
    energy = jnp.sum(cost_diag * (state_re * state_re + state_im * state_im)) / STATE
    return energy.reshape(1), state_re, state_im
```

```python
import functools
import jax
import jax.numpy as jnp
from jax import lax
from jax.experimental import pallas as pl
from jax.experimental.pallas import tpu as pltpu
from jax.sharding import PartitionSpec as P

LANES = 128
LAYERS = 8
HIGH = (8, 4)
LOW = (4, 8)


def rotate(re, im, cos_half, sin_half):
    count = len(re)
    step = 1
    while step < count:
        new_re = [cos_half * re[i] + sin_half * im[i ^ step] for i in range(count)]
        new_im = [cos_half * im[i] - sin_half * re[i ^ step] for i in range(count)]
        re, im = new_re, new_im
        step *= 2
    return re, im


def sublane_rotate(re, im, cos_half, sin_half):
    row = lax.broadcasted_iota(jnp.int32, (8, LANES), 0)
    for step in (1, 2, 4):
        bit_set = (row & step) != 0

        def flip(value):
            down = pltpu.roll(value, step, 0)
            if step == 4:
                return down
            return jnp.where(bit_set, down, pltpu.roll(value, 8 - step, 0))

        flip_re = [flip(value) for value in re]
        flip_im = [flip(value) for value in im]
        re, im = ([cos_half * r + sin_half * fi for r, fi in zip(re, flip_im)],
                  [cos_half * i - sin_half * fr for i, fr in zip(im, flip_re)])
    return re, im


def lane_matrix(cos_half, sin_half):
    row = lax.broadcasted_iota(jnp.int32, (LANES, LANES), 0)
    col = lax.broadcasted_iota(jnp.int32, (LANES, LANES), 1)
    diff = row ^ col
    cos_full = jnp.broadcast_to(cos_half[0:1], (LANES, LANES))
    sin_full = jnp.broadcast_to(sin_half[0:1], (LANES, LANES))
    mag = jnp.ones((LANES, LANES), jnp.float32)
    weight = jnp.zeros((LANES, LANES), jnp.int32)
    for bit in range(7):
        on = (diff >> bit) & 1
        mag = mag * jnp.where(on == 1, sin_full, cos_full)
        weight = weight + on
    quarter = weight & 3
    zero = jnp.zeros_like(mag)
    real = jnp.where(quarter == 0, mag, jnp.where(quarter == 2, -mag, zero))
    imag = jnp.where(quarter == 1, -mag, jnp.where(quarter == 3, mag, zero))
    return real, imag


def kernel(cost, gammas, betas, energy, out_re, out_im,
           cost_swap, recv_high, recv_low, send_high, send_low, work, cos_buf, sin_buf,
           rows_in, rows_out, matrix, energy_part, energy_all,
           cost_send, cost_recv, high_send, high_recv, low_send, low_recv, e_send, e_recv):
    qx = lax.axis_index('qx')
    qy = lax.axis_index('qy')
    bits = (qy, qx % 2, qx // 2)

    def flipped(offset):
        return [1 - bit if (offset >> i) & 1 else bit for i, bit in enumerate(bits)]

    def block(offset):
        y, core, x = flipped(offset)
        return (x * 2 + core) * 2 + y

    def peer(offset):
        y, core, x = flipped(offset)
        return {'qy': y, 'qx': x * 2 + core}

    barrier = pltpu.get_barrier_semaphore()
    for offset in range(1, 8):
        pl.semaphore_signal(barrier, inc=1, device_id=peer(offset), device_id_type=pl.DeviceIdType.MESH)
    pl.semaphore_wait(barrier, 7)

    for offset in range(1, 8):
        pltpu.make_async_remote_copy(
            src_ref=cost.at[block(offset)], dst_ref=cost_swap.at[offset],
            send_sem=cost_send, recv_sem=cost_recv,
            device_id=peer(offset), device_id_type=pl.DeviceIdType.MESH).start()

    def half_angle(layer):
        angle = jnp.full((8, LANES), 0.5 * betas[layer], jnp.float32)
        return jnp.cos(angle), jnp.sin(angle)

    def group(split, chunk, j):
        if split is HIGH:
            return pl.multiple_of((chunk * 4 + j) * 8, 8)
        return pl.multiple_of((j * 4 + chunk) * 8, 8)

    def cost_rows(swapped, offset, start):
        if swapped:
            return cost_swap[offset, pl.ds(start, 8), :]
        return cost[block(offset), pl.ds(start, 8), :]

    def trig(layer, split, swapped, chunk):
        gamma = gammas[layer]

        def body(j, carry):
            start = group(split, chunk, j)
            row = pl.multiple_of(j * 8, 8)
            for offset in range(8):
                angle = gamma * cost_rows(swapped, offset, start)
                cos_buf[offset, pl.ds(row, 8), :] = jnp.cos(angle)
                sin_buf[offset, pl.ds(row, 8), :] = jnp.sin(angle)
            return carry

        lax.fori_loop(0, split[1], body, 0)

    def wait_all(buffer, sem, chunk):
        part = buffer.at[chunk, pl.ds(1, 7)]
        pltpu.make_async_copy(part, part, sem.at[chunk]).wait()

    def layer_step(layer, split, first):
        swapped = split is HIGH
        if swapped:
            recv, recv_sem, send, send_sem, target, target_sem, out_split = (
                recv_high, high_recv, send_low, low_send, recv_low, low_recv, LOW)
        else:
            recv, recv_sem, send, send_sem, target, target_sem, out_split = (
                recv_low, low_recv, send_high, high_send, recv_high, high_recv, HIGH)
        chunks, per_slot = split
        cos_half, sin_half = half_angle(layer)
        if not first:
            cos_prev, sin_prev = half_angle(layer - 1)
        real, imag = lane_matrix(cos_half, sin_half)
        matrix[0:LANES, 0:LANES] = real
        matrix[0:LANES, LANES:] = imag
        matrix[LANES:, 0:LANES] = -imag
        matrix[LANES:, LANES:] = real

        def in_chunk(chunk, carry):
            trig(layer, split, swapped, chunk)
            if not first:
                wait_all(recv, recv_sem, chunk)

            def slots(j, carry):
                row = pl.multiple_of(j * 8, 8)
                cos_phase = [cos_buf[o, pl.ds(row, 8), :] for o in range(8)]
                sin_phase = [sin_buf[o, pl.ds(row, 8), :] for o in range(8)]
                if first:
                    re = cos_phase
                    im = [-value for value in sin_phase]
                else:
                    old_re = [recv[chunk, o, 0, pl.ds(row, 8), :] for o in range(8)]
                    old_im = [recv[chunk, o, 1, pl.ds(row, 8), :] for o in range(8)]
                    old_re, old_im = rotate(old_re, old_im, cos_prev, sin_prev)
                    re = [r * c + i * s for r, i, c, s in zip(old_re, old_im, cos_phase, sin_phase)]
                    im = [i * c - r * s for r, i, c, s in zip(old_re, old_im, cos_phase, sin_phase)]
                re, im = rotate(re, im, cos_half, sin_half)
                re, im = sublane_rotate(re, im, cos_half, sin_half)
                for o in range(8):
                    at = pl.multiple_of(o * per_slot * 8 + row, 8)
                    rows_in[pl.ds(at, 8), 0:LANES] = re[o]
                    rows_in[pl.ds(at, 8), LANES:] = im[o]
                return carry

            lax.fori_loop(0, per_slot, slots, 0)
            count = 64 * per_slot
            for base in range(0, count, 256):
                rows_out[base:base + 256, :] = lax.dot(
                    rows_in[base:base + 256, :], matrix[...],
                    precision=lax.Precision.HIGHEST, preferred_element_type=jnp.float32)

            def within(o, carry):
                base = pl.multiple_of(o * per_slot * 8, 8)
                re = [rows_out[pl.ds(base + 8 * j, 8), 0:LANES] for j in range(per_slot)]
                im = [rows_out[pl.ds(base + 8 * j, 8), LANES:] for j in range(per_slot)]
                re, im = rotate(re, im, cos_half, sin_half)
                for j in range(per_slot):
                    start = group(split, chunk, j)
                    work[o, 0, pl.ds(start, 8), :] = re[j]
                    work[o, 1, pl.ds(start, 8), :] = im[j]
                return carry

            lax.fori_loop(0, 8, within, 0)
            return carry

        lax.fori_loop(0, chunks, in_chunk, 0)

        out_chunks, out_per_slot = out_split

        def out_chunk(chunk, carry):
            def across(o, slot_target):
                re = [work[o, 0, pl.ds(group(out_split, chunk, j), 8), :] for j in range(out_per_slot)]
                im = [work[o, 1, pl.ds(group(out_split, chunk, j), 8), :] for j in range(out_per_slot)]
                re, im = rotate(re, im, cos_half, sin_half)
                for j in range(out_per_slot):
                    slot_target[chunk, o, 0, 8 * j:8 * j + 8, :] = re[j]
                    slot_target[chunk, o, 1, 8 * j:8 * j + 8, :] = im[j]

            def body(o, carry):
                across(o, send)
                return carry

            lax.fori_loop(1, 8, body, 0)
            for offset in range(1, 8):
                pltpu.make_async_remote_copy(
                    src_ref=send.at[chunk, offset], dst_ref=target.at[chunk, offset],
                    send_sem=send_sem.at[chunk], recv_sem=target_sem.at[chunk],
                    device_id=peer(offset), device_id_type=pl.DeviceIdType.MESH).start()
            across(0, target)
            return carry

        def drain(chunk, carry):
            wait_all(send, send_sem, chunk)
            return carry

        return out_chunk, drain, out_chunks

    def run_layer(layer, split, first, reuse):
        out_chunk, drain, out_chunks = layer_step(layer, split, first)
        if reuse:
            lax.fori_loop(0, out_chunks, drain, 0)
        lax.fori_loop(0, out_chunks, out_chunk, 0)

    run_layer(0, LOW, True, False)
    cost_swap[0] = cost[block(0)]
    part = cost_swap.at[pl.ds(1, 7)]
    pltpu.make_async_copy(part, part, cost_recv).wait()
    run_layer(1, HIGH, False, False)

    def pair(i, carry):
        run_layer(2 * i + 2, LOW, False, True)
        run_layer(2 * i + 3, HIGH, False, True)
        return carry

    lax.fori_loop(0, LAYERS // 2 - 1, pair, 0)

    cos_half, sin_half = half_angle(LAYERS - 1)
    energy_part[...] = jnp.zeros((8, LANES), jnp.float32)

    def final_chunk(chunk, carry):
        wait_all(recv_low, low_recv, chunk)

        def slots(j, carry):
            row = pl.multiple_of(j * 8, 8)
            start = group(LOW, chunk, j)
            re = [recv_low[chunk, o, 0, pl.ds(row, 8), :] for o in range(8)]
            im = [recv_low[chunk, o, 1, pl.ds(row, 8), :] for o in range(8)]
            re, im = rotate(re, im, cos_half, sin_half)
            total = energy_part[...]
            for o in range(8):
                at = block(o)
                out_re[at, pl.ds(start, 8), :] = re[o]
                out_im[at, pl.ds(start, 8), :] = im[o]
                total = total + cost[at, pl.ds(start, 8), :] * (re[o] * re[o] + im[o] * im[o])
            energy_part[...] = total
            return carry

        lax.fori_loop(0, LOW[1], slots, 0)
        return carry

    lax.fori_loop(0, LOW[0], final_chunk, 0)

    me = block(0)
    for offset in range(1, 8):
        pltpu.make_async_remote_copy(
            src_ref=energy_part, dst_ref=energy_all.at[me],
            send_sem=e_send.at[offset], recv_sem=e_recv.at[offset],
            device_id=peer(offset), device_id_type=pl.DeviceIdType.MESH).start()
    energy_all[me] = energy_part[...]
    for chunk in range(HIGH[0]):
        wait_all(send_high, high_send, chunk)
    for chunk in range(LOW[0]):
        wait_all(send_low, low_send, chunk)
    part = cost.at[pl.ds(1, 7)]
    pltpu.make_async_copy(part, part, cost_send).wait()
    for offset in range(1, 8):
        pltpu.make_async_copy(energy_part, energy_part, e_send.at[offset]).wait()
        pltpu.make_async_copy(energy_part, energy_part, e_recv.at[offset]).wait()
    total = energy_all[0]
    for i in range(1, 8):
        total = total + energy_all[i]
    energy[0] = jnp.sum(total) * (1.0 / (1 << 21))


def solution(mesh):
    state_spec = P(('inst', 'qx', 'qy'))

    def device_body(cost_local, gammas, betas):
        local_len = cost_local.shape[0]
        rows = local_len // (8 * LANES)
        shape = (8, rows, LANES)
        f32 = jnp.float32
        vmem = pl.BlockSpec(memory_space=pltpu.VMEM)
        smem = pl.BlockSpec(memory_space=pltpu.SMEM)
        dma = pltpu.SemaphoreType.DMA
        high = (HIGH[0], 8, 2, 8 * HIGH[1], LANES)
        low = (LOW[0], 8, 2, 8 * LOW[1], LANES)
        energy, state_re, state_im = pl.pallas_call(
            kernel,
            out_shape=(jax.ShapeDtypeStruct((1,), f32),
                       jax.ShapeDtypeStruct(shape, f32), jax.ShapeDtypeStruct(shape, f32)),
            in_specs=[vmem, smem, smem],
            out_specs=(smem, vmem, vmem),
            scratch_shapes=[
                pltpu.VMEM(shape, f32),
                pltpu.VMEM(high, f32), pltpu.VMEM(low, f32),
                pltpu.VMEM(high, f32), pltpu.VMEM(low, f32),
                pltpu.VMEM((8, 2, rows, LANES), f32),
                pltpu.VMEM((8, 8 * LOW[1], LANES), f32), pltpu.VMEM((8, 8 * LOW[1], LANES), f32),
                pltpu.VMEM((64 * LOW[1], 2 * LANES), f32), pltpu.VMEM((64 * LOW[1], 2 * LANES), f32),
                pltpu.VMEM((2 * LANES, 2 * LANES), f32),
                pltpu.VMEM((8, LANES), f32), pltpu.VMEM((8, 8, LANES), f32),
                dma, dma,
                dma((HIGH[0],)), dma((HIGH[0],)), dma((LOW[0],)), dma((LOW[0],)),
                dma((8,)), dma((8,)),
            ],
            compiler_params=pltpu.CompilerParams(collective_id=0, has_side_effects=True),
            name='qaoa',
        )(cost_local.reshape(shape), gammas, betas)
        return energy, state_re.reshape(local_len), state_im.reshape(local_len)

    return jax.shard_map(device_body, mesh=mesh, in_specs=(state_spec, P(), P()),
                         out_specs=(P('inst'), state_spec, state_spec), check_vma=False)
```

```python
import jax
import jax.numpy as jnp
from jax import lax
from jax.experimental import pallas as pl
from jax.experimental.pallas import tpu as pltpu
from jax.sharding import PartitionSpec as P

LANES = 128
LAYERS = 8
SUB = 2
PER_SUB = 8 // SUB


def rotate(re, im, cos_half, sin_half):
    count = len(re)
    step = 1
    while step < count:
        new_re = [cos_half * re[i] + sin_half * im[i ^ step] for i in range(count)]
        new_im = [cos_half * im[i] - sin_half * re[i ^ step] for i in range(count)]
        re, im = new_re, new_im
        step *= 2
    return re, im


def sublane_rotate(re, im, cos_half, sin_half):
    row = lax.broadcasted_iota(jnp.int32, (8, LANES), 0)
    for step in (1, 2, 4):
        bit_set = (row & step) != 0

        def flip(value):
            down = pltpu.roll(value, step, 0)
            if step == 4:
                return down
            return jnp.where(bit_set, down, pltpu.roll(value, 8 - step, 0))

        flip_re = [flip(value) for value in re]
        flip_im = [flip(value) for value in im]
        re, im = ([cos_half * r + sin_half * fi for r, fi in zip(re, flip_im)],
                  [cos_half * i - sin_half * fr for i, fr in zip(im, flip_re)])
    return re, im


def lane_matrix(cos_half, sin_half):
    row = lax.broadcasted_iota(jnp.int32, (LANES, LANES), 0)
    col = lax.broadcasted_iota(jnp.int32, (LANES, LANES), 1)
    diff = row ^ col
    cos_full = jnp.broadcast_to(cos_half[0:1], (LANES, LANES))
    sin_full = jnp.broadcast_to(sin_half[0:1], (LANES, LANES))
    mag = jnp.ones((LANES, LANES), jnp.float32)
    weight = jnp.zeros((LANES, LANES), jnp.int32)
    for bit in range(7):
        on = (diff >> bit) & 1
        mag = mag * jnp.where(on == 1, sin_full, cos_full)
        weight = weight + on
    quarter = weight & 3
    zero = jnp.zeros_like(mag)
    real = jnp.where(quarter == 0, mag, jnp.where(quarter == 2, -mag, zero))
    imag = jnp.where(quarter == 1, -mag, jnp.where(quarter == 3, mag, zero))
    return real, imag


def kernel(cost, gammas, betas, energy, out_re, out_im,
           cost_swap, recv, send, work, cos_buf, sin_buf, rows_in, matrix,
           energy_part, energy_all, cost_send, cost_recv, send_sem, recv_sem, e_send, e_recv):
    qx = lax.axis_index('qx')
    qy = lax.axis_index('qy')
    bits = (qy, qx % 2, qx // 2)

    def flipped(offset):
        return [1 - bit if (offset >> i) & 1 else bit for i, bit in enumerate(bits)]

    def block(offset):
        y, core, x = flipped(offset)
        return (x * 2 + core) * 2 + y

    def peer(offset):
        y, core, x = flipped(offset)
        return {'qy': y, 'qx': x * 2 + core}

    barrier = pltpu.get_barrier_semaphore()
    for offset in range(1, 8):
        pl.semaphore_signal(barrier, inc=1, device_id=peer(offset), device_id_type=pl.DeviceIdType.MESH)
    pl.semaphore_wait(barrier, 7)

    for offset in range(1, 8):
        pltpu.make_async_remote_copy(
            src_ref=cost.at[block(offset)], dst_ref=cost_swap.at[offset],
            send_sem=cost_send, recv_sem=cost_recv,
            device_id=peer(offset), device_id_type=pl.DeviceIdType.MESH).start()

    def half_angle(layer):
        angle = jnp.full((8, LANES), 0.5 * betas[layer], jnp.float32)
        return jnp.cos(angle), jnp.sin(angle)

    def wait_all(buffer, sem, at):
        part = buffer.at[(*at, pl.ds(1, 7))]
        pltpu.make_async_copy(part, part, sem.at[at]).wait()

    def run_layer(layer, odd, first, reuse):
        source, target = (0, 1) if odd else (1, 0)

        def quarter(held, mixed):
            return (held, mixed) if odd else (mixed, held)

        cos_half, sin_half = half_angle(layer)
        if not first:
            cos_prev, sin_prev = half_angle(layer - 1)
        gamma = gammas[layer]
        real, imag = lane_matrix(cos_half, sin_half)
        matrix[0:LANES, 0:LANES] = real
        matrix[0:LANES, LANES:] = imag
        matrix[LANES:, 0:LANES] = -imag
        matrix[LANES:, LANES:] = real

        def half(held, carry):
            def trig(r, carry):
                row = pl.multiple_of(r * 8, 8)
                for mixed in range(2):
                    a, b = quarter(held, mixed)
                    start = pl.multiple_of((a * 16 + b * 8 + r) * 8, 8)
                    for o in range(8):
                        if odd:
                            rows = cost[block(o), pl.ds(start, 8), :]
                        else:
                            rows = cost_swap[o, pl.ds(start, 8), :]
                        angle = gamma * rows
                        cos_buf[mixed * 8 + o, pl.ds(row, 8), :] = jnp.cos(angle)
                        sin_buf[mixed * 8 + o, pl.ds(row, 8), :] = jnp.sin(angle)
                return carry

            lax.fori_loop(0, 8, trig, 0)

            def sub_step(sub, carry):
                if not first:
                    for mixed in range(2):
                        wait_all(recv, recv_sem, (source, *quarter(held, mixed), sub))

                def pair_step(pair, carry):
                    def slots(i, carry):
                        row = pl.multiple_of((sub * PER_SUB + pair * 2 + i) * 8, 8)
                        cos_phase = [cos_buf[o, pl.ds(row, 8), :] for o in range(16)]
                        sin_phase = [sin_buf[o, pl.ds(row, 8), :] for o in range(16)]
                        if first:
                            re = cos_phase
                            im = [-value for value in sin_phase]
                        else:
                            local = pl.multiple_of((pair * 2 + i) * 8, 8)
                            old = [[recv[(source, *quarter(held, mixed), sub, o, c, pl.ds(local, 8))]
                                    for mixed in range(2) for o in range(8)] for c in range(2)]
                            old_re, old_im = rotate(*old, cos_prev, sin_prev)
                            re = [r * c + i * s for r, i, c, s in zip(old_re, old_im, cos_phase, sin_phase)]
                            im = [i * c - r * s for r, i, c, s in zip(old_re, old_im, cos_phase, sin_phase)]
                        re, im = rotate(re, im, cos_half, sin_half)
                        re, im = sublane_rotate(re, im, cos_half, sin_half)
                        for o in range(16):
                            at = pl.multiple_of(o * 16 + i * 8, 8)
                            rows_in[pl.ds(at, 8), 0:LANES] = re[o]
                            rows_in[pl.ds(at, 8), LANES:] = im[o]
                        return carry

                    lax.fori_loop(0, 2, slots, 0)
                    work[sub * (PER_SUB // 2) + pair] = lax.dot(
                        rows_in[...], matrix[...],
                        precision=lax.Precision.HIGHEST, preferred_element_type=jnp.float32)
                    return carry

                lax.fori_loop(0, PER_SUB // 2, pair_step, 0)
                return carry

            lax.fori_loop(0, SUB, sub_step, 0)

            if reuse:
                for mixed in range(2):
                    for sub in range(SUB):
                        wait_all(send, send_sem, (target, *quarter(held, mixed), sub))

            def emit(mixed, carry):
                a, b = quarter(held, mixed)

                def across(o, buffer):
                    def part(r, c):
                        at = pl.multiple_of((mixed * 8 + o) * 16 + (r % 2) * 8, 8)
                        return work[r // 2, pl.ds(at, 8), c * LANES:(c + 1) * LANES]

                    re = [part(r, 0) for r in range(8)]
                    im = [part(r, 1) for r in range(8)]
                    re, im = rotate(re, im, cos_half, sin_half)
                    for r in range(8):
                        row = (r % PER_SUB) * 8
                        buffer[target, a, b, r // PER_SUB, o, 0, row:row + 8, :] = re[r]
                        buffer[target, a, b, r // PER_SUB, o, 1, row:row + 8, :] = im[r]

                def body(o, carry):
                    across(o, send)
                    return carry

                lax.fori_loop(1, 8, body, 0)
                for sub in range(SUB):
                    for offset in range(1, 8):
                        pltpu.make_async_remote_copy(
                            src_ref=send.at[target, a, b, sub, offset],
                            dst_ref=recv.at[target, a, b, sub, offset],
                            send_sem=send_sem.at[target, a, b, sub],
                            recv_sem=recv_sem.at[target, a, b, sub],
                            device_id=peer(offset), device_id_type=pl.DeviceIdType.MESH).start()
                across(0, recv)
                return carry

            lax.fori_loop(0, 2, emit, 0)
            return carry

        lax.fori_loop(0, 2, half, 0)

    run_layer(0, True, True, False)
    cost_swap[0] = cost[block(0)]
    part = cost_swap.at[pl.ds(1, 7)]
    pltpu.make_async_copy(part, part, cost_recv).wait()
    run_layer(1, False, False, False)

    def layer_pair(i, carry):
        run_layer(2 * i + 2, True, False, True)
        run_layer(2 * i + 3, False, False, True)
        return carry

    lax.fori_loop(0, LAYERS // 2 - 1, layer_pair, 0)

    cos_half, sin_half = half_angle(LAYERS - 1)
    energy_part[...] = jnp.zeros((8, LANES), jnp.float32)

    def final_half(a, carry):
        def final_sub(sub, carry):
            for b in range(2):
                wait_all(recv, recv_sem, (0, a, b, sub))

            def slots(i, carry):
                row = pl.multiple_of(i * 8, 8)
                old = [[recv[0, a, b, sub, o, c, pl.ds(row, 8), :] for b in range(2) for o in range(8)]
                       for c in range(2)]
                re, im = rotate(*old, cos_half, sin_half)
                total = energy_part[...]
                for b in range(2):
                    start = pl.multiple_of((a * 16 + b * 8 + sub * PER_SUB + i) * 8, 8)
                    for o in range(8):
                        at = block(o)
                        r, m = re[b * 8 + o], im[b * 8 + o]
                        out_re[at, pl.ds(start, 8), :] = r
                        out_im[at, pl.ds(start, 8), :] = m
                        total = total + cost[at, pl.ds(start, 8), :] * (r * r + m * m)
                energy_part[...] = total
                return carry

            lax.fori_loop(0, PER_SUB, slots, 0)
            return carry

        lax.fori_loop(0, SUB, final_sub, 0)
        return carry

    lax.fori_loop(0, 2, final_half, 0)

    me = block(0)
    for offset in range(1, 8):
        pltpu.make_async_remote_copy(
            src_ref=energy_part, dst_ref=energy_all.at[me],
            send_sem=e_send.at[offset], recv_sem=e_recv.at[offset],
            device_id=peer(offset), device_id_type=pl.DeviceIdType.MESH).start()
    energy_all[me] = energy_part[...]
    for par in range(2):
        for a in range(2):
            for b in range(2):
                for sub in range(SUB):
                    wait_all(send, send_sem, (par, a, b, sub))
    part = cost.at[pl.ds(1, 7)]
    pltpu.make_async_copy(part, part, cost_send).wait()
    for offset in range(1, 8):
        pltpu.make_async_copy(energy_part, energy_part, e_send.at[offset]).wait()
        pltpu.make_async_copy(energy_part, energy_part, e_recv.at[offset]).wait()
    total = energy_all[0]
    for i in range(1, 8):
        total = total + energy_all[i]
    energy[0] = jnp.sum(total) * (1.0 / (1 << 21))


def solution(mesh):
    state_spec = P(('inst', 'qx', 'qy'))

    def device_body(cost_local, gammas, betas):
        local_len = cost_local.shape[0]
        rows = local_len // (8 * LANES)
        shape = (8, rows, LANES)
        f32 = jnp.float32
        vmem = pl.BlockSpec(memory_space=pltpu.VMEM)
        smem = pl.BlockSpec(memory_space=pltpu.SMEM)
        dma = pltpu.SemaphoreType.DMA
        parts = (2, 2, 2, SUB, 8, 2, 8 * PER_SUB, LANES)
        energy, state_re, state_im = pl.pallas_call(
            kernel,
            out_shape=(jax.ShapeDtypeStruct((1,), f32),
                       jax.ShapeDtypeStruct(shape, f32), jax.ShapeDtypeStruct(shape, f32)),
            in_specs=[vmem, smem, smem],
            out_specs=(smem, vmem, vmem),
            scratch_shapes=[
                pltpu.VMEM(shape, f32),
                pltpu.VMEM(parts, f32), pltpu.VMEM(parts, f32),
                pltpu.VMEM((4, 2 * LANES, 2 * LANES), f32),
                pltpu.VMEM((16, 64, LANES), f32), pltpu.VMEM((16, 64, LANES), f32),
                pltpu.VMEM((2 * LANES, 2 * LANES), f32), pltpu.VMEM((2 * LANES, 2 * LANES), f32),
                pltpu.VMEM((8, LANES), f32), pltpu.VMEM((8, 8, LANES), f32),
                dma, dma,
                dma((2, 2, 2, SUB)), dma((2, 2, 2, SUB)),
                dma((8,)), dma((8,)),
            ],
            compiler_params=pltpu.CompilerParams(collective_id=0, has_side_effects=True),
            name='qaoa',
        )(cost_local.reshape(shape), gammas, betas)
        return energy, state_re.reshape(local_len), state_im.reshape(local_len)

    return jax.shard_map(device_body, mesh=mesh, in_specs=(state_spec, P(), P()),
                         out_specs=(P('inst'), state_spec, state_spec), check_vma=False)
```

```python
import jax
import jax.numpy as jnp
from jax import lax
from jax.experimental import pallas as pl
from jax.experimental.pallas import tpu as pltpu
from jax.sharding import PartitionSpec as P

LANES = 128
LAYERS = 8
SUB = 4
PER_SUB = 8 // SUB


def rotate(re, im, cos_half, sin_half):
    count = len(re)
    step = 1
    while step < count:
        new_re = [cos_half * re[i] + sin_half * im[i ^ step] for i in range(count)]
        new_im = [cos_half * im[i] - sin_half * re[i ^ step] for i in range(count)]
        re, im = new_re, new_im
        step *= 2
    return re, im


def sublane_rotate(re, im, cos_half, sin_half):
    row = lax.broadcasted_iota(jnp.int32, (8, LANES), 0)
    for step in (1, 2, 4):
        bit_set = (row & step) != 0

        def flip(value):
            down = pltpu.roll(value, step, 0)
            if step == 4:
                return down
            return jnp.where(bit_set, down, pltpu.roll(value, 8 - step, 0))

        flip_re = [flip(value) for value in re]
        flip_im = [flip(value) for value in im]
        re, im = ([cos_half * r + sin_half * fi for r, fi in zip(re, flip_im)],
                  [cos_half * i - sin_half * fr for i, fr in zip(im, flip_re)])
    return re, im


def lane_matrix(cos_half, sin_half):
    row = lax.broadcasted_iota(jnp.int32, (LANES, LANES), 0)
    col = lax.broadcasted_iota(jnp.int32, (LANES, LANES), 1)
    diff = row ^ col
    cos_full = jnp.broadcast_to(cos_half[0:1], (LANES, LANES))
    sin_full = jnp.broadcast_to(sin_half[0:1], (LANES, LANES))
    mag = jnp.ones((LANES, LANES), jnp.float32)
    weight = jnp.zeros((LANES, LANES), jnp.int32)
    for bit in range(7):
        on = (diff >> bit) & 1
        mag = mag * jnp.where(on == 1, sin_full, cos_full)
        weight = weight + on
    quarter = weight & 3
    zero = jnp.zeros_like(mag)
    real = jnp.where(quarter == 0, mag, jnp.where(quarter == 2, -mag, zero))
    imag = jnp.where(quarter == 1, -mag, jnp.where(quarter == 3, mag, zero))
    return real, imag


def kernel(cost_hbm, gammas, betas, energy_all, out_re, out_im,
           cost, cost_swap, recv, send, work, cos_buf, sin_buf, rows_in, matrix,
           energy_part, cost_in, cost_send, cost_recv, send_sem, recv_sem, e_send, e_recv):
    load = pltpu.make_async_copy(cost_hbm, cost, cost_in)
    load.start()
    qx = lax.axis_index('qx')
    qy = lax.axis_index('qy')
    bits = (qy, qx % 2, qx // 2)

    def flipped(offset):
        return [1 - bit if (offset >> i) & 1 else bit for i, bit in enumerate(bits)]

    def block(offset):
        y, core, x = flipped(offset)
        return (x * 2 + core) * 2 + y

    def peer(offset):
        y, core, x = flipped(offset)
        return {'qy': y, 'qx': x * 2 + core}

    barrier = pltpu.get_barrier_semaphore()
    for offset in range(1, 8):
        pl.semaphore_signal(barrier, inc=1, device_id=peer(offset), device_id_type=pl.DeviceIdType.MESH)
    pl.semaphore_wait(barrier, 7)
    load.wait()

    for offset in range(1, 8):
        pltpu.make_async_remote_copy(
            src_ref=cost.at[block(offset)], dst_ref=cost_swap.at[offset],
            send_sem=cost_send, recv_sem=cost_recv,
            device_id=peer(offset), device_id_type=pl.DeviceIdType.MESH).start()

    def half_angle(layer):
        angle = jnp.full((8, LANES), 0.5 * betas[layer], jnp.float32)
        return jnp.cos(angle), jnp.sin(angle)

    def wait_all(buffer, sem, at):
        part = buffer.at[(*at, pl.ds(1, 7))]
        pltpu.make_async_copy(part, part, sem.at[at]).wait()

    def run_layer(layer, odd, first, reuse):
        source, target = (0, 1) if odd else (1, 0)

        def quarter(held, mixed):
            return (held, mixed) if odd else (mixed, held)

        cos_half, sin_half = half_angle(layer)
        if not first:
            cos_prev, sin_prev = half_angle(layer - 1)
        gamma = gammas[layer]
        real, imag = lane_matrix(cos_half, sin_half)
        matrix[0:LANES, 0:LANES] = real
        matrix[0:LANES, LANES:] = imag
        matrix[LANES:, 0:LANES] = -imag
        matrix[LANES:, LANES:] = real

        def half(held, carry):
            def trig(r, carry):
                row = pl.multiple_of(r * 8, 8)
                for mixed in range(2):
                    a, b = quarter(held, mixed)
                    start = pl.multiple_of((a * 16 + b * 8 + r) * 8, 8)
                    for o in range(8):
                        if odd:
                            rows = cost[block(o), pl.ds(start, 8), :]
                        else:
                            rows = cost_swap[o, pl.ds(start, 8), :]
                        angle = gamma * rows
                        cos_buf[mixed * 8 + o, pl.ds(row, 8), :] = jnp.cos(angle)
                        sin_buf[mixed * 8 + o, pl.ds(row, 8), :] = jnp.sin(angle)
                return carry

            lax.fori_loop(0, 8, trig, 0)

            def sub_step(sub, carry):
                if not first:
                    for mixed in range(2):
                        wait_all(recv, recv_sem, (source, *quarter(held, mixed), sub))

                def pair_step(pair, carry):
                    def slots(i, carry):
                        row = pl.multiple_of((sub * PER_SUB + pair * 2 + i) * 8, 8)
                        cos_phase = [cos_buf[o, pl.ds(row, 8), :] for o in range(16)]
                        sin_phase = [sin_buf[o, pl.ds(row, 8), :] for o in range(16)]
                        if first:
                            re = cos_phase
                            im = [-value for value in sin_phase]
                        else:
                            local = pl.multiple_of((pair * 2 + i) * 8, 8)
                            old = [[recv[(source, *quarter(held, mixed), sub, o, c, pl.ds(local, 8))]
                                    for mixed in range(2) for o in range(8)] for c in range(2)]
                            old_re, old_im = rotate(*old, cos_prev, sin_prev)
                            re = [r * c + i * s for r, i, c, s in zip(old_re, old_im, cos_phase, sin_phase)]
                            im = [i * c - r * s for r, i, c, s in zip(old_re, old_im, cos_phase, sin_phase)]
                        re, im = rotate(re, im, cos_half, sin_half)
                        re, im = sublane_rotate(re, im, cos_half, sin_half)
                        for o in range(16):
                            at = pl.multiple_of(o * 16 + i * 8, 8)
                            rows_in[pl.ds(at, 8), 0:LANES] = re[o]
                            rows_in[pl.ds(at, 8), LANES:] = im[o]
                        return carry

                    lax.fori_loop(0, 2, slots, 0)
                    work[sub * (PER_SUB // 2) + pair] = lax.dot(
                        rows_in[...], matrix[...],
                        precision=lax.Precision.HIGHEST, preferred_element_type=jnp.float32)
                    return carry

                lax.fori_loop(0, PER_SUB // 2, pair_step, 0)
                return carry

            lax.fori_loop(0, SUB, sub_step, 0)

            if reuse:
                for mixed in range(2):
                    for sub in range(SUB):
                        wait_all(send, send_sem, (target, *quarter(held, mixed), sub))

            def emit(mixed, carry):
                a, b = quarter(held, mixed)

                def across(o, buffer):
                    def part(r, c):
                        at = pl.multiple_of((mixed * 8 + o) * 16 + (r % 2) * 8, 8)
                        return work[r // 2, pl.ds(at, 8), c * LANES:(c + 1) * LANES]

                    re = [part(r, 0) for r in range(8)]
                    im = [part(r, 1) for r in range(8)]
                    re, im = rotate(re, im, cos_half, sin_half)
                    for r in range(8):
                        row = (r % PER_SUB) * 8
                        buffer[target, a, b, r // PER_SUB, o, 0, row:row + 8, :] = re[r]
                        buffer[target, a, b, r // PER_SUB, o, 1, row:row + 8, :] = im[r]

                def body(o, carry):
                    across(o, send)
                    return carry

                lax.fori_loop(1, 8, body, 0)
                for sub in range(SUB):
                    for offset in range(1, 8):
                        pltpu.make_async_remote_copy(
                            src_ref=send.at[target, a, b, sub, offset],
                            dst_ref=recv.at[target, a, b, sub, offset],
                            send_sem=send_sem.at[target, a, b, sub],
                            recv_sem=recv_sem.at[target, a, b, sub],
                            device_id=peer(offset), device_id_type=pl.DeviceIdType.MESH).start()
                across(0, recv)
                return carry

            lax.fori_loop(0, 2, emit, 0)
            return carry

        lax.fori_loop(0, 2, half, 0)

    run_layer(0, True, True, False)
    cost_swap[0] = cost[block(0)]
    part = cost_swap.at[pl.ds(1, 7)]
    pltpu.make_async_copy(part, part, cost_recv).wait()
    run_layer(1, False, False, False)

    def layer_pair(i, carry):
        run_layer(2 * i + 2, True, False, True)
        run_layer(2 * i + 3, False, False, True)
        return carry

    lax.fori_loop(0, LAYERS // 2 - 1, layer_pair, 0)

    cos_half, sin_half = half_angle(LAYERS - 1)
    energy_part[...] = jnp.zeros((8, LANES), jnp.float32)

    def final_half(a, carry):
        def final_sub(sub, carry):
            for b in range(2):
                wait_all(recv, recv_sem, (0, a, b, sub))

            def slots(i, carry):
                row = pl.multiple_of(i * 8, 8)
                old = [[recv[0, a, b, sub, o, c, pl.ds(row, 8), :] for b in range(2) for o in range(8)]
                       for c in range(2)]
                re, im = rotate(*old, cos_half, sin_half)
                total = energy_part[...]
                for b in range(2):
                    start = pl.multiple_of((a * 16 + b * 8 + sub * PER_SUB + i) * 8, 8)
                    for o in range(8):
                        at = block(o)
                        r, m = re[b * 8 + o], im[b * 8 + o]
                        out_re[at, pl.ds(start, 8), :] = r
                        out_im[at, pl.ds(start, 8), :] = m
                        total = total + cost[at, pl.ds(start, 8), :] * (r * r + m * m)
                energy_part[...] = total
                return carry

            lax.fori_loop(0, PER_SUB, slots, 0)
            return carry

        lax.fori_loop(0, SUB, final_sub, 0)
        return carry

    lax.fori_loop(0, 2, final_half, 0)

    me = block(0)
    for offset in range(1, 8):
        pltpu.make_async_remote_copy(
            src_ref=energy_part, dst_ref=energy_all.at[me],
            send_sem=e_send.at[offset], recv_sem=e_recv.at[offset],
            device_id=peer(offset), device_id_type=pl.DeviceIdType.MESH).start()
    energy_all[me] = energy_part[...]
    for par in range(2):
        for a in range(2):
            for b in range(2):
                for sub in range(SUB):
                    wait_all(send, send_sem, (par, a, b, sub))
    part = cost.at[pl.ds(1, 7)]
    pltpu.make_async_copy(part, part, cost_send).wait()
    for offset in range(1, 8):
        pltpu.make_async_copy(energy_part, energy_part, e_send.at[offset]).wait()
        pltpu.make_async_copy(energy_part, energy_part, e_recv.at[offset]).wait()


def write_out(energy_all, in_re, in_im, energy, out_re, out_im, sem):
    copies = [pltpu.make_async_copy(in_re, out_re, sem.at[0]), pltpu.make_async_copy(in_im, out_im, sem.at[1])]
    for copy in copies:
        copy.start()
    total = energy_all[0]
    for i in range(1, 8):
        total = total + energy_all[i]
    energy[0] = jnp.sum(total) * (1.0 / (1 << 21))
    for copy in copies:
        copy.wait()


def solution(mesh):
    state_spec = P(('inst', 'qx', 'qy'))

    def device_body(cost_local, gammas, betas):
        local_len = cost_local.shape[0]
        rows = local_len // (8 * LANES)
        shape = (8, rows, LANES)
        f32 = jnp.float32
        vmem = pl.BlockSpec(memory_space=pltpu.VMEM)
        smem = pl.BlockSpec(memory_space=pltpu.SMEM)
        dma = pltpu.SemaphoreType.DMA
        parts = (2, 2, 2, SUB, 8, 2, 8 * PER_SUB, LANES)
        hbm = pl.BlockSpec(memory_space=pl.ANY)
        results = pl.pallas_call(
            kernel,
            out_shape=(pltpu.VMEM((8, 8, LANES), f32), pltpu.VMEM(shape, f32), pltpu.VMEM(shape, f32)),
            in_specs=[hbm, smem, smem],
            out_specs=(vmem, vmem, vmem),
            scratch_shapes=[
                pltpu.VMEM(shape, f32), pltpu.VMEM(shape, f32),
                pltpu.VMEM(parts, f32), pltpu.VMEM(parts, f32),
                pltpu.VMEM((4, 2 * LANES, 2 * LANES), f32),
                pltpu.VMEM((16, 64, LANES), f32), pltpu.VMEM((16, 64, LANES), f32),
                pltpu.VMEM((2 * LANES, 2 * LANES), f32), pltpu.VMEM((2 * LANES, 2 * LANES), f32),
                pltpu.VMEM((8, LANES), f32),
                dma, dma, dma,
                dma((2, 2, 2, SUB)), dma((2, 2, 2, SUB)),
                dma((8,)), dma((8,)),
            ],
            compiler_params=pltpu.CompilerParams(collective_id=0, has_side_effects=True),
            name='qaoa',
        )(cost_local.reshape(shape), gammas, betas)
        energy, state_re, state_im = pl.pallas_call(
            write_out,
            out_shape=(jax.ShapeDtypeStruct((1,), f32),
                       jax.ShapeDtypeStruct(shape, f32), jax.ShapeDtypeStruct(shape, f32)),
            in_specs=[vmem, vmem, vmem],
            out_specs=(smem, hbm, hbm),
            scratch_shapes=[dma((2,))],
            name='write_out',
        )(*[pltpu.with_memory_space_constraint(value, pltpu.VMEM) for value in results])
        return energy, state_re.reshape(local_len), state_im.reshape(local_len)

    return jax.shard_map(device_body, mesh=mesh, in_specs=(state_spec, P(), P()),
                         out_specs=(P('inst'), state_spec, state_spec), check_vma=False)
```

```python
import jax
import jax.numpy as jnp
from jax import lax
from jax.experimental import pallas as pl
from jax.experimental.pallas import tpu as pltpu
from jax.sharding import PartitionSpec as P

LANES = 128
LAYERS = 8
SUB = 4
PER_SUB = 8 // SUB
SEND_ORDER = (5, 7, 4, 6, 1, 3, 2)


def rotate(re, im, cos_half, sin_half):
    count = len(re)
    step = 1
    while step < count:
        new_re = [cos_half * re[i] + sin_half * im[i ^ step] for i in range(count)]
        new_im = [cos_half * im[i] - sin_half * re[i ^ step] for i in range(count)]
        re, im = new_re, new_im
        step *= 2
    return re, im


def sublane_rotate(re, im, cos_half, sin_half):
    row = lax.broadcasted_iota(jnp.int32, (8, LANES), 0)
    for step in (1, 2, 4):
        bit_set = (row & step) != 0

        def flip(value):
            down = pltpu.roll(value, step, 0)
            if step == 4:
                return down
            return jnp.where(bit_set, down, pltpu.roll(value, 8 - step, 0))

        flip_re = [flip(value) for value in re]
        flip_im = [flip(value) for value in im]
        re, im = ([cos_half * r + sin_half * fi for r, fi in zip(re, flip_im)],
                  [cos_half * i - sin_half * fr for i, fr in zip(im, flip_re)])
    return re, im


def lane_matrix(cos_half, sin_half):
    row = lax.broadcasted_iota(jnp.int32, (LANES, LANES), 0)
    col = lax.broadcasted_iota(jnp.int32, (LANES, LANES), 1)
    diff = row ^ col
    cos_full = jnp.broadcast_to(cos_half[0:1], (LANES, LANES))
    sin_full = jnp.broadcast_to(sin_half[0:1], (LANES, LANES))
    mag = jnp.ones((LANES, LANES), jnp.float32)
    weight = jnp.zeros((LANES, LANES), jnp.int32)
    for bit in range(7):
        on = (diff >> bit) & 1
        mag = mag * jnp.where(on == 1, sin_full, cos_full)
        weight = weight + on
    quarter = weight & 3
    zero = jnp.zeros_like(mag)
    real = jnp.where(quarter == 0, mag, jnp.where(quarter == 2, -mag, zero))
    imag = jnp.where(quarter == 1, -mag, jnp.where(quarter == 3, mag, zero))
    return real, imag


def kernel(cost_hbm, gammas, betas, energy_all, out_re, out_im,
           cost, cost_swap, recv, send, work, cos_buf, sin_buf, rows_in, matrix,
           energy_part, cost_in, cost_send, cost_recv, send_sem, recv_sem, e_send, e_recv):
    load = pltpu.make_async_copy(cost_hbm, cost, cost_in)
    load.start()
    qx = lax.axis_index('qx')
    qy = lax.axis_index('qy')
    bits = (qy, qx % 2, qx // 2)

    def flipped(offset):
        return [1 - bit if (offset >> i) & 1 else bit for i, bit in enumerate(bits)]

    def block(offset):
        y, core, x = flipped(offset)
        return (x * 2 + core) * 2 + y

    def peer(offset):
        y, core, x = flipped(offset)
        return {'qy': y, 'qx': x * 2 + core}

    barrier = pltpu.get_barrier_semaphore()
    for offset in range(1, 8):
        pl.semaphore_signal(barrier, inc=1, device_id=peer(offset), device_id_type=pl.DeviceIdType.MESH)
    pl.semaphore_wait(barrier, 7)
    load.wait()

    for offset in range(1, 8):
        pltpu.make_async_remote_copy(
            src_ref=cost.at[block(offset)], dst_ref=cost_swap.at[offset],
            send_sem=cost_send, recv_sem=cost_recv,
            device_id=peer(offset), device_id_type=pl.DeviceIdType.MESH).start()

    def half_angle(layer):
        angle = jnp.full((8, LANES), 0.5 * betas[layer], jnp.float32)
        return jnp.cos(angle), jnp.sin(angle)

    def wait_all(buffer, sem, at):
        part = buffer.at[(*at, pl.ds(1, 7))]
        pltpu.make_async_copy(part, part, sem.at[at]).wait()

    def run_layer(layer, odd, first, reuse):
        source, target = (0, 1) if odd else (1, 0)

        def quarter(held, mixed):
            return (held, mixed) if odd else (mixed, held)

        cos_half, sin_half = half_angle(layer)
        if not first:
            cos_prev, sin_prev = half_angle(layer - 1)
        gamma = gammas[layer]
        real, imag = lane_matrix(cos_half, sin_half)
        matrix[0:LANES, 0:LANES] = real
        matrix[0:LANES, LANES:] = imag
        matrix[LANES:, 0:LANES] = -imag
        matrix[LANES:, LANES:] = real

        def half(held, carry):
            def trig(r, carry):
                row = pl.multiple_of(r * 8, 8)
                for mixed in range(2):
                    a, b = quarter(held, mixed)
                    start = pl.multiple_of((a * 16 + b * 8 + r) * 8, 8)
                    for o in range(8):
                        if odd:
                            rows = cost[block(o), pl.ds(start, 8), :]
                        else:
                            rows = cost_swap[o, pl.ds(start, 8), :]
                        angle = gamma * rows
                        cos_buf[mixed * 8 + o, pl.ds(row, 8), :] = jnp.cos(angle)
                        sin_buf[mixed * 8 + o, pl.ds(row, 8), :] = jnp.sin(angle)
                return carry

            lax.fori_loop(0, 8, trig, 0)

            def sub_step(sub, carry):
                if not first:
                    for mixed in range(2):
                        wait_all(recv, recv_sem, (source, *quarter(held, mixed), sub))

                def pair_step(pair, carry):
                    def slots(i, carry):
                        row = pl.multiple_of((sub * PER_SUB + pair * 2 + i) * 8, 8)
                        cos_phase = [cos_buf[o, pl.ds(row, 8), :] for o in range(16)]
                        sin_phase = [sin_buf[o, pl.ds(row, 8), :] for o in range(16)]
                        if first:
                            re = cos_phase
                            im = [-value for value in sin_phase]
                        else:
                            local = pl.multiple_of((pair * 2 + i) * 8, 8)
                            old = [[recv[(source, *quarter(held, mixed), sub, o, c, pl.ds(local, 8))]
                                    for mixed in range(2) for o in range(8)] for c in range(2)]
                            old_re, old_im = rotate(*old, cos_prev, sin_prev)
                            re = [r * c + i * s for r, i, c, s in zip(old_re, old_im, cos_phase, sin_phase)]
                            im = [i * c - r * s for r, i, c, s in zip(old_re, old_im, cos_phase, sin_phase)]
                        re, im = rotate(re, im, cos_half, sin_half)
                        re, im = sublane_rotate(re, im, cos_half, sin_half)
                        for o in range(16):
                            at = pl.multiple_of(o * 16 + i * 8, 8)
                            rows_in[pl.ds(at, 8), 0:LANES] = re[o]
                            rows_in[pl.ds(at, 8), LANES:] = im[o]
                        return carry

                    lax.fori_loop(0, 2, slots, 0)
                    work[sub * (PER_SUB // 2) + pair] = lax.dot(
                        rows_in[...], matrix[...],
                        precision=lax.Precision.HIGHEST, preferred_element_type=jnp.float32)
                    return carry

                lax.fori_loop(0, PER_SUB // 2, pair_step, 0)
                return carry

            lax.fori_loop(0, SUB, sub_step, 0)

            if reuse:
                for mixed in range(2):
                    for sub in range(SUB):
                        wait_all(send, send_sem, (target, *quarter(held, mixed), sub))

            def emit(mixed, carry):
                a, b = quarter(held, mixed)

                def across(o, buffer):
                    def part(r, c):
                        at = pl.multiple_of((mixed * 8 + o) * 16 + (r % 2) * 8, 8)
                        return work[r // 2, pl.ds(at, 8), c * LANES:(c + 1) * LANES]

                    re = [part(r, 0) for r in range(8)]
                    im = [part(r, 1) for r in range(8)]
                    re, im = rotate(re, im, cos_half, sin_half)
                    for r in range(8):
                        row = (r % PER_SUB) * 8
                        buffer[target, a, b, r // PER_SUB, o, 0, row:row + 8, :] = re[r]
                        buffer[target, a, b, r // PER_SUB, o, 1, row:row + 8, :] = im[r]

                def body(o, carry):
                    across(o, send)
                    return carry

                lax.fori_loop(1, 8, body, 0)
                for sub in range(SUB):
                    for offset in SEND_ORDER:
                        pltpu.make_async_remote_copy(
                            src_ref=send.at[target, a, b, sub, offset],
                            dst_ref=recv.at[target, a, b, sub, offset],
                            send_sem=send_sem.at[target, a, b, sub],
                            recv_sem=recv_sem.at[target, a, b, sub],
                            device_id=peer(offset), device_id_type=pl.DeviceIdType.MESH).start()
                across(0, recv)
                return carry

            lax.fori_loop(0, 2, emit, 0)
            return carry

        lax.fori_loop(0, 2, half, 0)

    run_layer(0, True, True, False)
    cost_swap[0] = cost[block(0)]
    part = cost_swap.at[pl.ds(1, 7)]
    pltpu.make_async_copy(part, part, cost_recv).wait()
    run_layer(1, False, False, False)

    def layer_pair(i, carry):
        run_layer(2 * i + 2, True, False, True)
        run_layer(2 * i + 3, False, False, True)
        return carry

    lax.fori_loop(0, LAYERS // 2 - 1, layer_pair, 0)

    cos_half, sin_half = half_angle(LAYERS - 1)
    energy_part[...] = jnp.zeros((8, LANES), jnp.float32)

    def final_half(a, carry):
        def final_sub(sub, carry):
            for b in range(2):
                wait_all(recv, recv_sem, (0, a, b, sub))

            def slots(i, carry):
                row = pl.multiple_of(i * 8, 8)
                old = [[recv[0, a, b, sub, o, c, pl.ds(row, 8), :] for b in range(2) for o in range(8)]
                       for c in range(2)]
                re, im = rotate(*old, cos_half, sin_half)
                total = energy_part[...]
                for b in range(2):
                    start = pl.multiple_of((a * 16 + b * 8 + sub * PER_SUB + i) * 8, 8)
                    for o in range(8):
                        at = block(o)
                        r, m = re[b * 8 + o], im[b * 8 + o]
                        out_re[at, pl.ds(start, 8), :] = r
                        out_im[at, pl.ds(start, 8), :] = m
                        total = total + cost[at, pl.ds(start, 8), :] * (r * r + m * m)
                energy_part[...] = total
                return carry

            lax.fori_loop(0, PER_SUB, slots, 0)
            return carry

        lax.fori_loop(0, SUB, final_sub, 0)
        return carry

    lax.fori_loop(0, 2, final_half, 0)

    me = block(0)
    for offset in range(1, 8):
        pltpu.make_async_remote_copy(
            src_ref=energy_part, dst_ref=energy_all.at[me],
            send_sem=e_send.at[offset], recv_sem=e_recv.at[offset],
            device_id=peer(offset), device_id_type=pl.DeviceIdType.MESH).start()
    energy_all[me] = energy_part[...]
    for par in range(2):
        for a in range(2):
            for b in range(2):
                for sub in range(SUB):
                    wait_all(send, send_sem, (par, a, b, sub))
    part = cost.at[pl.ds(1, 7)]
    pltpu.make_async_copy(part, part, cost_send).wait()
    for offset in range(1, 8):
        pltpu.make_async_copy(energy_part, energy_part, e_send.at[offset]).wait()
        pltpu.make_async_copy(energy_part, energy_part, e_recv.at[offset]).wait()


def write_out(energy_all, in_re, in_im, energy, out_re, out_im, sem):
    copies = [pltpu.make_async_copy(source.at[i], result.at[i], sem.at[c, i])
              for i in range(8) for c, (source, result) in enumerate(((in_re, out_re), (in_im, out_im)))]
    for copy in copies:
        copy.start()
    total = energy_all[0]
    for i in range(1, 8):
        total = total + energy_all[i]
    energy[0] = jnp.sum(total) * (1.0 / (1 << 21))
    for copy in copies:
        copy.wait()


def solution(mesh):
    state_spec = P(('inst', 'qx', 'qy'))

    def device_body(cost_local, gammas, betas):
        local_len = cost_local.shape[0]
        rows = local_len // (8 * LANES)
        shape = (8, rows, LANES)
        f32 = jnp.float32
        vmem = pl.BlockSpec(memory_space=pltpu.VMEM)
        smem = pl.BlockSpec(memory_space=pltpu.SMEM)
        dma = pltpu.SemaphoreType.DMA
        parts = (2, 2, 2, SUB, 8, 2, 8 * PER_SUB, LANES)
        hbm = pl.BlockSpec(memory_space=pl.ANY)
        results = pl.pallas_call(
            kernel,
            out_shape=(pltpu.VMEM((8, 8, LANES), f32), pltpu.VMEM(shape, f32), pltpu.VMEM(shape, f32)),
            in_specs=[hbm, smem, smem],
            out_specs=(vmem, vmem, vmem),
            scratch_shapes=[
                pltpu.VMEM(shape, f32), pltpu.VMEM(shape, f32),
                pltpu.VMEM(parts, f32), pltpu.VMEM(parts, f32),
                pltpu.VMEM((4, 2 * LANES, 2 * LANES), f32),
                pltpu.VMEM((16, 64, LANES), f32), pltpu.VMEM((16, 64, LANES), f32),
                pltpu.VMEM((2 * LANES, 2 * LANES), f32), pltpu.VMEM((2 * LANES, 2 * LANES), f32),
                pltpu.VMEM((8, LANES), f32),
                dma, dma, dma,
                dma((2, 2, 2, SUB)), dma((2, 2, 2, SUB)),
                dma((8,)), dma((8,)),
            ],
            compiler_params=pltpu.CompilerParams(collective_id=0, has_side_effects=True),
            name='qaoa',
        )(cost_local.reshape(shape), gammas, betas)
        energy, state_re, state_im = pl.pallas_call(
            write_out,
            out_shape=(jax.ShapeDtypeStruct((1,), f32),
                       jax.ShapeDtypeStruct(shape, f32), jax.ShapeDtypeStruct(shape, f32)),
            in_specs=[vmem, vmem, vmem],
            out_specs=(smem, hbm, hbm),
            scratch_shapes=[dma((2, 8))],
            name='write_out',
        )(*[pltpu.with_memory_space_constraint(value, pltpu.VMEM) for value in results])
        return energy, state_re.reshape(local_len), state_im.reshape(local_len)

    return jax.shard_map(device_body, mesh=mesh, in_specs=(state_spec, P(), P()),
                         out_specs=(P('inst'), state_spec, state_spec), check_vma=False)
```

```python
import jax
import jax.numpy as jnp
from jax import lax
from jax.experimental import pallas as pl
from jax.experimental.pallas import tpu as pltpu
from jax.sharding import PartitionSpec as P

LANES = 128
LAYERS = 8
SUB = 4
PER_SUB = 8 // SUB
SEND_ORDER = (5, 7, 4, 6, 1, 3, 2)
NEAR = (4, 1)


def rotate(re, im, cos_half, sin_half, steps=None):
    count = len(re)
    for step in steps or [1 << i for i in range(count.bit_length() - 1)]:
        new_re = [cos_half * re[i] + sin_half * im[i ^ step] for i in range(count)]
        new_im = [cos_half * im[i] - sin_half * re[i ^ step] for i in range(count)]
        re, im = new_re, new_im
    return re, im


def sublane_rotate(re, im, cos_half, sin_half):
    row = lax.broadcasted_iota(jnp.int32, (8, LANES), 0)
    for step in (1, 2, 4):
        bit_set = (row & step) != 0

        def flip(value):
            down = pltpu.roll(value, step, 0)
            if step == 4:
                return down
            return jnp.where(bit_set, down, pltpu.roll(value, 8 - step, 0))

        flip_re = [flip(value) for value in re]
        flip_im = [flip(value) for value in im]
        re, im = ([cos_half * r + sin_half * fi for r, fi in zip(re, flip_im)],
                  [cos_half * i - sin_half * fr for i, fr in zip(im, flip_re)])
    return re, im


def lane_matrix(cos_half, sin_half):
    row = lax.broadcasted_iota(jnp.int32, (LANES, LANES), 0)
    col = lax.broadcasted_iota(jnp.int32, (LANES, LANES), 1)
    diff = row ^ col
    cos_full = jnp.broadcast_to(cos_half[0:1], (LANES, LANES))
    sin_full = jnp.broadcast_to(sin_half[0:1], (LANES, LANES))
    mag = jnp.ones((LANES, LANES), jnp.float32)
    weight = jnp.zeros((LANES, LANES), jnp.int32)
    for bit in range(7):
        on = (diff >> bit) & 1
        mag = mag * jnp.where(on == 1, sin_full, cos_full)
        weight = weight + on
    quarter = weight & 3
    zero = jnp.zeros_like(mag)
    real = jnp.where(quarter == 0, mag, jnp.where(quarter == 2, -mag, zero))
    imag = jnp.where(quarter == 1, -mag, jnp.where(quarter == 3, mag, zero))
    return real, imag


def kernel(cost_hbm, gammas, betas, energy_all, out_re, out_im,
           cost, cost_near, cost_swap, recv, send, work, cos_buf, sin_buf, cos_near, sin_near,
           rows_in, matrix, energy_part, cost_in, near_send, near_recv, cost_send, cost_recv,
           send_sem, recv_sem, e_send, e_recv):
    load = pltpu.make_async_copy(cost_hbm, cost, cost_in)
    load.start()
    qx = lax.axis_index('qx')
    qy = lax.axis_index('qy')
    bits = (qy, qx % 2, qx // 2)

    def flipped(offset):
        return [1 - bit if (offset >> i) & 1 else bit for i, bit in enumerate(bits)]

    def block(offset):
        y, core, x = flipped(offset)
        return (x * 2 + core) * 2 + y

    def peer(offset):
        y, core, x = flipped(offset)
        return {'qy': y, 'qx': x * 2 + core}

    def remote(source, target, send_at, recv_at, offset):
        pltpu.make_async_remote_copy(
            src_ref=source, dst_ref=target, send_sem=send_at, recv_sem=recv_at,
            device_id=peer(offset), device_id_type=pl.DeviceIdType.MESH).start()

    barrier = pltpu.get_barrier_semaphore()
    for offset in range(1, 8):
        pl.semaphore_signal(barrier, inc=1, device_id=peer(offset), device_id_type=pl.DeviceIdType.MESH)
    pl.semaphore_wait(barrier, 7)
    load.wait()

    def half_angle(layer):
        angle = jnp.full((8, LANES), 0.5 * betas[layer], jnp.float32)
        return jnp.cos(angle), jnp.sin(angle)

    def wait_bytes(part, sem):
        pltpu.make_async_copy(part, part, sem).wait()

    def wait_all(buffer, sem, at, count):
        wait_bytes(buffer.at[(*at, pl.ds(0, count))], sem.at[at])

    def rows_of(r):
        return pl.ds(pl.multiple_of(r * 8, 8), 8)

    def set_matrix(cos_half, sin_half):
        real, imag = lane_matrix(cos_half, sin_half)
        matrix[0:LANES, 0:LANES] = real
        matrix[0:LANES, LANES:] = imag
        matrix[LANES:, 0:LANES] = -imag
        matrix[LANES:, LANES:] = real

    def put_rows(i, re, im):
        for o in range(16):
            at = pl.multiple_of(o * 16 + i * 8, 8)
            rows_in[pl.ds(at, 8), 0:LANES] = re[o]
            rows_in[pl.ds(at, 8), LANES:] = im[o]

    def lanes(a_held, at):
        work[a_held, at] = lax.dot(
            rows_in[...], matrix[...],
            precision=lax.Precision.HIGHEST, preferred_element_type=jnp.float32)

    def emit(held, mixed, target, a, b, cos_half, sin_half, order, route, local):
        def across(o, buffer):
            def part(r, c):
                at = pl.multiple_of((mixed * 8 + o) * 16 + (r % 2) * 8, 8)
                return work[held, r // 2, pl.ds(at, 8), c * LANES:(c + 1) * LANES]

            re = [part(r, 0) for r in range(8)]
            im = [part(r, 1) for r in range(8)]
            re, im = rotate(re, im, cos_half, sin_half)
            for r in range(8):
                row = (r % PER_SUB) * 8
                buffer[target, a, b, r // PER_SUB, o, 0, row:row + 8, :] = re[r]
                buffer[target, a, b, r // PER_SUB, o, 1, row:row + 8, :] = im[r]

        def body(o, carry):
            across(o, send)
            return carry

        lax.fori_loop(1, 8, body, 0)
        for sub in range(SUB):
            at = (target, a, b, sub)
            for o in order:
                remote(send.at[(*at, o)], recv.at[(*at, o)], send_sem.at[at], recv_sem.at[at], route(o))
        for o in local:
            across(o, recv)

    def first_layer():
        def sub_rows(sub):
            return pl.ds(pl.multiple_of(sub * 8 * PER_SUB, 8), 8 * PER_SUB)

        for sub in range(SUB):
            for a in range(2):
                remote(cost.at[:, a, :, sub_rows(sub)], cost_near.at[:, a, :, sub_rows(sub)],
                       near_send.at[a, sub], near_recv.at[a, sub], NEAR[a])
        for a in range(2):
            for o in range(1, 8):
                if not o & NEAR[a]:
                    remote(cost.at[block(o), a], cost_swap.at[o, a], cost_send, cost_recv, o)

        gamma = gammas[0]
        cos_half, sin_half = half_angle(0)
        set_matrix(cos_half, sin_half)

        def own_trig(r, carry):
            for a in range(2):
                for b in range(2):
                    for o in range(8):
                        angle = gamma * cost[block(o), a, b, rows_of(r), :]
                        cos_buf[a, b * 8 + o, rows_of(r), :] = jnp.cos(angle)
                        sin_buf[a, b * 8 + o, rows_of(r), :] = jnp.sin(angle)
            return carry

        lax.fori_loop(0, 8, own_trig, 0)

        def sub_step(sub, carry):
            for a in range(2):
                bit = NEAR[a]
                part = cost_near.at[:, a, :, sub_rows(sub)]
                wait_bytes(part, near_recv.at[a, sub])
                for o in range(1, 8):
                    if not o & bit:
                        remote(cost_near.at[block(o), a, :, sub_rows(sub)],
                               cost_swap.at[o | bit, a, :, sub_rows(sub)], cost_send, cost_recv, o)

                def slots(i, carry):
                    r = sub * PER_SUB + i
                    for b in range(2):
                        for o in range(8):
                            angle = gamma * cost_near[block(o), a, b, rows_of(r), :]
                            cos_near[b * 8 + o] = jnp.cos(angle)
                            sin_near[b * 8 + o] = jnp.sin(angle)
                    re, im = [None] * 16, [None] * 16
                    for b in range(2):
                        for o in range(8):
                            if o & bit:
                                continue
                            here, there = b * 8 + o, b * 8 + (o | bit)
                            for slot, cos_at, sin_at in (
                                    (here, lambda k: cos_buf[a, k, rows_of(r), :], lambda k: sin_buf[a, k, rows_of(r), :]),
                                    (there, lambda k: cos_near[k], lambda k: sin_near[k])):
                                re[slot] = cos_half * cos_at(here) - sin_half * sin_at(there)
                                im[slot] = -(cos_half * sin_at(here)) - sin_half * cos_at(there)
                    re, im = rotate(re, im, cos_half, sin_half, [step for step in (1, 2, 4, 8) if step != bit])
                    re, im = sublane_rotate(re, im, cos_half, sin_half)
                    put_rows(i, re, im)
                    return carry

                lax.fori_loop(0, PER_SUB, slots, 0)
                lanes(a, sub)
            return carry

        lax.fori_loop(0, SUB, sub_step, 0)

        def quarters(b, carry):
            for a in range(2):
                bit = NEAR[a]
                emit(a, b, 1, a, b, cos_half, sin_half,
                     [o for o in (3, 6, 7, 1, 4, 5, 2) if o & ~bit], lambda o: o & ~bit, (0, bit))
            return carry

        lax.fori_loop(0, 2, quarters, 0)
        cost_swap[0] = cost[block(0)]
        for a in range(2):
            cost_swap[NEAR[a], a] = cost_near[block(0), a]
        wait_bytes(cost_swap.at[pl.ds(0, 6)], cost_recv)

    def run_layer(layer, odd, arrived, drained):
        source, target = (0, 1) if odd else (1, 0)

        def quarter(held, mixed):
            return (held, mixed) if odd else (mixed, held)

        cos_half, sin_half = half_angle(layer)
        cos_prev, sin_prev = half_angle(layer - 1)
        gamma = gammas[layer]
        set_matrix(cos_half, sin_half)

        def half(held, carry):
            def trig(r, carry):
                for mixed in range(2):
                    for o in range(8):
                        at = (block(o) if odd else o, *quarter(held, mixed), rows_of(r))
                        angle = gamma * (cost if odd else cost_swap)[at]
                        cos_buf[held, mixed * 8 + o, rows_of(r), :] = jnp.cos(angle)
                        sin_buf[held, mixed * 8 + o, rows_of(r), :] = jnp.sin(angle)
                return carry

            lax.fori_loop(0, 8, trig, 0)

            def sub_step(sub, carry):
                for mixed in range(2):
                    wait_all(recv, recv_sem, (source, *quarter(held, mixed), sub), arrived)

                def slots(i, carry):
                    r = sub * PER_SUB + i
                    cos_phase = [cos_buf[held, o, rows_of(r), :] for o in range(16)]
                    sin_phase = [sin_buf[held, o, rows_of(r), :] for o in range(16)]
                    old = [[recv[(source, *quarter(held, mixed), sub, o, c, rows_of(i))]
                            for mixed in range(2) for o in range(8)] for c in range(2)]
                    old_re, old_im = rotate(*old, cos_prev, sin_prev)
                    re = [r * c + i * s for r, i, c, s in zip(old_re, old_im, cos_phase, sin_phase)]
                    im = [i * c - r * s for r, i, c, s in zip(old_re, old_im, cos_phase, sin_phase)]
                    re, im = rotate(re, im, cos_half, sin_half)
                    re, im = sublane_rotate(re, im, cos_half, sin_half)
                    put_rows(i, re, im)
                    return carry

                lax.fori_loop(0, PER_SUB, slots, 0)
                lanes(held, sub)
                return carry

            lax.fori_loop(0, SUB, sub_step, 0)

            if drained:
                for mixed in range(2):
                    for sub in range(SUB):
                        wait_all(send, send_sem, (target, *quarter(held, mixed), sub), drained)

            def quarters(mixed, carry):
                emit(held, mixed, target, *quarter(held, mixed), cos_half, sin_half, SEND_ORDER, lambda o: o, (0,))
                return carry

            lax.fori_loop(0, 2, quarters, 0)
            return carry

        lax.fori_loop(0, 2, half, 0)

    first_layer()
    run_layer(1, False, 6, 0)
    run_layer(2, True, 7, 6)

    def layer_pair(i, carry):
        run_layer(2 * i + 3, False, 7, 7)
        run_layer(2 * i + 4, True, 7, 7)
        return carry

    lax.fori_loop(0, LAYERS // 2 - 2, layer_pair, 0)
    run_layer(LAYERS - 1, False, 7, 7)

    cos_half, sin_half = half_angle(LAYERS - 1)
    energy_part[...] = jnp.zeros((8, LANES), jnp.float32)

    def final_half(a, carry):
        def final_sub(sub, carry):
            for b in range(2):
                wait_all(recv, recv_sem, (0, a, b, sub), 7)

            def slots(i, carry):
                r = sub * PER_SUB + i
                old = [[recv[0, a, b, sub, o, c, rows_of(i), :] for b in range(2) for o in range(8)]
                       for c in range(2)]
                re, im = rotate(*old, cos_half, sin_half)
                total = energy_part[...]
                for b in range(2):
                    for o in range(8):
                        at = (block(o), a, b, rows_of(r))
                        x, y = re[b * 8 + o], im[b * 8 + o]
                        out_re[at] = x
                        out_im[at] = y
                        total = total + cost[at] * (x * x + y * y)
                energy_part[...] = total
                return carry

            lax.fori_loop(0, PER_SUB, slots, 0)
            return carry

        lax.fori_loop(0, SUB, final_sub, 0)
        return carry

    lax.fori_loop(0, 2, final_half, 0)

    me = block(0)
    for offset in range(1, 8):
        remote(energy_part, energy_all.at[me], e_send.at[offset], e_recv.at[offset], offset)
    energy_all[me] = energy_part[...]
    for par in range(2):
        for a in range(2):
            for b in range(2):
                for sub in range(SUB):
                    wait_all(send, send_sem, (par, a, b, sub), 7)
    for a in range(2):
        for sub in range(SUB):
            wait_bytes(cost.at[:, a, :, pl.ds(sub * 8 * PER_SUB, 8 * PER_SUB)], near_send.at[a, sub])
    wait_bytes(cost_swap.at[pl.ds(0, 6)], cost_send)
    for offset in range(1, 8):
        wait_bytes(energy_part, e_send.at[offset])
        wait_bytes(energy_part, e_recv.at[offset])


def write_out(energy_all, in_re, in_im, energy, out_re, out_im, sem):
    copies = [pltpu.make_async_copy(in_re, out_re, sem.at[0]), pltpu.make_async_copy(in_im, out_im, sem.at[1])]
    for copy in copies:
        copy.start()
    total = energy_all[0]
    for i in range(1, 8):
        total = total + energy_all[i]
    energy[0] = jnp.sum(total) * (1.0 / (1 << 21))
    for copy in copies:
        copy.wait()


def solution(mesh):
    state_spec = P(('inst', 'qx', 'qy'))

    def device_body(cost_local, gammas, betas):
        local_len = cost_local.shape[0]
        shape = (8, 2, 2, local_len // (32 * LANES), LANES)
        f32 = jnp.float32
        vmem = pl.BlockSpec(memory_space=pltpu.VMEM)
        smem = pl.BlockSpec(memory_space=pltpu.SMEM)
        dma = pltpu.SemaphoreType.DMA
        parts = (2, 2, 2, SUB, 8, 2, 8 * PER_SUB, LANES)
        hbm = pl.BlockSpec(memory_space=pl.ANY)
        results = pl.pallas_call(
            kernel,
            out_shape=(pltpu.VMEM((8, 8, LANES), f32), pltpu.VMEM(shape, f32), pltpu.VMEM(shape, f32)),
            in_specs=[hbm, smem, smem],
            out_specs=(vmem, vmem, vmem),
            scratch_shapes=[
                pltpu.VMEM(shape, f32), pltpu.VMEM(shape, f32), pltpu.VMEM(shape, f32),
                pltpu.VMEM(parts, f32), pltpu.VMEM(parts, f32),
                pltpu.VMEM((2, 4, 2 * LANES, 2 * LANES), f32),
                pltpu.VMEM((2, 16, 64, LANES), f32), pltpu.VMEM((2, 16, 64, LANES), f32),
                pltpu.VMEM((16, 8, LANES), f32), pltpu.VMEM((16, 8, LANES), f32),
                pltpu.VMEM((2 * LANES, 2 * LANES), f32), pltpu.VMEM((2 * LANES, 2 * LANES), f32),
                pltpu.VMEM((8, LANES), f32),
                dma, dma((2, SUB)), dma((2, SUB)), dma, dma,
                dma((2, 2, 2, SUB)), dma((2, 2, 2, SUB)),
                dma((8,)), dma((8,)),
            ],
            compiler_params=pltpu.CompilerParams(collective_id=0, has_side_effects=True),
            name='qaoa',
        )(cost_local.reshape(shape), gammas, betas)
        energy, state_re, state_im = pl.pallas_call(
            write_out,
            out_shape=(jax.ShapeDtypeStruct((1,), f32),
                       jax.ShapeDtypeStruct(shape, f32), jax.ShapeDtypeStruct(shape, f32)),
            in_specs=[vmem, vmem, vmem],
            out_specs=(smem, hbm, hbm),
            scratch_shapes=[dma((2,))],
            name='write_out',
        )(*[pltpu.with_memory_space_constraint(value, pltpu.VMEM) for value in results])
        return energy, state_re.reshape(local_len), state_im.reshape(local_len)

    return jax.shard_map(device_body, mesh=mesh, in_specs=(state_spec, P(), P()),
                         out_specs=(P('inst'), state_spec, state_spec), check_vma=False)
```

```python
import jax
import jax.numpy as jnp
from jax import lax
from jax.experimental import pallas as pl
from jax.experimental.pallas import tpu as pltpu
from jax.sharding import PartitionSpec as P

LANES = 128
LAYERS = 8
SUB = 4
PER_SUB = 8 // SUB
SEND_ORDER = (5, 7, 4, 6, 1, 3, 2)
NEAR = (4, 1)


def rotate(re, im, cos_half, sin_half, steps=None):
    count = len(re)
    for step in steps or [1 << i for i in range(count.bit_length() - 1)]:
        new_re = [cos_half * re[i] + sin_half * im[i ^ step] for i in range(count)]
        new_im = [cos_half * im[i] - sin_half * re[i ^ step] for i in range(count)]
        re, im = new_re, new_im
    return re, im


def sublane_rotate(re, im, cos_half, sin_half):
    row = lax.broadcasted_iota(jnp.int32, (8, LANES), 0)
    for step in (1, 2, 4):
        bit_set = (row & step) != 0

        def flip(value):
            down = pltpu.roll(value, step, 0)
            if step == 4:
                return down
            return jnp.where(bit_set, down, pltpu.roll(value, 8 - step, 0))

        flip_re = [flip(value) for value in re]
        flip_im = [flip(value) for value in im]
        re, im = ([cos_half * r + sin_half * fi for r, fi in zip(re, flip_im)],
                  [cos_half * i - sin_half * fr for i, fr in zip(im, flip_re)])
    return re, im


def lane_matrix(cos_half, sin_half):
    row = lax.broadcasted_iota(jnp.int32, (LANES, LANES), 0)
    col = lax.broadcasted_iota(jnp.int32, (LANES, LANES), 1)
    diff = row ^ col
    cos_full = jnp.broadcast_to(cos_half[0:1], (LANES, LANES))
    sin_full = jnp.broadcast_to(sin_half[0:1], (LANES, LANES))
    mag = jnp.ones((LANES, LANES), jnp.float32)
    weight = jnp.zeros((LANES, LANES), jnp.int32)
    for bit in range(7):
        on = (diff >> bit) & 1
        mag = mag * jnp.where(on == 1, sin_full, cos_full)
        weight = weight + on
    quarter = weight & 3
    zero = jnp.zeros_like(mag)
    real = jnp.where(quarter == 0, mag, jnp.where(quarter == 2, -mag, zero))
    imag = jnp.where(quarter == 1, -mag, jnp.where(quarter == 3, mag, zero))
    return real, imag


def kernel(cost_hbm, gammas, betas, energy_all, out_re, out_im,
           cost, cost_near, cost_swap, recv, send, work, cos_buf, sin_buf, cos_near, sin_near,
           rows_in, matrix, energy_part, energy_row, cost_in, near_send, near_recv, cost_send, cost_recv,
           send_sem, recv_sem, e_send, e_recv):
    loads = [pltpu.make_async_copy(cost_hbm.at[:, :, :, pl.ds(sub * 8 * PER_SUB, 8 * PER_SUB)],
                                   cost.at[:, :, :, pl.ds(sub * 8 * PER_SUB, 8 * PER_SUB)], cost_in.at[sub])
             for sub in range(SUB)]
    for load in loads:
        load.start()
    qx = lax.axis_index('qx')
    qy = lax.axis_index('qy')
    bits = (qy, qx % 2, qx // 2)

    def flipped(offset):
        return [1 - bit if (offset >> i) & 1 else bit for i, bit in enumerate(bits)]

    def block(offset):
        y, core, x = flipped(offset)
        return (x * 2 + core) * 2 + y

    def peer(offset):
        y, core, x = flipped(offset)
        return {'qy': y, 'qx': x * 2 + core}

    def remote(source, target, send_at, recv_at, offset):
        pltpu.make_async_remote_copy(
            src_ref=source, dst_ref=target, send_sem=send_at, recv_sem=recv_at,
            device_id=peer(offset), device_id_type=pl.DeviceIdType.MESH).start()

    barrier = pltpu.get_barrier_semaphore()
    for offset in range(1, 8):
        pl.semaphore_signal(barrier, inc=1, device_id=peer(offset), device_id_type=pl.DeviceIdType.MESH)
    pl.semaphore_wait(barrier, 7)

    def half_angle(layer):
        angle = jnp.full((8, LANES), 0.5 * betas[layer], jnp.float32)
        return jnp.cos(angle), jnp.sin(angle)

    def wait_bytes(part, sem):
        pltpu.make_async_copy(part, part, sem).wait()

    def wait_all(buffer, sem, at, count):
        wait_bytes(buffer.at[(*at, pl.ds(0, count))], sem.at[at])

    def rows_of(r):
        return pl.ds(pl.multiple_of(r * 8, 8), 8)

    def set_matrix(cos_half, sin_half):
        real, imag = lane_matrix(cos_half, sin_half)
        matrix[0:LANES, 0:LANES] = real
        matrix[0:LANES, LANES:] = imag
        matrix[LANES:, 0:LANES] = -imag
        matrix[LANES:, LANES:] = real

    def put_rows(i, re, im):
        for o in range(16):
            at = pl.multiple_of(o * 16 + i * 8, 8)
            rows_in[pl.ds(at, 8), 0:LANES] = re[o]
            rows_in[pl.ds(at, 8), LANES:] = im[o]

    def lanes(a_held, at):
        work[a_held, at] = lax.dot(
            rows_in[...], matrix[...],
            precision=lax.Precision.HIGHEST, preferred_element_type=jnp.float32)

    def emit(held, mixed, target, a, b, cos_half, sin_half, order, route, local):
        def across(o, buffer):
            def part(r, c):
                at = pl.multiple_of((mixed * 8 + o) * 16 + (r % 2) * 8, 8)
                return work[held, r // 2, pl.ds(at, 8), c * LANES:(c + 1) * LANES]

            re = [part(r, 0) for r in range(8)]
            im = [part(r, 1) for r in range(8)]
            re, im = rotate(re, im, cos_half, sin_half)
            for r in range(8):
                row = (r % PER_SUB) * 8
                buffer[target, a, b, r // PER_SUB, o, 0, row:row + 8, :] = re[r]
                buffer[target, a, b, r // PER_SUB, o, 1, row:row + 8, :] = im[r]

        def body(o, carry):
            across(o, send)
            return carry

        lax.fori_loop(1, 8, body, 0)
        for sub in range(SUB):
            at = (target, a, b, sub)
            for o in order:
                remote(send.at[(*at, o)], recv.at[(*at, o)], send_sem.at[at], recv_sem.at[at], route(o))
        for o in local:
            across(o, recv)

    def first_layer():
        def sub_rows(sub):
            return pl.ds(pl.multiple_of(sub * 8 * PER_SUB, 8), 8 * PER_SUB)

        for sub in range(SUB):
            loads[sub].wait()
            for a in range(2):
                remote(cost.at[:, a, :, sub_rows(sub)], cost_near.at[:, a, :, sub_rows(sub)],
                       near_send.at[a, sub], near_recv.at[a, sub], NEAR[a])
        for a in range(2):
            for o in range(1, 8):
                if not o & NEAR[a]:
                    remote(cost.at[block(o), a], cost_swap.at[o, a], cost_send, cost_recv, o)

        gamma = gammas[0]
        cos_half, sin_half = half_angle(0)
        set_matrix(cos_half, sin_half)

        def own_trig(r, carry):
            for a in range(2):
                for b in range(2):
                    for o in range(8):
                        angle = gamma * cost[block(o), a, b, rows_of(r), :]
                        cos_buf[a, b * 8 + o, rows_of(r), :] = jnp.cos(angle)
                        sin_buf[a, b * 8 + o, rows_of(r), :] = jnp.sin(angle)
            return carry

        lax.fori_loop(0, 8, own_trig, 0)

        def sub_step(sub, carry):
            for a in range(2):
                bit = NEAR[a]
                part = cost_near.at[:, a, :, sub_rows(sub)]
                wait_bytes(part, near_recv.at[a, sub])
                for o in range(1, 8):
                    if not o & bit:
                        remote(cost_near.at[block(o), a, :, sub_rows(sub)],
                               cost_swap.at[o | bit, a, :, sub_rows(sub)], cost_send, cost_recv, o)

                def slots(i, carry):
                    r = sub * PER_SUB + i
                    for b in range(2):
                        for o in range(8):
                            angle = gamma * cost_near[block(o), a, b, rows_of(r), :]
                            cos_near[b * 8 + o] = jnp.cos(angle)
                            sin_near[b * 8 + o] = jnp.sin(angle)
                    re, im = [None] * 16, [None] * 16
                    for b in range(2):
                        for o in range(8):
                            if o & bit:
                                continue
                            here, there = b * 8 + o, b * 8 + (o | bit)
                            for slot, cos_at, sin_at in (
                                    (here, lambda k: cos_buf[a, k, rows_of(r), :], lambda k: sin_buf[a, k, rows_of(r), :]),
                                    (there, lambda k: cos_near[k], lambda k: sin_near[k])):
                                re[slot] = cos_half * cos_at(here) - sin_half * sin_at(there)
                                im[slot] = -(cos_half * sin_at(here)) - sin_half * cos_at(there)
                    re, im = rotate(re, im, cos_half, sin_half, [step for step in (1, 2, 4, 8) if step != bit])
                    re, im = sublane_rotate(re, im, cos_half, sin_half)
                    put_rows(i, re, im)
                    return carry

                lax.fori_loop(0, PER_SUB, slots, 0)
                lanes(a, sub)
            return carry

        lax.fori_loop(0, SUB, sub_step, 0)

        def quarters(b, carry):
            for a in range(2):
                bit = NEAR[a]
                emit(a, b, 1, a, b, cos_half, sin_half,
                     [o for o in (3, 6, 7, 1, 4, 5, 2) if o & ~bit], lambda o: o & ~bit, (0, bit))
            return carry

        lax.fori_loop(0, 2, quarters, 0)
        cost_swap[0] = cost[block(0)]
        for a in range(2):
            cost_swap[NEAR[a], a] = cost_near[block(0), a]
        wait_bytes(cost_swap.at[pl.ds(0, 6)], cost_recv)

    def run_layer(layer, odd, arrived, drained):
        source, target = (0, 1) if odd else (1, 0)

        def quarter(held, mixed):
            return (held, mixed) if odd else (mixed, held)

        cos_half, sin_half = half_angle(layer)
        cos_prev, sin_prev = half_angle(layer - 1)
        gamma = gammas[layer]
        set_matrix(cos_half, sin_half)

        def half(held, carry):
            def trig(r, carry):
                for mixed in range(2):
                    for o in range(8):
                        at = (block(o) if odd else o, *quarter(held, mixed), rows_of(r))
                        angle = gamma * (cost if odd else cost_swap)[at]
                        cos_buf[held, mixed * 8 + o, rows_of(r), :] = jnp.cos(angle)
                        sin_buf[held, mixed * 8 + o, rows_of(r), :] = jnp.sin(angle)
                return carry

            lax.fori_loop(0, 8, trig, 0)

            def sub_step(sub, carry):
                for mixed in range(2):
                    wait_all(recv, recv_sem, (source, *quarter(held, mixed), sub), arrived)

                def slots(i, carry):
                    r = sub * PER_SUB + i
                    cos_phase = [cos_buf[held, o, rows_of(r), :] for o in range(16)]
                    sin_phase = [sin_buf[held, o, rows_of(r), :] for o in range(16)]
                    old = [[recv[(source, *quarter(held, mixed), sub, o, c, rows_of(i))]
                            for mixed in range(2) for o in range(8)] for c in range(2)]
                    old_re, old_im = rotate(*old, cos_prev, sin_prev)
                    re = [r * c + i * s for r, i, c, s in zip(old_re, old_im, cos_phase, sin_phase)]
                    im = [i * c - r * s for r, i, c, s in zip(old_re, old_im, cos_phase, sin_phase)]
                    re, im = rotate(re, im, cos_half, sin_half)
                    re, im = sublane_rotate(re, im, cos_half, sin_half)
                    put_rows(i, re, im)
                    return carry

                lax.fori_loop(0, PER_SUB, slots, 0)
                lanes(held, sub)
                return carry

            lax.fori_loop(0, SUB, sub_step, 0)

            if drained:
                for mixed in range(2):
                    for sub in range(SUB):
                        wait_all(send, send_sem, (target, *quarter(held, mixed), sub), drained)

            def quarters(mixed, carry):
                emit(held, mixed, target, *quarter(held, mixed), cos_half, sin_half, SEND_ORDER, lambda o: o, (0,))
                return carry

            lax.fori_loop(0, 2, quarters, 0)
            return carry

        lax.fori_loop(0, 2, half, 0)

    first_layer()
    run_layer(1, False, 6, 0)
    run_layer(2, True, 7, 6)

    def layer_pair(i, carry):
        run_layer(2 * i + 3, False, 7, 7)
        run_layer(2 * i + 4, True, 7, 7)
        return carry

    lax.fori_loop(0, LAYERS // 2 - 2, layer_pair, 0)
    run_layer(LAYERS - 1, False, 7, 7)

    cos_half, sin_half = half_angle(LAYERS - 1)
    energy_part[...] = jnp.zeros((8, LANES), jnp.float32)

    def final_half(a, carry):
        def final_sub(sub, carry):
            for b in range(2):
                wait_all(recv, recv_sem, (0, a, b, sub), 7)

            def slots(i, carry):
                r = sub * PER_SUB + i
                old = [[recv[0, a, b, sub, o, c, rows_of(i), :] for b in range(2) for o in range(8)]
                       for c in range(2)]
                re, im = rotate(*old, cos_half, sin_half)
                total = energy_part[...]
                for b in range(2):
                    for o in range(8):
                        at = (block(o), a, b, rows_of(r))
                        x, y = re[b * 8 + o], im[b * 8 + o]
                        out_re[at] = x
                        out_im[at] = y
                        total = total + cost[at] * (x * x + y * y)
                energy_part[...] = total
                return carry

            lax.fori_loop(0, PER_SUB, slots, 0)
            return carry

        lax.fori_loop(0, SUB, final_sub, 0)
        return carry

    lax.fori_loop(0, 2, final_half, 0)

    me = block(0)
    energy_row[...] = jnp.sum(energy_part[...], axis=0, keepdims=True)
    for offset in range(1, 8):
        remote(energy_row, energy_all.at[me], e_send.at[offset], e_recv.at[offset], offset)
    energy_all[me] = energy_row[...]
    for par in range(2):
        for a in range(2):
            for b in range(2):
                for sub in range(SUB):
                    wait_all(send, send_sem, (par, a, b, sub), 7)
    for a in range(2):
        for sub in range(SUB):
            wait_bytes(cost.at[:, a, :, pl.ds(sub * 8 * PER_SUB, 8 * PER_SUB)], near_send.at[a, sub])
    wait_bytes(cost_swap.at[pl.ds(0, 6)], cost_send)
    for offset in range(1, 8):
        wait_bytes(energy_row, e_send.at[offset])
        wait_bytes(energy_row, e_recv.at[offset])


def write_out(energy_all, in_re, in_im, energy, out_re, out_im, value, sem):
    copies = [pltpu.make_async_copy(in_re, out_re, sem.at[0]), pltpu.make_async_copy(in_im, out_im, sem.at[1])]
    for copy in copies:
        copy.start()
    total = energy_all[0]
    for i in range(1, 8):
        total = total + energy_all[i]
    value[0] = jnp.sum(total) * (1.0 / (1 << 21))
    copies.append(pltpu.make_async_copy(value, energy, sem.at[2]))
    copies[2].start()
    for copy in copies:
        copy.wait()


def solution(mesh):
    state_spec = P(('inst', 'qx', 'qy'))

    def device_body(cost_local, gammas, betas):
        local_len = cost_local.shape[0]
        shape = (8, 2, 2, local_len // (32 * LANES), LANES)
        f32 = jnp.float32
        vmem = pl.BlockSpec(memory_space=pltpu.VMEM)
        smem = pl.BlockSpec(memory_space=pltpu.SMEM)
        dma = pltpu.SemaphoreType.DMA
        parts = (2, 2, 2, SUB, 8, 2, 8 * PER_SUB, LANES)
        hbm = pl.BlockSpec(memory_space=pl.ANY)
        results = pl.pallas_call(
            kernel,
            out_shape=(pltpu.VMEM((8, 1, LANES), f32), pltpu.VMEM(shape, f32), pltpu.VMEM(shape, f32)),
            in_specs=[hbm, smem, smem],
            out_specs=(vmem, vmem, vmem),
            scratch_shapes=[
                pltpu.VMEM(shape, f32), pltpu.VMEM(shape, f32), pltpu.VMEM(shape, f32),
                pltpu.VMEM(parts, f32), pltpu.VMEM(parts, f32),
                pltpu.VMEM((2, 4, 2 * LANES, 2 * LANES), f32),
                pltpu.VMEM((2, 16, 64, LANES), f32), pltpu.VMEM((2, 16, 64, LANES), f32),
                pltpu.VMEM((16, 8, LANES), f32), pltpu.VMEM((16, 8, LANES), f32),
                pltpu.VMEM((2 * LANES, 2 * LANES), f32), pltpu.VMEM((2 * LANES, 2 * LANES), f32),
                pltpu.VMEM((8, LANES), f32), pltpu.VMEM((1, LANES), f32),
                dma((SUB,)), dma((2, SUB)), dma((2, SUB)), dma, dma,
                dma((2, 2, 2, SUB)), dma((2, 2, 2, SUB)),
                dma((8,)), dma((8,)),
            ],
            compiler_params=pltpu.CompilerParams(collective_id=0, has_side_effects=True),
            name='qaoa',
        )(cost_local.reshape(shape), gammas, betas)
        energy, state_re, state_im = pl.pallas_call(
            write_out,
            out_shape=(jax.ShapeDtypeStruct((1,), f32),
                       jax.ShapeDtypeStruct(shape, f32), jax.ShapeDtypeStruct(shape, f32)),
            in_specs=[vmem, vmem, vmem],
            out_specs=(hbm, hbm, hbm),
            scratch_shapes=[pltpu.SMEM((1,), f32), dma((3,))],
            name='write_out',
        )(*[pltpu.with_memory_space_constraint(value, pltpu.VMEM) for value in results])
        return energy, state_re.reshape(local_len), state_im.reshape(local_len)

    return jax.shard_map(device_body, mesh=mesh, in_specs=(state_spec, P(), P()),
                         out_specs=(P('inst'), state_spec, state_spec), check_vma=False)
```

```python
import jax
import jax.numpy as jnp
from jax import lax
from jax.experimental import pallas as pl
from jax.experimental.pallas import tpu as pltpu
from jax.sharding import PartitionSpec as P

LANES = 128
LAYERS = 8
SUB = 4
PER_SUB = 8 // SUB
SEND_ORDER = (5, 7, 4, 6, 1, 3, 2)
NEAR = (4, 1)


def rotate(re, im, cos_half, sin_half, steps=None):
    count = len(re)
    for step in steps or [1 << i for i in range(count.bit_length() - 1)]:
        new_re = [cos_half * re[i] + sin_half * im[i ^ step] for i in range(count)]
        new_im = [cos_half * im[i] - sin_half * re[i ^ step] for i in range(count)]
        re, im = new_re, new_im
    return re, im


def sublane_rotate(re, im, cos_half, sin_half):
    row = lax.broadcasted_iota(jnp.int32, (8, LANES), 0)
    for step in (1, 2, 4):
        bit_set = (row & step) != 0

        def flip(value):
            down = pltpu.roll(value, step, 0)
            if step == 4:
                return down
            return jnp.where(bit_set, down, pltpu.roll(value, 8 - step, 0))

        flip_re = [flip(value) for value in re]
        flip_im = [flip(value) for value in im]
        re, im = ([cos_half * r + sin_half * fi for r, fi in zip(re, flip_im)],
                  [cos_half * i - sin_half * fr for i, fr in zip(im, flip_re)])
    return re, im


def lane_matrix(cos_half, sin_half):
    row = lax.broadcasted_iota(jnp.int32, (LANES, LANES), 0)
    col = lax.broadcasted_iota(jnp.int32, (LANES, LANES), 1)
    diff = row ^ col
    cos_full = jnp.broadcast_to(cos_half[0:1], (LANES, LANES))
    sin_full = jnp.broadcast_to(sin_half[0:1], (LANES, LANES))
    mag = jnp.ones((LANES, LANES), jnp.float32)
    weight = jnp.zeros((LANES, LANES), jnp.int32)
    for bit in range(7):
        on = (diff >> bit) & 1
        mag = mag * jnp.where(on == 1, sin_full, cos_full)
        weight = weight + on
    quarter = weight & 3
    zero = jnp.zeros_like(mag)
    real = jnp.where(quarter == 0, mag, jnp.where(quarter == 2, -mag, zero))
    imag = jnp.where(quarter == 1, -mag, jnp.where(quarter == 3, mag, zero))
    return real, imag


def kernel(cost_hbm, gammas_hbm, betas_hbm, energy_all, out_re, out_im,
           cost, cost_near, cost_swap, recv, send, work, cos_buf, sin_buf, cos_near, sin_near,
           rows_in, matrix, energy_part, energy_row, gammas, betas, angle_in, cost_in, near_send, near_recv, cost_send, cost_recv,
           send_sem, recv_sem, e_send, e_recv):
    loads = [pltpu.make_async_copy(cost_hbm.at[:, :, :, pl.ds(sub * 8 * PER_SUB, 8 * PER_SUB)],
                                   cost.at[:, :, :, pl.ds(sub * 8 * PER_SUB, 8 * PER_SUB)], cost_in.at[sub])
             for sub in range(SUB)]
    for load in loads:
        load.start()
    angle_loads = [pltpu.make_async_copy(gammas_hbm, gammas, angle_in.at[0]),
                   pltpu.make_async_copy(betas_hbm, betas, angle_in.at[1])]
    for load in angle_loads:
        load.start()
    qx = lax.axis_index('qx')
    qy = lax.axis_index('qy')
    bits = (qy, qx % 2, qx // 2)

    def flipped(offset):
        return [1 - bit if (offset >> i) & 1 else bit for i, bit in enumerate(bits)]

    def block(offset):
        y, core, x = flipped(offset)
        return (x * 2 + core) * 2 + y

    def peer(offset):
        y, core, x = flipped(offset)
        return {'qy': y, 'qx': x * 2 + core}

    def remote(source, target, send_at, recv_at, offset):
        pltpu.make_async_remote_copy(
            src_ref=source, dst_ref=target, send_sem=send_at, recv_sem=recv_at,
            device_id=peer(offset), device_id_type=pl.DeviceIdType.MESH).start()

    barrier = pltpu.get_barrier_semaphore()
    for offset in range(1, 8):
        pl.semaphore_signal(barrier, inc=1, device_id=peer(offset), device_id_type=pl.DeviceIdType.MESH)
    pl.semaphore_wait(barrier, 7)

    def half_angle(layer):
        angle = jnp.full((8, LANES), 0.5 * betas[layer], jnp.float32)
        return jnp.cos(angle), jnp.sin(angle)

    def wait_bytes(part, sem):
        pltpu.make_async_copy(part, part, sem).wait()

    def wait_all(buffer, sem, at, count):
        wait_bytes(buffer.at[(*at, pl.ds(0, count))], sem.at[at])

    def rows_of(r):
        return pl.ds(pl.multiple_of(r * 8, 8), 8)

    def set_matrix(cos_half, sin_half):
        real, imag = lane_matrix(cos_half, sin_half)
        matrix[0:LANES, 0:LANES] = real
        matrix[0:LANES, LANES:] = imag
        matrix[LANES:, 0:LANES] = -imag
        matrix[LANES:, LANES:] = real

    def put_rows(i, re, im):
        for o in range(16):
            at = pl.multiple_of(o * 16 + i * 8, 8)
            rows_in[pl.ds(at, 8), 0:LANES] = re[o]
            rows_in[pl.ds(at, 8), LANES:] = im[o]

    def lanes(a_held, at):
        work[a_held, at] = lax.dot(
            rows_in[...], matrix[...],
            precision=lax.Precision.HIGHEST, preferred_element_type=jnp.float32)

    def emit(held, mixed, target, a, b, cos_half, sin_half, order, route, local):
        def across(o, buffer):
            def part(r, c):
                at = pl.multiple_of((mixed * 8 + o) * 16 + (r % 2) * 8, 8)
                return work[held, r // 2, pl.ds(at, 8), c * LANES:(c + 1) * LANES]

            re = [part(r, 0) for r in range(8)]
            im = [part(r, 1) for r in range(8)]
            re, im = rotate(re, im, cos_half, sin_half)
            for r in range(8):
                row = (r % PER_SUB) * 8
                buffer[target, a, b, r // PER_SUB, o, 0, row:row + 8, :] = re[r]
                buffer[target, a, b, r // PER_SUB, o, 1, row:row + 8, :] = im[r]

        def body(o, carry):
            across(o, send)
            return carry

        lax.fori_loop(1, 8, body, 0)
        for sub in range(SUB):
            at = (target, a, b, sub)
            for o in order:
                remote(send.at[(*at, o)], recv.at[(*at, o)], send_sem.at[at], recv_sem.at[at], route(o))
        for o in local:
            across(o, recv)

    def first_layer():
        def sub_rows(sub):
            return pl.ds(pl.multiple_of(sub * 8 * PER_SUB, 8), 8 * PER_SUB)

        for sub in range(SUB):
            loads[sub].wait()
            for a in range(2):
                remote(cost.at[:, a, :, sub_rows(sub)], cost_near.at[:, a, :, sub_rows(sub)],
                       near_send.at[a, sub], near_recv.at[a, sub], NEAR[a])
        for a in range(2):
            for o in range(1, 8):
                if not o & NEAR[a]:
                    remote(cost.at[block(o), a], cost_swap.at[o, a], cost_send, cost_recv, o)

        for load in angle_loads:
            load.wait()
        gamma = gammas[0]
        cos_half, sin_half = half_angle(0)
        set_matrix(cos_half, sin_half)

        def own_trig(r, carry):
            for a in range(2):
                for b in range(2):
                    for o in range(8):
                        angle = gamma * cost[block(o), a, b, rows_of(r), :]
                        cos_buf[a, b * 8 + o, rows_of(r), :] = jnp.cos(angle)
                        sin_buf[a, b * 8 + o, rows_of(r), :] = jnp.sin(angle)
            return carry

        lax.fori_loop(0, 8, own_trig, 0)

        def sub_step(sub, carry):
            for a in range(2):
                bit = NEAR[a]
                part = cost_near.at[:, a, :, sub_rows(sub)]
                wait_bytes(part, near_recv.at[a, sub])
                for o in range(1, 8):
                    if not o & bit:
                        remote(cost_near.at[block(o), a, :, sub_rows(sub)],
                               cost_swap.at[o | bit, a, :, sub_rows(sub)], cost_send, cost_recv, o)

                def slots(i, carry):
                    r = sub * PER_SUB + i
                    for b in range(2):
                        for o in range(8):
                            angle = gamma * cost_near[block(o), a, b, rows_of(r), :]
                            cos_near[b * 8 + o] = jnp.cos(angle)
                            sin_near[b * 8 + o] = jnp.sin(angle)
                    re, im = [None] * 16, [None] * 16
                    for b in range(2):
                        for o in range(8):
                            if o & bit:
                                continue
                            here, there = b * 8 + o, b * 8 + (o | bit)
                            for slot, cos_at, sin_at in (
                                    (here, lambda k: cos_buf[a, k, rows_of(r), :], lambda k: sin_buf[a, k, rows_of(r), :]),
                                    (there, lambda k: cos_near[k], lambda k: sin_near[k])):
                                re[slot] = cos_half * cos_at(here) - sin_half * sin_at(there)
                                im[slot] = -(cos_half * sin_at(here)) - sin_half * cos_at(there)
                    re, im = rotate(re, im, cos_half, sin_half, [step for step in (1, 2, 4, 8) if step != bit])
                    re, im = sublane_rotate(re, im, cos_half, sin_half)
                    put_rows(i, re, im)
                    return carry

                lax.fori_loop(0, PER_SUB, slots, 0)
                lanes(a, sub)
            return carry

        lax.fori_loop(0, SUB, sub_step, 0)

        def quarters(b, carry):
            for a in range(2):
                bit = NEAR[a]
                emit(a, b, 1, a, b, cos_half, sin_half,
                     [o for o in (3, 6, 7, 1, 4, 5, 2) if o & ~bit], lambda o: o & ~bit, (0, bit))
            return carry

        lax.fori_loop(0, 2, quarters, 0)
        cost_swap[0] = cost[block(0)]
        for a in range(2):
            cost_swap[NEAR[a], a] = cost_near[block(0), a]
        wait_bytes(cost_swap.at[pl.ds(0, 6)], cost_recv)

    def run_layer(layer, odd, arrived, drained):
        source, target = (0, 1) if odd else (1, 0)

        def quarter(held, mixed):
            return (held, mixed) if odd else (mixed, held)

        cos_half, sin_half = half_angle(layer)
        cos_prev, sin_prev = half_angle(layer - 1)
        gamma = gammas[layer]
        set_matrix(cos_half, sin_half)

        def half(held, carry):
            def trig(r, carry):
                for mixed in range(2):
                    for o in range(8):
                        at = (block(o) if odd else o, *quarter(held, mixed), rows_of(r))
                        angle = gamma * (cost if odd else cost_swap)[at]
                        cos_buf[held, mixed * 8 + o, rows_of(r), :] = jnp.cos(angle)
                        sin_buf[held, mixed * 8 + o, rows_of(r), :] = jnp.sin(angle)
                return carry

            lax.fori_loop(0, 8, trig, 0)

            def sub_step(sub, carry):
                for mixed in range(2):
                    wait_all(recv, recv_sem, (source, *quarter(held, mixed), sub), arrived)

                def slots(i, carry):
                    r = sub * PER_SUB + i
                    cos_phase = [cos_buf[held, o, rows_of(r), :] for o in range(16)]
                    sin_phase = [sin_buf[held, o, rows_of(r), :] for o in range(16)]
                    old = [[recv[(source, *quarter(held, mixed), sub, o, c, rows_of(i))]
                            for mixed in range(2) for o in range(8)] for c in range(2)]
                    old_re, old_im = rotate(*old, cos_prev, sin_prev)
                    re = [r * c + i * s for r, i, c, s in zip(old_re, old_im, cos_phase, sin_phase)]
                    im = [i * c - r * s for r, i, c, s in zip(old_re, old_im, cos_phase, sin_phase)]
                    re, im = rotate(re, im, cos_half, sin_half)
                    re, im = sublane_rotate(re, im, cos_half, sin_half)
                    put_rows(i, re, im)
                    return carry

                lax.fori_loop(0, PER_SUB, slots, 0)
                lanes(held, sub)
                return carry

            lax.fori_loop(0, SUB, sub_step, 0)

            if drained:
                for mixed in range(2):
                    for sub in range(SUB):
                        wait_all(send, send_sem, (target, *quarter(held, mixed), sub), drained)

            def quarters(mixed, carry):
                emit(held, mixed, target, *quarter(held, mixed), cos_half, sin_half, SEND_ORDER, lambda o: o, (0,))
                return carry

            lax.fori_loop(0, 2, quarters, 0)
            return carry

        lax.fori_loop(0, 2, half, 0)

    first_layer()
    run_layer(1, False, 6, 0)
    run_layer(2, True, 7, 6)

    def layer_pair(i, carry):
        run_layer(2 * i + 3, False, 7, 7)
        run_layer(2 * i + 4, True, 7, 7)
        return carry

    lax.fori_loop(0, LAYERS // 2 - 2, layer_pair, 0)
    run_layer(LAYERS - 1, False, 7, 7)

    cos_half, sin_half = half_angle(LAYERS - 1)
    energy_part[...] = jnp.zeros((8, LANES), jnp.float32)

    def final_half(a, carry):
        def final_sub(sub, carry):
            for b in range(2):
                wait_all(recv, recv_sem, (0, a, b, sub), 7)

            def slots(i, carry):
                r = sub * PER_SUB + i
                old = [[recv[0, a, b, sub, o, c, rows_of(i), :] for b in range(2) for o in range(8)]
                       for c in range(2)]
                re, im = rotate(*old, cos_half, sin_half)
                total = energy_part[...]
                for b in range(2):
                    for o in range(8):
                        at = (block(o), a, b, rows_of(r))
                        x, y = re[b * 8 + o], im[b * 8 + o]
                        out_re[at] = x
                        out_im[at] = y
                        total = total + cost[at] * (x * x + y * y)
                energy_part[...] = total
                return carry

            lax.fori_loop(0, PER_SUB, slots, 0)
            return carry

        lax.fori_loop(0, SUB, final_sub, 0)
        return carry

    lax.fori_loop(0, 2, final_half, 0)

    me = block(0)
    energy_row[...] = jnp.sum(energy_part[...], axis=0, keepdims=True)
    for offset in range(1, 8):
        remote(energy_row, energy_all.at[me], e_send.at[offset], e_recv.at[offset], offset)
    energy_all[me] = energy_row[...]
    for par in range(2):
        for a in range(2):
            for b in range(2):
                for sub in range(SUB):
                    wait_all(send, send_sem, (par, a, b, sub), 7)
    for a in range(2):
        for sub in range(SUB):
            wait_bytes(cost.at[:, a, :, pl.ds(sub * 8 * PER_SUB, 8 * PER_SUB)], near_send.at[a, sub])
    wait_bytes(cost_swap.at[pl.ds(0, 6)], cost_send)
    for offset in range(1, 8):
        wait_bytes(energy_row, e_send.at[offset])
        wait_bytes(energy_row, e_recv.at[offset])


def write_out(energy_all, in_re, in_im, energy, out_re, out_im, value, sem):
    copies = [pltpu.make_async_copy(in_re, out_re, sem.at[0]), pltpu.make_async_copy(in_im, out_im, sem.at[1])]
    for copy in copies:
        copy.start()
    total = energy_all[0]
    for i in range(1, 8):
        total = total + energy_all[i]
    value[0] = jnp.sum(total) * (1.0 / (1 << 21))
    copies.append(pltpu.make_async_copy(value, energy, sem.at[2]))
    copies[2].start()
    for copy in copies:
        copy.wait()


def solution(mesh):
    state_spec = P(('inst', 'qx', 'qy'))

    def device_body(cost_local, gammas, betas):
        local_len = cost_local.shape[0]
        shape = (8, 2, 2, local_len // (32 * LANES), LANES)
        f32 = jnp.float32
        vmem = pl.BlockSpec(memory_space=pltpu.VMEM)
        dma = pltpu.SemaphoreType.DMA
        parts = (2, 2, 2, SUB, 8, 2, 8 * PER_SUB, LANES)
        hbm = pl.BlockSpec(memory_space=pl.ANY)
        results = pl.pallas_call(
            kernel,
            out_shape=(pltpu.VMEM((8, 1, LANES), f32), pltpu.VMEM(shape, f32), pltpu.VMEM(shape, f32)),
            in_specs=[hbm, hbm, hbm],
            out_specs=(vmem, vmem, vmem),
            scratch_shapes=[
                pltpu.VMEM(shape, f32), pltpu.VMEM(shape, f32), pltpu.VMEM(shape, f32),
                pltpu.VMEM(parts, f32), pltpu.VMEM(parts, f32),
                pltpu.VMEM((2, 4, 2 * LANES, 2 * LANES), f32),
                pltpu.VMEM((2, 16, 64, LANES), f32), pltpu.VMEM((2, 16, 64, LANES), f32),
                pltpu.VMEM((16, 8, LANES), f32), pltpu.VMEM((16, 8, LANES), f32),
                pltpu.VMEM((2 * LANES, 2 * LANES), f32), pltpu.VMEM((2 * LANES, 2 * LANES), f32),
                pltpu.VMEM((8, LANES), f32), pltpu.VMEM((1, LANES), f32),
                pltpu.SMEM((LAYERS,), f32), pltpu.SMEM((LAYERS,), f32), dma((2,)),
                dma((SUB,)), dma((2, SUB)), dma((2, SUB)), dma, dma,
                dma((2, 2, 2, SUB)), dma((2, 2, 2, SUB)),
                dma((8,)), dma((8,)),
            ],
            compiler_params=pltpu.CompilerParams(collective_id=0, has_side_effects=True),
            name='qaoa',
        )(cost_local.reshape(shape), gammas, betas)
        energy, state_re, state_im = pl.pallas_call(
            write_out,
            out_shape=(jax.ShapeDtypeStruct((1,), f32),
                       jax.ShapeDtypeStruct(shape, f32), jax.ShapeDtypeStruct(shape, f32)),
            in_specs=[vmem, vmem, vmem],
            out_specs=(hbm, hbm, hbm),
            scratch_shapes=[pltpu.SMEM((1,), f32), dma((3,))],
            name='write_out',
        )(*[pltpu.with_memory_space_constraint(value, pltpu.VMEM) for value in results])
        return energy, state_re.reshape(local_len), state_im.reshape(local_len)

    return jax.shard_map(device_body, mesh=mesh, in_specs=(state_spec, P(), P()),
                         out_specs=(P('inst'), state_spec, state_spec), check_vma=False)
```

```python
import jax
import jax.numpy as jnp
from jax import lax
from jax.experimental import pallas as pl
from jax.experimental.pallas import tpu as pltpu
from jax.sharding import PartitionSpec as P

LANES = 128
LAYERS = 8
SUB = 4
PER_SUB = 8 // SUB
SEND_ORDER = (1, 3, 2)
NEAR = (4, 1)


def rotate(re, im, cos_half, sin_half, steps=None):
    count = len(re)
    for step in steps or [1 << i for i in range(count.bit_length() - 1)]:
        new_re = [cos_half * re[i] + sin_half * im[i ^ step] for i in range(count)]
        new_im = [cos_half * im[i] - sin_half * re[i ^ step] for i in range(count)]
        re, im = new_re, new_im
    return re, im


def sublane_rotate(re, im, cos_half, sin_half):
    row = lax.broadcasted_iota(jnp.int32, (8, LANES), 0)
    for step in (1, 2, 4):
        bit_set = (row & step) != 0

        def flip(value):
            down = pltpu.roll(value, step, 0)
            if step == 4:
                return down
            return jnp.where(bit_set, down, pltpu.roll(value, 8 - step, 0))

        flip_re = [flip(value) for value in re]
        flip_im = [flip(value) for value in im]
        re, im = ([cos_half * r + sin_half * fi for r, fi in zip(re, flip_im)],
                  [cos_half * i - sin_half * fr for i, fr in zip(im, flip_re)])
    return re, im


def lane_matrix(cos_half, sin_half):
    row = lax.broadcasted_iota(jnp.int32, (LANES, LANES), 0)
    col = lax.broadcasted_iota(jnp.int32, (LANES, LANES), 1)
    diff = row ^ col
    cos_full = jnp.broadcast_to(cos_half[0:1], (LANES, LANES))
    sin_full = jnp.broadcast_to(sin_half[0:1], (LANES, LANES))
    mag = jnp.ones((LANES, LANES), jnp.float32)
    weight = jnp.zeros((LANES, LANES), jnp.int32)
    for bit in range(7):
        on = (diff >> bit) & 1
        mag = mag * jnp.where(on == 1, sin_full, cos_full)
        weight = weight + on
    quarter = weight & 3
    zero = jnp.zeros_like(mag)
    real = jnp.where(quarter == 0, mag, jnp.where(quarter == 2, -mag, zero))
    imag = jnp.where(quarter == 1, -mag, jnp.where(quarter == 3, mag, zero))
    return real, imag


def kernel(cost_hbm, gammas_hbm, betas_hbm, energy_all, out_re, out_im,
           cost, cost_near, cost_swap, recv, send, work, cos_buf, sin_buf, cos_near, sin_near,
           rows_in, matrix, energy_part, energy_row, gammas, betas, angle_in, cost_in, near_send, near_recv, cost_send, cost_recv,
           send_sem, recv_sem, e_send, e_recv):
    loads = [pltpu.make_async_copy(cost_hbm.at[:, :, :, pl.ds(sub * 8 * PER_SUB, 8 * PER_SUB)],
                                   cost.at[:, :, :, pl.ds(sub * 8 * PER_SUB, 8 * PER_SUB)], cost_in.at[sub])
             for sub in range(SUB)]
    for load in loads:
        load.start()
    angle_loads = [pltpu.make_async_copy(gammas_hbm, gammas, angle_in.at[0]),
                   pltpu.make_async_copy(betas_hbm, betas, angle_in.at[1])]
    for load in angle_loads:
        load.start()
    qx = lax.axis_index('qx')
    qy = lax.axis_index('qy')
    bits = (qy, qx % 2, qx // 2)

    def flipped(offset):
        return [1 - bit if (offset >> i) & 1 else bit for i, bit in enumerate(bits)]

    def block(offset):
        y, core, x = flipped(offset)
        return (x * 2 + core) * 2 + y

    def peer(offset):
        y, core, x = flipped(offset)
        return {'qy': y, 'qx': x * 2 + core}

    def remote(source, target, send_at, recv_at, offset):
        pltpu.make_async_remote_copy(
            src_ref=source, dst_ref=target, send_sem=send_at, recv_sem=recv_at,
            device_id=peer(offset), device_id_type=pl.DeviceIdType.MESH).start()

    barrier = pltpu.get_barrier_semaphore()
    for offset in range(1, 8):
        pl.semaphore_signal(barrier, inc=1, device_id=peer(offset), device_id_type=pl.DeviceIdType.MESH)
    pl.semaphore_wait(barrier, 7)

    def half_angle(layer):
        angle = jnp.full((8, LANES), 0.5 * betas[layer], jnp.float32)
        return jnp.cos(angle), jnp.sin(angle)

    def wait_bytes(part, sem):
        pltpu.make_async_copy(part, part, sem).wait()

    def wait_all(buffer, sem, at, count):
        wait_bytes(buffer.at[(*at, pl.ds(0, count))], sem.at[at])

    def rows_of(r):
        return pl.ds(pl.multiple_of(r * 8, 8), 8)

    def set_matrix(cos_half, sin_half):
        real, imag = lane_matrix(cos_half, sin_half)
        matrix[0:LANES, 0:LANES] = real
        matrix[0:LANES, LANES:] = imag
        matrix[LANES:, 0:LANES] = -imag
        matrix[LANES:, LANES:] = real

    def put_rows(i, re, im):
        for o in range(16):
            at = pl.multiple_of(o * 16 + i * 8, 8)
            rows_in[pl.ds(at, 8), 0:LANES] = re[o]
            rows_in[pl.ds(at, 8), LANES:] = im[o]

    def lanes(a_held, at):
        work[a_held, at] = lax.dot(
            rows_in[...], matrix[...],
            precision=lax.Precision.HIGHEST, preferred_element_type=jnp.float32)

    def emit(held, mixed, target, a, b, cos_half, sin_half, order, route, local):
        def across(o, buffer):
            def part(r, c):
                at = pl.multiple_of((mixed * 8 + o) * 16 + (r % 2) * 8, 8)
                return work[held, r // 2, pl.ds(at, 8), c * LANES:(c + 1) * LANES]

            re = [part(r, 0) for r in range(8)]
            im = [part(r, 1) for r in range(8)]
            re, im = rotate(re, im, cos_half, sin_half)
            for r in range(8):
                row = (r % PER_SUB) * 8
                buffer[target, a, b, r // PER_SUB, o, 0, row:row + 8, :] = re[r]
                buffer[target, a, b, r // PER_SUB, o, 1, row:row + 8, :] = im[r]

        def body(o, carry):
            across(o, send)
            return carry

        lax.fori_loop(1, 8, body, 0)
        for sub in range(SUB):
            at = (target, a, b, sub)
            for o in order:
                remote(send.at[(*at, o)], recv.at[(*at, o)], send_sem.at[at], recv_sem.at[at], route(o))
            if len(local) == 1:
                y, core, x = bits
                for turn in (1 - core, core):
                    for across_core in range(2):
                        o = 4 + 2 * across_core + turn
                        pltpu.make_async_remote_copy(
                            src_ref=send.at[(*at, o)], dst_ref=recv.at[(*at, o)],
                            send_sem=send_sem.at[at], recv_sem=recv_sem.at[at],
                            device_id={'qy': (y + turn) % 2, 'qx': (1 - x) * 2 + (core + across_core) % 2},
                            device_id_type=pl.DeviceIdType.MESH).start()
        for o in local:
            across(o, recv)

    def first_layer():
        def sub_rows(sub):
            return pl.ds(pl.multiple_of(sub * 8 * PER_SUB, 8), 8 * PER_SUB)

        for sub in range(SUB):
            loads[sub].wait()
            for a in range(2):
                remote(cost.at[:, a, :, sub_rows(sub)], cost_near.at[:, a, :, sub_rows(sub)],
                       near_send.at[a, sub], near_recv.at[a, sub], NEAR[a])
        for a in range(2):
            for o in range(1, 8):
                if not o & NEAR[a]:
                    remote(cost.at[block(o), a], cost_swap.at[o, a], cost_send, cost_recv, o)

        for load in angle_loads:
            load.wait()
        gamma = gammas[0]
        cos_half, sin_half = half_angle(0)
        set_matrix(cos_half, sin_half)

        def own_trig(r, carry):
            for a in range(2):
                for b in range(2):
                    for o in range(8):
                        angle = gamma * cost[block(o), a, b, rows_of(r), :]
                        cos_buf[a, b * 8 + o, rows_of(r), :] = jnp.cos(angle)
                        sin_buf[a, b * 8 + o, rows_of(r), :] = jnp.sin(angle)
            return carry

        lax.fori_loop(0, 8, own_trig, 0)

        def sub_step(sub, carry):
            for a in range(2):
                bit = NEAR[a]
                part = cost_near.at[:, a, :, sub_rows(sub)]
                wait_bytes(part, near_recv.at[a, sub])
                for o in range(1, 8):
                    if not o & bit:
                        remote(cost_near.at[block(o), a, :, sub_rows(sub)],
                               cost_swap.at[o | bit, a, :, sub_rows(sub)], cost_send, cost_recv, o)

                def slots(i, carry):
                    r = sub * PER_SUB + i
                    for b in range(2):
                        for o in range(8):
                            angle = gamma * cost_near[block(o), a, b, rows_of(r), :]
                            cos_near[b * 8 + o] = jnp.cos(angle)
                            sin_near[b * 8 + o] = jnp.sin(angle)
                    re, im = [None] * 16, [None] * 16
                    for b in range(2):
                        for o in range(8):
                            if o & bit:
                                continue
                            here, there = b * 8 + o, b * 8 + (o | bit)
                            for slot, cos_at, sin_at in (
                                    (here, lambda k: cos_buf[a, k, rows_of(r), :], lambda k: sin_buf[a, k, rows_of(r), :]),
                                    (there, lambda k: cos_near[k], lambda k: sin_near[k])):
                                re[slot] = cos_half * cos_at(here) - sin_half * sin_at(there)
                                im[slot] = -(cos_half * sin_at(here)) - sin_half * cos_at(there)
                    re, im = rotate(re, im, cos_half, sin_half, [step for step in (1, 2, 4, 8) if step != bit])
                    re, im = sublane_rotate(re, im, cos_half, sin_half)
                    put_rows(i, re, im)
                    return carry

                lax.fori_loop(0, PER_SUB, slots, 0)
                lanes(a, sub)
            return carry

        lax.fori_loop(0, SUB, sub_step, 0)

        def quarters(b, carry):
            for a in range(2):
                bit = NEAR[a]
                emit(a, b, 1, a, b, cos_half, sin_half,
                     [o for o in (3, 6, 7, 1, 4, 5, 2) if o & ~bit], lambda o: o & ~bit, (0, bit))
            return carry

        lax.fori_loop(0, 2, quarters, 0)
        cost_swap[0] = cost[block(0)]
        for a in range(2):
            cost_swap[NEAR[a], a] = cost_near[block(0), a]
        wait_bytes(cost_swap.at[pl.ds(0, 6)], cost_recv)

    def run_layer(layer, odd, arrived, drained):
        source, target = (0, 1) if odd else (1, 0)

        def quarter(held, mixed):
            return (held, mixed) if odd else (mixed, held)

        cos_half, sin_half = half_angle(layer)
        cos_prev, sin_prev = half_angle(layer - 1)
        gamma = gammas[layer]
        set_matrix(cos_half, sin_half)

        def half(held, carry):
            def trig(r, carry):
                for mixed in range(2):
                    for o in range(8):
                        at = (block(o) if odd else o, *quarter(held, mixed), rows_of(r))
                        angle = gamma * (cost if odd else cost_swap)[at]
                        cos_buf[held, mixed * 8 + o, rows_of(r), :] = jnp.cos(angle)
                        sin_buf[held, mixed * 8 + o, rows_of(r), :] = jnp.sin(angle)
                return carry

            lax.fori_loop(0, 8, trig, 0)

            def sub_step(sub, carry):
                for mixed in range(2):
                    wait_all(recv, recv_sem, (source, *quarter(held, mixed), sub), arrived)

                def slots(i, carry):
                    r = sub * PER_SUB + i
                    cos_phase = [cos_buf[held, o, rows_of(r), :] for o in range(16)]
                    sin_phase = [sin_buf[held, o, rows_of(r), :] for o in range(16)]
                    old = [[recv[(source, *quarter(held, mixed), sub, o, c, rows_of(i))]
                            for mixed in range(2) for o in range(8)] for c in range(2)]
                    old_re, old_im = rotate(*old, cos_prev, sin_prev)
                    re = [r * c + i * s for r, i, c, s in zip(old_re, old_im, cos_phase, sin_phase)]
                    im = [i * c - r * s for r, i, c, s in zip(old_re, old_im, cos_phase, sin_phase)]
                    re, im = rotate(re, im, cos_half, sin_half)
                    re, im = sublane_rotate(re, im, cos_half, sin_half)
                    put_rows(i, re, im)
                    return carry

                lax.fori_loop(0, PER_SUB, slots, 0)
                lanes(held, sub)
                return carry

            lax.fori_loop(0, SUB, sub_step, 0)

            if drained:
                for mixed in range(2):
                    for sub in range(SUB):
                        wait_all(send, send_sem, (target, *quarter(held, mixed), sub), drained)

            def quarters(mixed, carry):
                emit(held, mixed, target, *quarter(held, mixed), cos_half, sin_half, SEND_ORDER, lambda o: o, (0,))
                return carry

            lax.fori_loop(0, 2, quarters, 0)
            return carry

        lax.fori_loop(0, 2, half, 0)

    first_layer()
    run_layer(1, False, 6, 0)
    run_layer(2, True, 7, 6)

    def layer_pair(i, carry):
        run_layer(2 * i + 3, False, 7, 7)
        run_layer(2 * i + 4, True, 7, 7)
        return carry

    lax.fori_loop(0, LAYERS // 2 - 2, layer_pair, 0)
    run_layer(LAYERS - 1, False, 7, 7)

    cos_half, sin_half = half_angle(LAYERS - 1)
    energy_part[...] = jnp.zeros((8, LANES), jnp.float32)

    def final_half(a, carry):
        def final_sub(sub, carry):
            for b in range(2):
                wait_all(recv, recv_sem, (0, a, b, sub), 7)

            def slots(i, carry):
                r = sub * PER_SUB + i
                old = [[recv[0, a, b, sub, o, c, rows_of(i), :] for b in range(2) for o in range(8)]
                       for c in range(2)]
                re, im = rotate(*old, cos_half, sin_half)
                total = energy_part[...]
                for b in range(2):
                    for o in range(8):
                        at = (block(o), a, b, rows_of(r))
                        x, y = re[b * 8 + o], im[b * 8 + o]
                        out_re[at] = x
                        out_im[at] = y
                        total = total + cost[at] * (x * x + y * y)
                energy_part[...] = total
                return carry

            lax.fori_loop(0, PER_SUB, slots, 0)
            return carry

        lax.fori_loop(0, SUB, final_sub, 0)
        return carry

    lax.fori_loop(0, 2, final_half, 0)

    me = block(0)
    energy_row[...] = jnp.sum(energy_part[...], axis=0, keepdims=True)
    for offset in range(1, 8):
        remote(energy_row, energy_all.at[me], e_send.at[offset], e_recv.at[offset], offset)
    energy_all[me] = energy_row[...]
    for par in range(2):
        for a in range(2):
            for b in range(2):
                for sub in range(SUB):
                    wait_all(send, send_sem, (par, a, b, sub), 7)
    for a in range(2):
        for sub in range(SUB):
            wait_bytes(cost.at[:, a, :, pl.ds(sub * 8 * PER_SUB, 8 * PER_SUB)], near_send.at[a, sub])
    wait_bytes(cost_swap.at[pl.ds(0, 6)], cost_send)
    for offset in range(1, 8):
        wait_bytes(energy_row, e_send.at[offset])
        wait_bytes(energy_row, e_recv.at[offset])


def write_out(energy_all, in_re, in_im, energy, out_re, out_im, value, sem):
    copies = [pltpu.make_async_copy(in_re, out_re, sem.at[0]), pltpu.make_async_copy(in_im, out_im, sem.at[1])]
    for copy in copies:
        copy.start()
    total = energy_all[0]
    for i in range(1, 8):
        total = total + energy_all[i]
    value[0] = jnp.sum(total) * (1.0 / (1 << 21))
    copies.append(pltpu.make_async_copy(value, energy, sem.at[2]))
    copies[2].start()
    for copy in copies:
        copy.wait()


def solution(mesh):
    state_spec = P(('inst', 'qx', 'qy'))

    def device_body(cost_local, gammas, betas):
        local_len = cost_local.shape[0]
        shape = (8, 2, 2, local_len // (32 * LANES), LANES)
        f32 = jnp.float32
        vmem = pl.BlockSpec(memory_space=pltpu.VMEM)
        dma = pltpu.SemaphoreType.DMA
        parts = (2, 2, 2, SUB, 8, 2, 8 * PER_SUB, LANES)
        hbm = pl.BlockSpec(memory_space=pl.ANY)
        results = pl.pallas_call(
            kernel,
            out_shape=(pltpu.VMEM((8, 1, LANES), f32), pltpu.VMEM(shape, f32), pltpu.VMEM(shape, f32)),
            in_specs=[hbm, hbm, hbm],
            out_specs=(vmem, vmem, vmem),
            scratch_shapes=[
                pltpu.VMEM(shape, f32), pltpu.VMEM(shape, f32), pltpu.VMEM(shape, f32),
                pltpu.VMEM(parts, f32), pltpu.VMEM(parts, f32),
                pltpu.VMEM((2, 4, 2 * LANES, 2 * LANES), f32),
                pltpu.VMEM((2, 16, 64, LANES), f32), pltpu.VMEM((2, 16, 64, LANES), f32),
                pltpu.VMEM((16, 8, LANES), f32), pltpu.VMEM((16, 8, LANES), f32),
                pltpu.VMEM((2 * LANES, 2 * LANES), f32), pltpu.VMEM((2 * LANES, 2 * LANES), f32),
                pltpu.VMEM((8, LANES), f32), pltpu.VMEM((1, LANES), f32),
                pltpu.SMEM((LAYERS,), f32), pltpu.SMEM((LAYERS,), f32), dma((2,)),
                dma((SUB,)), dma((2, SUB)), dma((2, SUB)), dma, dma,
                dma((2, 2, 2, SUB)), dma((2, 2, 2, SUB)),
                dma((8,)), dma((8,)),
            ],
            compiler_params=pltpu.CompilerParams(collective_id=0, has_side_effects=True),
            name='qaoa',
        )(cost_local.reshape(shape), gammas, betas)
        energy, state_re, state_im = pl.pallas_call(
            write_out,
            out_shape=(jax.ShapeDtypeStruct((1,), f32),
                       jax.ShapeDtypeStruct(shape, f32), jax.ShapeDtypeStruct(shape, f32)),
            in_specs=[vmem, vmem, vmem],
            out_specs=(hbm, hbm, hbm),
            scratch_shapes=[pltpu.SMEM((1,), f32), dma((3,))],
            name='write_out',
        )(*[pltpu.with_memory_space_constraint(value, pltpu.VMEM) for value in results])
        return energy, state_re.reshape(local_len), state_im.reshape(local_len)

    return jax.shard_map(device_body, mesh=mesh, in_specs=(state_spec, P(), P()),
                         out_specs=(P('inst'), state_spec, state_spec), check_vma=False)
```

```python
import jax
import jax.numpy as jnp
from jax import lax
from jax.experimental import pallas as pl
from jax.experimental.pallas import tpu as pltpu
from jax.sharding import PartitionSpec as P

LANES = 128
LAYERS = 8
SUB = 4
PER_SUB = 8 // SUB
SEND_ORDER = (5, 7, 4, 6, 1, 3, 2)
NEAR = (4, 1)


def rotate(re, im, cos_half, sin_half, steps=None):
    count = len(re)
    for step in steps or [1 << i for i in range(count.bit_length() - 1)]:
        new_re = [cos_half * re[i] + sin_half * im[i ^ step] for i in range(count)]
        new_im = [cos_half * im[i] - sin_half * re[i ^ step] for i in range(count)]
        re, im = new_re, new_im
    return re, im


def sublane_rotate(re, im, cos_half, sin_half):
    row = lax.broadcasted_iota(jnp.int32, (8, LANES), 0)
    for step in (1, 2, 4):
        bit_set = (row & step) != 0

        def flip(value):
            down = pltpu.roll(value, step, 0)
            if step == 4:
                return down
            return jnp.where(bit_set, down, pltpu.roll(value, 8 - step, 0))

        flip_re = [flip(value) for value in re]
        flip_im = [flip(value) for value in im]
        re, im = ([cos_half * r + sin_half * fi for r, fi in zip(re, flip_im)],
                  [cos_half * i - sin_half * fr for i, fr in zip(im, flip_re)])
    return re, im


def lane_matrix(cos_half, sin_half):
    row = lax.broadcasted_iota(jnp.int32, (LANES, LANES), 0)
    col = lax.broadcasted_iota(jnp.int32, (LANES, LANES), 1)
    diff = row ^ col
    cos_full = jnp.broadcast_to(cos_half[0:1], (LANES, LANES))
    sin_full = jnp.broadcast_to(sin_half[0:1], (LANES, LANES))
    mag = jnp.ones((LANES, LANES), jnp.float32)
    weight = jnp.zeros((LANES, LANES), jnp.int32)
    for bit in range(7):
        on = (diff >> bit) & 1
        mag = mag * jnp.where(on == 1, sin_full, cos_full)
        weight = weight + on
    quarter = weight & 3
    zero = jnp.zeros_like(mag)
    real = jnp.where(quarter == 0, mag, jnp.where(quarter == 2, -mag, zero))
    imag = jnp.where(quarter == 1, -mag, jnp.where(quarter == 3, mag, zero))
    return real, imag


def kernel(cost_hbm, gammas_hbm, betas_hbm, energy_all, out_re, out_im,
           cost, cost_near, cost_swap, recv, send, work, cos_buf, sin_buf, cos_near, sin_near,
           rows_in, matrix, energy_part, energy_row, gammas, betas, angle_in, near_in, cost_in, near_send, near_recv, cost_send, cost_recv,
           send_sem, recv_sem, e_send, e_recv):
    loads = [pltpu.make_async_copy(cost_hbm.at[:, :, :, pl.ds(sub * 8 * PER_SUB, 8 * PER_SUB)],
                                   cost.at[:, :, :, pl.ds(sub * 8 * PER_SUB, 8 * PER_SUB)], cost_in.at[sub])
             for sub in range(SUB)]
    for load in loads:
        load.start()
    angle_loads = [pltpu.make_async_copy(gammas_hbm, gammas, angle_in.at[0]),
                   pltpu.make_async_copy(betas_hbm, betas, angle_in.at[1])]
    for load in angle_loads:
        load.start()
    qx = lax.axis_index('qx')
    qy = lax.axis_index('qy')
    bits = (qy, qx % 2, qx // 2)

    def flipped(offset):
        return [1 - bit if (offset >> i) & 1 else bit for i, bit in enumerate(bits)]

    def block(offset):
        y, core, x = flipped(offset)
        return (x * 2 + core) * 2 + y

    def peer(offset):
        y, core, x = flipped(offset)
        return {'qy': y, 'qx': x * 2 + core}

    def remote(source, target, send_at, recv_at, offset):
        pltpu.make_async_remote_copy(
            src_ref=source, dst_ref=target, send_sem=send_at, recv_sem=recv_at,
            device_id=peer(offset), device_id_type=pl.DeviceIdType.MESH).start()

    barrier = pltpu.get_barrier_semaphore()
    def signal_next(sem):
        for offset in (4, 1, 2):
            pl.semaphore_signal(sem, inc=1, device_id=peer(offset), device_id_type=pl.DeviceIdType.MESH)

    signal_next(barrier)
    pl.semaphore_wait(barrier, 3)

    def half_angle(layer):
        angle = jnp.full((8, LANES), 0.5 * betas[layer], jnp.float32)
        return jnp.cos(angle), jnp.sin(angle)

    def wait_bytes(part, sem):
        pltpu.make_async_copy(part, part, sem).wait()

    def wait_all(buffer, sem, at, count):
        wait_bytes(buffer.at[(*at, pl.ds(0, count))], sem.at[at])

    def rows_of(r):
        return pl.ds(pl.multiple_of(r * 8, 8), 8)

    def set_matrix(cos_half, sin_half):
        real, imag = lane_matrix(cos_half, sin_half)
        matrix[0:LANES, 0:LANES] = real
        matrix[0:LANES, LANES:] = imag
        matrix[LANES:, 0:LANES] = -imag
        matrix[LANES:, LANES:] = real

    def put_rows(i, re, im):
        for o in range(16):
            at = pl.multiple_of(o * 16 + i * 8, 8)
            rows_in[pl.ds(at, 8), 0:LANES] = re[o]
            rows_in[pl.ds(at, 8), LANES:] = im[o]

    def lanes(a_held, at):
        work[a_held, at] = lax.dot(
            rows_in[...], matrix[...],
            precision=lax.Precision.HIGHEST, preferred_element_type=jnp.float32)

    def emit(held, mixed, target, a, b, cos_half, sin_half, order, route, local):
        def across(o, buffer):
            def part(r, c):
                at = pl.multiple_of((mixed * 8 + o) * 16 + (r % 2) * 8, 8)
                return work[held, r // 2, pl.ds(at, 8), c * LANES:(c + 1) * LANES]

            re = [part(r, 0) for r in range(8)]
            im = [part(r, 1) for r in range(8)]
            re, im = rotate(re, im, cos_half, sin_half)
            for r in range(8):
                row = (r % PER_SUB) * 8
                buffer[target, a, b, r // PER_SUB, o, 0, row:row + 8, :] = re[r]
                buffer[target, a, b, r // PER_SUB, o, 1, row:row + 8, :] = im[r]

        def body(o, carry):
            across(o, send)
            return carry

        lax.fori_loop(1, 8, body, 0)
        for o in local:
            across(o, recv)
        for sub in range(SUB):
            at = (target, a, b, sub)
            for o in order:
                remote(send.at[(*at, o)], recv.at[(*at, o)], send_sem.at[at], recv_sem.at[at], route(o))

    def first_layer():
        def sub_rows(sub):
            return pl.ds(pl.multiple_of(sub * 8 * PER_SUB, 8), 8 * PER_SUB)

        for sub in range(SUB):
            loads[sub].wait()
            for a in range(2):
                remote(cost.at[:, a, :, sub_rows(sub)], cost_near.at[:, a, :, sub_rows(sub)],
                       near_send.at[a, sub], near_recv.at[a, sub], NEAR[a])
        signal_next(near_in.at[0])
        for load in angle_loads:
            load.wait()
        gamma = gammas[0]
        cos_half, sin_half = half_angle(0)
        set_matrix(cos_half, sin_half)

        def own_trig(r, carry):
            for a in range(2):
                for b in range(2):
                    for o in range(8):
                        angle = gamma * cost[block(o), a, b, rows_of(r), :]
                        cos_buf[a, b * 8 + o, rows_of(r), :] = jnp.cos(angle)
                        sin_buf[a, b * 8 + o, rows_of(r), :] = jnp.sin(angle)
            return carry

        for round_id in range(2):
            lax.fori_loop(4 * round_id, 4 * round_id + 4, own_trig, 0)
            pl.semaphore_wait(near_in.at[round_id], 3)
            if round_id == 0:
                signal_next(near_in.at[1])
        for a in range(2):
            for o in range(1, 8):
                if not o & NEAR[a]:
                    remote(cost.at[block(o), a], cost_swap.at[o, a], cost_send, cost_recv, o)

        def sub_step(sub, carry):
            for a in range(2):
                bit = NEAR[a]
                part = cost_near.at[:, a, :, sub_rows(sub)]
                wait_bytes(part, near_recv.at[a, sub])
                for o in range(1, 8):
                    if not o & bit:
                        remote(cost_near.at[block(o), a, :, sub_rows(sub)],
                               cost_swap.at[o | bit, a, :, sub_rows(sub)], cost_send, cost_recv, o)

                def slots(i, carry):
                    r = sub * PER_SUB + i
                    for b in range(2):
                        for o in range(8):
                            angle = gamma * cost_near[block(o), a, b, rows_of(r), :]
                            cos_near[b * 8 + o] = jnp.cos(angle)
                            sin_near[b * 8 + o] = jnp.sin(angle)
                    re, im = [None] * 16, [None] * 16
                    for b in range(2):
                        for o in range(8):
                            if o & bit:
                                continue
                            here, there = b * 8 + o, b * 8 + (o | bit)
                            for slot, cos_at, sin_at in (
                                    (here, lambda k: cos_buf[a, k, rows_of(r), :], lambda k: sin_buf[a, k, rows_of(r), :]),
                                    (there, lambda k: cos_near[k], lambda k: sin_near[k])):
                                re[slot] = cos_half * cos_at(here) - sin_half * sin_at(there)
                                im[slot] = -(cos_half * sin_at(here)) - sin_half * cos_at(there)
                    re, im = rotate(re, im, cos_half, sin_half, [step for step in (1, 2, 4, 8) if step != bit])
                    re, im = sublane_rotate(re, im, cos_half, sin_half)
                    put_rows(i, re, im)
                    return carry

                lax.fori_loop(0, PER_SUB, slots, 0)
                lanes(a, sub)
            return carry

        lax.fori_loop(0, SUB, sub_step, 0)

        def quarters(b, carry):
            for a in range(2):
                bit = NEAR[a]
                emit(a, b, 1, a, b, cos_half, sin_half,
                     [o for o in (3, 6, 7, 1, 4, 5, 2) if o & ~bit], lambda o: o & ~bit, (0, bit))
            return carry

        lax.fori_loop(0, 2, quarters, 0)
        cost_swap[0] = cost[block(0)]
        for a in range(2):
            cost_swap[NEAR[a], a] = cost_near[block(0), a]
        wait_bytes(cost_swap.at[pl.ds(0, 6)], cost_recv)

    def run_layer(layer, odd, arrived, drained):
        source, target = (0, 1) if odd else (1, 0)

        def quarter(held, mixed):
            return (held, mixed) if odd else (mixed, held)

        cos_half, sin_half = half_angle(layer)
        cos_prev, sin_prev = half_angle(layer - 1)
        gamma = gammas[layer]
        set_matrix(cos_half, sin_half)

        def half(held, carry):
            def trig(r, carry):
                for mixed in range(2):
                    for o in range(8):
                        at = (block(o) if odd else o, *quarter(held, mixed), rows_of(r))
                        angle = gamma * (cost if odd else cost_swap)[at]
                        cos_buf[held, mixed * 8 + o, rows_of(r), :] = jnp.cos(angle)
                        sin_buf[held, mixed * 8 + o, rows_of(r), :] = jnp.sin(angle)
                return carry

            lax.fori_loop(0, 8, trig, 0)

            def sub_step(sub, carry):
                for mixed in range(2):
                    wait_all(recv, recv_sem, (source, *quarter(held, mixed), sub), arrived)

                def slots(i, carry):
                    r = sub * PER_SUB + i
                    cos_phase = [cos_buf[held, o, rows_of(r), :] for o in range(16)]
                    sin_phase = [sin_buf[held, o, rows_of(r), :] for o in range(16)]
                    old = [[recv[(source, *quarter(held, mixed), sub, o, c, rows_of(i))]
                            for mixed in range(2) for o in range(8)] for c in range(2)]
                    old_re, old_im = rotate(*old, cos_prev, sin_prev)
                    re = [r * c + i * s for r, i, c, s in zip(old_re, old_im, cos_phase, sin_phase)]
                    im = [i * c - r * s for r, i, c, s in zip(old_re, old_im, cos_phase, sin_phase)]
                    re, im = rotate(re, im, cos_half, sin_half)
                    re, im = sublane_rotate(re, im, cos_half, sin_half)
                    put_rows(i, re, im)
                    return carry

                lax.fori_loop(0, PER_SUB, slots, 0)
                lanes(held, sub)
                return carry

            lax.fori_loop(0, SUB, sub_step, 0)

            if drained:
                for mixed in range(2):
                    for sub in range(SUB):
                        wait_all(send, send_sem, (target, *quarter(held, mixed), sub), drained)

            def quarters(mixed, carry):
                emit(held, mixed, target, *quarter(held, mixed), cos_half, sin_half, SEND_ORDER, lambda o: o, (0,))
                return carry

            lax.fori_loop(0, 2, quarters, 0)
            return carry

        lax.fori_loop(0, 2, half, 0)

    first_layer()
    run_layer(1, False, 6, 0)
    run_layer(2, True, 7, 6)

    def layer_pair(i, carry):
        run_layer(2 * i + 3, False, 7, 7)
        run_layer(2 * i + 4, True, 7, 7)
        return carry

    lax.fori_loop(0, LAYERS // 2 - 2, layer_pair, 0)
    run_layer(LAYERS - 1, False, 7, 7)

    cos_half, sin_half = half_angle(LAYERS - 1)
    energy_part[...] = jnp.zeros((8, LANES), jnp.float32)

    def final_half(a, carry):
        def final_sub(sub, carry):
            for b in range(2):
                wait_all(recv, recv_sem, (0, a, b, sub), 7)

            def slots(i, carry):
                r = sub * PER_SUB + i
                old = [[recv[0, a, b, sub, o, c, rows_of(i), :] for b in range(2) for o in range(8)]
                       for c in range(2)]
                re, im = rotate(*old, cos_half, sin_half)
                total = energy_part[...]
                for b in range(2):
                    for o in range(8):
                        at = (block(o), a, b, rows_of(r))
                        x, y = re[b * 8 + o], im[b * 8 + o]
                        out_re[at] = x
                        out_im[at] = y
                        total = total + cost[at] * (x * x + y * y)
                energy_part[...] = total
                return carry

            lax.fori_loop(0, PER_SUB, slots, 0)
            return carry

        lax.fori_loop(0, SUB, final_sub, 0)
        return carry

    lax.fori_loop(0, 2, final_half, 0)

    me = block(0)
    energy_row[...] = jnp.sum(energy_part[...], axis=0, keepdims=True)
    for offset in range(1, 8):
        remote(energy_row, energy_all.at[me], e_send.at[offset], e_recv.at[offset], offset)
    energy_all[me] = energy_row[...]
    for par in range(2):
        for a in range(2):
            for b in range(2):
                for sub in range(SUB):
                    wait_all(send, send_sem, (par, a, b, sub), 7)
    for a in range(2):
        for sub in range(SUB):
            wait_bytes(cost.at[:, a, :, pl.ds(sub * 8 * PER_SUB, 8 * PER_SUB)], near_send.at[a, sub])
    wait_bytes(cost_swap.at[pl.ds(0, 6)], cost_send)
    for offset in range(1, 8):
        wait_bytes(energy_row, e_send.at[offset])
        wait_bytes(energy_row, e_recv.at[offset])


def write_out(energy_all, in_re, in_im, energy, out_re, out_im, value, sem):
    copies = [pltpu.make_async_copy(in_re, out_re, sem.at[0]), pltpu.make_async_copy(in_im, out_im, sem.at[1])]
    for copy in copies:
        copy.start()
    total = energy_all[0]
    for i in range(1, 8):
        total = total + energy_all[i]
    value[0] = jnp.sum(total) * (1.0 / (1 << 21))
    copies.append(pltpu.make_async_copy(value, energy, sem.at[2]))
    copies[2].start()
    for copy in copies:
        copy.wait()


def solution(mesh):
    state_spec = P(('inst', 'qx', 'qy'))

    def device_body(cost_local, gammas, betas):
        local_len = cost_local.shape[0]
        shape = (8, 2, 2, local_len // (32 * LANES), LANES)
        f32 = jnp.float32
        vmem = pl.BlockSpec(memory_space=pltpu.VMEM)
        dma = pltpu.SemaphoreType.DMA
        parts = (2, 2, 2, SUB, 8, 2, 8 * PER_SUB, LANES)
        hbm = pl.BlockSpec(memory_space=pl.ANY)
        results = pl.pallas_call(
            kernel,
            out_shape=(pltpu.VMEM((8, 1, LANES), f32), pltpu.VMEM(shape, f32), pltpu.VMEM(shape, f32)),
            in_specs=[hbm, hbm, hbm],
            out_specs=(vmem, vmem, vmem),
            scratch_shapes=[
                pltpu.VMEM(shape, f32), pltpu.VMEM(shape, f32), pltpu.VMEM(shape, f32),
                pltpu.VMEM(parts, f32), pltpu.VMEM(parts, f32),
                pltpu.VMEM((2, 4, 2 * LANES, 2 * LANES), f32),
                pltpu.VMEM((2, 16, 64, LANES), f32), pltpu.VMEM((2, 16, 64, LANES), f32),
                pltpu.VMEM((16, 8, LANES), f32), pltpu.VMEM((16, 8, LANES), f32),
                pltpu.VMEM((2 * LANES, 2 * LANES), f32), pltpu.VMEM((2 * LANES, 2 * LANES), f32),
                pltpu.VMEM((8, LANES), f32), pltpu.VMEM((1, LANES), f32),
                pltpu.SMEM((LAYERS,), f32), pltpu.SMEM((LAYERS,), f32), dma((2,)), pltpu.SemaphoreType.REGULAR((2,)),
                dma((SUB,)), dma((2, SUB)), dma((2, SUB)), dma, dma,
                dma((2, 2, 2, SUB)), dma((2, 2, 2, SUB)),
                dma((8,)), dma((8,)),
            ],
            compiler_params=pltpu.CompilerParams(collective_id=0, has_side_effects=True),
            name='qaoa',
        )(cost_local.reshape(shape), gammas, betas)
        energy, state_re, state_im = pl.pallas_call(
            write_out,
            out_shape=(jax.ShapeDtypeStruct((1,), f32),
                       jax.ShapeDtypeStruct(shape, f32), jax.ShapeDtypeStruct(shape, f32)),
            in_specs=[vmem, vmem, vmem],
            out_specs=(hbm, hbm, hbm),
            scratch_shapes=[pltpu.SMEM((1,), f32), dma((3,))],
            name='write_out',
        )(*[pltpu.with_memory_space_constraint(value, pltpu.VMEM) for value in results])
        return energy, state_re.reshape(local_len), state_im.reshape(local_len)

    return jax.shard_map(device_body, mesh=mesh, in_specs=(state_spec, P(), P()),
                         out_specs=(P('inst'), state_spec, state_spec), check_vma=False)
```

```python
import jax
import jax.numpy as jnp
from jax import lax
from jax.experimental import pallas as pl
from jax.experimental.pallas import tpu as pltpu
from jax.sharding import PartitionSpec as P

LANES = 128
LAYERS = 8
SUB = 2
PER_SUB = 8 // SUB
SEND_ORDER = (5, 7, 4, 6, 1, 3, 2)
NEAR = (4, 1)


def rotate(re, im, cos_half, sin_half, steps=None):
    count = len(re)
    for step in steps or [1 << i for i in range(count.bit_length() - 1)]:
        new_re = [cos_half * re[i] + sin_half * im[i ^ step] for i in range(count)]
        new_im = [cos_half * im[i] - sin_half * re[i ^ step] for i in range(count)]
        re, im = new_re, new_im
    return re, im


def sublane_rotate(re, im, cos_half, sin_half):
    row = lax.broadcasted_iota(jnp.int32, (8, LANES), 0)
    for step in (1, 2, 4):
        bit_set = (row & step) != 0

        def flip(value):
            down = pltpu.roll(value, step, 0)
            if step == 4:
                return down
            return jnp.where(bit_set, down, pltpu.roll(value, 8 - step, 0))

        flip_re = [flip(value) for value in re]
        flip_im = [flip(value) for value in im]
        re, im = ([cos_half * r + sin_half * fi for r, fi in zip(re, flip_im)],
                  [cos_half * i - sin_half * fr for i, fr in zip(im, flip_re)])
    return re, im


def lane_matrix(cos_half, sin_half):
    row = lax.broadcasted_iota(jnp.int32, (LANES, LANES), 0)
    col = lax.broadcasted_iota(jnp.int32, (LANES, LANES), 1)
    diff = row ^ col
    cos_full = jnp.broadcast_to(cos_half[0:1], (LANES, LANES))
    sin_full = jnp.broadcast_to(sin_half[0:1], (LANES, LANES))
    mag = jnp.ones((LANES, LANES), jnp.float32)
    weight = jnp.zeros((LANES, LANES), jnp.int32)
    for bit in range(7):
        on = (diff >> bit) & 1
        mag = mag * jnp.where(on == 1, sin_full, cos_full)
        weight = weight + on
    quarter = weight & 3
    zero = jnp.zeros_like(mag)
    real = jnp.where(quarter == 0, mag, jnp.where(quarter == 2, -mag, zero))
    imag = jnp.where(quarter == 1, -mag, jnp.where(quarter == 3, mag, zero))
    return real, imag


def kernel(cost_hbm, gammas_hbm, betas_hbm, energy_all, out_re, out_im,
           cost, cost_near, cost_swap, recv, send, work, cos_buf, sin_buf, cos_near, sin_near,
           rows_in, matrix, energy_part, energy_row, gammas, betas, angle_in, near_in, cost_in, near_send, near_recv, cost_send, cost_recv,
           send_sem, recv_sem, e_send, e_recv):
    loads = [pltpu.make_async_copy(cost_hbm.at[:, :, :, pl.ds(sub * 8 * PER_SUB, 8 * PER_SUB)],
                                   cost.at[:, :, :, pl.ds(sub * 8 * PER_SUB, 8 * PER_SUB)], cost_in.at[sub])
             for sub in range(SUB)]
    for load in loads:
        load.start()
    angle_loads = [pltpu.make_async_copy(gammas_hbm, gammas, angle_in.at[0]),
                   pltpu.make_async_copy(betas_hbm, betas, angle_in.at[1])]
    for load in angle_loads:
        load.start()
    qx = lax.axis_index('qx')
    qy = lax.axis_index('qy')
    bits = (qy, qx % 2, qx // 2)

    def flipped(offset):
        return [1 - bit if (offset >> i) & 1 else bit for i, bit in enumerate(bits)]

    def block(offset):
        y, core, x = flipped(offset)
        return (x * 2 + core) * 2 + y

    def peer(offset):
        y, core, x = flipped(offset)
        return {'qy': y, 'qx': x * 2 + core}

    def remote(source, target, send_at, recv_at, offset):
        pltpu.make_async_remote_copy(
            src_ref=source, dst_ref=target, send_sem=send_at, recv_sem=recv_at,
            device_id=peer(offset), device_id_type=pl.DeviceIdType.MESH).start()

    barrier = pltpu.get_barrier_semaphore()
    def signal_next(sem):
        for offset in (4, 1, 2):
            pl.semaphore_signal(sem, inc=1, device_id=peer(offset), device_id_type=pl.DeviceIdType.MESH)

    signal_next(barrier)
    pl.semaphore_wait(barrier, 3)

    def half_angle(layer):
        angle = jnp.full((8, LANES), 0.5 * betas[layer], jnp.float32)
        return jnp.cos(angle), jnp.sin(angle)

    def wait_bytes(part, sem):
        pltpu.make_async_copy(part, part, sem).wait()

    def wait_all(buffer, sem, at, count):
        wait_bytes(buffer.at[(*at, pl.ds(0, count))], sem.at[at])

    def rows_of(r):
        return pl.ds(pl.multiple_of(r * 8, 8), 8)

    def set_matrix(cos_half, sin_half):
        real, imag = lane_matrix(cos_half, sin_half)
        matrix[0:LANES, 0:LANES] = real
        matrix[0:LANES, LANES:] = imag
        matrix[LANES:, 0:LANES] = -imag
        matrix[LANES:, LANES:] = real

    def put_rows(i, re, im):
        for o in range(16):
            at = pl.multiple_of(o * 16 + i * 8, 8)
            rows_in[pl.ds(at, 8), 0:LANES] = re[o]
            rows_in[pl.ds(at, 8), LANES:] = im[o]

    def lanes(a_held, at):
        work[a_held, at] = lax.dot(
            rows_in[...], matrix[...],
            precision=lax.Precision.HIGHEST, preferred_element_type=jnp.float32)

    def emit(held, mixed, target, a, b, cos_half, sin_half, order, route, local):
        def across(o, buffer):
            def part(r, c):
                at = pl.multiple_of((mixed * 8 + o) * 16 + (r % 2) * 8, 8)
                return work[held, r // 2, pl.ds(at, 8), c * LANES:(c + 1) * LANES]

            re = [part(r, 0) for r in range(8)]
            im = [part(r, 1) for r in range(8)]
            re, im = rotate(re, im, cos_half, sin_half)
            for r in range(8):
                row = (r % PER_SUB) * 8
                buffer[target, a, b, r // PER_SUB, o, 0, row:row + 8, :] = re[r]
                buffer[target, a, b, r // PER_SUB, o, 1, row:row + 8, :] = im[r]

        def body(o, carry):
            across(o, send)
            return carry

        lax.fori_loop(1, 8, body, 0)
        for o in local:
            across(o, recv)
        for sub in range(SUB):
            at = (target, a, b, sub)
            for o in order:
                remote(send.at[(*at, o)], recv.at[(*at, o)], send_sem.at[at], recv_sem.at[at], route(o))

    def first_layer():
        def sub_rows(sub):
            return pl.ds(pl.multiple_of(sub * 8 * PER_SUB, 8), 8 * PER_SUB)

        for sub in range(SUB):
            loads[sub].wait()
            for a in range(2):
                remote(cost.at[:, a, :, sub_rows(sub)], cost_near.at[:, a, :, sub_rows(sub)],
                       near_send.at[a, sub], near_recv.at[a, sub], NEAR[a])
        signal_next(near_in.at[0])
        for load in angle_loads:
            load.wait()
        gamma = gammas[0]
        cos_half, sin_half = half_angle(0)
        set_matrix(cos_half, sin_half)

        def own_trig(r, carry):
            for a in range(2):
                for b in range(2):
                    for o in range(8):
                        angle = gamma * cost[block(o), a, b, rows_of(r), :]
                        cos_buf[a, b * 8 + o, rows_of(r), :] = jnp.cos(angle)
                        sin_buf[a, b * 8 + o, rows_of(r), :] = jnp.sin(angle)
            return carry

        for round_id in range(2):
            lax.fori_loop(4 * round_id, 4 * round_id + 4, own_trig, 0)
            pl.semaphore_wait(near_in.at[round_id], 3)
            if round_id == 0:
                signal_next(near_in.at[1])
        for a in range(2):
            for o in range(1, 8):
                if not o & NEAR[a]:
                    remote(cost.at[block(o), a], cost_swap.at[o, a], cost_send, cost_recv, o)

        def sub_step(sub, carry):
            for a in range(2):
                bit = NEAR[a]
                part = cost_near.at[:, a, :, sub_rows(sub)]
                wait_bytes(part, near_recv.at[a, sub])
                for o in range(1, 8):
                    if not o & bit:
                        remote(cost_near.at[block(o), a, :, sub_rows(sub)],
                               cost_swap.at[o | bit, a, :, sub_rows(sub)], cost_send, cost_recv, o)

                def slots(i, carry):
                    r = sub * PER_SUB + i
                    for b in range(2):
                        for o in range(8):
                            angle = gamma * cost_near[block(o), a, b, rows_of(r), :]
                            cos_near[b * 8 + o] = jnp.cos(angle)
                            sin_near[b * 8 + o] = jnp.sin(angle)
                    re, im = [None] * 16, [None] * 16
                    for b in range(2):
                        for o in range(8):
                            if o & bit:
                                continue
                            here, there = b * 8 + o, b * 8 + (o | bit)
                            for slot, cos_at, sin_at in (
                                    (here, lambda k: cos_buf[a, k, rows_of(r), :], lambda k: sin_buf[a, k, rows_of(r), :]),
                                    (there, lambda k: cos_near[k], lambda k: sin_near[k])):
                                re[slot] = cos_half * cos_at(here) - sin_half * sin_at(there)
                                im[slot] = -(cos_half * sin_at(here)) - sin_half * cos_at(there)
                    re, im = rotate(re, im, cos_half, sin_half, [step for step in (1, 2, 4, 8) if step != bit])
                    re, im = sublane_rotate(re, im, cos_half, sin_half)
                    put_rows(i % 2, re, im)
                    return carry

                def blocks(k, carry):
                    lax.fori_loop(2 * k, 2 * k + 2, slots, 0)
                    lanes(a, sub * (PER_SUB // 2) + k)
                    return carry

                lax.fori_loop(0, PER_SUB // 2, blocks, 0)
            return carry

        lax.fori_loop(0, SUB, sub_step, 0)

        def quarters(b, carry):
            for a in range(2):
                bit = NEAR[a]
                emit(a, b, 1, a, b, cos_half, sin_half,
                     [o for o in (3, 6, 7, 1, 4, 5, 2) if o & ~bit], lambda o: o & ~bit, (0, bit))
            return carry

        lax.fori_loop(0, 2, quarters, 0)
        cost_swap[0] = cost[block(0)]
        for a in range(2):
            cost_swap[NEAR[a], a] = cost_near[block(0), a]
        wait_bytes(cost_swap.at[pl.ds(0, 6)], cost_recv)

    def run_layer(layer, odd, arrived, drained):
        source, target = (0, 1) if odd else (1, 0)

        def quarter(held, mixed):
            return (held, mixed) if odd else (mixed, held)

        cos_half, sin_half = half_angle(layer)
        cos_prev, sin_prev = half_angle(layer - 1)
        gamma = gammas[layer]
        set_matrix(cos_half, sin_half)

        def half(held, carry):
            def trig(r, carry):
                for mixed in range(2):
                    for o in range(8):
                        at = (block(o) if odd else o, *quarter(held, mixed), rows_of(r))
                        angle = gamma * (cost if odd else cost_swap)[at]
                        cos_buf[held, mixed * 8 + o, rows_of(r), :] = jnp.cos(angle)
                        sin_buf[held, mixed * 8 + o, rows_of(r), :] = jnp.sin(angle)
                return carry

            lax.fori_loop(0, 8, trig, 0)

            def sub_step(sub, carry):
                for mixed in range(2):
                    wait_all(recv, recv_sem, (source, *quarter(held, mixed), sub), arrived)

                def slots(i, carry):
                    r = sub * PER_SUB + i
                    cos_phase = [cos_buf[held, o, rows_of(r), :] for o in range(16)]
                    sin_phase = [sin_buf[held, o, rows_of(r), :] for o in range(16)]
                    old = [[recv[(source, *quarter(held, mixed), sub, o, c, rows_of(i))]
                            for mixed in range(2) for o in range(8)] for c in range(2)]
                    old_re, old_im = rotate(*old, cos_prev, sin_prev)
                    re = [r * c + i * s for r, i, c, s in zip(old_re, old_im, cos_phase, sin_phase)]
                    im = [i * c - r * s for r, i, c, s in zip(old_re, old_im, cos_phase, sin_phase)]
                    re, im = rotate(re, im, cos_half, sin_half)
                    re, im = sublane_rotate(re, im, cos_half, sin_half)
                    put_rows(i % 2, re, im)
                    return carry

                def blocks(k, carry):
                    lax.fori_loop(2 * k, 2 * k + 2, slots, 0)
                    lanes(held, sub * (PER_SUB // 2) + k)
                    return carry

                lax.fori_loop(0, PER_SUB // 2, blocks, 0)
                return carry

            lax.fori_loop(0, SUB, sub_step, 0)

            if drained:
                for mixed in range(2):
                    for sub in range(SUB):
                        wait_all(send, send_sem, (target, *quarter(held, mixed), sub), drained)

            def quarters(mixed, carry):
                emit(held, mixed, target, *quarter(held, mixed), cos_half, sin_half, SEND_ORDER, lambda o: o, (0,))
                return carry

            lax.fori_loop(0, 2, quarters, 0)
            return carry

        lax.fori_loop(0, 2, half, 0)

    first_layer()
    run_layer(1, False, 6, 0)
    run_layer(2, True, 7, 6)

    def layer_pair(i, carry):
        run_layer(2 * i + 3, False, 7, 7)
        run_layer(2 * i + 4, True, 7, 7)
        return carry

    lax.fori_loop(0, LAYERS // 2 - 2, layer_pair, 0)
    run_layer(LAYERS - 1, False, 7, 7)

    cos_half, sin_half = half_angle(LAYERS - 1)
    energy_part[...] = jnp.zeros((8, LANES), jnp.float32)

    def final_half(a, carry):
        def final_sub(sub, carry):
            for b in range(2):
                wait_all(recv, recv_sem, (0, a, b, sub), 7)

            def slots(i, carry):
                r = sub * PER_SUB + i
                old = [[recv[0, a, b, sub, o, c, rows_of(i), :] for b in range(2) for o in range(8)]
                       for c in range(2)]
                re, im = rotate(*old, cos_half, sin_half)
                total = energy_part[...]
                for b in range(2):
                    for o in range(8):
                        at = (block(o), a, b, rows_of(r))
                        x, y = re[b * 8 + o], im[b * 8 + o]
                        out_re[at] = x
                        out_im[at] = y
                        total = total + cost[at] * (x * x + y * y)
                energy_part[...] = total
                return carry

            lax.fori_loop(0, PER_SUB, slots, 0)
            return carry

        lax.fori_loop(0, SUB, final_sub, 0)
        return carry

    lax.fori_loop(0, 2, final_half, 0)

    me = block(0)
    energy_row[...] = jnp.sum(energy_part[...], axis=0, keepdims=True)
    for offset in range(1, 8):
        remote(energy_row, energy_all.at[me], e_send.at[offset], e_recv.at[offset], offset)
    energy_all[me] = energy_row[...]
    for par in range(2):
        for a in range(2):
            for b in range(2):
                for sub in range(SUB):
                    wait_all(send, send_sem, (par, a, b, sub), 7)
    for a in range(2):
        for sub in range(SUB):
            wait_bytes(cost.at[:, a, :, pl.ds(sub * 8 * PER_SUB, 8 * PER_SUB)], near_send.at[a, sub])
    wait_bytes(cost_swap.at[pl.ds(0, 6)], cost_send)
    for offset in range(1, 8):
        wait_bytes(energy_row, e_send.at[offset])
        wait_bytes(energy_row, e_recv.at[offset])


def write_out(energy_all, in_re, in_im, energy, out_re, out_im, value, sem):
    copies = [pltpu.make_async_copy(in_re, out_re, sem.at[0]), pltpu.make_async_copy(in_im, out_im, sem.at[1])]
    for copy in copies:
        copy.start()
    total = energy_all[0]
    for i in range(1, 8):
        total = total + energy_all[i]
    value[0] = jnp.sum(total) * (1.0 / (1 << 21))
    copies.append(pltpu.make_async_copy(value, energy, sem.at[2]))
    copies[2].start()
    for copy in copies:
        copy.wait()


def solution(mesh):
    state_spec = P(('inst', 'qx', 'qy'))

    def device_body(cost_local, gammas, betas):
        local_len = cost_local.shape[0]
        shape = (8, 2, 2, local_len // (32 * LANES), LANES)
        f32 = jnp.float32
        vmem = pl.BlockSpec(memory_space=pltpu.VMEM)
        dma = pltpu.SemaphoreType.DMA
        parts = (2, 2, 2, SUB, 8, 2, 8 * PER_SUB, LANES)
        hbm = pl.BlockSpec(memory_space=pl.ANY)
        results = pl.pallas_call(
            kernel,
            out_shape=(pltpu.VMEM((8, 1, LANES), f32), pltpu.VMEM(shape, f32), pltpu.VMEM(shape, f32)),
            in_specs=[hbm, hbm, hbm],
            out_specs=(vmem, vmem, vmem),
            scratch_shapes=[
                pltpu.VMEM(shape, f32), pltpu.VMEM(shape, f32), pltpu.VMEM(shape, f32),
                pltpu.VMEM(parts, f32), pltpu.VMEM(parts, f32),
                pltpu.VMEM((2, 4, 2 * LANES, 2 * LANES), f32),
                pltpu.VMEM((2, 16, 64, LANES), f32), pltpu.VMEM((2, 16, 64, LANES), f32),
                pltpu.VMEM((16, 8, LANES), f32), pltpu.VMEM((16, 8, LANES), f32),
                pltpu.VMEM((2 * LANES, 2 * LANES), f32), pltpu.VMEM((2 * LANES, 2 * LANES), f32),
                pltpu.VMEM((8, LANES), f32), pltpu.VMEM((1, LANES), f32),
                pltpu.SMEM((LAYERS,), f32), pltpu.SMEM((LAYERS,), f32), dma((2,)), pltpu.SemaphoreType.REGULAR((2,)),
                dma((SUB,)), dma((2, SUB)), dma((2, SUB)), dma, dma,
                dma((2, 2, 2, SUB)), dma((2, 2, 2, SUB)),
                dma((8,)), dma((8,)),
            ],
            compiler_params=pltpu.CompilerParams(collective_id=0, has_side_effects=True),
            name='qaoa',
        )(cost_local.reshape(shape), gammas, betas)
        energy, state_re, state_im = pl.pallas_call(
            write_out,
            out_shape=(jax.ShapeDtypeStruct((1,), f32),
                       jax.ShapeDtypeStruct(shape, f32), jax.ShapeDtypeStruct(shape, f32)),
            in_specs=[vmem, vmem, vmem],
            out_specs=(hbm, hbm, hbm),
            scratch_shapes=[pltpu.SMEM((1,), f32), dma((3,))],
            name='write_out',
        )(*[pltpu.with_memory_space_constraint(value, pltpu.VMEM) for value in results])
        return energy, state_re.reshape(local_len), state_im.reshape(local_len)

    return jax.shard_map(device_body, mesh=mesh, in_specs=(state_spec, P(), P()),
                         out_specs=(P('inst'), state_spec, state_spec), check_vma=False)
```

```python
import jax
import jax.numpy as jnp
from jax import lax
from jax.experimental import pallas as pl
from jax.experimental.pallas import tpu as pltpu
from jax.sharding import PartitionSpec as P

LANES = 128
LAYERS = 8
PAIRS = 4
SEND_ORDER = (5, 7, 4, 6, 1, 3, 2)
NEAR = (4, 1)


def rotate(re, im, cos_half, sin_half, steps=None):
    count = len(re)
    for step in steps or [1 << i for i in range(count.bit_length() - 1)]:
        new_re = [cos_half * re[i] + sin_half * im[i ^ step] for i in range(count)]
        new_im = [cos_half * im[i] - sin_half * re[i ^ step] for i in range(count)]
        re, im = new_re, new_im
    return re, im


def sublane_rotate(re, im, cos_half, sin_half):
    row = lax.broadcasted_iota(jnp.int32, (8, LANES), 0)
    for step in (1, 2, 4):
        bit_set = (row & step) != 0

        def flip(value):
            down = pltpu.roll(value, step, 0)
            if step == 4:
                return down
            return jnp.where(bit_set, down, pltpu.roll(value, 8 - step, 0))

        flip_re = [flip(value) for value in re]
        flip_im = [flip(value) for value in im]
        re, im = ([cos_half * r + sin_half * fi for r, fi in zip(re, flip_im)],
                  [cos_half * i - sin_half * fr for i, fr in zip(im, flip_re)])
    return re, im


def lane_matrix(cos_half, sin_half):
    row = lax.broadcasted_iota(jnp.int32, (LANES, LANES), 0)
    col = lax.broadcasted_iota(jnp.int32, (LANES, LANES), 1)
    diff = row ^ col
    cos_full = jnp.broadcast_to(cos_half[0:1], (LANES, LANES))
    sin_full = jnp.broadcast_to(sin_half[0:1], (LANES, LANES))
    mag = jnp.ones((LANES, LANES), jnp.float32)
    weight = jnp.zeros((LANES, LANES), jnp.int32)
    for bit in range(7):
        on = (diff >> bit) & 1
        mag = mag * jnp.where(on == 1, sin_full, cos_full)
        weight = weight + on
    quarter = weight & 3
    zero = jnp.zeros_like(mag)
    real = jnp.where(quarter == 0, mag, jnp.where(quarter == 2, -mag, zero))
    imag = jnp.where(quarter == 1, -mag, jnp.where(quarter == 3, mag, zero))
    return real, imag


def kernel(cost_hbm, gammas_hbm, betas_hbm, energy_all, out_re, out_im,
           cost, cost_near, cost_swap, recv, send, work, cos_buf, sin_buf, cos_near, sin_near,
           rows_in, matrix, energy_part, energy_row, gammas, betas, angle_in, near_in, cost_in, near_send, near_recv, cost_send, cost_recv,
           send_sem, recv_sem, e_send, e_recv):
    loads = [pltpu.make_async_copy(cost_hbm.at[:, :, :, pl.ds(sub * 16, 16)],
                                   cost.at[:, :, :, pl.ds(sub * 16, 16)], cost_in.at[sub])
             for sub in range(PAIRS)]
    for load in loads:
        load.start()
    angle_loads = [pltpu.make_async_copy(gammas_hbm, gammas, angle_in.at[0]),
                   pltpu.make_async_copy(betas_hbm, betas, angle_in.at[1])]
    for load in angle_loads:
        load.start()
    qx = lax.axis_index('qx')
    qy = lax.axis_index('qy')
    bits = (qy, qx % 2, qx // 2)

    def flipped(offset):
        return [1 - bit if (offset >> i) & 1 else bit for i, bit in enumerate(bits)]

    def block(offset):
        y, core, x = flipped(offset)
        return (x * 2 + core) * 2 + y

    def peer(offset):
        y, core, x = flipped(offset)
        return {'qy': y, 'qx': x * 2 + core}

    def remote(source, target, send_at, recv_at, offset):
        pltpu.make_async_remote_copy(
            src_ref=source, dst_ref=target, send_sem=send_at, recv_sem=recv_at,
            device_id=peer(offset), device_id_type=pl.DeviceIdType.MESH).start()

    barrier = pltpu.get_barrier_semaphore()
    def signal_next(sem):
        for offset in (4, 1, 2):
            pl.semaphore_signal(sem, inc=1, device_id=peer(offset), device_id_type=pl.DeviceIdType.MESH)

    signal_next(barrier)
    pl.semaphore_wait(barrier, 3)

    def half_angle(layer):
        angle = jnp.full((8, LANES), 0.5 * betas[layer], jnp.float32)
        return jnp.cos(angle), jnp.sin(angle)

    def wait_bytes(part, sem):
        pltpu.make_async_copy(part, part, sem).wait()

    def wait_all(buffer, sem, at, count):
        wait_bytes(buffer.at[(*at, pl.ds(0, count))], sem.at[at])

    def rows_of(r):
        return pl.ds(pl.multiple_of(r * 8, 8), 8)

    def set_matrix(cos_half, sin_half):
        real, imag = lane_matrix(cos_half, sin_half)
        matrix[0:LANES, 0:LANES] = real
        matrix[0:LANES, LANES:] = imag
        matrix[LANES:, 0:LANES] = -imag
        matrix[LANES:, LANES:] = real

    def put_rows(i, re, im):
        for o in range(16):
            at = pl.multiple_of(o * 16 + i * 8, 8)
            rows_in[pl.ds(at, 8), 0:LANES] = re[o]
            rows_in[pl.ds(at, 8), LANES:] = im[o]

    def lanes(a_held, at):
        work[a_held, at] = lax.dot(
            rows_in[...], matrix[...],
            precision=lax.Precision.HIGHEST, preferred_element_type=jnp.float32)

    def emit(held, mixed, target, a, b, cos_half, sin_half, order, route, local):
        def across(o, buffer):
            def part(r, c):
                at = pl.multiple_of((mixed * 8 + o) * 16 + (r % 2) * 8, 8)
                return work[held, r // 2, pl.ds(at, 8), c * LANES:(c + 1) * LANES]

            re = [part(r, 0) for r in range(8)]
            im = [part(r, 1) for r in range(8)]
            re, im = rotate(re, im, cos_half, sin_half)
            for r in range(8):
                buffer[target, a, b, r, o, 0] = re[r]
                buffer[target, a, b, r, o, 1] = im[r]

        def body(o, carry):
            across(o, send)
            return carry

        lax.fori_loop(1, 8, body, 0)
        for o in local:
            across(o, recv)
        for r in range(8):
            at = (target, a, b, r)
            for o in order:
                remote(send.at[(*at, o)], recv.at[(*at, o)], send_sem.at[at], recv_sem.at[at], route(o))

    def first_layer():
        def sub_rows(sub):
            return pl.ds(pl.multiple_of(sub * 16, 8), 16)

        for sub in range(PAIRS):
            loads[sub].wait()
            for a in range(2):
                remote(cost.at[:, a, :, sub_rows(sub)], cost_near.at[:, a, :, sub_rows(sub)],
                       near_send.at[a, sub], near_recv.at[a, sub], NEAR[a])
        signal_next(near_in.at[0])
        for load in angle_loads:
            load.wait()
        gamma = gammas[0]
        cos_half, sin_half = half_angle(0)
        set_matrix(cos_half, sin_half)

        def own_trig(r, carry):
            for a in range(2):
                for b in range(2):
                    for o in range(8):
                        angle = gamma * cost[block(o), a, b, rows_of(r), :]
                        cos_buf[a, b * 8 + o, rows_of(r), :] = jnp.cos(angle)
                        sin_buf[a, b * 8 + o, rows_of(r), :] = jnp.sin(angle)
            return carry

        for round_id in range(2):
            lax.fori_loop(4 * round_id, 4 * round_id + 4, own_trig, 0)
            pl.semaphore_wait(near_in.at[round_id], 3)
            if round_id == 0:
                signal_next(near_in.at[1])
        for a in range(2):
            for o in range(1, 8):
                if not o & NEAR[a]:
                    remote(cost.at[block(o), a], cost_swap.at[o, a], cost_send, cost_recv, o)

        def sub_step(sub, carry):
            for a in range(2):
                bit = NEAR[a]
                part = cost_near.at[:, a, :, sub_rows(sub)]
                wait_bytes(part, near_recv.at[a, sub])
                for o in range(1, 8):
                    if not o & bit:
                        remote(cost_near.at[block(o), a, :, sub_rows(sub)],
                               cost_swap.at[o | bit, a, :, sub_rows(sub)], cost_send, cost_recv, o)

                def slots(i, carry):
                    r = 2 * sub + i
                    for b in range(2):
                        for o in range(8):
                            angle = gamma * cost_near[block(o), a, b, rows_of(r), :]
                            cos_near[b * 8 + o] = jnp.cos(angle)
                            sin_near[b * 8 + o] = jnp.sin(angle)
                    re, im = [None] * 16, [None] * 16
                    for b in range(2):
                        for o in range(8):
                            if o & bit:
                                continue
                            here, there = b * 8 + o, b * 8 + (o | bit)
                            for slot, cos_at, sin_at in (
                                    (here, lambda k: cos_buf[a, k, rows_of(r), :], lambda k: sin_buf[a, k, rows_of(r), :]),
                                    (there, lambda k: cos_near[k], lambda k: sin_near[k])):
                                re[slot] = cos_half * cos_at(here) - sin_half * sin_at(there)
                                im[slot] = -(cos_half * sin_at(here)) - sin_half * cos_at(there)
                    re, im = rotate(re, im, cos_half, sin_half, [step for step in (1, 2, 4, 8) if step != bit])
                    re, im = sublane_rotate(re, im, cos_half, sin_half)
                    put_rows(i, re, im)
                    return carry

                lax.fori_loop(0, 2, slots, 0)
                lanes(a, sub)
            return carry

        lax.fori_loop(0, PAIRS, sub_step, 0)

        def quarters(b, carry):
            for a in range(2):
                bit = NEAR[a]
                emit(a, b, 1, a, b, cos_half, sin_half,
                     [o for o in (3, 6, 7, 1, 4, 5, 2) if o & ~bit], lambda o: o & ~bit, (0, bit))
            return carry

        lax.fori_loop(0, 2, quarters, 0)
        cost_swap[0] = cost[block(0)]
        for a in range(2):
            cost_swap[NEAR[a], a] = cost_near[block(0), a]
        wait_bytes(cost_swap.at[pl.ds(0, 6)], cost_recv)

    def run_layer(layer, odd, arrived, drained):
        source, target = (0, 1) if odd else (1, 0)

        def quarter(held, mixed):
            return (held, mixed) if odd else (mixed, held)

        cos_half, sin_half = half_angle(layer)
        cos_prev, sin_prev = half_angle(layer - 1)
        gamma = gammas[layer]
        set_matrix(cos_half, sin_half)

        def half(held, carry):
            def trig(r, carry):
                for mixed in range(2):
                    for o in range(8):
                        at = (block(o) if odd else o, *quarter(held, mixed), rows_of(r))
                        angle = gamma * (cost if odd else cost_swap)[at]
                        cos_buf[held, mixed * 8 + o, rows_of(r), :] = jnp.cos(angle)
                        sin_buf[held, mixed * 8 + o, rows_of(r), :] = jnp.sin(angle)
                return carry

            lax.fori_loop(0, 8, trig, 0)

            def sub_step(sub, carry):
                for i in range(2):
                    for mixed in range(2):
                        wait_all(recv, recv_sem, (source, *quarter(held, mixed), 2 * sub + i), arrived)

                def slots(i, carry):
                    r = 2 * sub + i
                    cos_phase = [cos_buf[held, o, rows_of(r), :] for o in range(16)]
                    sin_phase = [sin_buf[held, o, rows_of(r), :] for o in range(16)]
                    old = [[recv[(source, *quarter(held, mixed), r, o, c)]
                            for mixed in range(2) for o in range(8)] for c in range(2)]
                    old_re, old_im = rotate(*old, cos_prev, sin_prev)
                    re = [r * c + i * s for r, i, c, s in zip(old_re, old_im, cos_phase, sin_phase)]
                    im = [i * c - r * s for r, i, c, s in zip(old_re, old_im, cos_phase, sin_phase)]
                    re, im = rotate(re, im, cos_half, sin_half)
                    re, im = sublane_rotate(re, im, cos_half, sin_half)
                    put_rows(i, re, im)
                    return carry

                lax.fori_loop(0, 2, slots, 0)
                lanes(held, sub)
                return carry

            lax.fori_loop(0, PAIRS, sub_step, 0)

            if drained:
                for mixed in range(2):
                    for r in range(8):
                        wait_all(send, send_sem, (target, *quarter(held, mixed), r), drained)

            def quarters(mixed, carry):
                emit(held, mixed, target, *quarter(held, mixed), cos_half, sin_half, SEND_ORDER, lambda o: o, (0,))
                return carry

            lax.fori_loop(0, 2, quarters, 0)
            return carry

        lax.fori_loop(0, 2, half, 0)

    first_layer()
    run_layer(1, False, 6, 0)
    run_layer(2, True, 7, 6)

    def layer_pair(i, carry):
        run_layer(2 * i + 3, False, 7, 7)
        run_layer(2 * i + 4, True, 7, 7)
        return carry

    lax.fori_loop(0, LAYERS // 2 - 2, layer_pair, 0)
    run_layer(LAYERS - 1, False, 7, 7)

    cos_half, sin_half = half_angle(LAYERS - 1)
    energy_part[...] = jnp.zeros((8, LANES), jnp.float32)

    def final_half(a, carry):
        def slots(r, carry):
            for b in range(2):
                wait_all(recv, recv_sem, (0, a, b, r), 7)
            old = [[recv[0, a, b, r, o, c] for b in range(2) for o in range(8)] for c in range(2)]
            re, im = rotate(*old, cos_half, sin_half)
            total = energy_part[...]
            for b in range(2):
                for o in range(8):
                    at = (block(o), a, b, rows_of(r))
                    x, y = re[b * 8 + o], im[b * 8 + o]
                    out_re[at] = x
                    out_im[at] = y
                    total = total + cost[at] * (x * x + y * y)
            energy_part[...] = total
            return carry

        lax.fori_loop(0, 8, slots, 0)
        return carry

    lax.fori_loop(0, 2, final_half, 0)

    me = block(0)
    energy_row[...] = jnp.sum(energy_part[...], axis=0, keepdims=True)
    for offset in range(1, 8):
        remote(energy_row, energy_all.at[me], e_send.at[offset], e_recv.at[offset], offset)
    energy_all[me] = energy_row[...]
    for par in range(2):
        for a in range(2):
            for b in range(2):
                for r in range(8):
                    wait_all(send, send_sem, (par, a, b, r), 7)
    for a in range(2):
        for sub in range(PAIRS):
            wait_bytes(cost.at[:, a, :, pl.ds(sub * 16, 16)], near_send.at[a, sub])
    wait_bytes(cost_swap.at[pl.ds(0, 6)], cost_send)
    for offset in range(1, 8):
        wait_bytes(energy_row, e_send.at[offset])
        wait_bytes(energy_row, e_recv.at[offset])


def write_out(energy_all, in_re, in_im, energy, out_re, out_im, value, sem):
    copies = [pltpu.make_async_copy(in_re, out_re, sem.at[0]), pltpu.make_async_copy(in_im, out_im, sem.at[1])]
    for copy in copies:
        copy.start()
    total = energy_all[0]
    for i in range(1, 8):
        total = total + energy_all[i]
    value[0] = jnp.sum(total) * (1.0 / (1 << 21))
    copies.append(pltpu.make_async_copy(value, energy, sem.at[2]))
    copies[2].start()
    for copy in copies:
        copy.wait()


def solution(mesh):
    state_spec = P(('inst', 'qx', 'qy'))

    def device_body(cost_local, gammas, betas):
        local_len = cost_local.shape[0]
        shape = (8, 2, 2, local_len // (32 * LANES), LANES)
        f32 = jnp.float32
        vmem = pl.BlockSpec(memory_space=pltpu.VMEM)
        dma = pltpu.SemaphoreType.DMA
        parts = (2, 2, 2, 8, 8, 2, 8, LANES)
        hbm = pl.BlockSpec(memory_space=pl.ANY)
        results = pl.pallas_call(
            kernel,
            out_shape=(pltpu.VMEM((8, 1, LANES), f32), pltpu.VMEM(shape, f32), pltpu.VMEM(shape, f32)),
            in_specs=[hbm, hbm, hbm],
            out_specs=(vmem, vmem, vmem),
            scratch_shapes=[
                pltpu.VMEM(shape, f32), pltpu.VMEM(shape, f32), pltpu.VMEM(shape, f32),
                pltpu.VMEM(parts, f32), pltpu.VMEM(parts, f32),
                pltpu.VMEM((2, 4, 2 * LANES, 2 * LANES), f32),
                pltpu.VMEM((2, 16, 64, LANES), f32), pltpu.VMEM((2, 16, 64, LANES), f32),
                pltpu.VMEM((16, 8, LANES), f32), pltpu.VMEM((16, 8, LANES), f32),
                pltpu.VMEM((2 * LANES, 2 * LANES), f32), pltpu.VMEM((2 * LANES, 2 * LANES), f32),
                pltpu.VMEM((8, LANES), f32), pltpu.VMEM((1, LANES), f32),
                pltpu.SMEM((LAYERS,), f32), pltpu.SMEM((LAYERS,), f32), dma((2,)), pltpu.SemaphoreType.REGULAR((2,)),
                dma((PAIRS,)), dma((2, PAIRS)), dma((2, PAIRS)), dma, dma,
                dma((2, 2, 2, 8)), dma((2, 2, 2, 8)),
                dma((8,)), dma((8,)),
            ],
            compiler_params=pltpu.CompilerParams(collective_id=0, has_side_effects=True),
            name='qaoa',
        )(cost_local.reshape(shape), gammas, betas)
        energy, state_re, state_im = pl.pallas_call(
            write_out,
            out_shape=(jax.ShapeDtypeStruct((1,), f32),
                       jax.ShapeDtypeStruct(shape, f32), jax.ShapeDtypeStruct(shape, f32)),
            in_specs=[vmem, vmem, vmem],
            out_specs=(hbm, hbm, hbm),
            scratch_shapes=[pltpu.SMEM((1,), f32), dma((3,))],
            name='write_out',
        )(*[pltpu.with_memory_space_constraint(value, pltpu.VMEM) for value in results])
        return energy, state_re.reshape(local_len), state_im.reshape(local_len)

    return jax.shard_map(device_body, mesh=mesh, in_specs=(state_spec, P(), P()),
                         out_specs=(P('inst'), state_spec, state_spec), check_vma=False)
```

```python
import jax
import jax.numpy as jnp
from jax import lax
from jax.experimental import pallas as pl
from jax.experimental.pallas import tpu as pltpu
from jax.sharding import PartitionSpec as P

LANES = 128
LAYERS = 8
COARSE = 4
FINE = 2
PAIRS = 4
SEND_ORDER = (5, 7, 4, 6, 1, 3, 2)
NEAR = (4, 1)


def rotate(re, im, cos_half, sin_half, steps=None):
    count = len(re)
    for step in steps or [1 << i for i in range(count.bit_length() - 1)]:
        new_re = [cos_half * re[i] + sin_half * im[i ^ step] for i in range(count)]
        new_im = [cos_half * im[i] - sin_half * re[i ^ step] for i in range(count)]
        re, im = new_re, new_im
    return re, im


def sublane_rotate(re, im, cos_half, sin_half):
    row = lax.broadcasted_iota(jnp.int32, (8, LANES), 0)
    for step in (1, 2, 4):
        bit_set = (row & step) != 0

        def flip(value):
            down = pltpu.roll(value, step, 0)
            if step == 4:
                return down
            return jnp.where(bit_set, down, pltpu.roll(value, 8 - step, 0))

        flip_re = [flip(value) for value in re]
        flip_im = [flip(value) for value in im]
        re, im = ([cos_half * r + sin_half * fi for r, fi in zip(re, flip_im)],
                  [cos_half * i - sin_half * fr for i, fr in zip(im, flip_re)])
    return re, im


def lane_matrix(cos_half, sin_half):
    row = lax.broadcasted_iota(jnp.int32, (LANES, LANES), 0)
    col = lax.broadcasted_iota(jnp.int32, (LANES, LANES), 1)
    diff = row ^ col
    cos_full = jnp.broadcast_to(cos_half[0:1], (LANES, LANES))
    sin_full = jnp.broadcast_to(sin_half[0:1], (LANES, LANES))
    mag = jnp.ones((LANES, LANES), jnp.float32)
    weight = jnp.zeros((LANES, LANES), jnp.int32)
    for bit in range(7):
        on = (diff >> bit) & 1
        mag = mag * jnp.where(on == 1, sin_full, cos_full)
        weight = weight + on
    quarter = weight & 3
    zero = jnp.zeros_like(mag)
    real = jnp.where(quarter == 0, mag, jnp.where(quarter == 2, -mag, zero))
    imag = jnp.where(quarter == 1, -mag, jnp.where(quarter == 3, mag, zero))
    return real, imag


def kernel(cost_hbm, gammas_hbm, betas_hbm, energy_all, out_re, out_im,
           cost, cost_near, cost_swap, recv, send, work, cos_buf, sin_buf, cos_near, sin_near,
           rows_in, matrix, energy_part, energy_row, gammas, betas, angle_in, near_in, cost_in, near_send, near_recv, cost_send, cost_recv,
           send_sem, recv_sem, e_send, e_recv):
    loads = [pltpu.make_async_copy(cost_hbm.at[:, :, :, pl.ds(sub * 16, 16)],
                                   cost.at[:, :, :, pl.ds(sub * 16, 16)], cost_in.at[sub])
             for sub in range(PAIRS)]
    for load in loads:
        load.start()
    angle_loads = [pltpu.make_async_copy(gammas_hbm, gammas, angle_in.at[0]),
                   pltpu.make_async_copy(betas_hbm, betas, angle_in.at[1])]
    for load in angle_loads:
        load.start()
    qx = lax.axis_index('qx')
    qy = lax.axis_index('qy')
    bits = (qy, qx % 2, qx // 2)

    def flipped(offset):
        return [1 - bit if (offset >> i) & 1 else bit for i, bit in enumerate(bits)]

    def block(offset):
        y, core, x = flipped(offset)
        return (x * 2 + core) * 2 + y

    def peer(offset):
        y, core, x = flipped(offset)
        return {'qy': y, 'qx': x * 2 + core}

    def remote(source, target, send_at, recv_at, offset):
        pltpu.make_async_remote_copy(
            src_ref=source, dst_ref=target, send_sem=send_at, recv_sem=recv_at,
            device_id=peer(offset), device_id_type=pl.DeviceIdType.MESH).start()

    barrier = pltpu.get_barrier_semaphore()
    def signal_next(sem):
        for offset in (4, 1, 2):
            pl.semaphore_signal(sem, inc=1, device_id=peer(offset), device_id_type=pl.DeviceIdType.MESH)

    signal_next(barrier)
    pl.semaphore_wait(barrier, 3)

    def half_angle(layer):
        angle = jnp.full((8, LANES), 0.5 * betas[layer], jnp.float32)
        return jnp.cos(angle), jnp.sin(angle)

    def wait_bytes(part, sem):
        pltpu.make_async_copy(part, part, sem).wait()

    def wait_all(buffer, sem, at, first_r, size, count):
        wait_bytes(buffer.at[(*at, pl.ds(0, count), pl.ds(0, size))], sem.at[(*at, first_r)])

    def rows_of(r):
        return pl.ds(pl.multiple_of(r * 8, 8), 8)

    def set_matrix(cos_half, sin_half):
        real, imag = lane_matrix(cos_half, sin_half)
        matrix[0:LANES, 0:LANES] = real
        matrix[0:LANES, LANES:] = imag
        matrix[LANES:, 0:LANES] = -imag
        matrix[LANES:, LANES:] = real

    def put_rows(i, re, im):
        for o in range(16):
            at = pl.multiple_of(o * 16 + i * 8, 8)
            rows_in[pl.ds(at, 8), 0:LANES] = re[o]
            rows_in[pl.ds(at, 8), LANES:] = im[o]

    def lanes(a_held, at):
        work[a_held, at] = lax.dot(
            rows_in[...], matrix[...],
            precision=lax.Precision.HIGHEST, preferred_element_type=jnp.float32)

    def emit(held, mixed, target, a, b, cos_half, sin_half, size, order, route, local):
        def across(o, buffer):
            def part(r, c):
                at = pl.multiple_of((mixed * 8 + o) * 16 + (r % 2) * 8, 8)
                return work[held, r // 2, pl.ds(at, 8), c * LANES:(c + 1) * LANES]

            re = [part(r, 0) for r in range(8)]
            im = [part(r, 1) for r in range(8)]
            re, im = rotate(re, im, cos_half, sin_half)
            for r in range(8):
                buffer[target, a, b, o, r, 0] = re[r]
                buffer[target, a, b, o, r, 1] = im[r]

        def body(o, carry):
            across(o, send)
            return carry

        lax.fori_loop(1, 8, body, 0)
        for o in local:
            across(o, recv)
        for r in range(0, 8, size):
            sem_at = (target, a, b, r)
            for o in order:
                at = (target, a, b, o, pl.ds(r, size))
                remote(send.at[at], recv.at[at], send_sem.at[sem_at], recv_sem.at[sem_at], route(o))

    def first_layer():
        def sub_rows(sub):
            return pl.ds(pl.multiple_of(sub * 16, 8), 16)

        for sub in range(PAIRS):
            loads[sub].wait()
            for a in range(2):
                remote(cost.at[:, a, :, sub_rows(sub)], cost_near.at[:, a, :, sub_rows(sub)],
                       near_send.at[a, sub], near_recv.at[a, sub], NEAR[a])
        signal_next(near_in.at[0])
        for load in angle_loads:
            load.wait()
        gamma = gammas[0]
        cos_half, sin_half = half_angle(0)
        set_matrix(cos_half, sin_half)

        def own_trig(r, carry):
            for a in range(2):
                for b in range(2):
                    for o in range(8):
                        angle = gamma * cost[block(o), a, b, rows_of(r), :]
                        cos_buf[a, b * 8 + o, rows_of(r), :] = jnp.cos(angle)
                        sin_buf[a, b * 8 + o, rows_of(r), :] = jnp.sin(angle)
            return carry

        for round_id in range(2):
            lax.fori_loop(4 * round_id, 4 * round_id + 4, own_trig, 0)
            pl.semaphore_wait(near_in.at[round_id], 3)
            if round_id == 0:
                signal_next(near_in.at[1])
        for a in range(2):
            for o in range(1, 8):
                if not o & NEAR[a]:
                    remote(cost.at[block(o), a], cost_swap.at[o, a], cost_send, cost_recv, o)

        def sub_step(sub, carry):
            for a in range(2):
                bit = NEAR[a]
                part = cost_near.at[:, a, :, sub_rows(sub)]
                wait_bytes(part, near_recv.at[a, sub])
                for o in range(1, 8):
                    if not o & bit:
                        remote(cost_near.at[block(o), a, :, sub_rows(sub)],
                               cost_swap.at[o | bit, a, :, sub_rows(sub)], cost_send, cost_recv, o)

                def slots(i, carry):
                    r = 2 * sub + i
                    for b in range(2):
                        for o in range(8):
                            angle = gamma * cost_near[block(o), a, b, rows_of(r), :]
                            cos_near[b * 8 + o] = jnp.cos(angle)
                            sin_near[b * 8 + o] = jnp.sin(angle)
                    re, im = [None] * 16, [None] * 16
                    for b in range(2):
                        for o in range(8):
                            if o & bit:
                                continue
                            here, there = b * 8 + o, b * 8 + (o | bit)
                            for slot, cos_at, sin_at in (
                                    (here, lambda k: cos_buf[a, k, rows_of(r), :], lambda k: sin_buf[a, k, rows_of(r), :]),
                                    (there, lambda k: cos_near[k], lambda k: sin_near[k])):
                                re[slot] = cos_half * cos_at(here) - sin_half * sin_at(there)
                                im[slot] = -(cos_half * sin_at(here)) - sin_half * cos_at(there)
                    re, im = rotate(re, im, cos_half, sin_half, [step for step in (1, 2, 4, 8) if step != bit])
                    re, im = sublane_rotate(re, im, cos_half, sin_half)
                    put_rows(i, re, im)
                    return carry

                lax.fori_loop(0, 2, slots, 0)
                lanes(a, sub)
            return carry

        lax.fori_loop(0, PAIRS, sub_step, 0)

        def quarters(b, carry):
            for a in range(2):
                bit = NEAR[a]
                emit(a, b, 1, a, b, cos_half, sin_half, COARSE,
                     [o for o in (3, 6, 7, 1, 4, 5, 2) if o & ~bit], lambda o: o & ~bit, (0, bit))
            return carry

        lax.fori_loop(0, 2, quarters, 0)
        cost_swap[0] = cost[block(0)]
        for a in range(2):
            cost_swap[NEAR[a], a] = cost_near[block(0), a]
        wait_bytes(cost_swap.at[pl.ds(0, 6)], cost_recv)

    def run_layer(layer, odd, arrived, drained, size=COARSE):
        source, target = (0, 1) if odd else (1, 0)

        def quarter(held, mixed):
            return (held, mixed) if odd else (mixed, held)

        cos_half, sin_half = half_angle(layer)
        cos_prev, sin_prev = half_angle(layer - 1)
        gamma = gammas[layer]
        set_matrix(cos_half, sin_half)

        def half(held, carry):
            def trig(r, carry):
                for mixed in range(2):
                    for o in range(8):
                        at = (block(o) if odd else o, *quarter(held, mixed), rows_of(r))
                        angle = gamma * (cost if odd else cost_swap)[at]
                        cos_buf[held, mixed * 8 + o, rows_of(r), :] = jnp.cos(angle)
                        sin_buf[held, mixed * 8 + o, rows_of(r), :] = jnp.sin(angle)
                return carry

            lax.fori_loop(0, 8, trig, 0)

            def block_step(sub):
                def slots(i, carry):
                    r = 2 * sub + i
                    cos_phase = [cos_buf[held, o, rows_of(r), :] for o in range(16)]
                    sin_phase = [sin_buf[held, o, rows_of(r), :] for o in range(16)]
                    old = [[recv[(source, *quarter(held, mixed), o, r, c)]
                            for mixed in range(2) for o in range(8)] for c in range(2)]
                    old_re, old_im = rotate(*old, cos_prev, sin_prev)
                    re = [r * c + i * s for r, i, c, s in zip(old_re, old_im, cos_phase, sin_phase)]
                    im = [i * c - r * s for r, i, c, s in zip(old_re, old_im, cos_phase, sin_phase)]
                    re, im = rotate(re, im, cos_half, sin_half)
                    re, im = sublane_rotate(re, im, cos_half, sin_half)
                    put_rows(i, re, im)
                    return carry

                lax.fori_loop(0, 2, slots, 0)
                lanes(held, sub)

            def message(i, carry):
                for mixed in range(2):
                    wait_all(recv, recv_sem, (source, *quarter(held, mixed)), i * COARSE, COARSE, arrived)

                def blocks(k, carry):
                    block_step(i * (COARSE // 2) + k)
                    return carry

                lax.fori_loop(0, COARSE // 2, blocks, 0)
                return carry

            lax.fori_loop(0, 8 // COARSE, message, 0)

            if drained:
                for mixed in range(2):
                    for r in range(0, 8, COARSE):
                        wait_all(send, send_sem, (target, *quarter(held, mixed)), r, COARSE, drained)

            def quarters(mixed, carry):
                emit(held, mixed, target, *quarter(held, mixed), cos_half, sin_half, size, SEND_ORDER, lambda o: o, (0,))
                return carry

            lax.fori_loop(0, 2, quarters, 0)
            return carry

        lax.fori_loop(0, 2, half, 0)

    first_layer()
    run_layer(1, False, 6, 0)
    run_layer(2, True, 7, 6)

    def layer_pair(i, carry):
        run_layer(2 * i + 3, False, 7, 7)
        run_layer(2 * i + 4, True, 7, 7)
        return carry

    lax.fori_loop(0, LAYERS // 2 - 2, layer_pair, 0)
    run_layer(LAYERS - 1, False, 7, 7, FINE)

    cos_half, sin_half = half_angle(LAYERS - 1)
    energy_part[...] = jnp.zeros((8, LANES), jnp.float32)

    def final_half(a, carry):
        def message(i, carry):
            for b in range(2):
                wait_all(recv, recv_sem, (0, a, b), i * FINE, FINE, 7)

            def slots(r, carry):
                old = [[recv[0, a, b, o, r, c] for b in range(2) for o in range(8)] for c in range(2)]
                re, im = rotate(*old, cos_half, sin_half)
                total = energy_part[...]
                for b in range(2):
                    for o in range(8):
                        at = (block(o), a, b, rows_of(r))
                        x, y = re[b * 8 + o], im[b * 8 + o]
                        out_re[at] = x
                        out_im[at] = y
                        total = total + cost[at] * (x * x + y * y)
                energy_part[...] = total
                return carry

            lax.fori_loop(i * FINE, (i + 1) * FINE, slots, 0)
            return carry

        lax.fori_loop(0, 8 // FINE, message, 0)
        return carry

    lax.fori_loop(0, 2, final_half, 0)

    me = block(0)
    energy_row[...] = jnp.sum(energy_part[...], axis=0, keepdims=True)
    for offset in range(1, 8):
        remote(energy_row, energy_all.at[me], e_send.at[offset], e_recv.at[offset], offset)
    energy_all[me] = energy_row[...]
    for par in range(2):
        for a in range(2):
            for b in range(2):
                size = COARSE if par else FINE
                for r in range(0, 8, size):
                    wait_all(send, send_sem, (par, a, b), r, size, 7)
    for a in range(2):
        for sub in range(PAIRS):
            wait_bytes(cost.at[:, a, :, pl.ds(sub * 16, 16)], near_send.at[a, sub])
    wait_bytes(cost_swap.at[pl.ds(0, 6)], cost_send)
    for offset in range(1, 8):
        wait_bytes(energy_row, e_send.at[offset])
        wait_bytes(energy_row, e_recv.at[offset])


def write_out(energy_all, in_re, in_im, energy, out_re, out_im, value, sem):
    copies = [pltpu.make_async_copy(in_re, out_re, sem.at[0]), pltpu.make_async_copy(in_im, out_im, sem.at[1])]
    for copy in copies:
        copy.start()
    total = energy_all[0]
    for i in range(1, 8):
        total = total + energy_all[i]
    value[0] = jnp.sum(total) * (1.0 / (1 << 21))
    copies.append(pltpu.make_async_copy(value, energy, sem.at[2]))
    copies[2].start()
    for copy in copies:
        copy.wait()


def solution(mesh):
    state_spec = P(('inst', 'qx', 'qy'))

    def device_body(cost_local, gammas, betas):
        local_len = cost_local.shape[0]
        shape = (8, 2, 2, local_len // (32 * LANES), LANES)
        f32 = jnp.float32
        vmem = pl.BlockSpec(memory_space=pltpu.VMEM)
        dma = pltpu.SemaphoreType.DMA
        parts = (2, 2, 2, 8, 8, 2, 8, LANES)
        hbm = pl.BlockSpec(memory_space=pl.ANY)
        results = pl.pallas_call(
            kernel,
            out_shape=(pltpu.VMEM((8, 1, LANES), f32), pltpu.VMEM(shape, f32), pltpu.VMEM(shape, f32)),
            in_specs=[hbm, hbm, hbm],
            out_specs=(vmem, vmem, vmem),
            scratch_shapes=[
                pltpu.VMEM(shape, f32), pltpu.VMEM(shape, f32), pltpu.VMEM(shape, f32),
                pltpu.VMEM(parts, f32), pltpu.VMEM(parts, f32),
                pltpu.VMEM((2, 4, 2 * LANES, 2 * LANES), f32),
                pltpu.VMEM((2, 16, 64, LANES), f32), pltpu.VMEM((2, 16, 64, LANES), f32),
                pltpu.VMEM((16, 8, LANES), f32), pltpu.VMEM((16, 8, LANES), f32),
                pltpu.VMEM((2 * LANES, 2 * LANES), f32), pltpu.VMEM((2 * LANES, 2 * LANES), f32),
                pltpu.VMEM((8, LANES), f32), pltpu.VMEM((1, LANES), f32),
                pltpu.SMEM((LAYERS,), f32), pltpu.SMEM((LAYERS,), f32), dma((2,)), pltpu.SemaphoreType.REGULAR((2,)),
                dma((PAIRS,)), dma((2, PAIRS)), dma((2, PAIRS)), dma, dma,
                dma((2, 2, 2, 8)), dma((2, 2, 2, 8)),
                dma((8,)), dma((8,)),
            ],
            compiler_params=pltpu.CompilerParams(collective_id=0, has_side_effects=True),
            name='qaoa',
        )(cost_local.reshape(shape), gammas, betas)
        energy, state_re, state_im = pl.pallas_call(
            write_out,
            out_shape=(jax.ShapeDtypeStruct((1,), f32),
                       jax.ShapeDtypeStruct(shape, f32), jax.ShapeDtypeStruct(shape, f32)),
            in_specs=[vmem, vmem, vmem],
            out_specs=(hbm, hbm, hbm),
            scratch_shapes=[pltpu.SMEM((1,), f32), dma((3,))],
            name='write_out',
        )(*[pltpu.with_memory_space_constraint(value, pltpu.VMEM) for value in results])
        return energy, state_re.reshape(local_len), state_im.reshape(local_len)

    return jax.shard_map(device_body, mesh=mesh, in_specs=(state_spec, P(), P()),
                         out_specs=(P('inst'), state_spec, state_spec), check_vma=False)
```

```python
import jax
import jax.numpy as jnp
from jax import lax
from jax.experimental import pallas as pl
from jax.experimental.pallas import tpu as pltpu
from jax.sharding import PartitionSpec as P

LANES = 128
LAYERS = 8
SUB = 4
PER_SUB = 8 // SUB
SEND_ORDER = (5, 7, 4, 6, 1, 3, 2)
NEAR = (4, 1)


def rotate(re, im, cos_half, sin_half, steps=None):
    count = len(re)
    for step in steps or [1 << i for i in range(count.bit_length() - 1)]:
        new_re = [cos_half * re[i] + sin_half * im[i ^ step] for i in range(count)]
        new_im = [cos_half * im[i] - sin_half * re[i ^ step] for i in range(count)]
        re, im = new_re, new_im
    return re, im


def sublane_rotate(re, im, cos_half, sin_half):
    row = lax.broadcasted_iota(jnp.int32, (8, LANES), 0)
    for step in (1, 2, 4):
        bit_set = (row & step) != 0

        def flip(value):
            down = pltpu.roll(value, step, 0)
            if step == 4:
                return down
            return jnp.where(bit_set, down, pltpu.roll(value, 8 - step, 0))

        flip_re = [flip(value) for value in re]
        flip_im = [flip(value) for value in im]
        re, im = ([cos_half * r + sin_half * fi for r, fi in zip(re, flip_im)],
                  [cos_half * i - sin_half * fr for i, fr in zip(im, flip_re)])
    return re, im


def lane_matrix(cos_half, sin_half):
    row = lax.broadcasted_iota(jnp.int32, (LANES, LANES), 0)
    col = lax.broadcasted_iota(jnp.int32, (LANES, LANES), 1)
    diff = row ^ col
    cos_full = jnp.broadcast_to(cos_half[0:1], (LANES, LANES))
    sin_full = jnp.broadcast_to(sin_half[0:1], (LANES, LANES))
    mag = jnp.ones((LANES, LANES), jnp.float32)
    weight = jnp.zeros((LANES, LANES), jnp.int32)
    for bit in range(7):
        on = (diff >> bit) & 1
        mag = mag * jnp.where(on == 1, sin_full, cos_full)
        weight = weight + on
    quarter = weight & 3
    zero = jnp.zeros_like(mag)
    real = jnp.where(quarter == 0, mag, jnp.where(quarter == 2, -mag, zero))
    imag = jnp.where(quarter == 1, -mag, jnp.where(quarter == 3, mag, zero))
    return real, imag


def kernel(cost_hbm, gammas_hbm, betas_hbm, energy_all, out_re, out_im,
           cost, cost_near, cost_swap, recv, send, work, cos_buf, sin_buf, cos_near, sin_near,
           rows_in, matrix, energy_part, energy_row, gammas, betas, angle_in, near_in, cost_in, near_send, near_recv, cost_send, cost_recv,
           send_sem, recv_sem, e_send, e_recv):
    loads = [pltpu.make_async_copy(cost_hbm.at[:, :, :, pl.ds(sub * 8 * PER_SUB, 8 * PER_SUB)],
                                   cost.at[:, :, :, pl.ds(sub * 8 * PER_SUB, 8 * PER_SUB)], cost_in.at[sub])
             for sub in range(SUB)]
    for load in loads:
        load.start()
    angle_loads = [pltpu.make_async_copy(gammas_hbm, gammas, angle_in.at[0]),
                   pltpu.make_async_copy(betas_hbm, betas, angle_in.at[1])]
    for load in angle_loads:
        load.start()
    qx = lax.axis_index('qx')
    qy = lax.axis_index('qy')
    bits = (qy, qx % 2, qx // 2)

    def flipped(offset):
        return [1 - bit if (offset >> i) & 1 else bit for i, bit in enumerate(bits)]

    def block(offset):
        y, core, x = flipped(offset)
        return (x * 2 + core) * 2 + y

    def peer(offset):
        y, core, x = flipped(offset)
        return {'qy': y, 'qx': x * 2 + core}

    def remote(source, target, send_at, recv_at, offset):
        pltpu.make_async_remote_copy(
            src_ref=source, dst_ref=target, send_sem=send_at, recv_sem=recv_at,
            device_id=peer(offset), device_id_type=pl.DeviceIdType.MESH).start()

    barrier = pltpu.get_barrier_semaphore()
    def signal_next(sem):
        for offset in (4, 1, 2):
            pl.semaphore_signal(sem, inc=1, device_id=peer(offset), device_id_type=pl.DeviceIdType.MESH)

    signal_next(barrier)
    pl.semaphore_wait(barrier, 3)

    def half_angle(layer):
        angle = jnp.full((8, LANES), 0.5 * betas[layer], jnp.float32)
        return jnp.cos(angle), jnp.sin(angle)

    def wait_bytes(part, sem):
        pltpu.make_async_copy(part, part, sem).wait()

    def wait_all(buffer, sem, at, count):
        wait_bytes(buffer.at[(*at, pl.ds(0, count))], sem.at[at])

    def rows_of(r):
        return pl.ds(pl.multiple_of(r * 8, 8), 8)

    def set_matrix(cos_half, sin_half):
        real, imag = lane_matrix(cos_half, sin_half)
        matrix[0:LANES, 0:LANES] = real
        matrix[0:LANES, LANES:] = imag
        matrix[LANES:, 0:LANES] = -imag
        matrix[LANES:, LANES:] = real

    def put_rows(i, re, im):
        for o in range(16):
            at = pl.multiple_of(o * 16 + i * 8, 8)
            rows_in[pl.ds(at, 8), 0:LANES] = re[o]
            rows_in[pl.ds(at, 8), LANES:] = im[o]

    def lanes(a_held, at):
        work[a_held, at] = lax.dot(
            rows_in[...], matrix[...],
            precision=lax.Precision.HIGHEST, preferred_element_type=jnp.float32)

    def send_parts(target, a, b, subs, order, route):
        for sub in subs:
            at = (target, a, b, sub)
            for o in order:
                remote(send.at[(*at, o)], recv.at[(*at, o)], send_sem.at[at], recv_sem.at[at], route(o))

    def emit(held, mixed, target, a, b, cos_half, sin_half, local):
        def across(o, buffer):
            def part(r, c):
                at = pl.multiple_of((mixed * 8 + o) * 16 + (r % 2) * 8, 8)
                return work[held, r // 2, pl.ds(at, 8), c * LANES:(c + 1) * LANES]

            re = [part(r, 0) for r in range(8)]
            im = [part(r, 1) for r in range(8)]
            re, im = rotate(re, im, cos_half, sin_half)
            for r in range(8):
                row = (r % PER_SUB) * 8
                buffer[target, a, b, r // PER_SUB, o, 0, row:row + 8, :] = re[r]
                buffer[target, a, b, r // PER_SUB, o, 1, row:row + 8, :] = im[r]

        def body(o, carry):
            across(o, send)
            return carry

        lax.fori_loop(1, 8, body, 0)
        for o in local:
            across(o, recv)
    def first_layer():
        def sub_rows(sub):
            return pl.ds(pl.multiple_of(sub * 8 * PER_SUB, 8), 8 * PER_SUB)

        for sub in range(SUB):
            loads[sub].wait()
            for a in range(2):
                remote(cost.at[:, a, :, sub_rows(sub)], cost_near.at[:, a, :, sub_rows(sub)],
                       near_send.at[a, sub], near_recv.at[a, sub], NEAR[a])
        signal_next(near_in.at[0])
        for load in angle_loads:
            load.wait()
        gamma = gammas[0]
        cos_half, sin_half = half_angle(0)
        set_matrix(cos_half, sin_half)

        def own_trig(r, carry):
            for a in range(2):
                for b in range(2):
                    for o in range(8):
                        angle = gamma * cost[block(o), a, b, rows_of(r), :]
                        cos_buf[a, b * 8 + o, rows_of(r), :] = jnp.cos(angle)
                        sin_buf[a, b * 8 + o, rows_of(r), :] = jnp.sin(angle)
            return carry

        for round_id in range(2):
            lax.fori_loop(4 * round_id, 4 * round_id + 4, own_trig, 0)
            pl.semaphore_wait(near_in.at[round_id], 3)
            if round_id == 0:
                signal_next(near_in.at[1])
        for a in range(2):
            for o in range(1, 8):
                if not o & NEAR[a]:
                    remote(cost.at[block(o), a], cost_swap.at[o, a], cost_send, cost_recv, o)

        def sub_step(sub, carry):
            for a in range(2):
                bit = NEAR[a]
                part = cost_near.at[:, a, :, sub_rows(sub)]
                wait_bytes(part, near_recv.at[a, sub])
                for o in range(1, 8):
                    if not o & bit:
                        remote(cost_near.at[block(o), a, :, sub_rows(sub)],
                               cost_swap.at[o | bit, a, :, sub_rows(sub)], cost_send, cost_recv, o)

                def slots(i, carry):
                    r = sub * PER_SUB + i
                    for b in range(2):
                        for o in range(8):
                            angle = gamma * cost_near[block(o), a, b, rows_of(r), :]
                            cos_near[b * 8 + o] = jnp.cos(angle)
                            sin_near[b * 8 + o] = jnp.sin(angle)
                    re, im = [None] * 16, [None] * 16
                    for b in range(2):
                        for o in range(8):
                            if o & bit:
                                continue
                            here, there = b * 8 + o, b * 8 + (o | bit)
                            for slot, cos_at, sin_at in (
                                    (here, lambda k: cos_buf[a, k, rows_of(r), :], lambda k: sin_buf[a, k, rows_of(r), :]),
                                    (there, lambda k: cos_near[k], lambda k: sin_near[k])):
                                re[slot] = cos_half * cos_at(here) - sin_half * sin_at(there)
                                im[slot] = -(cos_half * sin_at(here)) - sin_half * cos_at(there)
                    re, im = rotate(re, im, cos_half, sin_half, [step for step in (1, 2, 4, 8) if step != bit])
                    re, im = sublane_rotate(re, im, cos_half, sin_half)
                    put_rows(i, re, im)
                    return carry

                lax.fori_loop(0, PER_SUB, slots, 0)
                lanes(a, sub)
            return carry

        lax.fori_loop(0, SUB, sub_step, 0)

        def quarters(b, carry):
            for a in range(2):
                bit = NEAR[a]
                emit(a, b, 1, a, b, cos_half, sin_half, (0, bit))
                send_parts(1, a, b, range(SUB), [o for o in (3, 6, 7, 1, 4, 5, 2) if o & ~bit], lambda o: o & ~bit)
            return carry

        lax.fori_loop(0, 2, quarters, 0)
        cost_swap[0] = cost[block(0)]
        for a in range(2):
            cost_swap[NEAR[a], a] = cost_near[block(0), a]
        wait_bytes(cost_swap.at[pl.ds(0, 6)], cost_recv)

    def run_layer(layer, odd, arrived, drained):
        source, target = (0, 1) if odd else (1, 0)

        def quarter(held, mixed):
            return (held, mixed) if odd else (mixed, held)

        cos_half, sin_half = half_angle(layer)
        cos_prev, sin_prev = half_angle(layer - 1)
        gamma = gammas[layer]
        set_matrix(cos_half, sin_half)

        def half(held, carry):
            def trig(r, carry):
                for mixed in range(2):
                    for o in range(8):
                        at = (block(o) if odd else o, *quarter(held, mixed), rows_of(r))
                        angle = gamma * (cost if odd else cost_swap)[at]
                        cos_buf[held, mixed * 8 + o, rows_of(r), :] = jnp.cos(angle)
                        sin_buf[held, mixed * 8 + o, rows_of(r), :] = jnp.sin(angle)
                return carry

            lax.fori_loop(0, 8, trig, 0)

            def sub_step(sub, carry):
                for mixed in range(2):
                    wait_all(recv, recv_sem, (source, *quarter(held, mixed), sub), arrived)

                def slots(i, carry):
                    r = sub * PER_SUB + i
                    cos_phase = [cos_buf[held, o, rows_of(r), :] for o in range(16)]
                    sin_phase = [sin_buf[held, o, rows_of(r), :] for o in range(16)]
                    old = [[recv[(source, *quarter(held, mixed), sub, o, c, rows_of(i))]
                            for mixed in range(2) for o in range(8)] for c in range(2)]
                    old_re, old_im = rotate(*old, cos_prev, sin_prev)
                    re = [r * c + i * s for r, i, c, s in zip(old_re, old_im, cos_phase, sin_phase)]
                    im = [i * c - r * s for r, i, c, s in zip(old_re, old_im, cos_phase, sin_phase)]
                    re, im = rotate(re, im, cos_half, sin_half)
                    re, im = sublane_rotate(re, im, cos_half, sin_half)
                    put_rows(i, re, im)
                    return carry

                lax.fori_loop(0, PER_SUB, slots, 0)
                lanes(held, sub)
                return carry

            lax.fori_loop(0, SUB, sub_step, 0)

            if drained:
                for mixed in range(2):
                    for sub in range(SUB):
                        wait_all(send, send_sem, (target, *quarter(held, mixed), sub), drained)

            def parts(held, mixed, subs):
                send_parts(target, *quarter(held, mixed), subs, SEND_ORDER, lambda o: o)

            emit(held, 0, target, *quarter(held, 0), cos_half, sin_half, (0,))
            parts(held, 0, range(SUB))

            @pl.when(held == 1)
            def _():
                parts(0, 1, range(SUB // 2, SUB))

            emit(held, 1, target, *quarter(held, 1), cos_half, sin_half, (0,))
            parts(held, 1, range(SUB // 2))

            @pl.when(held == 1)
            def _():
                parts(1, 1, range(SUB // 2, SUB))

            return carry

        lax.fori_loop(0, 2, half, 0)

    first_layer()
    run_layer(1, False, 6, 0)
    run_layer(2, True, 7, 6)

    def layer_pair(i, carry):
        run_layer(2 * i + 3, False, 7, 7)
        run_layer(2 * i + 4, True, 7, 7)
        return carry

    lax.fori_loop(0, LAYERS // 2 - 2, layer_pair, 0)
    run_layer(LAYERS - 1, False, 7, 7)

    cos_half, sin_half = half_angle(LAYERS - 1)
    energy_part[...] = jnp.zeros((8, LANES), jnp.float32)

    def final_half(a, carry):
        def final_sub(sub, carry):
            for b in range(2):
                wait_all(recv, recv_sem, (0, a, b, sub), 7)

            def slots(i, carry):
                r = sub * PER_SUB + i
                old = [[recv[0, a, b, sub, o, c, rows_of(i), :] for b in range(2) for o in range(8)]
                       for c in range(2)]
                re, im = rotate(*old, cos_half, sin_half)
                total = energy_part[...]
                for b in range(2):
                    for o in range(8):
                        at = (block(o), a, b, rows_of(r))
                        x, y = re[b * 8 + o], im[b * 8 + o]
                        out_re[at] = x
                        out_im[at] = y
                        total = total + cost[at] * (x * x + y * y)
                energy_part[...] = total
                return carry

            lax.fori_loop(0, PER_SUB, slots, 0)
            return carry

        lax.fori_loop(0, SUB, final_sub, 0)
        return carry

    lax.fori_loop(0, 2, final_half, 0)

    me = block(0)
    energy_row[...] = jnp.sum(energy_part[...], axis=0, keepdims=True)
    for offset in range(1, 8):
        remote(energy_row, energy_all.at[me], e_send.at[offset], e_recv.at[offset], offset)
    energy_all[me] = energy_row[...]
    for par in range(2):
        for a in range(2):
            for b in range(2):
                for sub in range(SUB):
                    wait_all(send, send_sem, (par, a, b, sub), 7)
    for a in range(2):
        for sub in range(SUB):
            wait_bytes(cost.at[:, a, :, pl.ds(sub * 8 * PER_SUB, 8 * PER_SUB)], near_send.at[a, sub])
    wait_bytes(cost_swap.at[pl.ds(0, 6)], cost_send)
    for offset in range(1, 8):
        wait_bytes(energy_row, e_send.at[offset])
        wait_bytes(energy_row, e_recv.at[offset])


def write_out(energy_all, in_re, in_im, energy, out_re, out_im, value, sem):
    copies = [pltpu.make_async_copy(in_re, out_re, sem.at[0]), pltpu.make_async_copy(in_im, out_im, sem.at[1])]
    for copy in copies:
        copy.start()
    total = energy_all[0]
    for i in range(1, 8):
        total = total + energy_all[i]
    value[0] = jnp.sum(total) * (1.0 / (1 << 21))
    copies.append(pltpu.make_async_copy(value, energy, sem.at[2]))
    copies[2].start()
    for copy in copies:
        copy.wait()


def solution(mesh):
    state_spec = P(('inst', 'qx', 'qy'))

    def device_body(cost_local, gammas, betas):
        local_len = cost_local.shape[0]
        shape = (8, 2, 2, local_len // (32 * LANES), LANES)
        f32 = jnp.float32
        vmem = pl.BlockSpec(memory_space=pltpu.VMEM)
        dma = pltpu.SemaphoreType.DMA
        parts = (2, 2, 2, SUB, 8, 2, 8 * PER_SUB, LANES)
        hbm = pl.BlockSpec(memory_space=pl.ANY)
        results = pl.pallas_call(
            kernel,
            out_shape=(pltpu.VMEM((8, 1, LANES), f32), pltpu.VMEM(shape, f32), pltpu.VMEM(shape, f32)),
            in_specs=[hbm, hbm, hbm],
            out_specs=(vmem, vmem, vmem),
            scratch_shapes=[
                pltpu.VMEM(shape, f32), pltpu.VMEM(shape, f32), pltpu.VMEM(shape, f32),
                pltpu.VMEM(parts, f32), pltpu.VMEM(parts, f32),
                pltpu.VMEM((2, 4, 2 * LANES, 2 * LANES), f32),
                pltpu.VMEM((2, 16, 64, LANES), f32), pltpu.VMEM((2, 16, 64, LANES), f32),
                pltpu.VMEM((16, 8, LANES), f32), pltpu.VMEM((16, 8, LANES), f32),
                pltpu.VMEM((2 * LANES, 2 * LANES), f32), pltpu.VMEM((2 * LANES, 2 * LANES), f32),
                pltpu.VMEM((8, LANES), f32), pltpu.VMEM((1, LANES), f32),
                pltpu.SMEM((LAYERS,), f32), pltpu.SMEM((LAYERS,), f32), dma((2,)), pltpu.SemaphoreType.REGULAR((2,)),
                dma((SUB,)), dma((2, SUB)), dma((2, SUB)), dma, dma,
                dma((2, 2, 2, SUB)), dma((2, 2, 2, SUB)),
                dma((8,)), dma((8,)),
            ],
            compiler_params=pltpu.CompilerParams(collective_id=0, has_side_effects=True),
            name='qaoa',
        )(cost_local.reshape(shape), gammas, betas)
        energy, state_re, state_im = pl.pallas_call(
            write_out,
            out_shape=(jax.ShapeDtypeStruct((1,), f32),
                       jax.ShapeDtypeStruct(shape, f32), jax.ShapeDtypeStruct(shape, f32)),
            in_specs=[vmem, vmem, vmem],
            out_specs=(hbm, hbm, hbm),
            scratch_shapes=[pltpu.SMEM((1,), f32), dma((3,))],
            name='write_out',
        )(*[pltpu.with_memory_space_constraint(value, pltpu.VMEM) for value in results])
        return energy, state_re.reshape(local_len), state_im.reshape(local_len)

    return jax.shard_map(device_body, mesh=mesh, in_specs=(state_spec, P(), P()),
                         out_specs=(P('inst'), state_spec, state_spec), check_vma=False)
```

```python
import jax
import jax.numpy as jnp
from jax import lax
from jax.experimental import pallas as pl
from jax.experimental.pallas import tpu as pltpu
from jax.sharding import PartitionSpec as P

LANES = 128
LAYERS = 8
SUB = 4
PER_SUB = 8 // SUB
NEAR = (4, 1)


def rotate(re, im, cos_half, sin_half, steps=None):
    count = len(re)
    for step in steps or [1 << i for i in range(count.bit_length() - 1)]:
        new_re = [cos_half * re[i] + sin_half * im[i ^ step] for i in range(count)]
        new_im = [cos_half * im[i] - sin_half * re[i ^ step] for i in range(count)]
        re, im = new_re, new_im
    return re, im


def sublane_rotate(re, im, cos_half, sin_half):
    row = lax.broadcasted_iota(jnp.int32, (8, LANES), 0)
    for step in (1, 2, 4):
        bit_set = (row & step) != 0

        def flip(value):
            down = pltpu.roll(value, step, 0)
            if step == 4:
                return down
            return jnp.where(bit_set, down, pltpu.roll(value, 8 - step, 0))

        flip_re = [flip(value) for value in re]
        flip_im = [flip(value) for value in im]
        re, im = ([cos_half * r + sin_half * fi for r, fi in zip(re, flip_im)],
                  [cos_half * i - sin_half * fr for i, fr in zip(im, flip_re)])
    return re, im


def lane_matrix(cos_half, sin_half):
    row = lax.broadcasted_iota(jnp.int32, (LANES, LANES), 0)
    col = lax.broadcasted_iota(jnp.int32, (LANES, LANES), 1)
    diff = row ^ col
    cos_full = jnp.broadcast_to(cos_half[0:1], (LANES, LANES))
    sin_full = jnp.broadcast_to(sin_half[0:1], (LANES, LANES))
    mag = jnp.ones((LANES, LANES), jnp.float32)
    weight = jnp.zeros((LANES, LANES), jnp.int32)
    for bit in range(7):
        on = (diff >> bit) & 1
        mag = mag * jnp.where(on == 1, sin_full, cos_full)
        weight = weight + on
    quarter = weight & 3
    zero = jnp.zeros_like(mag)
    real = jnp.where(quarter == 0, mag, jnp.where(quarter == 2, -mag, zero))
    imag = jnp.where(quarter == 1, -mag, jnp.where(quarter == 3, mag, zero))
    return real, imag


def kernel(cost_hbm, gammas_hbm, betas_hbm, energy_all, out_re, out_im,
           cost, cost_near, cost_swap, recv, send, work, cos_buf, sin_buf, cos_near, sin_near,
           rows_in, matrix, energy_part, energy_row, gammas, betas, angle_in, near_in, cost_in, near_send, near_recv, cost_send, cost_recv,
           send_sem, recv_sem, e_send, e_recv):
    loads = [pltpu.make_async_copy(cost_hbm.at[:, :, :, pl.ds(sub * 8 * PER_SUB, 8 * PER_SUB)],
                                   cost.at[:, :, :, pl.ds(sub * 8 * PER_SUB, 8 * PER_SUB)], cost_in.at[sub])
             for sub in range(SUB)]
    for load in loads:
        load.start()
    angle_loads = [pltpu.make_async_copy(gammas_hbm, gammas, angle_in.at[0]),
                   pltpu.make_async_copy(betas_hbm, betas, angle_in.at[1])]
    for load in angle_loads:
        load.start()
    qx = lax.axis_index('qx')
    qy = lax.axis_index('qy')
    bits = (qy, qx % 2, qx // 2)

    def flipped(offset):
        return [1 - bit if (offset >> i) & 1 else bit for i, bit in enumerate(bits)]

    def block(offset):
        y, core, x = flipped(offset)
        return (x * 2 + core) * 2 + y

    def peer(offset):
        y, core, x = flipped(offset)
        return {'qy': y, 'qx': x * 2 + core}

    def remote(source, target, send_at, recv_at, offset):
        pltpu.make_async_remote_copy(
            src_ref=source, dst_ref=target, send_sem=send_at, recv_sem=recv_at,
            device_id=peer(offset), device_id_type=pl.DeviceIdType.MESH).start()

    barrier = pltpu.get_barrier_semaphore()
    def signal_next(sem):
        for offset in (4, 1, 2):
            pl.semaphore_signal(sem, inc=1, device_id=peer(offset), device_id_type=pl.DeviceIdType.MESH)

    signal_next(barrier)
    pl.semaphore_wait(barrier, 3)

    def half_angle(layer):
        angle = jnp.full((8, LANES), 0.5 * betas[layer], jnp.float32)
        return jnp.cos(angle), jnp.sin(angle)

    def wait_bytes(part, sem):
        pltpu.make_async_copy(part, part, sem).wait()

    def wait_all(buffer, sem, at, count):
        wait_bytes(buffer.at[(*at, pl.ds(0, count))], sem.at[at])

    def rows_of(r):
        return pl.ds(pl.multiple_of(r * 8, 8), 8)

    def set_matrix(cos_half, sin_half):
        real, imag = lane_matrix(cos_half, sin_half)
        matrix[0:LANES, 0:LANES] = real
        matrix[0:LANES, LANES:] = imag
        matrix[LANES:, 0:LANES] = -imag
        matrix[LANES:, LANES:] = real

    def put_rows(i, re, im):
        for o in range(16):
            at = pl.multiple_of(o * 16 + i * 8, 8)
            rows_in[pl.ds(at, 8), 0:LANES] = re[o]
            rows_in[pl.ds(at, 8), LANES:] = im[o]

    def lanes(a_held, at):
        work[a_held, at] = lax.dot(
            rows_in[...], matrix[...],
            precision=lax.Precision.HIGHEST, preferred_element_type=jnp.float32)

    def emit(held, mixed, target, a, b, cos_half, sin_half, order, route, local):
        def across(o, buffer):
            def part(r, c):
                at = pl.multiple_of((mixed * 8 + o) * 16 + (r % 2) * 8, 8)
                return work[held, r // 2, pl.ds(at, 8), c * LANES:(c + 1) * LANES]

            re = [part(r, 0) for r in range(8)]
            im = [part(r, 1) for r in range(8)]
            re, im = rotate(re, im, cos_half, sin_half)
            for r in range(8):
                row = (r % PER_SUB) * 8
                buffer[target, a, b, r // PER_SUB, o, 0, row:row + 8, :] = re[r]
                buffer[target, a, b, r // PER_SUB, o, 1, row:row + 8, :] = im[r]

        def body(o, carry):
            across(o, send)
            return carry

        lax.fori_loop(1, 8, body, 0)
        for o in local:
            across(o, recv)
        for sub in range(SUB):
            at = (target, a, b, sub)
            if route is None:
                y, core, x = bits
                for x_step, y_step in ((1, 1), (1, 0), (0, 1)):
                    for turn in (core, 1 - core):
                        o = 4 * x_step + 2 * turn + y_step
                        pltpu.make_async_remote_copy(
                            src_ref=send.at[(*at, o)], dst_ref=recv.at[(*at, o)],
                            send_sem=send_sem.at[at], recv_sem=recv_sem.at[at],
                            device_id={'qy': (y + y_step) % 2, 'qx': (x + x_step) % 2 * 2 + (core + turn) % 2},
                            device_id_type=pl.DeviceIdType.MESH).start()
                remote(send.at[(*at, 2)], recv.at[(*at, 2)], send_sem.at[at], recv_sem.at[at], 2)
                continue
            for o in order:
                remote(send.at[(*at, o)], recv.at[(*at, o)], send_sem.at[at], recv_sem.at[at], route(o))

    def first_layer():
        def sub_rows(sub):
            return pl.ds(pl.multiple_of(sub * 8 * PER_SUB, 8), 8 * PER_SUB)

        for sub in range(SUB):
            loads[sub].wait()
            for a in range(2):
                remote(cost.at[:, a, :, sub_rows(sub)], cost_near.at[:, a, :, sub_rows(sub)],
                       near_send.at[a, sub], near_recv.at[a, sub], NEAR[a])
        signal_next(near_in.at[0])
        for load in angle_loads:
            load.wait()
        gamma = gammas[0]
        cos_half, sin_half = half_angle(0)
        set_matrix(cos_half, sin_half)

        def own_trig(r, carry):
            for a in range(2):
                for b in range(2):
                    for o in range(8):
                        angle = gamma * cost[block(o), a, b, rows_of(r), :]
                        cos_buf[a, b * 8 + o, rows_of(r), :] = jnp.cos(angle)
                        sin_buf[a, b * 8 + o, rows_of(r), :] = jnp.sin(angle)
            return carry

        for round_id in range(2):
            lax.fori_loop(4 * round_id, 4 * round_id + 4, own_trig, 0)
            pl.semaphore_wait(near_in.at[round_id], 3)
            if round_id == 0:
                signal_next(near_in.at[1])
        for a in range(2):
            for o in range(1, 8):
                if not o & NEAR[a]:
                    remote(cost.at[block(o), a], cost_swap.at[o, a], cost_send, cost_recv, o)

        def sub_step(sub, carry):
            for a in range(2):
                bit = NEAR[a]
                part = cost_near.at[:, a, :, sub_rows(sub)]
                wait_bytes(part, near_recv.at[a, sub])
                for o in range(1, 8):
                    if not o & bit:
                        remote(cost_near.at[block(o), a, :, sub_rows(sub)],
                               cost_swap.at[o | bit, a, :, sub_rows(sub)], cost_send, cost_recv, o)

                def slots(i, carry):
                    r = sub * PER_SUB + i
                    for b in range(2):
                        for o in range(8):
                            angle = gamma * cost_near[block(o), a, b, rows_of(r), :]
                            cos_near[b * 8 + o] = jnp.cos(angle)
                            sin_near[b * 8 + o] = jnp.sin(angle)
                    re, im = [None] * 16, [None] * 16
                    for b in range(2):
                        for o in range(8):
                            if o & bit:
                                continue
                            here, there = b * 8 + o, b * 8 + (o | bit)
                            for slot, cos_at, sin_at in (
                                    (here, lambda k: cos_buf[a, k, rows_of(r), :], lambda k: sin_buf[a, k, rows_of(r), :]),
                                    (there, lambda k: cos_near[k], lambda k: sin_near[k])):
                                re[slot] = cos_half * cos_at(here) - sin_half * sin_at(there)
                                im[slot] = -(cos_half * sin_at(here)) - sin_half * cos_at(there)
                    re, im = rotate(re, im, cos_half, sin_half, [step for step in (1, 2, 4, 8) if step != bit])
                    re, im = sublane_rotate(re, im, cos_half, sin_half)
                    put_rows(i, re, im)
                    return carry

                lax.fori_loop(0, PER_SUB, slots, 0)
                lanes(a, sub)
            return carry

        lax.fori_loop(0, SUB, sub_step, 0)

        def quarters(b, carry):
            for a in range(2):
                bit = NEAR[a]
                emit(a, b, 1, a, b, cos_half, sin_half,
                     [o for o in (3, 6, 7, 1, 4, 5, 2) if o & ~bit], lambda o: o & ~bit, (0, bit))
            return carry

        lax.fori_loop(0, 2, quarters, 0)
        cost_swap[0] = cost[block(0)]
        for a in range(2):
            cost_swap[NEAR[a], a] = cost_near[block(0), a]
        wait_bytes(cost_swap.at[pl.ds(0, 6)], cost_recv)

    def run_layer(layer, odd, arrived, drained):
        source, target = (0, 1) if odd else (1, 0)

        def quarter(held, mixed):
            return (held, mixed) if odd else (mixed, held)

        cos_half, sin_half = half_angle(layer)
        cos_prev, sin_prev = half_angle(layer - 1)
        gamma = gammas[layer]
        set_matrix(cos_half, sin_half)

        def half(held, carry):
            def trig(r, carry):
                for mixed in range(2):
                    for o in range(8):
                        at = (block(o) if odd else o, *quarter(held, mixed), rows_of(r))
                        angle = gamma * (cost if odd else cost_swap)[at]
                        cos_buf[held, mixed * 8 + o, rows_of(r), :] = jnp.cos(angle)
                        sin_buf[held, mixed * 8 + o, rows_of(r), :] = jnp.sin(angle)
                return carry

            lax.fori_loop(0, 8, trig, 0)

            def sub_step(sub, carry):
                for mixed in range(2):
                    wait_all(recv, recv_sem, (source, *quarter(held, mixed), sub), arrived)

                def slots(i, carry):
                    r = sub * PER_SUB + i
                    cos_phase = [cos_buf[held, o, rows_of(r), :] for o in range(16)]
                    sin_phase = [sin_buf[held, o, rows_of(r), :] for o in range(16)]
                    old = [[recv[(source, *quarter(held, mixed), sub, o, c, rows_of(i))]
                            for mixed in range(2) for o in range(8)] for c in range(2)]
                    old_re, old_im = rotate(*old, cos_prev, sin_prev)
                    re = [r * c + i * s for r, i, c, s in zip(old_re, old_im, cos_phase, sin_phase)]
                    im = [i * c - r * s for r, i, c, s in zip(old_re, old_im, cos_phase, sin_phase)]
                    re, im = rotate(re, im, cos_half, sin_half)
                    re, im = sublane_rotate(re, im, cos_half, sin_half)
                    put_rows(i, re, im)
                    return carry

                lax.fori_loop(0, PER_SUB, slots, 0)
                lanes(held, sub)
                return carry

            lax.fori_loop(0, SUB, sub_step, 0)

            if drained:
                for mixed in range(2):
                    for sub in range(SUB):
                        wait_all(send, send_sem, (target, *quarter(held, mixed), sub), drained)

            def quarters(mixed, carry):
                emit(held, mixed, target, *quarter(held, mixed), cos_half, sin_half, (), None, (0,))
                return carry

            lax.fori_loop(0, 2, quarters, 0)
            return carry

        lax.fori_loop(0, 2, half, 0)

    first_layer()
    run_layer(1, False, 6, 0)
    run_layer(2, True, 7, 6)

    def layer_pair(i, carry):
        run_layer(2 * i + 3, False, 7, 7)
        run_layer(2 * i + 4, True, 7, 7)
        return carry

    lax.fori_loop(0, LAYERS // 2 - 2, layer_pair, 0)
    run_layer(LAYERS - 1, False, 7, 7)

    cos_half, sin_half = half_angle(LAYERS - 1)
    energy_part[...] = jnp.zeros((8, LANES), jnp.float32)

    def final_half(a, carry):
        def final_sub(sub, carry):
            for b in range(2):
                wait_all(recv, recv_sem, (0, a, b, sub), 7)

            def slots(i, carry):
                r = sub * PER_SUB + i
                old = [[recv[0, a, b, sub, o, c, rows_of(i), :] for b in range(2) for o in range(8)]
                       for c in range(2)]
                re, im = rotate(*old, cos_half, sin_half)
                total = energy_part[...]
                for b in range(2):
                    for o in range(8):
                        at = (block(o), a, b, rows_of(r))
                        x, y = re[b * 8 + o], im[b * 8 + o]
                        out_re[at] = x
                        out_im[at] = y
                        total = total + cost[at] * (x * x + y * y)
                energy_part[...] = total
                return carry

            lax.fori_loop(0, PER_SUB, slots, 0)
            return carry

        lax.fori_loop(0, SUB, final_sub, 0)
        return carry

    lax.fori_loop(0, 2, final_half, 0)

    me = block(0)
    energy_row[...] = jnp.sum(energy_part[...], axis=0, keepdims=True)
    for offset in range(1, 8):
        remote(energy_row, energy_all.at[me], e_send.at[offset], e_recv.at[offset], offset)
    energy_all[me] = energy_row[...]
    for par in range(2):
        for a in range(2):
            for b in range(2):
                for sub in range(SUB):
                    wait_all(send, send_sem, (par, a, b, sub), 7)
    for a in range(2):
        for sub in range(SUB):
            wait_bytes(cost.at[:, a, :, pl.ds(sub * 8 * PER_SUB, 8 * PER_SUB)], near_send.at[a, sub])
    wait_bytes(cost_swap.at[pl.ds(0, 6)], cost_send)
    for offset in range(1, 8):
        wait_bytes(energy_row, e_send.at[offset])
        wait_bytes(energy_row, e_recv.at[offset])


def write_out(energy_all, in_re, in_im, energy, out_re, out_im, value, sem):
    copies = [pltpu.make_async_copy(in_re, out_re, sem.at[0]), pltpu.make_async_copy(in_im, out_im, sem.at[1])]
    for copy in copies:
        copy.start()
    total = energy_all[0]
    for i in range(1, 8):
        total = total + energy_all[i]
    value[0] = jnp.sum(total) * (1.0 / (1 << 21))
    copies.append(pltpu.make_async_copy(value, energy, sem.at[2]))
    copies[2].start()
    for copy in copies:
        copy.wait()


def solution(mesh):
    state_spec = P(('inst', 'qx', 'qy'))

    def device_body(cost_local, gammas, betas):
        local_len = cost_local.shape[0]
        shape = (8, 2, 2, local_len // (32 * LANES), LANES)
        f32 = jnp.float32
        vmem = pl.BlockSpec(memory_space=pltpu.VMEM)
        dma = pltpu.SemaphoreType.DMA
        parts = (2, 2, 2, SUB, 8, 2, 8 * PER_SUB, LANES)
        hbm = pl.BlockSpec(memory_space=pl.ANY)
        results = pl.pallas_call(
            kernel,
            out_shape=(pltpu.VMEM((8, 1, LANES), f32), pltpu.VMEM(shape, f32), pltpu.VMEM(shape, f32)),
            in_specs=[hbm, hbm, hbm],
            out_specs=(vmem, vmem, vmem),
            scratch_shapes=[
                pltpu.VMEM(shape, f32), pltpu.VMEM(shape, f32), pltpu.VMEM(shape, f32),
                pltpu.VMEM(parts, f32), pltpu.VMEM(parts, f32),
                pltpu.VMEM((2, 4, 2 * LANES, 2 * LANES), f32),
                pltpu.VMEM((2, 16, 64, LANES), f32), pltpu.VMEM((2, 16, 64, LANES), f32),
                pltpu.VMEM((16, 8, LANES), f32), pltpu.VMEM((16, 8, LANES), f32),
                pltpu.VMEM((2 * LANES, 2 * LANES), f32), pltpu.VMEM((2 * LANES, 2 * LANES), f32),
                pltpu.VMEM((8, LANES), f32), pltpu.VMEM((1, LANES), f32),
                pltpu.SMEM((LAYERS,), f32), pltpu.SMEM((LAYERS,), f32), dma((2,)), pltpu.SemaphoreType.REGULAR((2,)),
                dma((SUB,)), dma((2, SUB)), dma((2, SUB)), dma, dma,
                dma((2, 2, 2, SUB)), dma((2, 2, 2, SUB)),
                dma((8,)), dma((8,)),
            ],
            compiler_params=pltpu.CompilerParams(collective_id=0, has_side_effects=True),
            name='qaoa',
        )(cost_local.reshape(shape), gammas, betas)
        energy, state_re, state_im = pl.pallas_call(
            write_out,
            out_shape=(jax.ShapeDtypeStruct((1,), f32),
                       jax.ShapeDtypeStruct(shape, f32), jax.ShapeDtypeStruct(shape, f32)),
            in_specs=[vmem, vmem, vmem],
            out_specs=(hbm, hbm, hbm),
            scratch_shapes=[pltpu.SMEM((1,), f32), dma((3,))],
            name='write_out',
        )(*[pltpu.with_memory_space_constraint(value, pltpu.VMEM) for value in results])
        return energy, state_re.reshape(local_len), state_im.reshape(local_len)

    return jax.shard_map(device_body, mesh=mesh, in_specs=(state_spec, P(), P()),
                         out_specs=(P('inst'), state_spec, state_spec), check_vma=False)
```

```python
import jax
import jax.numpy as jnp
from jax import lax
from jax.experimental import pallas as pl
from jax.experimental.pallas import tpu as pltpu
from jax.sharding import PartitionSpec as P

LANES = 128
LAYERS = 8
FIRST = 2
REST = 1
PAIRS = 4
SEND_ORDER = (5, 7, 4, 6, 1, 3, 2)
NEAR = (4, 1)


def rotate(re, im, cos_half, sin_half, steps=None):
    count = len(re)
    for step in steps or [1 << i for i in range(count.bit_length() - 1)]:
        new_re = [cos_half * re[i] + sin_half * im[i ^ step] for i in range(count)]
        new_im = [cos_half * im[i] - sin_half * re[i ^ step] for i in range(count)]
        re, im = new_re, new_im
    return re, im


def sublane_rotate(re, im, cos_half, sin_half):
    row = lax.broadcasted_iota(jnp.int32, (8, LANES), 0)
    for step in (1, 2, 4):
        bit_set = (row & step) != 0

        def flip(value):
            down = pltpu.roll(value, step, 0)
            if step == 4:
                return down
            return jnp.where(bit_set, down, pltpu.roll(value, 8 - step, 0))

        flip_re = [flip(value) for value in re]
        flip_im = [flip(value) for value in im]
        re, im = ([cos_half * r + sin_half * fi for r, fi in zip(re, flip_im)],
                  [cos_half * i - sin_half * fr for i, fr in zip(im, flip_re)])
    return re, im


def lane_matrix(cos_half, sin_half):
    row = lax.broadcasted_iota(jnp.int32, (LANES, LANES), 0)
    col = lax.broadcasted_iota(jnp.int32, (LANES, LANES), 1)
    diff = row ^ col
    cos_full = jnp.broadcast_to(cos_half[0:1], (LANES, LANES))
    sin_full = jnp.broadcast_to(sin_half[0:1], (LANES, LANES))
    mag = jnp.ones((LANES, LANES), jnp.float32)
    weight = jnp.zeros((LANES, LANES), jnp.int32)
    for bit in range(7):
        on = (diff >> bit) & 1
        mag = mag * jnp.where(on == 1, sin_full, cos_full)
        weight = weight + on
    quarter = weight & 3
    zero = jnp.zeros_like(mag)
    real = jnp.where(quarter == 0, mag, jnp.where(quarter == 2, -mag, zero))
    imag = jnp.where(quarter == 1, -mag, jnp.where(quarter == 3, mag, zero))
    return real, imag


def kernel(cost_hbm, gammas_hbm, betas_hbm, energy_all, out_re, out_im,
           cost, cost_near, cost_swap, recv, send, work, cos_buf, sin_buf, cos_near, sin_near,
           rows_in, matrix, energy_part, energy_row, gammas, betas, angle_in, near_in, cost_in, near_send, near_recv, cost_send, cost_recv,
           send_sem, recv_sem, e_send, e_recv):
    loads = [pltpu.make_async_copy(cost_hbm.at[:, :, :, pl.ds(sub * 16, 16)],
                                   cost.at[:, :, :, pl.ds(sub * 16, 16)], cost_in.at[sub])
             for sub in range(PAIRS)]
    for load in loads:
        load.start()
    angle_loads = [pltpu.make_async_copy(gammas_hbm, gammas, angle_in.at[0]),
                   pltpu.make_async_copy(betas_hbm, betas, angle_in.at[1])]
    for load in angle_loads:
        load.start()
    qx = lax.axis_index('qx')
    qy = lax.axis_index('qy')
    bits = (qy, qx % 2, qx // 2)

    def flipped(offset):
        return [1 - bit if (offset >> i) & 1 else bit for i, bit in enumerate(bits)]

    def block(offset):
        y, core, x = flipped(offset)
        return (x * 2 + core) * 2 + y

    def peer(offset):
        y, core, x = flipped(offset)
        return {'qy': y, 'qx': x * 2 + core}

    def remote(source, target, send_at, recv_at, offset):
        pltpu.make_async_remote_copy(
            src_ref=source, dst_ref=target, send_sem=send_at, recv_sem=recv_at,
            device_id=peer(offset), device_id_type=pl.DeviceIdType.MESH).start()

    barrier = pltpu.get_barrier_semaphore()
    def signal_next(sem):
        for offset in (4, 1, 2):
            pl.semaphore_signal(sem, inc=1, device_id=peer(offset), device_id_type=pl.DeviceIdType.MESH)

    signal_next(barrier)
    pl.semaphore_wait(barrier, 3)

    def half_angle(layer):
        angle = jnp.full((8, LANES), 0.5 * betas[layer], jnp.float32)
        return jnp.cos(angle), jnp.sin(angle)

    def wait_bytes(part, sem):
        pltpu.make_async_copy(part, part, sem).wait()

    def wait_all(buffer, sem, at, first_r, size, count):
        wait_bytes(buffer.at[(*at, pl.ds(0, count), pl.ds(0, size))], sem.at[(*at, first_r)])

    def rows_of(r):
        return pl.ds(pl.multiple_of(r * 8, 8), 8)

    def set_matrix(cos_half, sin_half):
        real, imag = lane_matrix(cos_half, sin_half)
        matrix[0:LANES, 0:LANES] = real
        matrix[0:LANES, LANES:] = imag
        matrix[LANES:, 0:LANES] = -imag
        matrix[LANES:, LANES:] = real

    def put_rows(i, re, im):
        for o in range(16):
            at = pl.multiple_of(o * 16 + i * 8, 8)
            rows_in[pl.ds(at, 8), 0:LANES] = re[o]
            rows_in[pl.ds(at, 8), LANES:] = im[o]

    def lanes(a_held, at):
        work[a_held, at] = lax.dot(
            rows_in[...], matrix[...],
            precision=lax.Precision.HIGHEST, preferred_element_type=jnp.float32)

    def emit(held, mixed, target, a, b, cos_half, sin_half, size, order, route, local):
        def across(o, buffer):
            def part(r, c):
                at = pl.multiple_of((mixed * 8 + o) * 16 + (r % 2) * 8, 8)
                return work[held, r // 2, pl.ds(at, 8), c * LANES:(c + 1) * LANES]

            re = [part(r, 0) for r in range(8)]
            im = [part(r, 1) for r in range(8)]
            re, im = rotate(re, im, cos_half, sin_half)
            for r in range(8):
                buffer[target, a, b, o, r, 0] = re[r]
                buffer[target, a, b, o, r, 1] = im[r]

        def body(o, carry):
            across(o, send)
            return carry

        lax.fori_loop(1, 8, body, 0)
        for o in local:
            across(o, recv)
        for r in range(0, 8, size):
            sem_at = (target, a, b, r)
            for o in order:
                at = (target, a, b, o, pl.ds(r, size))
                remote(send.at[at], recv.at[at], send_sem.at[sem_at], recv_sem.at[sem_at], route(o))

    def first_layer():
        def sub_rows(sub):
            return pl.ds(pl.multiple_of(sub * 16, 8), 16)

        for sub in range(PAIRS):
            loads[sub].wait()
            for a in range(2):
                remote(cost.at[:, a, :, sub_rows(sub)], cost_near.at[:, a, :, sub_rows(sub)],
                       near_send.at[a, sub], near_recv.at[a, sub], NEAR[a])
        signal_next(near_in.at[0])
        for load in angle_loads:
            load.wait()
        gamma = gammas[0]
        cos_half, sin_half = half_angle(0)
        set_matrix(cos_half, sin_half)

        def own_trig(r, carry):
            for a in range(2):
                for b in range(2):
                    for o in range(8):
                        angle = gamma * cost[block(o), a, b, rows_of(r), :]
                        cos_buf[a, b * 8 + o, rows_of(r), :] = jnp.cos(angle)
                        sin_buf[a, b * 8 + o, rows_of(r), :] = jnp.sin(angle)
            return carry

        for round_id in range(2):
            lax.fori_loop(4 * round_id, 4 * round_id + 4, own_trig, 0)
            pl.semaphore_wait(near_in.at[round_id], 3)
            if round_id == 0:
                signal_next(near_in.at[1])
        for a in range(2):
            for o in range(1, 8):
                if not o & NEAR[a]:
                    remote(cost.at[block(o), a], cost_swap.at[o, a], cost_send, cost_recv, o)

        def sub_step(sub, carry):
            for a in range(2):
                bit = NEAR[a]
                part = cost_near.at[:, a, :, sub_rows(sub)]
                wait_bytes(part, near_recv.at[a, sub])
                for o in range(1, 8):
                    if not o & bit:
                        remote(cost_near.at[block(o), a, :, sub_rows(sub)],
                               cost_swap.at[o | bit, a, :, sub_rows(sub)], cost_send, cost_recv, o)

                def slots(i, carry):
                    r = 2 * sub + i
                    for b in range(2):
                        for o in range(8):
                            angle = gamma * cost_near[block(o), a, b, rows_of(r), :]
                            cos_near[b * 8 + o] = jnp.cos(angle)
                            sin_near[b * 8 + o] = jnp.sin(angle)
                    re, im = [None] * 16, [None] * 16
                    for b in range(2):
                        for o in range(8):
                            if o & bit:
                                continue
                            here, there = b * 8 + o, b * 8 + (o | bit)
                            for slot, cos_at, sin_at in (
                                    (here, lambda k: cos_buf[a, k, rows_of(r), :], lambda k: sin_buf[a, k, rows_of(r), :]),
                                    (there, lambda k: cos_near[k], lambda k: sin_near[k])):
                                re[slot] = cos_half * cos_at(here) - sin_half * sin_at(there)
                                im[slot] = -(cos_half * sin_at(here)) - sin_half * cos_at(there)
                    re, im = rotate(re, im, cos_half, sin_half, [step for step in (1, 2, 4, 8) if step != bit])
                    re, im = sublane_rotate(re, im, cos_half, sin_half)
                    put_rows(i, re, im)
                    return carry

                lax.fori_loop(0, 2, slots, 0)
                lanes(a, sub)
            return carry

        lax.fori_loop(0, PAIRS, sub_step, 0)

        def quarters(b, carry):
            for a in range(2):
                bit = NEAR[a]
                emit(a, b, 1, a, b, cos_half, sin_half, FIRST,
                     [o for o in (3, 6, 7, 1, 4, 5, 2) if o & ~bit], lambda o: o & ~bit, (0, bit))
            return carry

        lax.fori_loop(0, 2, quarters, 0)
        cost_swap[0] = cost[block(0)]
        for a in range(2):
            cost_swap[NEAR[a], a] = cost_near[block(0), a]
        wait_bytes(cost_swap.at[pl.ds(0, 6)], cost_recv)

    def run_layer(layer, odd, arrived, drained, size_in=REST, size_drained=REST):
        source, target = (0, 1) if odd else (1, 0)

        def quarter(held, mixed):
            return (held, mixed) if odd else (mixed, held)

        cos_half, sin_half = half_angle(layer)
        cos_prev, sin_prev = half_angle(layer - 1)
        gamma = gammas[layer]
        set_matrix(cos_half, sin_half)

        def half(held, carry):
            def trig(r, carry):
                for mixed in range(2):
                    for o in range(8):
                        at = (block(o) if odd else o, *quarter(held, mixed), rows_of(r))
                        angle = gamma * (cost if odd else cost_swap)[at]
                        cos_buf[held, mixed * 8 + o, rows_of(r), :] = jnp.cos(angle)
                        sin_buf[held, mixed * 8 + o, rows_of(r), :] = jnp.sin(angle)
                return carry

            lax.fori_loop(0, 8, trig, 0)

            def block_step(sub, carry):
                for i in range(0, 2, size_in):
                    for mixed in range(2):
                        wait_all(recv, recv_sem, (source, *quarter(held, mixed)), 2 * sub + i, size_in, arrived)

                def slots(i, carry):
                    r = 2 * sub + i
                    cos_phase = [cos_buf[held, o, rows_of(r), :] for o in range(16)]
                    sin_phase = [sin_buf[held, o, rows_of(r), :] for o in range(16)]
                    old = [[recv[(source, *quarter(held, mixed), o, r, c)]
                            for mixed in range(2) for o in range(8)] for c in range(2)]
                    old_re, old_im = rotate(*old, cos_prev, sin_prev)
                    re = [r * c + i * s for r, i, c, s in zip(old_re, old_im, cos_phase, sin_phase)]
                    im = [i * c - r * s for r, i, c, s in zip(old_re, old_im, cos_phase, sin_phase)]
                    re, im = rotate(re, im, cos_half, sin_half)
                    re, im = sublane_rotate(re, im, cos_half, sin_half)
                    put_rows(i, re, im)
                    return carry

                lax.fori_loop(0, 2, slots, 0)
                lanes(held, sub)
                return carry

            lax.fori_loop(0, PAIRS, block_step, 0)

            if drained:
                for mixed in range(2):
                    for r in range(0, 8, size_drained):
                        wait_all(send, send_sem, (target, *quarter(held, mixed)), r, size_drained, drained)

            def quarters(mixed, carry):
                emit(held, mixed, target, *quarter(held, mixed), cos_half, sin_half, REST, SEND_ORDER, lambda o: o, (0,))
                return carry

            lax.fori_loop(0, 2, quarters, 0)
            return carry

        lax.fori_loop(0, 2, half, 0)

    first_layer()
    run_layer(1, False, 6, 0, size_in=FIRST)
    run_layer(2, True, 7, 6, size_drained=FIRST)

    def layer_pair(i, carry):
        run_layer(2 * i + 3, False, 7, 7)
        run_layer(2 * i + 4, True, 7, 7)
        return carry

    lax.fori_loop(0, LAYERS // 2 - 2, layer_pair, 0)
    run_layer(LAYERS - 1, False, 7, 7)

    cos_half, sin_half = half_angle(LAYERS - 1)
    energy_part[...] = jnp.zeros((8, LANES), jnp.float32)

    def final_half(a, carry):
        def message(i, carry):
            for b in range(2):
                wait_all(recv, recv_sem, (0, a, b), i * REST, REST, 7)

            def slots(r, carry):
                old = [[recv[0, a, b, o, r, c] for b in range(2) for o in range(8)] for c in range(2)]
                re, im = rotate(*old, cos_half, sin_half)
                total = energy_part[...]
                for b in range(2):
                    for o in range(8):
                        at = (block(o), a, b, rows_of(r))
                        x, y = re[b * 8 + o], im[b * 8 + o]
                        out_re[at] = x
                        out_im[at] = y
                        total = total + cost[at] * (x * x + y * y)
                energy_part[...] = total
                return carry

            lax.fori_loop(i * REST, (i + 1) * REST, slots, 0)
            return carry

        lax.fori_loop(0, 8 // REST, message, 0)
        return carry

    lax.fori_loop(0, 2, final_half, 0)

    me = block(0)
    energy_row[...] = jnp.sum(energy_part[...], axis=0, keepdims=True)
    for offset in range(1, 8):
        remote(energy_row, energy_all.at[me], e_send.at[offset], e_recv.at[offset], offset)
    energy_all[me] = energy_row[...]
    for par in range(2):
        for a in range(2):
            for b in range(2):
                for r in range(0, 8, REST):
                    wait_all(send, send_sem, (par, a, b), r, REST, 7)
    for a in range(2):
        for sub in range(PAIRS):
            wait_bytes(cost.at[:, a, :, pl.ds(sub * 16, 16)], near_send.at[a, sub])
    wait_bytes(cost_swap.at[pl.ds(0, 6)], cost_send)
    for offset in range(1, 8):
        wait_bytes(energy_row, e_send.at[offset])
        wait_bytes(energy_row, e_recv.at[offset])


def write_out(energy_all, in_re, in_im, energy, out_re, out_im, value, sem):
    copies = [pltpu.make_async_copy(in_re, out_re, sem.at[0]), pltpu.make_async_copy(in_im, out_im, sem.at[1])]
    for copy in copies:
        copy.start()
    total = energy_all[0]
    for i in range(1, 8):
        total = total + energy_all[i]
    value[0] = jnp.sum(total) * (1.0 / (1 << 21))
    copies.append(pltpu.make_async_copy(value, energy, sem.at[2]))
    copies[2].start()
    for copy in copies:
        copy.wait()


def solution(mesh):
    state_spec = P(('inst', 'qx', 'qy'))

    def device_body(cost_local, gammas, betas):
        local_len = cost_local.shape[0]
        shape = (8, 2, 2, local_len // (32 * LANES), LANES)
        f32 = jnp.float32
        vmem = pl.BlockSpec(memory_space=pltpu.VMEM)
        dma = pltpu.SemaphoreType.DMA
        parts = (2, 2, 2, 8, 8, 2, 8, LANES)
        hbm = pl.BlockSpec(memory_space=pl.ANY)
        results = pl.pallas_call(
            kernel,
            out_shape=(pltpu.VMEM((8, 1, LANES), f32), pltpu.VMEM(shape, f32), pltpu.VMEM(shape, f32)),
            in_specs=[hbm, hbm, hbm],
            out_specs=(vmem, vmem, vmem),
            scratch_shapes=[
                pltpu.VMEM(shape, f32), pltpu.VMEM(shape, f32), pltpu.VMEM(shape, f32),
                pltpu.VMEM(parts, f32), pltpu.VMEM(parts, f32),
                pltpu.VMEM((2, 4, 2 * LANES, 2 * LANES), f32),
                pltpu.VMEM((2, 16, 64, LANES), f32), pltpu.VMEM((2, 16, 64, LANES), f32),
                pltpu.VMEM((16, 8, LANES), f32), pltpu.VMEM((16, 8, LANES), f32),
                pltpu.VMEM((2 * LANES, 2 * LANES), f32), pltpu.VMEM((2 * LANES, 2 * LANES), f32),
                pltpu.VMEM((8, LANES), f32), pltpu.VMEM((1, LANES), f32),
                pltpu.SMEM((LAYERS,), f32), pltpu.SMEM((LAYERS,), f32), dma((2,)), pltpu.SemaphoreType.REGULAR((2,)),
                dma((PAIRS,)), dma((2, PAIRS)), dma((2, PAIRS)), dma, dma,
                dma((2, 2, 2, 8)), dma((2, 2, 2, 8)),
                dma((8,)), dma((8,)),
            ],
            compiler_params=pltpu.CompilerParams(collective_id=0, has_side_effects=True),
            name='qaoa',
        )(cost_local.reshape(shape), gammas, betas)
        energy, state_re, state_im = pl.pallas_call(
            write_out,
            out_shape=(jax.ShapeDtypeStruct((1,), f32),
                       jax.ShapeDtypeStruct(shape, f32), jax.ShapeDtypeStruct(shape, f32)),
            in_specs=[vmem, vmem, vmem],
            out_specs=(hbm, hbm, hbm),
            scratch_shapes=[pltpu.SMEM((1,), f32), dma((3,))],
            name='write_out',
        )(*[pltpu.with_memory_space_constraint(value, pltpu.VMEM) for value in results])
        return energy, state_re.reshape(local_len), state_im.reshape(local_len)

    return jax.shard_map(device_body, mesh=mesh, in_specs=(state_spec, P(), P()),
                         out_specs=(P('inst'), state_spec, state_spec), check_vma=False)
```

```python
import jax
import jax.numpy as jnp
from jax import lax
from jax.experimental import pallas as pl
from jax.experimental.pallas import tpu as pltpu
from jax.sharding import PartitionSpec as P

LANES = 128
LAYERS = 8
SUB = 4
PER_SUB = 8 // SUB
SEND_ORDER = (5, 7, 4, 6, 1, 3, 2)
NEAR = (4, 1)


def rotate(re, im, cos_half, sin_half, steps=None):
    count = len(re)
    for step in steps or [1 << i for i in range(count.bit_length() - 1)]:
        new_re = [cos_half * re[i] + sin_half * im[i ^ step] for i in range(count)]
        new_im = [cos_half * im[i] - sin_half * re[i ^ step] for i in range(count)]
        re, im = new_re, new_im
    return re, im


def sublane_rotate(re, im, cos_half, sin_half):
    row = lax.broadcasted_iota(jnp.int32, (8, LANES), 0)
    for step in (1, 2, 4):
        bit_set = (row & step) != 0

        def flip(value):
            down = pltpu.roll(value, step, 0)
            if step == 4:
                return down
            return jnp.where(bit_set, down, pltpu.roll(value, 8 - step, 0))

        flip_re = [flip(value) for value in re]
        flip_im = [flip(value) for value in im]
        re, im = ([cos_half * r + sin_half * fi for r, fi in zip(re, flip_im)],
                  [cos_half * i - sin_half * fr for i, fr in zip(im, flip_re)])
    return re, im


def lane_matrix(cos_half, sin_half):
    row = lax.broadcasted_iota(jnp.int32, (LANES, LANES), 0)
    col = lax.broadcasted_iota(jnp.int32, (LANES, LANES), 1)
    diff = row ^ col
    cos_full = jnp.broadcast_to(cos_half[0:1], (LANES, LANES))
    sin_full = jnp.broadcast_to(sin_half[0:1], (LANES, LANES))
    mag = jnp.ones((LANES, LANES), jnp.float32)
    weight = jnp.zeros((LANES, LANES), jnp.int32)
    for bit in range(7):
        on = (diff >> bit) & 1
        mag = mag * jnp.where(on == 1, sin_full, cos_full)
        weight = weight + on
    quarter = weight & 3
    zero = jnp.zeros_like(mag)
    real = jnp.where(quarter == 0, mag, jnp.where(quarter == 2, -mag, zero))
    imag = jnp.where(quarter == 1, -mag, jnp.where(quarter == 3, mag, zero))
    return real, imag


def kernel(cost_hbm, gammas_hbm, betas_hbm, energy_all, out_re, out_im,
           cost, cost_near, cost_swap, recv, send, work, cos_buf, sin_buf, cos_near, sin_near,
           rows_in, matrix, energy_part, energy_row, gammas, betas, angle_in, near_in, cost_in, near_send, near_recv, cost_send, cost_recv,
           send_sem, recv_sem, e_send, e_recv):
    qx = lax.axis_index('qx')
    qy = lax.axis_index('qy')
    bits = (qy, qx % 2, qx // 2)

    def flipped(offset):
        return [1 - bit if (offset >> i) & 1 else bit for i, bit in enumerate(bits)]

    def block(offset):
        y, core, x = flipped(offset)
        return (x * 2 + core) * 2 + y

    def peer(offset):
        y, core, x = flipped(offset)
        return {'qy': y, 'qx': x * 2 + core}

    def remote(source, target, send_at, recv_at, offset):
        pltpu.make_async_remote_copy(
            src_ref=source, dst_ref=target, send_sem=send_at, recv_sem=recv_at,
            device_id=peer(offset), device_id_type=pl.DeviceIdType.MESH).start()

    barrier = pltpu.get_barrier_semaphore()

    def signal_next(sem):
        for offset in (4, 1, 2):
            pl.semaphore_signal(sem, inc=1, device_id=peer(offset), device_id_type=pl.DeviceIdType.MESH)

    signal_next(barrier)
    loads = [pltpu.make_async_copy(cost_hbm.at[:, :, :, pl.ds(sub * 8 * PER_SUB, 8 * PER_SUB)],
                                   cost.at[:, :, :, pl.ds(sub * 8 * PER_SUB, 8 * PER_SUB)], cost_in.at[sub])
             for sub in range(SUB)]
    for load in loads:
        load.start()
    angle_loads = [pltpu.make_async_copy(gammas_hbm, gammas, angle_in.at[0]),
                   pltpu.make_async_copy(betas_hbm, betas, angle_in.at[1])]
    for load in angle_loads:
        load.start()
    pl.semaphore_wait(barrier, 3)

    def half_angle(layer):
        angle = jnp.full((8, LANES), 0.5 * betas[layer], jnp.float32)
        return jnp.cos(angle), jnp.sin(angle)

    def wait_bytes(part, sem):
        pltpu.make_async_copy(part, part, sem).wait()

    def wait_all(buffer, sem, at, count):
        wait_bytes(buffer.at[(*at, pl.ds(0, count))], sem.at[at])

    def rows_of(r):
        return pl.ds(pl.multiple_of(r * 8, 8), 8)

    def set_matrix(cos_half, sin_half):
        real, imag = lane_matrix(cos_half, sin_half)
        matrix[0:LANES, 0:LANES] = real
        matrix[0:LANES, LANES:] = imag
        matrix[LANES:, 0:LANES] = -imag
        matrix[LANES:, LANES:] = real

    def put_rows(i, re, im, base=0):
        for o in range(16):
            at = pl.multiple_of(base + o * 16 + i * 8, 8)
            rows_in[pl.ds(at, 8), 0:LANES] = re[o]
            rows_in[pl.ds(at, 8), LANES:] = im[o]

    def lanes(count):
        return lax.dot(rows_in[0:count, :], matrix[...],
                       precision=lax.Precision.HIGHEST, preferred_element_type=jnp.float32)

    def emit(held, mixed, target, a, b, cos_half, sin_half, order, route, local):
        def across(o, buffer):
            def part(r, c):
                at = pl.multiple_of((mixed * 8 + o) * 16 + (r % 2) * 8, 8)
                return work[held, r // 2, pl.ds(at, 8), c * LANES:(c + 1) * LANES]

            re = [part(r, 0) for r in range(8)]
            im = [part(r, 1) for r in range(8)]
            re, im = rotate(re, im, cos_half, sin_half)
            for r in range(8):
                row = (r % PER_SUB) * 8
                buffer[target, a, b, r // PER_SUB, o, 0, row:row + 8, :] = re[r]
                buffer[target, a, b, r // PER_SUB, o, 1, row:row + 8, :] = im[r]

        def body(o, carry):
            across(o, send)
            return carry

        lax.fori_loop(1, 8, body, 0)
        for o in local:
            across(o, recv)
        for sub in range(SUB):
            at = (target, a, b, sub)
            for o in order:
                remote(send.at[(*at, o)], recv.at[(*at, o)], send_sem.at[at], recv_sem.at[at], route(o))

    def first_layer():
        def sub_rows(sub):
            return pl.ds(pl.multiple_of(sub * 8 * PER_SUB, 8), 8 * PER_SUB)

        for sub in range(SUB):
            loads[sub].wait()
            for a in range(2):
                remote(cost.at[:, a, :, sub_rows(sub)], cost_near.at[:, a, :, sub_rows(sub)],
                       near_send.at[a, sub], near_recv.at[a, sub], NEAR[a])
        signal_next(near_in.at[0])
        for load in angle_loads:
            load.wait()
        gamma = gammas[0]
        cos_half, sin_half = half_angle(0)
        set_matrix(cos_half, sin_half)

        def own_trig(r, carry):
            for a in range(2):
                for b in range(2):
                    for o in range(8):
                        angle = gamma * cost[block(o), a, b, rows_of(r), :]
                        cos_buf[a, b * 8 + o, rows_of(r), :] = jnp.cos(angle)
                        sin_buf[a, b * 8 + o, rows_of(r), :] = jnp.sin(angle)
            return carry

        for round_id in range(2):
            lax.fori_loop(4 * round_id, 4 * round_id + 4, own_trig, 0)
            pl.semaphore_wait(near_in.at[round_id], 3)
            if round_id == 0:
                signal_next(near_in.at[1])
        for a in range(2):
            for o in range(1, 8):
                if not o & NEAR[a]:
                    remote(cost.at[block(o), a], cost_swap.at[o, a], cost_send, cost_recv, o)

        def sub_step(sub, carry):
            for a in range(2):
                bit = NEAR[a]
                part = cost_near.at[:, a, :, sub_rows(sub)]
                wait_bytes(part, near_recv.at[a, sub])
                for o in range(1, 8):
                    if not o & bit:
                        remote(cost_near.at[block(o), a, :, sub_rows(sub)],
                               cost_swap.at[o | bit, a, :, sub_rows(sub)], cost_send, cost_recv, o)

                def slots(i, carry):
                    r = sub * PER_SUB + i
                    for b in range(2):
                        for o in range(8):
                            angle = gamma * cost_near[block(o), a, b, rows_of(r), :]
                            cos_near[b * 8 + o] = jnp.cos(angle)
                            sin_near[b * 8 + o] = jnp.sin(angle)
                    re, im = [None] * 16, [None] * 16
                    for b in range(2):
                        for o in range(8):
                            if o & bit:
                                continue
                            here, there = b * 8 + o, b * 8 + (o | bit)
                            for slot, cos_at, sin_at in (
                                    (here, lambda k: cos_buf[a, k, rows_of(r), :], lambda k: sin_buf[a, k, rows_of(r), :]),
                                    (there, lambda k: cos_near[k], lambda k: sin_near[k])):
                                re[slot] = cos_half * cos_at(here) - sin_half * sin_at(there)
                                im[slot] = -(cos_half * sin_at(here)) - sin_half * cos_at(there)
                    re, im = rotate(re, im, cos_half, sin_half, [step for step in (1, 2, 4, 8) if step != bit])
                    re, im = sublane_rotate(re, im, cos_half, sin_half)
                    put_rows(i, re, im, a * 2 * LANES)
                    return carry

                lax.fori_loop(0, PER_SUB, slots, 0)
            rows = lanes(4 * LANES)
            for a in range(2):
                work[a, sub] = rows[a * 2 * LANES:(a + 1) * 2 * LANES]
            return carry

        lax.fori_loop(0, SUB, sub_step, 0)

        def quarters(b, carry):
            for a in range(2):
                bit = NEAR[a]
                emit(a, b, 1, a, b, cos_half, sin_half,
                     [o for o in (3, 6, 7, 1, 4, 5, 2) if o & ~bit], lambda o: o & ~bit, (0, bit))
            return carry

        lax.fori_loop(0, 2, quarters, 0)
        cost_swap[0] = cost[block(0)]
        for a in range(2):
            cost_swap[NEAR[a], a] = cost_near[block(0), a]
        wait_bytes(cost_swap.at[pl.ds(0, 6)], cost_recv)

    def run_layer(layer, odd, arrived, drained):
        source, target = (0, 1) if odd else (1, 0)

        def quarter(held, mixed):
            return (held, mixed) if odd else (mixed, held)

        cos_half, sin_half = half_angle(layer)
        cos_prev, sin_prev = half_angle(layer - 1)
        gamma = gammas[layer]
        set_matrix(cos_half, sin_half)

        def half(held, carry):
            def trig(r, carry):
                for mixed in range(2):
                    for o in range(8):
                        at = (block(o) if odd else o, *quarter(held, mixed), rows_of(r))
                        angle = gamma * (cost if odd else cost_swap)[at]
                        cos_buf[held, mixed * 8 + o, rows_of(r), :] = jnp.cos(angle)
                        sin_buf[held, mixed * 8 + o, rows_of(r), :] = jnp.sin(angle)
                return carry

            lax.fori_loop(0, 8, trig, 0)

            def sub_step(sub, carry):
                for mixed in range(2):
                    wait_all(recv, recv_sem, (source, *quarter(held, mixed), sub), arrived)

                def slots(i, carry):
                    r = sub * PER_SUB + i
                    cos_phase = [cos_buf[held, o, rows_of(r), :] for o in range(16)]
                    sin_phase = [sin_buf[held, o, rows_of(r), :] for o in range(16)]
                    old = [[recv[(source, *quarter(held, mixed), sub, o, c, rows_of(i))]
                            for mixed in range(2) for o in range(8)] for c in range(2)]
                    old_re, old_im = rotate(*old, cos_prev, sin_prev)
                    re = [r * c + i * s for r, i, c, s in zip(old_re, old_im, cos_phase, sin_phase)]
                    im = [i * c - r * s for r, i, c, s in zip(old_re, old_im, cos_phase, sin_phase)]
                    re, im = rotate(re, im, cos_half, sin_half)
                    re, im = sublane_rotate(re, im, cos_half, sin_half)
                    put_rows(i, re, im)
                    return carry

                lax.fori_loop(0, PER_SUB, slots, 0)
                work[held, sub] = lanes(2 * LANES)
                return carry

            lax.fori_loop(0, SUB, sub_step, 0)

            if drained:
                for mixed in range(2):
                    for sub in range(SUB):
                        wait_all(send, send_sem, (target, *quarter(held, mixed), sub), drained)

            def quarters(mixed, carry):
                emit(held, mixed, target, *quarter(held, mixed), cos_half, sin_half, SEND_ORDER, lambda o: o, (0,))
                return carry

            lax.fori_loop(0, 2, quarters, 0)
            return carry

        lax.fori_loop(0, 2, half, 0)

    first_layer()
    run_layer(1, False, 6, 0)
    run_layer(2, True, 7, 6)

    def layer_pair(i, carry):
        run_layer(2 * i + 3, False, 7, 7)
        run_layer(2 * i + 4, True, 7, 7)
        return carry

    lax.fori_loop(0, LAYERS // 2 - 2, layer_pair, 0)
    run_layer(LAYERS - 1, False, 7, 7)

    cos_half, sin_half = half_angle(LAYERS - 1)
    energy_part[...] = jnp.zeros((8, LANES), jnp.float32)

    def final_half(a, carry):
        def final_sub(sub, carry):
            for b in range(2):
                wait_all(recv, recv_sem, (0, a, b, sub), 7)

            def slots(i, carry):
                r = sub * PER_SUB + i
                old = [[recv[0, a, b, sub, o, c, rows_of(i), :] for b in range(2) for o in range(8)]
                       for c in range(2)]
                re, im = rotate(*old, cos_half, sin_half)
                total = energy_part[...]
                for b in range(2):
                    for o in range(8):
                        at = (block(o), a, b, rows_of(r))
                        x, y = re[b * 8 + o], im[b * 8 + o]
                        out_re[at] = x
                        out_im[at] = y
                        total = total + cost[at] * (x * x + y * y)
                energy_part[...] = total
                return carry

            lax.fori_loop(0, PER_SUB, slots, 0)
            return carry

        lax.fori_loop(0, SUB, final_sub, 0)
        return carry

    lax.fori_loop(0, 2, final_half, 0)

    me = block(0)
    energy_row[...] = jnp.sum(energy_part[...], axis=0, keepdims=True)
    for offset in range(1, 8):
        remote(energy_row, energy_all.at[me], e_send.at[offset], e_recv.at[offset], offset)
    energy_all[me] = energy_row[...]
    for par in range(2):
        for a in range(2):
            for b in range(2):
                for sub in range(SUB):
                    wait_all(send, send_sem, (par, a, b, sub), 7)
    for a in range(2):
        for sub in range(SUB):
            wait_bytes(cost.at[:, a, :, pl.ds(sub * 8 * PER_SUB, 8 * PER_SUB)], near_send.at[a, sub])
    wait_bytes(cost_swap.at[pl.ds(0, 6)], cost_send)
    for offset in range(1, 8):
        wait_bytes(energy_row, e_send.at[offset])
        wait_bytes(energy_row, e_recv.at[offset])


def write_out(energy_all, in_re, in_im, energy, out_re, out_im, value, sem):
    copies = [pltpu.make_async_copy(in_re, out_re, sem.at[0]), pltpu.make_async_copy(in_im, out_im, sem.at[1])]
    for copy in copies:
        copy.start()
    total = energy_all[0]
    for i in range(1, 8):
        total = total + energy_all[i]
    value[0] = jnp.sum(total) * (1.0 / (1 << 21))
    copies.append(pltpu.make_async_copy(value, energy, sem.at[2]))
    copies[2].start()
    for copy in copies:
        copy.wait()


def solution(mesh):
    state_spec = P(('inst', 'qx', 'qy'))

    def device_body(cost_local, gammas, betas):
        local_len = cost_local.shape[0]
        shape = (8, 2, 2, local_len // (32 * LANES), LANES)
        f32 = jnp.float32
        vmem = pl.BlockSpec(memory_space=pltpu.VMEM)
        dma = pltpu.SemaphoreType.DMA
        parts = (2, 2, 2, SUB, 8, 2, 8 * PER_SUB, LANES)
        hbm = pl.BlockSpec(memory_space=pl.ANY)
        results = pl.pallas_call(
            kernel,
            out_shape=(pltpu.VMEM((8, 1, LANES), f32), pltpu.VMEM(shape, f32), pltpu.VMEM(shape, f32)),
            in_specs=[hbm, hbm, hbm],
            out_specs=(vmem, vmem, vmem),
            scratch_shapes=[
                pltpu.VMEM(shape, f32), pltpu.VMEM(shape, f32), pltpu.VMEM(shape, f32),
                pltpu.VMEM(parts, f32), pltpu.VMEM(parts, f32),
                pltpu.VMEM((2, 4, 2 * LANES, 2 * LANES), f32),
                pltpu.VMEM((2, 16, 64, LANES), f32), pltpu.VMEM((2, 16, 64, LANES), f32),
                pltpu.VMEM((16, 8, LANES), f32), pltpu.VMEM((16, 8, LANES), f32),
                pltpu.VMEM((4 * LANES, 2 * LANES), f32), pltpu.VMEM((2 * LANES, 2 * LANES), f32),
                pltpu.VMEM((8, LANES), f32), pltpu.VMEM((1, LANES), f32),
                pltpu.SMEM((LAYERS,), f32), pltpu.SMEM((LAYERS,), f32), dma((2,)), pltpu.SemaphoreType.REGULAR((2,)),
                dma((SUB,)), dma((2, SUB)), dma((2, SUB)), dma, dma,
                dma((2, 2, 2, SUB)), dma((2, 2, 2, SUB)),
                dma((8,)), dma((8,)),
            ],
            compiler_params=pltpu.CompilerParams(collective_id=0, has_side_effects=True),
            name='qaoa',
        )(cost_local.reshape(shape), gammas, betas)
        energy, state_re, state_im = pl.pallas_call(
            write_out,
            out_shape=(jax.ShapeDtypeStruct((1,), f32),
                       jax.ShapeDtypeStruct(shape, f32), jax.ShapeDtypeStruct(shape, f32)),
            in_specs=[vmem, vmem, vmem],
            out_specs=(hbm, hbm, hbm),
            scratch_shapes=[pltpu.SMEM((1,), f32), dma((3,))],
            name='write_out',
        )(*[pltpu.with_memory_space_constraint(value, pltpu.VMEM) for value in results])
        return energy, state_re.reshape(local_len), state_im.reshape(local_len)

    return jax.shard_map(device_body, mesh=mesh, in_specs=(state_spec, P(), P()),
                         out_specs=(P('inst'), state_spec, state_spec), check_vma=False)
```

```python
import jax
import jax.numpy as jnp
from jax import lax
from jax.experimental import pallas as pl
from jax.experimental.pallas import tpu as pltpu
from jax.sharding import PartitionSpec as P

LANES = 128
LAYERS = 8
SUB = 4
PER_SUB = 8 // SUB
SEND_ORDER = (5, 7, 4, 6, 1, 3, 2)
NEAR = (4, 1)


def rotate(re, im, cos_half, sin_half, steps=None):
    count = len(re)
    for step in steps or [1 << i for i in range(count.bit_length() - 1)]:
        new_re = [cos_half * re[i] + sin_half * im[i ^ step] for i in range(count)]
        new_im = [cos_half * im[i] - sin_half * re[i ^ step] for i in range(count)]
        re, im = new_re, new_im
    return re, im


def sublane_rotate(re, im, cos_half, sin_half):
    row = lax.broadcasted_iota(jnp.int32, (8, LANES), 0)
    for step in (1, 2, 4):
        bit_set = (row & step) != 0

        def flip(value):
            down = pltpu.roll(value, step, 0)
            if step == 4:
                return down
            return jnp.where(bit_set, down, pltpu.roll(value, 8 - step, 0))

        flip_re = [flip(value) for value in re]
        flip_im = [flip(value) for value in im]
        re, im = ([cos_half * r + sin_half * fi for r, fi in zip(re, flip_im)],
                  [cos_half * i - sin_half * fr for i, fr in zip(im, flip_re)])
    return re, im


def lane_matrix(cos_half, sin_half):
    row = lax.broadcasted_iota(jnp.int32, (LANES, LANES), 0)
    col = lax.broadcasted_iota(jnp.int32, (LANES, LANES), 1)
    diff = row ^ col
    cos_full = jnp.broadcast_to(cos_half[0:1], (LANES, LANES))
    sin_full = jnp.broadcast_to(sin_half[0:1], (LANES, LANES))
    mag = jnp.ones((LANES, LANES), jnp.float32)
    weight = jnp.zeros((LANES, LANES), jnp.int32)
    for bit in range(7):
        on = (diff >> bit) & 1
        mag = mag * jnp.where(on == 1, sin_full, cos_full)
        weight = weight + on
    quarter = weight & 3
    zero = jnp.zeros_like(mag)
    real = jnp.where(quarter == 0, mag, jnp.where(quarter == 2, -mag, zero))
    imag = jnp.where(quarter == 1, -mag, jnp.where(quarter == 3, mag, zero))
    return real, imag


def kernel(cost_hbm, gammas_hbm, betas_hbm, energy_all, out_re, out_im,
           cost, cost_near, cost_swap, recv, send, work, cos_buf, sin_buf, cos_near, sin_near,
           rows_in, matrix, energy_part, energy_row, gammas, betas, angle_in, near_in, cost_in, near_send, near_recv, cost_send, cost_recv,
           send_sem, recv_sem, e_send, e_recv):
    qx = lax.axis_index('qx')
    qy = lax.axis_index('qy')
    bits = (qy, qx % 2, qx // 2)

    def flipped(offset):
        return [1 - bit if (offset >> i) & 1 else bit for i, bit in enumerate(bits)]

    def block(offset):
        y, core, x = flipped(offset)
        return (x * 2 + core) * 2 + y

    def peer(offset):
        y, core, x = flipped(offset)
        return {'qy': y, 'qx': x * 2 + core}

    def remote(source, target, send_at, recv_at, offset):
        pltpu.make_async_remote_copy(
            src_ref=source, dst_ref=target, send_sem=send_at, recv_sem=recv_at,
            device_id=peer(offset), device_id_type=pl.DeviceIdType.MESH).start()

    barrier = pltpu.get_barrier_semaphore()

    def signal_next(sem):
        for offset in (4, 1, 2):
            pl.semaphore_signal(sem, inc=1, device_id=peer(offset), device_id_type=pl.DeviceIdType.MESH)

    signal_next(barrier)
    loads = [pltpu.make_async_copy(cost_hbm.at[:, :, :, pl.ds(sub * 8 * PER_SUB, 8 * PER_SUB)],
                                   cost.at[:, :, :, pl.ds(sub * 8 * PER_SUB, 8 * PER_SUB)], cost_in.at[sub])
             for sub in range(SUB)]
    for load in loads:
        load.start()
    angle_loads = [pltpu.make_async_copy(gammas_hbm, gammas, angle_in.at[0]),
                   pltpu.make_async_copy(betas_hbm, betas, angle_in.at[1])]
    for load in angle_loads:
        load.start()
    pl.semaphore_wait(barrier, 3)

    def half_angle(layer):
        angle = jnp.full((8, LANES), 0.5 * betas[layer], jnp.float32)
        return jnp.cos(angle), jnp.sin(angle)

    def wait_bytes(part, sem):
        pltpu.make_async_copy(part, part, sem).wait()

    def wait_all(buffer, sem, at, count):
        wait_bytes(buffer.at[(*at, pl.ds(0, count))], sem.at[at])

    def rows_of(r):
        return pl.ds(pl.multiple_of(r * 8, 8), 8)

    def set_matrix(cos_half, sin_half):
        real, imag = lane_matrix(cos_half, sin_half)
        matrix[0:LANES, 0:LANES] = real
        matrix[0:LANES, LANES:] = imag
        matrix[LANES:, 0:LANES] = -imag
        matrix[LANES:, LANES:] = real

    def put_rows(i, re, im, base=0):
        for o in range(16):
            at = pl.multiple_of(base + o * 16 + i * 8, 8)
            rows_in[pl.ds(at, 8), 0:LANES] = re[o]
            rows_in[pl.ds(at, 8), LANES:] = im[o]

    def lanes(count):
        return lax.dot(rows_in[0:count, :], matrix[...],
                       precision=lax.Precision.HIGHEST, preferred_element_type=jnp.float32)

    def emit(held, mixed, target, a, b, cos_half, sin_half, order, route, local):
        def across(o, buffer):
            def part(r, c):
                at = pl.multiple_of((mixed * 8 + o) * 16 + (r % 2) * 8, 8)
                return work[held, r // 2, pl.ds(at, 8), c * LANES:(c + 1) * LANES]

            re = [part(r, 0) for r in range(8)]
            im = [part(r, 1) for r in range(8)]
            re, im = rotate(re, im, cos_half, sin_half)
            for r in range(8):
                row = (r % PER_SUB) * 8
                buffer[target, a, b, r // PER_SUB, o, 0, row:row + 8, :] = re[r]
                buffer[target, a, b, r // PER_SUB, o, 1, row:row + 8, :] = im[r]

        def body(o, carry):
            across(o, send)
            return carry

        lax.fori_loop(1, 8, body, 0)
        for o in local:
            across(o, recv)
        for sub in range(SUB):
            at = (target, a, b, sub)
            for o in order:
                remote(send.at[(*at, o)], recv.at[(*at, o)], send_sem.at[at], recv_sem.at[at], route(o))

    def first_layer():
        def sub_rows(sub):
            return pl.ds(pl.multiple_of(sub * 8 * PER_SUB, 8), 8 * PER_SUB)

        for sub in range(SUB):
            loads[sub].wait()
            for a in range(2):
                remote(cost.at[:, a, :, sub_rows(sub)], cost_near.at[:, a, :, sub_rows(sub)],
                       near_send.at[a, sub], near_recv.at[a, sub], NEAR[a])
        signal_next(near_in.at[0])
        for load in angle_loads:
            load.wait()
        gamma = gammas[0]
        cos_half, sin_half = half_angle(0)
        set_matrix(cos_half, sin_half)

        def own_trig(r, carry):
            for a in range(2):
                for b in range(2):
                    for o in range(8):
                        angle = gamma * cost[block(o), a, b, rows_of(r), :]
                        cos_buf[a, b * 8 + o, rows_of(r), :] = jnp.cos(angle)
                        sin_buf[a, b * 8 + o, rows_of(r), :] = jnp.sin(angle)
            return carry

        for round_id in range(2):
            lax.fori_loop(4 * round_id, 4 * round_id + 4, own_trig, 0)
            pl.semaphore_wait(near_in.at[round_id], 3)
            if round_id == 0:
                signal_next(near_in.at[1])
        for a in range(2):
            for o in range(1, 8):
                if not o & NEAR[a]:
                    remote(cost.at[block(o), a], cost_swap.at[o, a], cost_send, cost_recv, o)

        def sub_step(sub, carry):
            for a in range(2):
                bit = NEAR[a]
                part = cost_near.at[:, a, :, sub_rows(sub)]
                wait_bytes(part, near_recv.at[a, sub])
                for o in range(1, 8):
                    if not o & bit:
                        remote(cost_near.at[block(o), a, :, sub_rows(sub)],
                               cost_swap.at[o | bit, a, :, sub_rows(sub)], cost_send, cost_recv, o)

                def slots(i, carry):
                    r = sub * PER_SUB + i
                    for b in range(2):
                        for o in range(8):
                            angle = gamma * cost_near[block(o), a, b, rows_of(r), :]
                            cos_near[b * 8 + o] = jnp.cos(angle)
                            sin_near[b * 8 + o] = jnp.sin(angle)
                    re, im = [None] * 16, [None] * 16
                    for b in range(2):
                        for o in range(8):
                            if o & bit:
                                continue
                            here, there = b * 8 + o, b * 8 + (o | bit)
                            for slot, cos_at, sin_at in (
                                    (here, lambda k: cos_buf[a, k, rows_of(r), :], lambda k: sin_buf[a, k, rows_of(r), :]),
                                    (there, lambda k: cos_near[k], lambda k: sin_near[k])):
                                re[slot] = cos_half * cos_at(here) - sin_half * sin_at(there)
                                im[slot] = -(cos_half * sin_at(here)) - sin_half * cos_at(there)
                    re, im = rotate(re, im, cos_half, sin_half, [step for step in (1, 2, 4, 8) if step != bit])
                    re, im = sublane_rotate(re, im, cos_half, sin_half)
                    put_rows(i, re, im, a * 2 * LANES)
                    return carry

                lax.fori_loop(0, PER_SUB, slots, 0)
            rows = lanes(4 * LANES)
            for a in range(2):
                work[a, sub] = rows[a * 2 * LANES:(a + 1) * 2 * LANES]
            return carry

        lax.fori_loop(0, SUB, sub_step, 0)

        def quarters(b, carry):
            for a in range(2):
                bit = NEAR[a]
                emit(a, b, 1, a, b, cos_half, sin_half,
                     [o for o in (3, 6, 7, 1, 4, 5, 2) if o & ~bit], lambda o: o & ~bit, (0, bit))
            return carry

        lax.fori_loop(0, 2, quarters, 0)
        cost_swap[0] = cost[block(0)]
        for a in range(2):
            cost_swap[NEAR[a], a] = cost_near[block(0), a]
        wait_bytes(cost_swap.at[pl.ds(0, 6)], cost_recv)

    def run_layer(layer, odd, arrived, drained):
        source, target = (0, 1) if odd else (1, 0)

        def quarter(held, mixed):
            return (held, mixed) if odd else (mixed, held)

        cos_half, sin_half = half_angle(layer)
        cos_prev, sin_prev = half_angle(layer - 1)
        gamma = gammas[layer]
        set_matrix(cos_half, sin_half)

        def half(held, carry):
            def trig(r, carry):
                for mixed in range(2):
                    for o in range(8):
                        at = (block(o) if odd else o, *quarter(held, mixed), rows_of(r))
                        angle = gamma * (cost if odd else cost_swap)[at]
                        cos_buf[held, mixed * 8 + o, rows_of(r), :] = jnp.cos(angle)
                        sin_buf[held, mixed * 8 + o, rows_of(r), :] = jnp.sin(angle)
                return carry

            lax.fori_loop(0, 8, trig, 0)

            def sub_step(sub, carry):
                for mixed in range(2):
                    wait_all(recv, recv_sem, (source, *quarter(held, mixed), sub), arrived)

                def slots(i, carry):
                    r = sub * PER_SUB + i
                    cos_phase = [cos_buf[held, o, rows_of(r), :] for o in range(16)]
                    sin_phase = [sin_buf[held, o, rows_of(r), :] for o in range(16)]
                    old = [[recv[(source, *quarter(held, mixed), sub, o, c, rows_of(i))]
                            for mixed in range(2) for o in range(8)] for c in range(2)]
                    old_re, old_im = rotate(*old, cos_prev, sin_prev)
                    re = [r * c + i * s for r, i, c, s in zip(old_re, old_im, cos_phase, sin_phase)]
                    im = [i * c - r * s for r, i, c, s in zip(old_re, old_im, cos_phase, sin_phase)]
                    re, im = rotate(re, im, cos_half, sin_half)
                    re, im = sublane_rotate(re, im, cos_half, sin_half)
                    put_rows(i, re, im)
                    return carry

                lax.fori_loop(0, PER_SUB, slots, 0)
                work[held, sub] = lanes(2 * LANES)
                return carry

            lax.fori_loop(0, SUB, sub_step, 0)

            if drained:
                for mixed in range(2):
                    for sub in range(SUB):
                        wait_all(send, send_sem, (target, *quarter(held, mixed), sub), drained)

            def quarters(mixed, carry):
                emit(held, mixed, target, *quarter(held, mixed), cos_half, sin_half, SEND_ORDER, lambda o: o, (0,))
                return carry

            lax.fori_loop(0, 2, quarters, 0)
            return carry

        lax.fori_loop(0, 2, half, 0)

    first_layer()
    run_layer(1, False, 6, 0)
    run_layer(2, True, 7, 6)

    def layer_pair(i, carry):
        run_layer(2 * i + 3, False, 7, 7)
        run_layer(2 * i + 4, True, 7, 7)
        return carry

    lax.fori_loop(0, LAYERS // 2 - 2, layer_pair, 0)
    run_layer(LAYERS - 1, False, 7, 7)

    cos_half, sin_half = half_angle(LAYERS - 1)
    energy_part[...] = jnp.zeros((8, LANES), jnp.float32)

    def final_half(a, carry):
        def final_sub(sub, carry):
            for b in range(2):
                wait_all(recv, recv_sem, (0, a, b, sub), 7)

            def slots(i, carry):
                r = sub * PER_SUB + i
                old = [[recv[0, a, b, sub, o, c, rows_of(i), :] for b in range(2) for o in range(8)]
                       for c in range(2)]
                re, im = rotate(*old, cos_half, sin_half)
                total = energy_part[...]
                for b in range(2):
                    for o in range(8):
                        at = (block(o), a, b, rows_of(r))
                        x, y = re[b * 8 + o], im[b * 8 + o]
                        out_re[at] = x
                        out_im[at] = y
                        total = total + cost[at] * (x * x + y * y)
                energy_part[...] = total
                return carry

            lax.fori_loop(0, PER_SUB, slots, 0)
            return carry

        lax.fori_loop(0, SUB, final_sub, 0)
        return carry

    lax.fori_loop(0, 2, final_half, 0)

    me = block(0)
    energy_row[...] = jnp.sum(energy_part[...], axis=0, keepdims=True)
    energy_all[me] = energy_row[...]

    def drain(par):
        for a in range(2):
            for b in range(2):
                for sub in range(SUB):
                    wait_all(send, send_sem, (par, a, b, sub), 7)

    drain(1)
    for a in range(2):
        for sub in range(SUB):
            wait_bytes(cost.at[:, a, :, pl.ds(sub * 8 * PER_SUB, 8 * PER_SUB)], near_send.at[a, sub])
    wait_bytes(cost_swap.at[pl.ds(0, 6)], cost_send)
    for offset in range(1, 8):
        remote(energy_row, energy_all.at[me], e_send.at[offset], e_recv.at[offset], offset)
    drain(0)
    for offset in range(1, 8):
        wait_bytes(energy_row, e_send.at[offset])
        wait_bytes(energy_row, e_recv.at[offset])


def write_out(energy_all, in_re, in_im, energy, out_re, out_im, value, sem):
    copies = [pltpu.make_async_copy(in_re, out_re, sem.at[0]), pltpu.make_async_copy(in_im, out_im, sem.at[1])]
    for copy in copies:
        copy.start()
    total = energy_all[0]
    for i in range(1, 8):
        total = total + energy_all[i]
    value[0] = jnp.sum(total) * (1.0 / (1 << 21))
    copies.append(pltpu.make_async_copy(value, energy, sem.at[2]))
    copies[2].start()
    for copy in copies:
        copy.wait()


def solution(mesh):
    state_spec = P(('inst', 'qx', 'qy'))

    def device_body(cost_local, gammas, betas):
        local_len = cost_local.shape[0]
        shape = (8, 2, 2, local_len // (32 * LANES), LANES)
        f32 = jnp.float32
        vmem = pl.BlockSpec(memory_space=pltpu.VMEM)
        dma = pltpu.SemaphoreType.DMA
        parts = (2, 2, 2, SUB, 8, 2, 8 * PER_SUB, LANES)
        hbm = pl.BlockSpec(memory_space=pl.ANY)
        results = pl.pallas_call(
            kernel,
            out_shape=(pltpu.VMEM((8, 1, LANES), f32), pltpu.VMEM(shape, f32), pltpu.VMEM(shape, f32)),
            in_specs=[hbm, hbm, hbm],
            out_specs=(vmem, vmem, vmem),
            scratch_shapes=[
                pltpu.VMEM(shape, f32), pltpu.VMEM(shape, f32), pltpu.VMEM(shape, f32),
                pltpu.VMEM(parts, f32), pltpu.VMEM(parts, f32),
                pltpu.VMEM((2, 4, 2 * LANES, 2 * LANES), f32),
                pltpu.VMEM((2, 16, 64, LANES), f32), pltpu.VMEM((2, 16, 64, LANES), f32),
                pltpu.VMEM((16, 8, LANES), f32), pltpu.VMEM((16, 8, LANES), f32),
                pltpu.VMEM((4 * LANES, 2 * LANES), f32), pltpu.VMEM((2 * LANES, 2 * LANES), f32),
                pltpu.VMEM((8, LANES), f32), pltpu.VMEM((1, LANES), f32),
                pltpu.SMEM((LAYERS,), f32), pltpu.SMEM((LAYERS,), f32), dma((2,)), pltpu.SemaphoreType.REGULAR((2,)),
                dma((SUB,)), dma((2, SUB)), dma((2, SUB)), dma, dma,
                dma((2, 2, 2, SUB)), dma((2, 2, 2, SUB)),
                dma((8,)), dma((8,)),
            ],
            compiler_params=pltpu.CompilerParams(collective_id=0, has_side_effects=True),
            name='qaoa',
        )(cost_local.reshape(shape), gammas, betas)
        energy, state_re, state_im = pl.pallas_call(
            write_out,
            out_shape=(jax.ShapeDtypeStruct((1,), f32),
                       jax.ShapeDtypeStruct(shape, f32), jax.ShapeDtypeStruct(shape, f32)),
            in_specs=[vmem, vmem, vmem],
            out_specs=(hbm, hbm, hbm),
            scratch_shapes=[pltpu.SMEM((1,), f32), dma((3,))],
            name='write_out',
        )(*[pltpu.with_memory_space_constraint(value, pltpu.VMEM) for value in results])
        return energy, state_re.reshape(local_len), state_im.reshape(local_len)

    return jax.shard_map(device_body, mesh=mesh, in_specs=(state_spec, P(), P()),
                         out_specs=(P('inst'), state_spec, state_spec), check_vma=False)
```

```python
import jax
import jax.numpy as jnp
from jax import lax
from jax.experimental import pallas as pl
from jax.experimental.pallas import tpu as pltpu
from jax.sharding import PartitionSpec as P

LANES = 128
LAYERS = 8
SUB = 4
PER_SUB = 8 // SUB
SEND_ORDER = (5, 7, 4, 6, 1, 3, 2)
NEAR = (4, 1)


def rotate(re, im, cos_half, sin_half, steps=None):
    count = len(re)
    for step in steps or [1 << i for i in range(count.bit_length() - 1)]:
        new_re = [cos_half * re[i] + sin_half * im[i ^ step] for i in range(count)]
        new_im = [cos_half * im[i] - sin_half * re[i ^ step] for i in range(count)]
        re, im = new_re, new_im
    return re, im


def sublane_rotate(re, im, cos_half, sin_half):
    row = lax.broadcasted_iota(jnp.int32, (8, LANES), 0)
    for step in (1, 2, 4):
        bit_set = (row & step) != 0

        def flip(value):
            down = pltpu.roll(value, step, 0)
            if step == 4:
                return down
            return jnp.where(bit_set, down, pltpu.roll(value, 8 - step, 0))

        flip_re = [flip(value) for value in re]
        flip_im = [flip(value) for value in im]
        re, im = ([cos_half * r + sin_half * fi for r, fi in zip(re, flip_im)],
                  [cos_half * i - sin_half * fr for i, fr in zip(im, flip_re)])
    return re, im


def lane_matrix(cos_half, sin_half):
    row = lax.broadcasted_iota(jnp.int32, (LANES, LANES), 0)
    col = lax.broadcasted_iota(jnp.int32, (LANES, LANES), 1)
    diff = row ^ col
    cos_full = jnp.broadcast_to(cos_half[0:1], (LANES, LANES))
    sin_full = jnp.broadcast_to(sin_half[0:1], (LANES, LANES))
    mag = jnp.ones((LANES, LANES), jnp.float32)
    weight = jnp.zeros((LANES, LANES), jnp.int32)
    for bit in range(7):
        on = (diff >> bit) & 1
        mag = mag * jnp.where(on == 1, sin_full, cos_full)
        weight = weight + on
    quarter = weight & 3
    zero = jnp.zeros_like(mag)
    real = jnp.where(quarter == 0, mag, jnp.where(quarter == 2, -mag, zero))
    imag = jnp.where(quarter == 1, -mag, jnp.where(quarter == 3, mag, zero))
    return real, imag


ENERGY_ORDER = (7, 5, 6, 4, 3, 1, 2)


def kernel(cost_hbm, gammas_hbm, betas_hbm, energy_all, out_re, out_im,
           cost, cost_near, cost_swap, recv, send, work, cos_buf, sin_buf, cos_near, sin_near,
           rows_in, matrix, energy_part, energy_row, gammas, betas, angle_in, near_in, cost_in, near_send, near_recv, cost_send, cost_recv,
           send_sem, recv_sem, e_send, e_recv):
    qx = lax.axis_index('qx')
    qy = lax.axis_index('qy')
    bits = (qy, qx % 2, qx // 2)

    def flipped(offset):
        return [1 - bit if (offset >> i) & 1 else bit for i, bit in enumerate(bits)]

    def block(offset):
        y, core, x = flipped(offset)
        return (x * 2 + core) * 2 + y

    def peer(offset):
        y, core, x = flipped(offset)
        return {'qy': y, 'qx': x * 2 + core}

    def remote(source, target, send_at, recv_at, offset):
        pltpu.make_async_remote_copy(
            src_ref=source, dst_ref=target, send_sem=send_at, recv_sem=recv_at,
            device_id=peer(offset), device_id_type=pl.DeviceIdType.MESH).start()

    barrier = pltpu.get_barrier_semaphore()

    def signal_next(sem):
        for offset in (4, 1, 2):
            pl.semaphore_signal(sem, inc=1, device_id=peer(offset), device_id_type=pl.DeviceIdType.MESH)

    signal_next(barrier)
    loads = [pltpu.make_async_copy(cost_hbm.at[:, :, :, pl.ds(sub * 8 * PER_SUB, 8 * PER_SUB)],
                                   cost.at[:, :, :, pl.ds(sub * 8 * PER_SUB, 8 * PER_SUB)], cost_in.at[sub])
             for sub in range(SUB)]
    for load in loads:
        load.start()
    angle_loads = [pltpu.make_async_copy(gammas_hbm, gammas, angle_in.at[0]),
                   pltpu.make_async_copy(betas_hbm, betas, angle_in.at[1])]
    for load in angle_loads:
        load.start()
    pl.semaphore_wait(barrier, 3)

    def half_angle(layer):
        angle = jnp.full((8, LANES), 0.5 * betas[layer], jnp.float32)
        return jnp.cos(angle), jnp.sin(angle)

    def wait_bytes(part, sem):
        pltpu.make_async_copy(part, part, sem).wait()

    def wait_all(buffer, sem, at, count):
        wait_bytes(buffer.at[(*at, pl.ds(0, count))], sem.at[at])

    def wait_last(buffer, sem, a, b, part):
        wait_bytes(buffer.at[0, a, b, 0, pl.ds(0, 7), :, pl.ds(0, 8)], sem.at[0, a, b, SUB - 1 + part])

    def rows_of(r):
        return pl.ds(pl.multiple_of(r * 8, 8), 8)

    def set_matrix(cos_half, sin_half):
        real, imag = lane_matrix(cos_half, sin_half)
        matrix[0:LANES, 0:LANES] = real
        matrix[0:LANES, LANES:] = imag
        matrix[LANES:, 0:LANES] = -imag
        matrix[LANES:, LANES:] = real

    def put_rows(i, re, im, base=0):
        for o in range(16):
            at = pl.multiple_of(base + o * 16 + i * 8, 8)
            rows_in[pl.ds(at, 8), 0:LANES] = re[o]
            rows_in[pl.ds(at, 8), LANES:] = im[o]

    def lanes(count):
        return lax.dot(rows_in[0:count, :], matrix[...],
                       precision=lax.Precision.HIGHEST, preferred_element_type=jnp.float32)

    def emit(held, mixed, target, a, b, cos_half, sin_half, order, route, local, last=False):
        def across(o, buffer):
            def part(r, c):
                at = pl.multiple_of((mixed * 8 + o) * 16 + (r % 2) * 8, 8)
                return work[held, r // 2, pl.ds(at, 8), c * LANES:(c + 1) * LANES]

            re = [part(r, 0) for r in range(8)]
            im = [part(r, 1) for r in range(8)]
            re, im = rotate(re, im, cos_half, sin_half)
            for r in range(8):
                row = (r % PER_SUB) * 8
                buffer[target, a, b, r // PER_SUB, o, 0, row:row + 8, :] = re[r]
                buffer[target, a, b, r // PER_SUB, o, 1, row:row + 8, :] = im[r]

        def body(o, carry):
            across(o, send)
            return carry

        lax.fori_loop(1, 8, body, 0)
        for o in local:
            across(o, recv)
        for sub in range(SUB - last):
            at = (target, a, b, sub)
            for o in order:
                remote(send.at[(*at, o)], recv.at[(*at, o)], send_sem.at[at], recv_sem.at[at], route(o))
        if last:
            for part in range(2):
                sem_at = (target, a, b, SUB - 1 + part)
                for o in order:
                    at = (target, a, b, SUB - 1, o, slice(None), pl.ds(8 * part, 8))
                    remote(send.at[at], recv.at[at], send_sem.at[sem_at], recv_sem.at[sem_at], route(o))

    def first_layer():
        def sub_rows(sub):
            return pl.ds(pl.multiple_of(sub * 8 * PER_SUB, 8), 8 * PER_SUB)

        for sub in range(SUB):
            loads[sub].wait()
            for a in range(2):
                remote(cost.at[:, a, :, sub_rows(sub)], cost_near.at[:, a, :, sub_rows(sub)],
                       near_send.at[a, sub], near_recv.at[a, sub], NEAR[a])
        signal_next(near_in.at[0])
        for load in angle_loads:
            load.wait()
        gamma = gammas[0]
        cos_half, sin_half = half_angle(0)
        set_matrix(cos_half, sin_half)

        def own_trig(r, carry):
            for a in range(2):
                for b in range(2):
                    for o in range(8):
                        angle = gamma * cost[block(o), a, b, rows_of(r), :]
                        cos_buf[a, b * 8 + o, rows_of(r), :] = jnp.cos(angle)
                        sin_buf[a, b * 8 + o, rows_of(r), :] = jnp.sin(angle)
            return carry

        for round_id in range(2):
            lax.fori_loop(4 * round_id, 4 * round_id + 4, own_trig, 0)
            pl.semaphore_wait(near_in.at[round_id], 3)
            if round_id == 0:
                signal_next(near_in.at[1])
        for a in range(2):
            for o in range(1, 8):
                if not o & NEAR[a]:
                    remote(cost.at[block(o), a], cost_swap.at[o, a], cost_send, cost_recv, o)

        def sub_step(sub, carry):
            for a in range(2):
                bit = NEAR[a]
                part = cost_near.at[:, a, :, sub_rows(sub)]
                wait_bytes(part, near_recv.at[a, sub])
                for o in range(1, 8):
                    if not o & bit:
                        remote(cost_near.at[block(o), a, :, sub_rows(sub)],
                               cost_swap.at[o | bit, a, :, sub_rows(sub)], cost_send, cost_recv, o)

                def slots(i, carry):
                    r = sub * PER_SUB + i
                    for b in range(2):
                        for o in range(8):
                            angle = gamma * cost_near[block(o), a, b, rows_of(r), :]
                            cos_near[b * 8 + o] = jnp.cos(angle)
                            sin_near[b * 8 + o] = jnp.sin(angle)
                    re, im = [None] * 16, [None] * 16
                    for b in range(2):
                        for o in range(8):
                            if o & bit:
                                continue
                            here, there = b * 8 + o, b * 8 + (o | bit)
                            for slot, cos_at, sin_at in (
                                    (here, lambda k: cos_buf[a, k, rows_of(r), :], lambda k: sin_buf[a, k, rows_of(r), :]),
                                    (there, lambda k: cos_near[k], lambda k: sin_near[k])):
                                re[slot] = cos_half * cos_at(here) - sin_half * sin_at(there)
                                im[slot] = -(cos_half * sin_at(here)) - sin_half * cos_at(there)
                    re, im = rotate(re, im, cos_half, sin_half, [step for step in (1, 2, 4, 8) if step != bit])
                    re, im = sublane_rotate(re, im, cos_half, sin_half)
                    put_rows(i, re, im, a * 2 * LANES)
                    return carry

                lax.fori_loop(0, PER_SUB, slots, 0)
            rows = lanes(4 * LANES)
            for a in range(2):
                work[a, sub] = rows[a * 2 * LANES:(a + 1) * 2 * LANES]
            return carry

        lax.fori_loop(0, SUB, sub_step, 0)

        def quarters(b, carry):
            for a in range(2):
                bit = NEAR[a]
                emit(a, b, 1, a, b, cos_half, sin_half,
                     [o for o in (3, 6, 7, 1, 4, 5, 2) if o & ~bit], lambda o: o & ~bit, (0, bit))
            return carry

        lax.fori_loop(0, 2, quarters, 0)
        cost_swap[0] = cost[block(0)]
        for a in range(2):
            cost_swap[NEAR[a], a] = cost_near[block(0), a]
        wait_bytes(cost_swap.at[pl.ds(0, 6)], cost_recv)

    def run_layer(layer, odd, arrived, drained, last=False):
        source, target = (0, 1) if odd else (1, 0)

        def quarter(held, mixed):
            return (held, mixed) if odd else (mixed, held)

        cos_half, sin_half = half_angle(layer)
        cos_prev, sin_prev = half_angle(layer - 1)
        gamma = gammas[layer]
        set_matrix(cos_half, sin_half)

        def half(held, carry):
            def trig(r, carry):
                for mixed in range(2):
                    for o in range(8):
                        at = (block(o) if odd else o, *quarter(held, mixed), rows_of(r))
                        angle = gamma * (cost if odd else cost_swap)[at]
                        cos_buf[held, mixed * 8 + o, rows_of(r), :] = jnp.cos(angle)
                        sin_buf[held, mixed * 8 + o, rows_of(r), :] = jnp.sin(angle)
                return carry

            lax.fori_loop(0, 8, trig, 0)

            def sub_step(sub, carry):
                for mixed in range(2):
                    wait_all(recv, recv_sem, (source, *quarter(held, mixed), sub), arrived)

                def slots(i, carry):
                    r = sub * PER_SUB + i
                    cos_phase = [cos_buf[held, o, rows_of(r), :] for o in range(16)]
                    sin_phase = [sin_buf[held, o, rows_of(r), :] for o in range(16)]
                    old = [[recv[(source, *quarter(held, mixed), sub, o, c, rows_of(i))]
                            for mixed in range(2) for o in range(8)] for c in range(2)]
                    old_re, old_im = rotate(*old, cos_prev, sin_prev)
                    re = [r * c + i * s for r, i, c, s in zip(old_re, old_im, cos_phase, sin_phase)]
                    im = [i * c - r * s for r, i, c, s in zip(old_re, old_im, cos_phase, sin_phase)]
                    re, im = rotate(re, im, cos_half, sin_half)
                    re, im = sublane_rotate(re, im, cos_half, sin_half)
                    put_rows(i, re, im)
                    return carry

                lax.fori_loop(0, PER_SUB, slots, 0)
                work[held, sub] = lanes(2 * LANES)
                return carry

            lax.fori_loop(0, SUB, sub_step, 0)

            if drained:
                for mixed in range(2):
                    for sub in range(SUB):
                        wait_all(send, send_sem, (target, *quarter(held, mixed), sub), drained)

            def quarters(mixed, carry):
                emit(held, mixed, target, *quarter(held, mixed), cos_half, sin_half, SEND_ORDER, lambda o: o, (0,), last)
                return carry

            lax.fori_loop(0, 2, quarters, 0)
            return carry

        lax.fori_loop(0, 2, half, 0)

    first_layer()
    run_layer(1, False, 6, 0)
    run_layer(2, True, 7, 6)

    def layer_pair(i, carry):
        run_layer(2 * i + 3, False, 7, 7)
        run_layer(2 * i + 4, True, 7, 7)
        return carry

    lax.fori_loop(0, LAYERS // 2 - 2, layer_pair, 0)
    run_layer(LAYERS - 1, False, 7, 7, True)

    cos_half, sin_half = half_angle(LAYERS - 1)
    energy_part[...] = jnp.zeros((8, LANES), jnp.float32)

    def final_half(a, carry):
        def slots(sub, i):
            r = sub * PER_SUB + i
            old = [[recv[0, a, b, sub, o, c, rows_of(i), :] for b in range(2) for o in range(8)]
                   for c in range(2)]
            re, im = rotate(*old, cos_half, sin_half)
            total = energy_part[...]
            for b in range(2):
                for o in range(8):
                    at = (block(o), a, b, rows_of(r))
                    x, y = re[b * 8 + o], im[b * 8 + o]
                    out_re[at] = x
                    out_im[at] = y
                    total = total + cost[at] * (x * x + y * y)
            energy_part[...] = total

        def final_sub(sub, carry):
            for b in range(2):
                wait_all(recv, recv_sem, (0, a, b, sub), 7)

            def body(i, carry):
                slots(sub, i)
                return carry

            lax.fori_loop(0, PER_SUB, body, 0)
            return carry

        def final_part(part, carry):
            for b in range(2):
                wait_last(recv, recv_sem, a, b, part)
            slots(SUB - 1, part)
            return carry

        lax.fori_loop(0, SUB - 1, final_sub, 0)
        lax.fori_loop(0, 2, final_part, 0)
        return carry

    lax.fori_loop(0, 2, final_half, 0)

    me = block(0)
    energy_row[...] = jnp.sum(energy_part[...], axis=0, keepdims=True)
    energy_all[me] = energy_row[...]

    def drain(par):
        for a in range(2):
            for b in range(2):
                for sub in range(SUB if par else SUB - 1):
                    wait_all(send, send_sem, (par, a, b, sub), 7)
                if not par:
                    wait_last(send, send_sem, a, b, 0)
                    wait_last(send, send_sem, a, b, 1)

    drain(1)
    for a in range(2):
        for sub in range(SUB):
            wait_bytes(cost.at[:, a, :, pl.ds(sub * 8 * PER_SUB, 8 * PER_SUB)], near_send.at[a, sub])
    wait_bytes(cost_swap.at[pl.ds(0, 6)], cost_send)
    for offset in ENERGY_ORDER:
        remote(energy_row, energy_all.at[me], e_send.at[offset], e_recv.at[offset], offset)
    drain(0)
    for offset in range(1, 8):
        wait_bytes(energy_row, e_send.at[offset])
        wait_bytes(energy_row, e_recv.at[offset])


def write_out(energy_all, in_re, in_im, energy, out_re, out_im, value, sem):
    copies = [pltpu.make_async_copy(in_re, out_re, sem.at[0]), pltpu.make_async_copy(in_im, out_im, sem.at[1])]
    for copy in copies:
        copy.start()
    total = energy_all[0]
    for i in range(1, 8):
        total = total + energy_all[i]
    value[0] = jnp.sum(total) * (1.0 / (1 << 21))
    copies.append(pltpu.make_async_copy(value, energy, sem.at[2]))
    copies[2].start()
    for copy in copies:
        copy.wait()


def solution(mesh):
    state_spec = P(('inst', 'qx', 'qy'))

    def device_body(cost_local, gammas, betas):
        local_len = cost_local.shape[0]
        shape = (8, 2, 2, local_len // (32 * LANES), LANES)
        f32 = jnp.float32
        vmem = pl.BlockSpec(memory_space=pltpu.VMEM)
        dma = pltpu.SemaphoreType.DMA
        parts = (2, 2, 2, SUB, 8, 2, 8 * PER_SUB, LANES)
        hbm = pl.BlockSpec(memory_space=pl.ANY)
        results = pl.pallas_call(
            kernel,
            out_shape=(pltpu.VMEM((8, 1, LANES), f32), pltpu.VMEM(shape, f32), pltpu.VMEM(shape, f32)),
            in_specs=[hbm, hbm, hbm],
            out_specs=(vmem, vmem, vmem),
            scratch_shapes=[
                pltpu.VMEM(shape, f32), pltpu.VMEM(shape, f32), pltpu.VMEM(shape, f32),
                pltpu.VMEM(parts, f32), pltpu.VMEM(parts, f32),
                pltpu.VMEM((2, 4, 2 * LANES, 2 * LANES), f32),
                pltpu.VMEM((2, 16, 64, LANES), f32), pltpu.VMEM((2, 16, 64, LANES), f32),
                pltpu.VMEM((16, 8, LANES), f32), pltpu.VMEM((16, 8, LANES), f32),
                pltpu.VMEM((4 * LANES, 2 * LANES), f32), pltpu.VMEM((2 * LANES, 2 * LANES), f32),
                pltpu.VMEM((8, LANES), f32), pltpu.VMEM((1, LANES), f32),
                pltpu.SMEM((LAYERS,), f32), pltpu.SMEM((LAYERS,), f32), dma((2,)), pltpu.SemaphoreType.REGULAR((2,)),
                dma((SUB,)), dma((2, SUB)), dma((2, SUB)), dma, dma,
                dma((2, 2, 2, SUB + 1)), dma((2, 2, 2, SUB + 1)),
                dma((8,)), dma((8,)),
            ],
            compiler_params=pltpu.CompilerParams(collective_id=0, has_side_effects=True),
            name='qaoa',
        )(cost_local.reshape(shape), gammas, betas)
        energy, state_re, state_im = pl.pallas_call(
            write_out,
            out_shape=(jax.ShapeDtypeStruct((1,), f32),
                       jax.ShapeDtypeStruct(shape, f32), jax.ShapeDtypeStruct(shape, f32)),
            in_specs=[vmem, vmem, vmem],
            out_specs=(hbm, hbm, hbm),
            scratch_shapes=[pltpu.SMEM((1,), f32), dma((3,))],
            name='write_out',
        )(*[pltpu.with_memory_space_constraint(value, pltpu.VMEM) for value in results])
        return energy, state_re.reshape(local_len), state_im.reshape(local_len)

    return jax.shard_map(device_body, mesh=mesh, in_specs=(state_spec, P(), P()),
                         out_specs=(P('inst'), state_spec, state_spec), check_vma=False)
```

```python
import jax
import jax.numpy as jnp
from jax import lax
from jax.experimental import pallas as pl
from jax.experimental.pallas import tpu as pltpu
from jax.sharding import PartitionSpec as P

LANES = 128
LAYERS = 8
SUB = 4
PER_SUB = 8 // SUB
SEND_ORDER = (5, 7, 4, 6, 1, 3, 2)
NEAR = (4, 1)


def rotate(re, im, cos_half, sin_half, steps=None):
    count = len(re)
    for step in steps or [1 << i for i in range(count.bit_length() - 1)]:
        new_re = [cos_half * re[i] + sin_half * im[i ^ step] for i in range(count)]
        new_im = [cos_half * im[i] - sin_half * re[i ^ step] for i in range(count)]
        re, im = new_re, new_im
    return re, im


def sublane_rotate(re, im, cos_half, sin_half):
    row = lax.broadcasted_iota(jnp.int32, (8, LANES), 0)
    for step in (1, 2, 4):
        bit_set = (row & step) != 0

        def flip(value):
            down = pltpu.roll(value, step, 0)
            if step == 4:
                return down
            return jnp.where(bit_set, down, pltpu.roll(value, 8 - step, 0))

        flip_re = [flip(value) for value in re]
        flip_im = [flip(value) for value in im]
        re, im = ([cos_half * r + sin_half * fi for r, fi in zip(re, flip_im)],
                  [cos_half * i - sin_half * fr for i, fr in zip(im, flip_re)])
    return re, im


def lane_matrix(cos_half, sin_half):
    row = lax.broadcasted_iota(jnp.int32, (LANES, LANES), 0)
    col = lax.broadcasted_iota(jnp.int32, (LANES, LANES), 1)
    diff = row ^ col
    cos_full = jnp.broadcast_to(cos_half[0:1], (LANES, LANES))
    sin_full = jnp.broadcast_to(sin_half[0:1], (LANES, LANES))
    mag = jnp.ones((LANES, LANES), jnp.float32)
    weight = jnp.zeros((LANES, LANES), jnp.int32)
    for bit in range(7):
        on = (diff >> bit) & 1
        mag = mag * jnp.where(on == 1, sin_full, cos_full)
        weight = weight + on
    quarter = weight & 3
    zero = jnp.zeros_like(mag)
    real = jnp.where(quarter == 0, mag, jnp.where(quarter == 2, -mag, zero))
    imag = jnp.where(quarter == 1, -mag, jnp.where(quarter == 3, mag, zero))
    return real, imag


def kernel(cost_hbm, gammas_hbm, betas_hbm, energy_all, out_re, out_im,
           cost, cost_near, cost_swap, recv, send, work, cos_buf, sin_buf, cos_near, sin_near,
           rows_in, matrix, energy_part, energy_row, gammas, betas, angle_in, near_in, cost_in, near_send, near_recv, cost_send, cost_recv,
           send_sem, recv_sem, e_send, e_recv):
    qx = lax.axis_index('qx')
    qy = lax.axis_index('qy')
    bits = (qy, qx % 2, qx // 2)

    def flipped(offset):
        return [1 - bit if (offset >> i) & 1 else bit for i, bit in enumerate(bits)]

    def block(offset):
        y, core, x = flipped(offset)
        return (x * 2 + core) * 2 + y

    def peer(offset):
        y, core, x = flipped(offset)
        return {'qy': y, 'qx': x * 2 + core}

    def remote(source, target, send_at, recv_at, offset):
        pltpu.make_async_remote_copy(
            src_ref=source, dst_ref=target, send_sem=send_at, recv_sem=recv_at,
            device_id=peer(offset), device_id_type=pl.DeviceIdType.MESH).start()

    barrier = pltpu.get_barrier_semaphore()

    def signal_next(sem):
        for offset in (4, 1, 2):
            pl.semaphore_signal(sem, inc=1, device_id=peer(offset), device_id_type=pl.DeviceIdType.MESH)

    signal_next(barrier)
    loads = [pltpu.make_async_copy(cost_hbm.at[:, :, :, pl.ds(sub * 8 * PER_SUB, 8 * PER_SUB)],
                                   cost.at[:, :, :, pl.ds(sub * 8 * PER_SUB, 8 * PER_SUB)], cost_in.at[sub])
             for sub in range(SUB)]
    for load in loads:
        load.start()
    angle_loads = [pltpu.make_async_copy(gammas_hbm, gammas, angle_in.at[0]),
                   pltpu.make_async_copy(betas_hbm, betas, angle_in.at[1])]
    for load in angle_loads:
        load.start()
    pl.semaphore_wait(barrier, 3)

    def half_angle(layer):
        angle = jnp.full((8, LANES), 0.5 * betas[layer], jnp.float32)
        return jnp.cos(angle), jnp.sin(angle)

    def wait_bytes(part, sem):
        pltpu.make_async_copy(part, part, sem).wait()

    def wait_all(buffer, sem, at, count):
        wait_bytes(buffer.at[(*at, pl.ds(0, count))], sem.at[at])

    def rows_of(r):
        return pl.ds(pl.multiple_of(r * 8, 8), 8)

    def set_matrix(cos_half, sin_half):
        real, imag = lane_matrix(cos_half, sin_half)
        matrix[0:LANES, 0:LANES] = real
        matrix[0:LANES, LANES:] = imag
        matrix[LANES:, 0:LANES] = -imag
        matrix[LANES:, LANES:] = real

    def put_rows(i, re, im, base=0):
        for o in range(16):
            at = pl.multiple_of(base + o * 16 + i * 8, 8)
            rows_in[pl.ds(at, 8), 0:LANES] = re[o]
            rows_in[pl.ds(at, 8), LANES:] = im[o]

    def lanes(count):
        return lax.dot(rows_in[0:count, :], matrix[...],
                       precision=lax.Precision.HIGHEST, preferred_element_type=jnp.float32)

    def emit(held, mixed, target, a, b, cos_half, sin_half, order, route, local):
        def across(o, buffer):
            def part(r, c):
                at = pl.multiple_of((mixed * 8 + o) * 16 + (r % 2) * 8, 8)
                return work[held, r // 2, pl.ds(at, 8), c * LANES:(c + 1) * LANES]

            re = [part(r, 0) for r in range(8)]
            im = [part(r, 1) for r in range(8)]
            re, im = rotate(re, im, cos_half, sin_half)
            for r in range(8):
                row = (r % PER_SUB) * 8
                buffer[target, a, b, r // PER_SUB, o, 0, row:row + 8, :] = re[r]
                buffer[target, a, b, r // PER_SUB, o, 1, row:row + 8, :] = im[r]

        def body(o, carry):
            across(o, send)
            return carry

        lax.fori_loop(1, 8, body, 0)
        for o in local:
            across(o, recv)
        for sub in range(SUB):
            at = (target, a, b, sub)
            for o in order:
                remote(send.at[(*at, o)], recv.at[(*at, o)], send_sem.at[at], recv_sem.at[at], route(o))

    def first_layer():
        def sub_rows(sub):
            return pl.ds(pl.multiple_of(sub * 8 * PER_SUB, 8), 8 * PER_SUB)

        for sub in range(SUB):
            loads[sub].wait()
            for a in range(2):
                remote(cost.at[:, a, :, sub_rows(sub)], cost_near.at[:, a, :, sub_rows(sub)],
                       near_send.at[a, sub], near_recv.at[a, sub], NEAR[a])
        signal_next(near_in.at[0])
        for load in angle_loads:
            load.wait()
        gamma = gammas[0]
        cos_half, sin_half = half_angle(0)
        set_matrix(cos_half, sin_half)

        def own_trig(r, carry):
            for a in range(2):
                for b in range(2):
                    for o in range(8):
                        angle = gamma * cost[block(o), a, b, rows_of(r), :]
                        cos_buf[a, b * 8 + o, rows_of(r), :] = jnp.cos(angle)
                        sin_buf[a, b * 8 + o, rows_of(r), :] = jnp.sin(angle)
            return carry

        for round_id in range(2):
            lax.fori_loop(4 * round_id, 4 * round_id + 4, own_trig, 0)
            pl.semaphore_wait(near_in.at[round_id], 3)
            if round_id == 0:
                signal_next(near_in.at[1])
        for a in range(2):
            for o in range(1, 8):
                if not o & NEAR[a]:
                    remote(cost.at[block(o), a], cost_swap.at[o, a], cost_send, cost_recv, o)

        def sub_step(sub, carry):
            for a in range(2):
                bit = NEAR[a]
                part = cost_near.at[:, a, :, sub_rows(sub)]
                wait_bytes(part, near_recv.at[a, sub])
                for o in range(1, 8):
                    if not o & bit:
                        remote(cost_near.at[block(o), a, :, sub_rows(sub)],
                               cost_swap.at[o | bit, a, :, sub_rows(sub)], cost_send, cost_recv, o)

                def slots(i, carry):
                    r = sub * PER_SUB + i
                    for b in range(2):
                        for o in range(8):
                            angle = gamma * cost_near[block(o), a, b, rows_of(r), :]
                            cos_near[b * 8 + o] = jnp.cos(angle)
                            sin_near[b * 8 + o] = jnp.sin(angle)
                    re, im = [None] * 16, [None] * 16
                    for b in range(2):
                        for o in range(8):
                            if o & bit:
                                continue
                            here, there = b * 8 + o, b * 8 + (o | bit)
                            for slot, cos_at, sin_at in (
                                    (here, lambda k: cos_buf[a, k, rows_of(r), :], lambda k: sin_buf[a, k, rows_of(r), :]),
                                    (there, lambda k: cos_near[k], lambda k: sin_near[k])):
                                re[slot] = cos_half * cos_at(here) - sin_half * sin_at(there)
                                im[slot] = -(cos_half * sin_at(here)) - sin_half * cos_at(there)
                    re, im = rotate(re, im, cos_half, sin_half, [step for step in (1, 2, 4, 8) if step != bit])
                    re, im = sublane_rotate(re, im, cos_half, sin_half)
                    put_rows(i, re, im, a * 2 * LANES)
                    return carry

                lax.fori_loop(0, PER_SUB, slots, 0)
            rows = lanes(4 * LANES)
            for a in range(2):
                work[a, sub] = rows[a * 2 * LANES:(a + 1) * 2 * LANES]
            return carry

        lax.fori_loop(0, SUB, sub_step, 0)

        def quarters(b, carry):
            for a in range(2):
                bit = NEAR[a]
                emit(a, b, 1, a, b, cos_half, sin_half,
                     [o for o in (3, 6, 7, 1, 4, 5, 2) if o & ~bit], lambda o: o & ~bit, (0, bit))
            return carry

        lax.fori_loop(0, 2, quarters, 0)
        cost_swap[0] = cost[block(0)]
        for a in range(2):
            cost_swap[NEAR[a], a] = cost_near[block(0), a]
        wait_bytes(cost_swap.at[pl.ds(0, 6)], cost_recv)

    def run_layer(layer, odd, arrived, drained):
        source, target = (0, 1) if odd else (1, 0)

        def quarter(held, mixed):
            return (held, mixed) if odd else (mixed, held)

        cos_half, sin_half = half_angle(layer)
        cos_prev, sin_prev = half_angle(layer - 1)
        gamma = gammas[layer]
        set_matrix(cos_half, sin_half)

        def half(held, carry):
            def trig(r, carry):
                for mixed in range(2):
                    for o in range(8):
                        at = (block(o) if odd else o, *quarter(held, mixed), rows_of(r))
                        angle = gamma * (cost if odd else cost_swap)[at]
                        cos_buf[held, mixed * 8 + o, rows_of(r), :] = jnp.cos(angle)
                        sin_buf[held, mixed * 8 + o, rows_of(r), :] = jnp.sin(angle)
                return carry

            lax.fori_loop(0, 8, trig, 0)

            def sub_step(sub, carry):
                for mixed in range(2):
                    wait_all(recv, recv_sem, (source, *quarter(held, mixed), sub), arrived)

                def slots(i, carry):
                    r = sub * PER_SUB + i
                    cos_phase = [cos_buf[held, o, rows_of(r), :] for o in range(16)]
                    sin_phase = [sin_buf[held, o, rows_of(r), :] for o in range(16)]
                    old = [[recv[(source, *quarter(held, mixed), sub, o, c, rows_of(i))]
                            for mixed in range(2) for o in range(8)] for c in range(2)]
                    old_re, old_im = rotate(*old, cos_prev, sin_prev)
                    re = [r * c + i * s for r, i, c, s in zip(old_re, old_im, cos_phase, sin_phase)]
                    im = [i * c - r * s for r, i, c, s in zip(old_re, old_im, cos_phase, sin_phase)]
                    re, im = rotate(re, im, cos_half, sin_half)
                    re, im = sublane_rotate(re, im, cos_half, sin_half)
                    put_rows(i, re, im)
                    return carry

                lax.fori_loop(0, PER_SUB, slots, 0)
                work[held, sub] = lanes(2 * LANES)
                return carry

            lax.fori_loop(0, SUB, sub_step, 0)

            if drained:
                for mixed in range(2):
                    for sub in range(SUB):
                        wait_all(send, send_sem, (target, *quarter(held, mixed), sub), drained)

            def quarters(mixed, carry):
                emit(held, mixed, target, *quarter(held, mixed), cos_half, sin_half, SEND_ORDER, lambda o: o, (0,))
                return carry

            lax.fori_loop(0, 2, quarters, 0)
            return carry

        lax.fori_loop(0, 2, half, 0)

    first_layer()
    run_layer(1, False, 6, 0)
    run_layer(2, True, 7, 6)

    def layer_pair(i, carry):
        run_layer(2 * i + 3, False, 7, 7)
        run_layer(2 * i + 4, True, 7, 7)
        return carry

    lax.fori_loop(0, LAYERS // 2 - 2, layer_pair, 0)
    run_layer(LAYERS - 1, False, 7, 7)

    cos_half, sin_half = half_angle(LAYERS - 1)
    energy_part[...] = jnp.zeros((8, LANES), jnp.float32)

    def final_half(a, carry):
        def final_sub(sub, carry):
            for b in range(2):
                wait_all(recv, recv_sem, (0, a, b, sub), 7)

            def slots(i, carry):
                r = sub * PER_SUB + i
                old = [[recv[0, a, b, sub, o, c, rows_of(i), :] for b in range(2) for o in range(8)]
                       for c in range(2)]
                re, im = rotate(*old, cos_half, sin_half)
                total = energy_part[...]
                for b in range(2):
                    for o in range(8):
                        at = (block(o), a, b, rows_of(r))
                        x, y = re[b * 8 + o], im[b * 8 + o]
                        out_re[at] = x
                        out_im[at] = y
                        total = total + cost[at] * (x * x + y * y)
                energy_part[...] = total
                return carry

            lax.fori_loop(0, PER_SUB, slots, 0)
            return carry

        lax.fori_loop(0, SUB, final_sub, 0)
        return carry

    lax.fori_loop(0, 2, final_half, 0)

    me = block(0)
    energy_row[...] = jnp.sum(energy_part[...], axis=0, keepdims=True)
    energy_all[me] = energy_row[...]

    def drain(par):
        for a in range(2):
            for b in range(2):
                for sub in range(SUB):
                    wait_all(send, send_sem, (par, a, b, sub), 7)

    for a in range(2):
        for sub in range(SUB):
            wait_bytes(cost.at[:, a, :, pl.ds(sub * 8 * PER_SUB, 8 * PER_SUB)], near_send.at[a, sub])
    wait_bytes(cost_swap.at[pl.ds(0, 6)], cost_send)
    for offset in (7, 5, 6, 4, 3, 1, 2):
        remote(energy_row, energy_all.at[me], e_send.at[offset], e_recv.at[offset], offset)
    drain(0)
    drain(1)
    for offset in range(1, 8):
        wait_bytes(energy_row, e_send.at[offset])
        wait_bytes(energy_row, e_recv.at[offset])


def write_out(energy_all, in_re, in_im, energy, out_re, out_im, value, sem):
    copies = [pltpu.make_async_copy(source.at[pl.ds(4 * i, 4)], result.at[pl.ds(4 * i, 4)], sem.at[2 * c + i])
              for i in range(2) for c, (source, result) in enumerate(((in_re, out_re), (in_im, out_im)))]
    for copy in copies:
        copy.start()
    total = energy_all[0]
    for i in range(1, 8):
        total = total + energy_all[i]
    value[0] = jnp.sum(total) * (1.0 / (1 << 21))
    copies.append(pltpu.make_async_copy(value, energy, sem.at[4]))
    copies[4].start()
    for copy in copies:
        copy.wait()


def solution(mesh):
    state_spec = P(('inst', 'qx', 'qy'))

    def device_body(cost_local, gammas, betas):
        local_len = cost_local.shape[0]
        shape = (8, 2, 2, local_len // (32 * LANES), LANES)
        f32 = jnp.float32
        vmem = pl.BlockSpec(memory_space=pltpu.VMEM)
        dma = pltpu.SemaphoreType.DMA
        parts = (2, 2, 2, SUB, 8, 2, 8 * PER_SUB, LANES)
        hbm = pl.BlockSpec(memory_space=pl.ANY)
        results = pl.pallas_call(
            kernel,
            out_shape=(pltpu.VMEM((8, 1, LANES), f32), pltpu.VMEM(shape, f32), pltpu.VMEM(shape, f32)),
            in_specs=[hbm, hbm, hbm],
            out_specs=(vmem, vmem, vmem),
            scratch_shapes=[
                pltpu.VMEM(shape, f32), pltpu.VMEM(shape, f32), pltpu.VMEM(shape, f32),
                pltpu.VMEM(parts, f32), pltpu.VMEM(parts, f32),
                pltpu.VMEM((2, 4, 2 * LANES, 2 * LANES), f32),
                pltpu.VMEM((2, 16, 64, LANES), f32), pltpu.VMEM((2, 16, 64, LANES), f32),
                pltpu.VMEM((16, 8, LANES), f32), pltpu.VMEM((16, 8, LANES), f32),
                pltpu.VMEM((4 * LANES, 2 * LANES), f32), pltpu.VMEM((2 * LANES, 2 * LANES), f32),
                pltpu.VMEM((8, LANES), f32), pltpu.VMEM((1, LANES), f32),
                pltpu.SMEM((LAYERS,), f32), pltpu.SMEM((LAYERS,), f32), dma((2,)), pltpu.SemaphoreType.REGULAR((2,)),
                dma((SUB,)), dma((2, SUB)), dma((2, SUB)), dma, dma,
                dma((2, 2, 2, SUB)), dma((2, 2, 2, SUB)),
                dma((8,)), dma((8,)),
            ],
            compiler_params=pltpu.CompilerParams(collective_id=0, has_side_effects=True),
            name='qaoa',
        )(cost_local.reshape(shape), gammas, betas)
        energy, state_re, state_im = pl.pallas_call(
            write_out,
            out_shape=(jax.ShapeDtypeStruct((1,), f32),
                       jax.ShapeDtypeStruct(shape, f32), jax.ShapeDtypeStruct(shape, f32)),
            in_specs=[vmem, vmem, vmem],
            out_specs=(hbm, hbm, hbm),
            scratch_shapes=[pltpu.SMEM((1,), f32), dma((5,))],
            name='write_out',
        )(*[pltpu.with_memory_space_constraint(value, pltpu.VMEM) for value in results])
        return energy, state_re.reshape(local_len), state_im.reshape(local_len)

    return jax.shard_map(device_body, mesh=mesh, in_specs=(state_spec, P(), P()),
                         out_specs=(P('inst'), state_spec, state_spec), check_vma=False)
```

```python
import jax
import jax.numpy as jnp
from jax import lax
from jax.experimental import pallas as pl
from jax.experimental.pallas import tpu as pltpu
from jax.sharding import PartitionSpec as P

LANES = 128
LAYERS = 8
SUB = 4
PER_SUB = 8 // SUB
SEND_ORDER = (5, 7, 4, 6, 1, 3, 2)
NEAR = (4, 1)


def rotate(re, im, cos_half, sin_half, steps=None):
    count = len(re)
    for step in steps or [1 << i for i in range(count.bit_length() - 1)]:
        new_re = [cos_half * re[i] + sin_half * im[i ^ step] for i in range(count)]
        new_im = [cos_half * im[i] - sin_half * re[i ^ step] for i in range(count)]
        re, im = new_re, new_im
    return re, im


def sublane_rotate(re, im, cos_half, sin_half):
    row = lax.broadcasted_iota(jnp.int32, (8, LANES), 0)
    for step in (1, 2, 4):
        bit_set = (row & step) != 0

        def flip(value):
            down = pltpu.roll(value, step, 0)
            if step == 4:
                return down
            return jnp.where(bit_set, down, pltpu.roll(value, 8 - step, 0))

        flip_re = [flip(value) for value in re]
        flip_im = [flip(value) for value in im]
        re, im = ([cos_half * r + sin_half * fi for r, fi in zip(re, flip_im)],
                  [cos_half * i - sin_half * fr for i, fr in zip(im, flip_re)])
    return re, im


def lane_matrix(cos_half, sin_half):
    row = lax.broadcasted_iota(jnp.int32, (LANES, LANES), 0)
    col = lax.broadcasted_iota(jnp.int32, (LANES, LANES), 1)
    diff = row ^ col
    cos_full = jnp.broadcast_to(cos_half[0:1], (LANES, LANES))
    sin_full = jnp.broadcast_to(sin_half[0:1], (LANES, LANES))
    mag = jnp.ones((LANES, LANES), jnp.float32)
    weight = jnp.zeros((LANES, LANES), jnp.int32)
    for bit in range(7):
        on = (diff >> bit) & 1
        mag = mag * jnp.where(on == 1, sin_full, cos_full)
        weight = weight + on
    quarter = weight & 3
    zero = jnp.zeros_like(mag)
    real = jnp.where(quarter == 0, mag, jnp.where(quarter == 2, -mag, zero))
    imag = jnp.where(quarter == 1, -mag, jnp.where(quarter == 3, mag, zero))
    return real, imag


def kernel(cost_hbm, gammas_hbm, betas_hbm, energy_all, out_re, out_im,
           cost, cost_near, cost_swap, recv, send, work, cos_buf, sin_buf, cos_near, sin_near,
           rows_in, matrix, energy_part, energy_row, gammas, betas, angle_in, near_in, cost_in, near_send, near_recv, cost_send, cost_recv,
           send_sem, recv_sem, e_send, e_recv):
    qx = lax.axis_index('qx')
    qy = lax.axis_index('qy')
    bits = (qy, qx % 2, qx // 2)

    def flipped(offset):
        return [1 - bit if (offset >> i) & 1 else bit for i, bit in enumerate(bits)]

    def block(offset):
        y, core, x = flipped(offset)
        return (x * 2 + core) * 2 + y

    def peer(offset):
        y, core, x = flipped(offset)
        return {'qy': y, 'qx': x * 2 + core}

    def remote(source, target, send_at, recv_at, offset):
        pltpu.make_async_remote_copy(
            src_ref=source, dst_ref=target, send_sem=send_at, recv_sem=recv_at,
            device_id=peer(offset), device_id_type=pl.DeviceIdType.MESH).start()

    barrier = pltpu.get_barrier_semaphore()

    def signal_next(sem):
        for offset in (4, 1, 2):
            pl.semaphore_signal(sem, inc=1, device_id=peer(offset), device_id_type=pl.DeviceIdType.MESH)

    signal_next(barrier)
    loads = [pltpu.make_async_copy(cost_hbm.at[:, :, :, pl.ds(sub * 8 * PER_SUB, 8 * PER_SUB)],
                                   cost.at[:, :, :, pl.ds(sub * 8 * PER_SUB, 8 * PER_SUB)], cost_in.at[sub])
             for sub in range(SUB)]
    for load in loads:
        load.start()
    angle_loads = [pltpu.make_async_copy(gammas_hbm, gammas, angle_in.at[0]),
                   pltpu.make_async_copy(betas_hbm, betas, angle_in.at[1])]
    for load in angle_loads:
        load.start()
    pl.semaphore_wait(barrier, 3)

    def half_angle(layer):
        angle = jnp.full((8, LANES), 0.5 * betas[layer], jnp.float32)
        return jnp.cos(angle), jnp.sin(angle)

    def wait_bytes(part, sem):
        pltpu.make_async_copy(part, part, sem).wait()

    def wait_all(buffer, sem, at, count):
        wait_bytes(buffer.at[(*at, pl.ds(0, count))], sem.at[at])

    def rows_of(r):
        return pl.ds(pl.multiple_of(r * 8, 8), 8)

    def set_matrix(cos_half, sin_half):
        real, imag = lane_matrix(cos_half, sin_half)
        matrix[0:LANES, 0:LANES] = real
        matrix[0:LANES, LANES:] = imag
        matrix[LANES:, 0:LANES] = -imag
        matrix[LANES:, LANES:] = real

    def put_rows(i, re, im, base=0):
        for o in range(16):
            at = pl.multiple_of(base + o * 16 + i * 8, 8)
            rows_in[pl.ds(at, 8), 0:LANES] = re[o]
            rows_in[pl.ds(at, 8), LANES:] = im[o]

    def lanes(count):
        return lax.dot(rows_in[0:count, :], matrix[...],
                       precision=lax.Precision.HIGHEST, preferred_element_type=jnp.float32)

    def emit(held, mixed, target, a, b, cos_half, sin_half, order, route, local):
        def across(o, buffer):
            def part(r, c):
                at = pl.multiple_of((mixed * 8 + o) * 16 + (r % 2) * 8, 8)
                return work[held, r // 2, pl.ds(at, 8), c * LANES:(c + 1) * LANES]

            re = [part(r, 0) for r in range(8)]
            im = [part(r, 1) for r in range(8)]
            re, im = rotate(re, im, cos_half, sin_half)
            for r in range(8):
                row = (r % PER_SUB) * 8
                buffer[target, a, b, r // PER_SUB, o, 0, row:row + 8, :] = re[r]
                buffer[target, a, b, r // PER_SUB, o, 1, row:row + 8, :] = im[r]

        def body(o, carry):
            across(o, send)
            return carry

        lax.fori_loop(1, 8, body, 0)
        for o in local:
            across(o, recv)
        for sub in range(SUB):
            at = (target, a, b, sub)
            for o in order:
                remote(send.at[(*at, o)], recv.at[(*at, o)], send_sem.at[at], recv_sem.at[at], route(o))

    def first_layer():
        def sub_rows(sub):
            return pl.ds(pl.multiple_of(sub * 8 * PER_SUB, 8), 8 * PER_SUB)

        for sub in range(SUB):
            loads[sub].wait()
            for a in range(2):
                remote(cost.at[:, a, :, sub_rows(sub)], cost_near.at[:, a, :, sub_rows(sub)],
                       near_send.at[a, sub], near_recv.at[a, sub], NEAR[a])
        signal_next(near_in.at[0])
        for load in angle_loads:
            load.wait()
        gamma = gammas[0]
        cos_half, sin_half = half_angle(0)
        set_matrix(cos_half, sin_half)

        def own_trig(r, carry):
            for a in range(2):
                for b in range(2):
                    for o in range(8):
                        angle = gamma * cost[block(o), a, b, rows_of(r), :]
                        cos_buf[a, b * 8 + o, rows_of(r), :] = jnp.cos(angle)
                        sin_buf[a, b * 8 + o, rows_of(r), :] = jnp.sin(angle)
            return carry

        for round_id in range(2):
            lax.fori_loop(4 * round_id, 4 * round_id + 4, own_trig, 0)
            pl.semaphore_wait(near_in.at[round_id], 3)
            if round_id == 0:
                signal_next(near_in.at[1])
        for a in range(2):
            for o in range(1, 8):
                if not o & NEAR[a]:
                    remote(cost.at[block(o), a], cost_swap.at[o, a], cost_send, cost_recv, o)

        def sub_step(sub, carry):
            for a in range(2):
                bit = NEAR[a]
                part = cost_near.at[:, a, :, sub_rows(sub)]
                wait_bytes(part, near_recv.at[a, sub])
                for o in range(1, 8):
                    if not o & bit:
                        remote(cost_near.at[block(o), a, :, sub_rows(sub)],
                               cost_swap.at[o | bit, a, :, sub_rows(sub)], cost_send, cost_recv, o)

                def slots(i, carry):
                    r = sub * PER_SUB + i
                    for b in range(2):
                        for o in range(8):
                            angle = gamma * cost_near[block(o), a, b, rows_of(r), :]
                            cos_near[b * 8 + o] = jnp.cos(angle)
                            sin_near[b * 8 + o] = jnp.sin(angle)
                    re, im = [None] * 16, [None] * 16
                    for b in range(2):
                        for o in range(8):
                            if o & bit:
                                continue
                            here, there = b * 8 + o, b * 8 + (o | bit)
                            for slot, cos_at, sin_at in (
                                    (here, lambda k: cos_buf[a, k, rows_of(r), :], lambda k: sin_buf[a, k, rows_of(r), :]),
                                    (there, lambda k: cos_near[k], lambda k: sin_near[k])):
                                re[slot] = cos_half * cos_at(here) - sin_half * sin_at(there)
                                im[slot] = -(cos_half * sin_at(here)) - sin_half * cos_at(there)
                    re, im = rotate(re, im, cos_half, sin_half, [step for step in (1, 2, 4, 8) if step != bit])
                    re, im = sublane_rotate(re, im, cos_half, sin_half)
                    put_rows(i, re, im, a * 2 * LANES)
                    return carry

                lax.fori_loop(0, PER_SUB, slots, 0)
            rows = lanes(4 * LANES)
            for a in range(2):
                work[a, sub] = rows[a * 2 * LANES:(a + 1) * 2 * LANES]
            return carry

        lax.fori_loop(0, SUB, sub_step, 0)

        def quarters(b, carry):
            for a in range(2):
                bit = NEAR[a]
                emit(a, b, 1, a, b, cos_half, sin_half,
                     [o for o in (3, 6, 7, 1, 4, 5, 2) if o & ~bit], lambda o: o & ~bit, (0, bit))
            return carry

        lax.fori_loop(0, 2, quarters, 0)
        cost_swap[0] = cost[block(0)]
        for a in range(2):
            cost_swap[NEAR[a], a] = cost_near[block(0), a]
        wait_bytes(cost_swap.at[pl.ds(0, 6)], cost_recv)

    def run_layer(layer, odd, arrived, drained):
        source, target = (0, 1) if odd else (1, 0)

        def quarter(held, mixed):
            return (held, mixed) if odd else (mixed, held)

        cos_half, sin_half = half_angle(layer)
        cos_prev, sin_prev = half_angle(layer - 1)
        gamma = gammas[layer]
        set_matrix(cos_half, sin_half)

        def half(held, carry):
            def trig(r, carry):
                for mixed in range(2):
                    for o in range(8):
                        at = (block(o) if odd else o, *quarter(held, mixed), rows_of(r))
                        angle = gamma * (cost if odd else cost_swap)[at]
                        cos_buf[held, mixed * 8 + o, rows_of(r), :] = jnp.cos(angle)
                        sin_buf[held, mixed * 8 + o, rows_of(r), :] = jnp.sin(angle)
                return carry

            lax.fori_loop(0, 8, trig, 0)

            def sub_step(sub, carry):
                for mixed in range(2):
                    wait_all(recv, recv_sem, (source, *quarter(held, mixed), sub), arrived)

                def slots(i, carry):
                    r = sub * PER_SUB + i
                    cos_phase = [cos_buf[held, o, rows_of(r), :] for o in range(16)]
                    sin_phase = [sin_buf[held, o, rows_of(r), :] for o in range(16)]
                    old = [[recv[(source, *quarter(held, mixed), sub, o, c, rows_of(i))]
                            for mixed in range(2) for o in range(8)] for c in range(2)]
                    old_re, old_im = rotate(*old, cos_prev, sin_prev)
                    re = [r * c + i * s for r, i, c, s in zip(old_re, old_im, cos_phase, sin_phase)]
                    im = [i * c - r * s for r, i, c, s in zip(old_re, old_im, cos_phase, sin_phase)]
                    re, im = rotate(re, im, cos_half, sin_half)
                    re, im = sublane_rotate(re, im, cos_half, sin_half)
                    put_rows(i, re, im)
                    return carry

                lax.fori_loop(0, PER_SUB, slots, 0)
                work[held, sub] = lanes(2 * LANES)
                return carry

            lax.fori_loop(0, SUB, sub_step, 0)

            if drained:
                for mixed in range(2):
                    for sub in range(SUB):
                        wait_all(send, send_sem, (target, *quarter(held, mixed), sub), drained)

            def quarters(mixed, carry):
                emit(held, mixed, target, *quarter(held, mixed), cos_half, sin_half, SEND_ORDER, lambda o: o, (0,))
                return carry

            lax.fori_loop(0, 2, quarters, 0)
            return carry

        lax.fori_loop(0, 2, half, 0)

    first_layer()
    run_layer(1, False, 6, 0)
    run_layer(2, True, 7, 6)

    def layer_pair(i, carry):
        run_layer(2 * i + 3, False, 7, 7)
        run_layer(2 * i + 4, True, 7, 7)
        return carry

    lax.fori_loop(0, LAYERS // 2 - 2, layer_pair, 0)
    run_layer(LAYERS - 1, False, 7, 7)

    cos_half, sin_half = half_angle(LAYERS - 1)
    energy_part[...] = jnp.zeros((8, LANES), jnp.float32)

    def slot_gates(a, b, sub, i):
        return rotate(*[[recv[0, a, b, sub, o, c, rows_of(i), :] for o in range(8)] for c in range(2)],
                      cos_half, sin_half)

    def early_half(a, carry):
        def early_sub(sub, carry):
            wait_all(recv, recv_sem, (0, a, 0, sub), 7)

            def slots(i, carry):
                for c, values in enumerate(slot_gates(a, 0, sub, i)):
                    for o in range(8):
                        recv[0, a, 0, sub, o, c, rows_of(i), :] = values[o]
                return carry

            lax.fori_loop(0, PER_SUB, slots, 0)
            return carry

        lax.fori_loop(0, SUB, early_sub, 0)
        return carry

    lax.fori_loop(0, 2, early_half, 0)

    def final_half(a, carry):
        def final_sub(sub, carry):
            wait_all(recv, recv_sem, (0, a, 1, sub), 7)

            def slots(i, carry):
                r = sub * PER_SUB + i
                re, im = slot_gates(a, 1, sub, i)
                total = energy_part[...]
                for o in range(8):
                    early = [recv[0, a, 0, sub, o, c, rows_of(i), :] for c in range(2)]
                    pair_re, pair_im = rotate([early[0], re[o]], [early[1], im[o]], cos_half, sin_half)
                    for b in range(2):
                        at = (block(o), a, b, rows_of(r))
                        x, y = pair_re[b], pair_im[b]
                        out_re[at] = x
                        out_im[at] = y
                        total = total + cost[at] * (x * x + y * y)
                energy_part[...] = total
                return carry

            lax.fori_loop(0, PER_SUB, slots, 0, unroll=True)
            return carry

        lax.fori_loop(0, SUB, final_sub, 0)
        return carry

    lax.fori_loop(0, 2, final_half, 0)

    me = block(0)
    energy_row[...] = jnp.sum(energy_part[...], axis=0, keepdims=True)
    energy_all[me] = energy_row[...]

    def drain(par):
        for a in range(2):
            for b in range(2):
                for sub in range(SUB):
                    wait_all(send, send_sem, (par, a, b, sub), 7)

    for a in range(2):
        for sub in range(SUB):
            wait_bytes(cost.at[:, a, :, pl.ds(sub * 8 * PER_SUB, 8 * PER_SUB)], near_send.at[a, sub])
    wait_bytes(cost_swap.at[pl.ds(0, 6)], cost_send)
    for offset in (7, 5, 6, 4, 3, 1, 2):
        remote(energy_row, energy_all.at[me], e_send.at[offset], e_recv.at[offset], offset)
    drain(0)
    drain(1)
    for offset in range(1, 8):
        wait_bytes(energy_row, e_send.at[offset])
        wait_bytes(energy_row, e_recv.at[offset])


def write_out(energy_all, in_re, in_im, energy, out_re, out_im, value, sem):
    copies = [pltpu.make_async_copy(in_re, out_re, sem.at[0]), pltpu.make_async_copy(in_im, out_im, sem.at[1])]
    for copy in copies:
        copy.start()
    total = energy_all[0]
    for i in range(1, 8):
        total = total + energy_all[i]
    value[0] = jnp.sum(total) * (1.0 / (1 << 21))
    copies.append(pltpu.make_async_copy(value, energy, sem.at[2]))
    copies[2].start()
    for copy in copies:
        copy.wait()


def solution(mesh):
    state_spec = P(('inst', 'qx', 'qy'))

    def device_body(cost_local, gammas, betas):
        local_len = cost_local.shape[0]
        shape = (8, 2, 2, local_len // (32 * LANES), LANES)
        f32 = jnp.float32
        vmem = pl.BlockSpec(memory_space=pltpu.VMEM)
        dma = pltpu.SemaphoreType.DMA
        parts = (2, 2, 2, SUB, 8, 2, 8 * PER_SUB, LANES)
        hbm = pl.BlockSpec(memory_space=pl.ANY)
        results = pl.pallas_call(
            kernel,
            out_shape=(pltpu.VMEM((8, 1, LANES), f32), pltpu.VMEM(shape, f32), pltpu.VMEM(shape, f32)),
            in_specs=[hbm, hbm, hbm],
            out_specs=(vmem, vmem, vmem),
            scratch_shapes=[
                pltpu.VMEM(shape, f32), pltpu.VMEM(shape, f32), pltpu.VMEM(shape, f32),
                pltpu.VMEM(parts, f32), pltpu.VMEM(parts, f32),
                pltpu.VMEM((2, 4, 2 * LANES, 2 * LANES), f32),
                pltpu.VMEM((2, 16, 64, LANES), f32), pltpu.VMEM((2, 16, 64, LANES), f32),
                pltpu.VMEM((16, 8, LANES), f32), pltpu.VMEM((16, 8, LANES), f32),
                pltpu.VMEM((4 * LANES, 2 * LANES), f32), pltpu.VMEM((2 * LANES, 2 * LANES), f32),
                pltpu.VMEM((8, LANES), f32), pltpu.VMEM((1, LANES), f32),
                pltpu.SMEM((LAYERS,), f32), pltpu.SMEM((LAYERS,), f32), dma((2,)), pltpu.SemaphoreType.REGULAR((2,)),
                dma((SUB,)), dma((2, SUB)), dma((2, SUB)), dma, dma,
                dma((2, 2, 2, SUB)), dma((2, 2, 2, SUB)),
                dma((8,)), dma((8,)),
            ],
            compiler_params=pltpu.CompilerParams(collective_id=0, has_side_effects=True),
            name='qaoa',
        )(cost_local.reshape(shape), gammas, betas)
        energy, state_re, state_im = pl.pallas_call(
            write_out,
            out_shape=(jax.ShapeDtypeStruct((1,), f32),
                       jax.ShapeDtypeStruct(shape, f32), jax.ShapeDtypeStruct(shape, f32)),
            in_specs=[vmem, vmem, vmem],
            out_specs=(hbm, hbm, hbm),
            scratch_shapes=[pltpu.SMEM((1,), f32), dma((3,))],
            name='write_out',
        )(*[pltpu.with_memory_space_constraint(value, pltpu.VMEM) for value in results])
        return energy, state_re.reshape(local_len), state_im.reshape(local_len)

    return jax.shard_map(device_body, mesh=mesh, in_specs=(state_spec, P(), P()),
                         out_specs=(P('inst'), state_spec, state_spec), check_vma=False)
```

```python
import jax
import jax.numpy as jnp
from jax import lax
from jax.experimental import pallas as pl
from jax.experimental.pallas import tpu as pltpu
from jax.sharding import PartitionSpec as P

LANES = 128
LAYERS = 8
SUB = 4
PER_SUB = 8 // SUB
SEND_ORDER = (5, 7, 4, 6, 1, 3, 2)
NEAR = (4, 1)


def rotate(re, im, cos_half, sin_half, steps=None):
    count = len(re)
    for step in steps or [1 << i for i in range(count.bit_length() - 1)]:
        new_re = [cos_half * re[i] + sin_half * im[i ^ step] for i in range(count)]
        new_im = [cos_half * im[i] - sin_half * re[i ^ step] for i in range(count)]
        re, im = new_re, new_im
    return re, im


def sublane_rotate(re, im, cos_half, sin_half):
    row = lax.broadcasted_iota(jnp.int32, (8, LANES), 0)
    for step in (1, 2, 4):
        bit_set = (row & step) != 0

        def flip(value):
            down = pltpu.roll(value, step, 0)
            if step == 4:
                return down
            return jnp.where(bit_set, down, pltpu.roll(value, 8 - step, 0))

        flip_re = [flip(value) for value in re]
        flip_im = [flip(value) for value in im]
        re, im = ([cos_half * r + sin_half * fi for r, fi in zip(re, flip_im)],
                  [cos_half * i - sin_half * fr for i, fr in zip(im, flip_re)])
    return re, im


def lane_matrix(cos_half, sin_half):
    row = lax.broadcasted_iota(jnp.int32, (LANES, LANES), 0)
    col = lax.broadcasted_iota(jnp.int32, (LANES, LANES), 1)
    diff = row ^ col
    cos_full = jnp.broadcast_to(cos_half[0:1], (LANES, LANES))
    sin_full = jnp.broadcast_to(sin_half[0:1], (LANES, LANES))
    mag = jnp.ones((LANES, LANES), jnp.float32)
    weight = jnp.zeros((LANES, LANES), jnp.int32)
    for bit in range(7):
        on = (diff >> bit) & 1
        mag = mag * jnp.where(on == 1, sin_full, cos_full)
        weight = weight + on
    quarter = weight & 3
    zero = jnp.zeros_like(mag)
    real = jnp.where(quarter == 0, mag, jnp.where(quarter == 2, -mag, zero))
    imag = jnp.where(quarter == 1, -mag, jnp.where(quarter == 3, mag, zero))
    return real, imag


def kernel(cost_hbm, gammas_hbm, betas_hbm, energy_all, out_re, out_im,
           cost, cost_near, cost_swap, recv, send, work, cos_buf, sin_buf, cos_near, sin_near,
           rows_in, matrix, energy_part, energy_row, gammas, betas, angle_in, near_in, cost_in, near_send, near_recv, cost_send, cost_recv,
           send_sem, recv_sem, e_send, e_recv):
    qx = lax.axis_index('qx')
    qy = lax.axis_index('qy')
    bits = (qy, qx % 2, qx // 2)

    def flipped(offset):
        return [1 - bit if (offset >> i) & 1 else bit for i, bit in enumerate(bits)]

    def block(offset):
        y, core, x = flipped(offset)
        return (x * 2 + core) * 2 + y

    def peer(offset):
        y, core, x = flipped(offset)
        return {'qy': y, 'qx': x * 2 + core}

    def remote(source, target, send_at, recv_at, offset):
        pltpu.make_async_remote_copy(
            src_ref=source, dst_ref=target, send_sem=send_at, recv_sem=recv_at,
            device_id=peer(offset), device_id_type=pl.DeviceIdType.MESH).start()

    barrier = pltpu.get_barrier_semaphore()

    def signal_next(sem):
        for offset in (4, 1, 2):
            pl.semaphore_signal(sem, inc=1, device_id=peer(offset), device_id_type=pl.DeviceIdType.MESH)

    signal_next(barrier)
    loads = [pltpu.make_async_copy(cost_hbm.at[:, :, :, pl.ds(sub * 8 * PER_SUB, 8 * PER_SUB)],
                                   cost.at[:, :, :, pl.ds(sub * 8 * PER_SUB, 8 * PER_SUB)], cost_in.at[sub])
             for sub in range(SUB)]
    for load in loads:
        load.start()
    angle_loads = [pltpu.make_async_copy(gammas_hbm, gammas, angle_in.at[0]),
                   pltpu.make_async_copy(betas_hbm, betas, angle_in.at[1])]
    for load in angle_loads:
        load.start()
    pl.semaphore_wait(barrier, 3)

    def half_angle(layer):
        angle = jnp.full((8, LANES), 0.5 * betas[layer], jnp.float32)
        return jnp.cos(angle), jnp.sin(angle)

    def wait_bytes(part, sem):
        pltpu.make_async_copy(part, part, sem).wait()

    def wait_all(buffer, sem, at, count):
        wait_bytes(buffer.at[(*at, pl.ds(0, count))], sem.at[at])

    def rows_of(r):
        return pl.ds(pl.multiple_of(r * 8, 8), 8)

    def set_matrix(cos_half, sin_half):
        real, imag = lane_matrix(cos_half, sin_half)
        matrix[0:LANES, 0:LANES] = real
        matrix[0:LANES, LANES:] = imag
        matrix[LANES:, 0:LANES] = -imag
        matrix[LANES:, LANES:] = real

    def put_rows(i, re, im, base=0):
        for o in range(16):
            at = pl.multiple_of(base + o * 16 + i * 8, 8)
            rows_in[pl.ds(at, 8), 0:LANES] = re[o]
            rows_in[pl.ds(at, 8), LANES:] = im[o]

    def lanes(count):
        return lax.dot(rows_in[0:count, :], matrix[...],
                       precision=lax.Precision.HIGHEST, preferred_element_type=jnp.float32)

    def emit(held, mixed, target, a, b, cos_half, sin_half, order, route, local):
        def across(o, buffer):
            def part(r, c):
                at = pl.multiple_of((mixed * 8 + o) * 16 + (r % 2) * 8, 8)
                return work[held, r // 2, pl.ds(at, 8), c * LANES:(c + 1) * LANES]

            re = [part(r, 0) for r in range(8)]
            im = [part(r, 1) for r in range(8)]
            re, im = rotate(re, im, cos_half, sin_half)
            for r in range(8):
                row = (r % PER_SUB) * 8
                buffer[target, a, b, r // PER_SUB, o, 0, row:row + 8, :] = re[r]
                buffer[target, a, b, r // PER_SUB, o, 1, row:row + 8, :] = im[r]

        def body(o, carry):
            across(o, send)
            return carry

        lax.fori_loop(1, 8, body, 0)
        for o in local:
            across(o, recv)
        for sub in range(SUB):
            at = (target, a, b, sub)
            for o in order:
                remote(send.at[(*at, o)], recv.at[(*at, o)], send_sem.at[at], recv_sem.at[at], route(o))

    def first_layer():
        def sub_rows(sub):
            return pl.ds(pl.multiple_of(sub * 8 * PER_SUB, 8), 8 * PER_SUB)

        for sub in range(SUB):
            loads[sub].wait()
            for a in range(2):
                remote(cost.at[:, a, :, sub_rows(sub)], cost_near.at[:, a, :, sub_rows(sub)],
                       near_send.at[a, sub], near_recv.at[a, sub], NEAR[a])
        signal_next(near_in.at[0])
        for load in angle_loads:
            load.wait()
        gamma = gammas[0]
        cos_half, sin_half = half_angle(0)
        set_matrix(cos_half, sin_half)

        def own_trig(r, carry):
            for a in range(2):
                for b in range(2):
                    for o in range(8):
                        angle = gamma * cost[block(o), a, b, rows_of(r), :]
                        cos_buf[a, b * 8 + o, rows_of(r), :] = jnp.cos(angle)
                        sin_buf[a, b * 8 + o, rows_of(r), :] = jnp.sin(angle)
            return carry

        for round_id in range(2):
            lax.fori_loop(4 * round_id, 4 * round_id + 4, own_trig, 0)
            pl.semaphore_wait(near_in.at[round_id], 3)
            if round_id == 0:
                signal_next(near_in.at[1])
        for a in range(2):
            for o in range(1, 8):
                if not o & NEAR[a]:
                    remote(cost.at[block(o), a], cost_swap.at[o, a], cost_send, cost_recv, o)

        def sub_step(sub, carry):
            for a in range(2):
                bit = NEAR[a]
                part = cost_near.at[:, a, :, sub_rows(sub)]
                wait_bytes(part, near_recv.at[a, sub])
                for o in range(1, 8):
                    if not o & bit:
                        remote(cost_near.at[block(o), a, :, sub_rows(sub)],
                               cost_swap.at[o | bit, a, :, sub_rows(sub)], cost_send, cost_recv, o)

                def slots(i, carry):
                    r = sub * PER_SUB + i
                    for b in range(2):
                        for o in range(8):
                            angle = gamma * cost_near[block(o), a, b, rows_of(r), :]
                            cos_near[b * 8 + o] = jnp.cos(angle)
                            sin_near[b * 8 + o] = jnp.sin(angle)
                    re, im = [None] * 16, [None] * 16
                    for b in range(2):
                        for o in range(8):
                            if o & bit:
                                continue
                            here, there = b * 8 + o, b * 8 + (o | bit)
                            for slot, cos_at, sin_at in (
                                    (here, lambda k: cos_buf[a, k, rows_of(r), :], lambda k: sin_buf[a, k, rows_of(r), :]),
                                    (there, lambda k: cos_near[k], lambda k: sin_near[k])):
                                re[slot] = cos_half * cos_at(here) - sin_half * sin_at(there)
                                im[slot] = -(cos_half * sin_at(here)) - sin_half * cos_at(there)
                    re, im = rotate(re, im, cos_half, sin_half, [step for step in (1, 2, 4, 8) if step != bit])
                    re, im = sublane_rotate(re, im, cos_half, sin_half)
                    put_rows(i, re, im, a * 2 * LANES)
                    return carry

                lax.fori_loop(0, PER_SUB, slots, 0)
            rows = lanes(4 * LANES)
            for a in range(2):
                work[a, sub] = rows[a * 2 * LANES:(a + 1) * 2 * LANES]
            return carry

        lax.fori_loop(0, SUB, sub_step, 0)

        def quarters(b, carry):
            for a in range(2):
                bit = NEAR[a]
                emit(a, b, 1, a, b, cos_half, sin_half,
                     [o for o in (3, 6, 7, 1, 4, 5, 2) if o & ~bit], lambda o: o & ~bit, (0, bit))
            return carry

        lax.fori_loop(0, 2, quarters, 0)
        cost_swap[0] = cost[block(0)]
        for a in range(2):
            cost_swap[NEAR[a], a] = cost_near[block(0), a]
        wait_bytes(cost_swap.at[pl.ds(0, 6)], cost_recv)

    def run_layer(layer, odd, arrived, drained):
        source, target = (0, 1) if odd else (1, 0)

        def quarter(held, mixed):
            return (held, mixed) if odd else (mixed, held)

        cos_half, sin_half = half_angle(layer)
        cos_prev, sin_prev = half_angle(layer - 1)
        gamma = gammas[layer]
        set_matrix(cos_half, sin_half)

        def half(held, carry):
            def trig(r, carry):
                for mixed in range(2):
                    for o in range(8):
                        at = (block(o) if odd else o, *quarter(held, mixed), rows_of(r))
                        angle = gamma * (cost if odd else cost_swap)[at]
                        cos_buf[held, mixed * 8 + o, rows_of(r), :] = jnp.cos(angle)
                        sin_buf[held, mixed * 8 + o, rows_of(r), :] = jnp.sin(angle)
                return carry

            lax.fori_loop(0, 8, trig, 0)

            def sub_step(sub, carry):
                for mixed in range(2):
                    wait_all(recv, recv_sem, (source, *quarter(held, mixed), sub), arrived)

                def slots(i, carry):
                    r = sub * PER_SUB + i
                    cos_phase = [cos_buf[held, o, rows_of(r), :] for o in range(16)]
                    sin_phase = [sin_buf[held, o, rows_of(r), :] for o in range(16)]
                    old = [[recv[(source, *quarter(held, mixed), sub, o, c, rows_of(i))]
                            for mixed in range(2) for o in range(8)] for c in range(2)]
                    old_re, old_im = rotate(*old, cos_prev, sin_prev)
                    re = [r * c + i * s for r, i, c, s in zip(old_re, old_im, cos_phase, sin_phase)]
                    im = [i * c - r * s for r, i, c, s in zip(old_re, old_im, cos_phase, sin_phase)]
                    re, im = rotate(re, im, cos_half, sin_half)
                    re, im = sublane_rotate(re, im, cos_half, sin_half)
                    put_rows(i, re, im)
                    return carry

                lax.fori_loop(0, PER_SUB, slots, 0)
                work[held, sub] = lanes(2 * LANES)
                return carry

            lax.fori_loop(0, SUB, sub_step, 0)

            if drained:
                for mixed in range(2):
                    for sub in range(SUB):
                        wait_all(send, send_sem, (target, *quarter(held, mixed), sub), drained)

            def quarters(mixed, carry):
                emit(held, mixed, target, *quarter(held, mixed), cos_half, sin_half, SEND_ORDER, lambda o: o, (0,))
                return carry

            lax.fori_loop(0, 2, quarters, 0)
            return carry

        lax.fori_loop(0, 2, half, 0)

    first_layer()
    run_layer(1, False, 6, 0)
    run_layer(2, True, 7, 6)

    def layer_pair(i, carry):
        run_layer(2 * i + 3, False, 7, 7)
        run_layer(2 * i + 4, True, 7, 7)
        return carry

    lax.fori_loop(0, LAYERS // 2 - 2, layer_pair, 0)
    run_layer(LAYERS - 1, False, 7, 7)

    cos_half, sin_half = half_angle(LAYERS - 1)
    energy_part[...] = jnp.zeros((8, LANES), jnp.float32)

    def slot_gates(a, b, sub, i):
        return rotate(*[[recv[0, a, b, sub, o, c, rows_of(i), :] for o in range(8)] for c in range(2)],
                      cos_half, sin_half)

    def early_half(a, carry):
        def early_sub(sub, carry):
            wait_all(recv, recv_sem, (0, a, 0, sub), 7)

            def slots(i, carry):
                for c, values in enumerate(slot_gates(a, 0, sub, i)):
                    for o in range(8):
                        recv[0, a, 0, sub, o, c, rows_of(i), :] = values[o]
                return carry

            lax.fori_loop(0, PER_SUB, slots, 0)
            return carry

        lax.fori_loop(0, SUB, early_sub, 0)
        return carry

    lax.fori_loop(0, 2, early_half, 0)

    def final_half(a, carry):
        def final_sub(sub, carry):
            wait_all(recv, recv_sem, (0, a, 1, sub), 7)

            def slots(i, carry):
                r = sub * PER_SUB + i
                re, im = slot_gates(a, 1, sub, i)
                terms = []
                for o in range(8):
                    early = [recv[0, a, 0, sub, o, c, rows_of(i), :] for c in range(2)]
                    pair_re, pair_im = rotate([early[0], re[o]], [early[1], im[o]], cos_half, sin_half)
                    for b in range(2):
                        at = (block(o), a, b, rows_of(r))
                        x, y = pair_re[b], pair_im[b]
                        out_re[at] = x
                        out_im[at] = y
                        terms.append(cost[at] * (x * x + y * y))
                while len(terms) > 1:
                    terms = [terms[k] + terms[k + 1] for k in range(0, len(terms), 2)]
                energy_part[...] = energy_part[...] + terms[0]
                return carry

            lax.fori_loop(0, PER_SUB, slots, 0, unroll=True)
            return carry

        lax.fori_loop(0, SUB, final_sub, 0)
        return carry

    lax.fori_loop(0, 2, final_half, 0)

    me = block(0)
    energy_row[...] = jnp.sum(energy_part[...], axis=0, keepdims=True)
    energy_all[me] = energy_row[...]

    def drain(par):
        for a in range(2):
            for b in range(2):
                for sub in range(SUB):
                    wait_all(send, send_sem, (par, a, b, sub), 7)

    for a in range(2):
        for sub in range(SUB):
            wait_bytes(cost.at[:, a, :, pl.ds(sub * 8 * PER_SUB, 8 * PER_SUB)], near_send.at[a, sub])
    wait_bytes(cost_swap.at[pl.ds(0, 6)], cost_send)
    for offset in (7, 5, 6, 4, 3, 1, 2):
        remote(energy_row, energy_all.at[me], e_send.at[offset], e_recv.at[offset], offset)
    drain(0)
    drain(1)
    for offset in range(1, 8):
        wait_bytes(energy_row, e_send.at[offset])
        wait_bytes(energy_row, e_recv.at[offset])


def write_out(energy_all, in_re, in_im, energy, out_re, out_im, value, sem):
    copies = [pltpu.make_async_copy(in_re, out_re, sem.at[0]), pltpu.make_async_copy(in_im, out_im, sem.at[1])]
    for copy in copies:
        copy.start()
    total = energy_all[0]
    for i in range(1, 8):
        total = total + energy_all[i]
    value[0] = jnp.sum(total) * (1.0 / (1 << 21))
    copies.append(pltpu.make_async_copy(value, energy, sem.at[2]))
    copies[2].start()
    for copy in copies:
        copy.wait()


def solution(mesh):
    state_spec = P(('inst', 'qx', 'qy'))

    def device_body(cost_local, gammas, betas):
        local_len = cost_local.shape[0]
        shape = (8, 2, 2, local_len // (32 * LANES), LANES)
        f32 = jnp.float32
        vmem = pl.BlockSpec(memory_space=pltpu.VMEM)
        dma = pltpu.SemaphoreType.DMA
        parts = (2, 2, 2, SUB, 8, 2, 8 * PER_SUB, LANES)
        hbm = pl.BlockSpec(memory_space=pl.ANY)
        results = pl.pallas_call(
            kernel,
            out_shape=(pltpu.VMEM((8, 1, LANES), f32), pltpu.VMEM(shape, f32), pltpu.VMEM(shape, f32)),
            in_specs=[hbm, hbm, hbm],
            out_specs=(vmem, vmem, vmem),
            scratch_shapes=[
                pltpu.VMEM(shape, f32), pltpu.VMEM(shape, f32), pltpu.VMEM(shape, f32),
                pltpu.VMEM(parts, f32), pltpu.VMEM(parts, f32),
                pltpu.VMEM((2, 4, 2 * LANES, 2 * LANES), f32),
                pltpu.VMEM((2, 16, 64, LANES), f32), pltpu.VMEM((2, 16, 64, LANES), f32),
                pltpu.VMEM((16, 8, LANES), f32), pltpu.VMEM((16, 8, LANES), f32),
                pltpu.VMEM((4 * LANES, 2 * LANES), f32), pltpu.VMEM((2 * LANES, 2 * LANES), f32),
                pltpu.VMEM((8, LANES), f32), pltpu.VMEM((1, LANES), f32),
                pltpu.SMEM((LAYERS,), f32), pltpu.SMEM((LAYERS,), f32), dma((2,)), pltpu.SemaphoreType.REGULAR((2,)),
                dma((SUB,)), dma((2, SUB)), dma((2, SUB)), dma, dma,
                dma((2, 2, 2, SUB)), dma((2, 2, 2, SUB)),
                dma((8,)), dma((8,)),
            ],
            compiler_params=pltpu.CompilerParams(collective_id=0, has_side_effects=True),
            name='qaoa',
        )(cost_local.reshape(shape), gammas, betas)
        energy, state_re, state_im = pl.pallas_call(
            write_out,
            out_shape=(jax.ShapeDtypeStruct((1,), f32),
                       jax.ShapeDtypeStruct(shape, f32), jax.ShapeDtypeStruct(shape, f32)),
            in_specs=[vmem, vmem, vmem],
            out_specs=(hbm, hbm, hbm),
            scratch_shapes=[pltpu.SMEM((1,), f32), dma((3,))],
            name='write_out',
        )(*[pltpu.with_memory_space_constraint(value, pltpu.VMEM) for value in results])
        return energy, state_re.reshape(local_len), state_im.reshape(local_len)

    return jax.shard_map(device_body, mesh=mesh, in_specs=(state_spec, P(), P()),
                         out_specs=(P('inst'), state_spec, state_spec), check_vma=False)
```

```python
import jax
import jax.numpy as jnp
from jax import lax
from jax.experimental import pallas as pl
from jax.experimental.pallas import tpu as pltpu
from jax.sharding import PartitionSpec as P

LANES = 128
LAYERS = 8
SUB = 4
PER_SUB = 8 // SUB
SEND_ORDER = (5, 7, 4, 6, 1, 3, 2)
NEAR = (4, 1)


def rotate(re, im, cos_half, sin_half, steps=None):
    count = len(re)
    for step in steps or [1 << i for i in range(count.bit_length() - 1)]:
        new_re = [cos_half * re[i] + sin_half * im[i ^ step] for i in range(count)]
        new_im = [cos_half * im[i] - sin_half * re[i ^ step] for i in range(count)]
        re, im = new_re, new_im
    return re, im


def sublane_rotate(re, im, cos_half, sin_half):
    row = lax.broadcasted_iota(jnp.int32, (8, LANES), 0)
    for step in (1, 2, 4):
        bit_set = (row & step) != 0

        def flip(value):
            down = pltpu.roll(value, step, 0)
            if step == 4:
                return down
            return jnp.where(bit_set, down, pltpu.roll(value, 8 - step, 0))

        flip_re = [flip(value) for value in re]
        flip_im = [flip(value) for value in im]
        re, im = ([cos_half * r + sin_half * fi for r, fi in zip(re, flip_im)],
                  [cos_half * i - sin_half * fr for i, fr in zip(im, flip_re)])
    return re, im


def lane_matrix(cos_half, sin_half):
    row = lax.broadcasted_iota(jnp.int32, (LANES, LANES), 0)
    col = lax.broadcasted_iota(jnp.int32, (LANES, LANES), 1)
    diff = row ^ col
    cos_full = jnp.broadcast_to(cos_half[0:1], (LANES, LANES))
    sin_full = jnp.broadcast_to(sin_half[0:1], (LANES, LANES))
    mag = jnp.ones((LANES, LANES), jnp.float32)
    weight = jnp.zeros((LANES, LANES), jnp.int32)
    for bit in range(7):
        on = (diff >> bit) & 1
        mag = mag * jnp.where(on == 1, sin_full, cos_full)
        weight = weight + on
    quarter = weight & 3
    zero = jnp.zeros_like(mag)
    real = jnp.where(quarter == 0, mag, jnp.where(quarter == 2, -mag, zero))
    imag = jnp.where(quarter == 1, -mag, jnp.where(quarter == 3, mag, zero))
    return real, imag


def kernel(cost_hbm, gammas_hbm, betas_hbm, energy_all, out_re, out_im,
           cost, cost_near, cost_swap, recv, send, work, cos_buf, sin_buf, cos_near, sin_near,
           rows_in, matrix, energy_part, energy_row, gammas, betas, angle_in, near_in, cost_in, near_send, near_recv, cost_send, cost_recv,
           send_sem, recv_sem, e_send, e_recv):
    qx = lax.axis_index('qx')
    qy = lax.axis_index('qy')
    bits = (qy, qx % 2, qx // 2)

    def flipped(offset):
        return [1 - bit if (offset >> i) & 1 else bit for i, bit in enumerate(bits)]

    def block(offset):
        y, core, x = flipped(offset)
        return (x * 2 + core) * 2 + y

    def peer(offset):
        y, core, x = flipped(offset)
        return {'qy': y, 'qx': x * 2 + core}

    def remote(source, target, send_at, recv_at, offset):
        pltpu.make_async_remote_copy(
            src_ref=source, dst_ref=target, send_sem=send_at, recv_sem=recv_at,
            device_id=peer(offset), device_id_type=pl.DeviceIdType.MESH).start()

    barrier = pltpu.get_barrier_semaphore()

    def signal_next(sem):
        for offset in (4, 1, 2):
            pl.semaphore_signal(sem, inc=1, device_id=peer(offset), device_id_type=pl.DeviceIdType.MESH)

    signal_next(barrier)
    loads = [pltpu.make_async_copy(cost_hbm.at[:, :, :, pl.ds(sub * 8 * PER_SUB, 8 * PER_SUB)],
                                   cost.at[:, :, :, pl.ds(sub * 8 * PER_SUB, 8 * PER_SUB)], cost_in.at[sub])
             for sub in range(SUB)]
    for load in loads:
        load.start()
    angle_loads = [pltpu.make_async_copy(gammas_hbm, gammas, angle_in.at[0]),
                   pltpu.make_async_copy(betas_hbm, betas, angle_in.at[1])]
    for load in angle_loads:
        load.start()
    pl.semaphore_wait(barrier, 3)

    def half_angle(layer):
        angle = jnp.full((8, LANES), 0.5 * betas[layer], jnp.float32)
        return jnp.cos(angle), jnp.sin(angle)

    def wait_bytes(part, sem):
        pltpu.make_async_copy(part, part, sem).wait()

    def wait_all(buffer, sem, at, count):
        wait_bytes(buffer.at[(*at, pl.ds(0, count))], sem.at[at])

    def rows_of(r):
        return pl.ds(pl.multiple_of(r * 8, 8), 8)

    def set_matrix(cos_half, sin_half):
        real, imag = lane_matrix(cos_half, sin_half)
        matrix[0:LANES, 0:LANES] = real
        matrix[0:LANES, LANES:] = imag
        matrix[LANES:, 0:LANES] = -imag
        matrix[LANES:, LANES:] = real

    def put_rows(i, re, im, base=0):
        for o in range(16):
            at = pl.multiple_of(base + o * 16 + i * 8, 8)
            rows_in[pl.ds(at, 8), 0:LANES] = re[o]
            rows_in[pl.ds(at, 8), LANES:] = im[o]

    def lanes(count):
        return lax.dot(rows_in[0:count, :], matrix[...],
                       precision=lax.Precision.HIGHEST, preferred_element_type=jnp.float32)

    def emit(held, mixed, target, a, b, cos_half, sin_half, order, route, local):
        def across(o, buffer):
            def part(r, c):
                at = pl.multiple_of((mixed * 8 + o) * 16 + (r % 2) * 8, 8)
                return work[held, r // 2, pl.ds(at, 8), c * LANES:(c + 1) * LANES]

            re = [part(r, 0) for r in range(8)]
            im = [part(r, 1) for r in range(8)]
            re, im = rotate(re, im, cos_half, sin_half)
            for r in range(8):
                row = (r % PER_SUB) * 8
                buffer[target, a, b, r // PER_SUB, o, 0, row:row + 8, :] = re[r]
                buffer[target, a, b, r // PER_SUB, o, 1, row:row + 8, :] = im[r]

        def body(o, carry):
            across(o, send)
            return carry

        lax.fori_loop(1, 8, body, 0)
        for o in local:
            across(o, recv)
        for sub in range(SUB):
            at = (target, a, b, sub)
            for o in order:
                remote(send.at[(*at, o)], recv.at[(*at, o)], send_sem.at[at], recv_sem.at[at], route(o))

    def first_layer():
        def sub_rows(sub):
            return pl.ds(pl.multiple_of(sub * 8 * PER_SUB, 8), 8 * PER_SUB)

        for sub in range(SUB):
            loads[sub].wait()
            for a in range(2):
                remote(cost.at[:, a, :, sub_rows(sub)], cost_near.at[:, a, :, sub_rows(sub)],
                       near_send.at[a, sub], near_recv.at[a, sub], NEAR[a])
        signal_next(near_in.at[0])
        for load in angle_loads:
            load.wait()
        gamma = gammas[0]
        cos_half, sin_half = half_angle(0)
        set_matrix(cos_half, sin_half)

        def own_trig(r, carry):
            for a in range(2):
                for b in range(2):
                    for o in range(8):
                        angle = gamma * cost[block(o), a, b, rows_of(r), :]
                        cos_buf[a, b * 8 + o, rows_of(r), :] = jnp.cos(angle)
                        sin_buf[a, b * 8 + o, rows_of(r), :] = jnp.sin(angle)
            return carry

        for round_id in range(2):
            lax.fori_loop(4 * round_id, 4 * round_id + 4, own_trig, 0)
            pl.semaphore_wait(near_in.at[round_id], 3)
            if round_id == 0:
                signal_next(near_in.at[1])
        for a in range(2):
            for o in range(1, 8):
                if not o & NEAR[a]:
                    remote(cost.at[block(o), a], cost_swap.at[o, a], cost_send, cost_recv, o)

        def sub_step(sub, carry):
            for a in range(2):
                bit = NEAR[a]
                part = cost_near.at[:, a, :, sub_rows(sub)]
                wait_bytes(part, near_recv.at[a, sub])
                @pl.when(sub % 2 == 1)
                def _():
                    rows = pl.ds(pl.multiple_of((sub - 1) * 8 * PER_SUB, 8), 16 * PER_SUB)
                    for o in range(1, 8):
                        if not o & bit:
                            remote(cost_near.at[block(o), a, :, rows], cost_swap.at[o | bit, a, :, rows],
                                   cost_send, cost_recv, o)

                def slots(i, carry):
                    r = sub * PER_SUB + i
                    for b in range(2):
                        for o in range(8):
                            angle = gamma * cost_near[block(o), a, b, rows_of(r), :]
                            cos_near[b * 8 + o] = jnp.cos(angle)
                            sin_near[b * 8 + o] = jnp.sin(angle)
                    re, im = [None] * 16, [None] * 16
                    for b in range(2):
                        for o in range(8):
                            if o & bit:
                                continue
                            here, there = b * 8 + o, b * 8 + (o | bit)
                            for slot, cos_at, sin_at in (
                                    (here, lambda k: cos_buf[a, k, rows_of(r), :], lambda k: sin_buf[a, k, rows_of(r), :]),
                                    (there, lambda k: cos_near[k], lambda k: sin_near[k])):
                                re[slot] = cos_half * cos_at(here) - sin_half * sin_at(there)
                                im[slot] = -(cos_half * sin_at(here)) - sin_half * cos_at(there)
                    re, im = rotate(re, im, cos_half, sin_half, [step for step in (1, 2, 4, 8) if step != bit])
                    re, im = sublane_rotate(re, im, cos_half, sin_half)
                    put_rows(i, re, im, a * 2 * LANES)
                    return carry

                lax.fori_loop(0, PER_SUB, slots, 0)
            rows = lanes(4 * LANES)
            for a in range(2):
                work[a, sub] = rows[a * 2 * LANES:(a + 1) * 2 * LANES]
            return carry

        lax.fori_loop(0, SUB, sub_step, 0)

        def quarters(b, carry):
            for a in range(2):
                bit = NEAR[a]
                emit(a, b, 1, a, b, cos_half, sin_half,
                     [o for o in (3, 6, 7, 1, 4, 5, 2) if o & ~bit], lambda o: o & ~bit, (0, bit))
            return carry

        lax.fori_loop(0, 2, quarters, 0)
        cost_swap[0] = cost[block(0)]
        for a in range(2):
            cost_swap[NEAR[a], a] = cost_near[block(0), a]
        wait_bytes(cost_swap.at[pl.ds(0, 6)], cost_recv)

    def run_layer(layer, odd, arrived, drained):
        source, target = (0, 1) if odd else (1, 0)

        def quarter(held, mixed):
            return (held, mixed) if odd else (mixed, held)

        cos_half, sin_half = half_angle(layer)
        cos_prev, sin_prev = half_angle(layer - 1)
        gamma = gammas[layer]
        set_matrix(cos_half, sin_half)

        def half(held, carry):
            def trig(r, carry):
                for mixed in range(2):
                    for o in range(8):
                        at = (block(o) if odd else o, *quarter(held, mixed), rows_of(r))
                        angle = gamma * (cost if odd else cost_swap)[at]
                        cos_buf[held, mixed * 8 + o, rows_of(r), :] = jnp.cos(angle)
                        sin_buf[held, mixed * 8 + o, rows_of(r), :] = jnp.sin(angle)
                return carry

            lax.fori_loop(0, 8, trig, 0)

            def sub_step(sub, carry):
                for mixed in range(2):
                    wait_all(recv, recv_sem, (source, *quarter(held, mixed), sub), arrived)

                def slots(i, carry):
                    r = sub * PER_SUB + i
                    cos_phase = [cos_buf[held, o, rows_of(r), :] for o in range(16)]
                    sin_phase = [sin_buf[held, o, rows_of(r), :] for o in range(16)]
                    old = [[recv[(source, *quarter(held, mixed), sub, o, c, rows_of(i))]
                            for mixed in range(2) for o in range(8)] for c in range(2)]
                    old_re, old_im = rotate(*old, cos_prev, sin_prev)
                    re = [r * c + i * s for r, i, c, s in zip(old_re, old_im, cos_phase, sin_phase)]
                    im = [i * c - r * s for r, i, c, s in zip(old_re, old_im, cos_phase, sin_phase)]
                    re, im = rotate(re, im, cos_half, sin_half)
                    re, im = sublane_rotate(re, im, cos_half, sin_half)
                    put_rows(i, re, im)
                    return carry

                lax.fori_loop(0, PER_SUB, slots, 0)
                work[held, sub] = lanes(2 * LANES)
                return carry

            lax.fori_loop(0, SUB, sub_step, 0)

            if drained:
                for mixed in range(2):
                    for sub in range(SUB):
                        wait_all(send, send_sem, (target, *quarter(held, mixed), sub), drained)

            def quarters(mixed, carry):
                emit(held, mixed, target, *quarter(held, mixed), cos_half, sin_half, SEND_ORDER, lambda o: o, (0,))
                return carry

            lax.fori_loop(0, 2, quarters, 0)
            return carry

        lax.fori_loop(0, 2, half, 0)

    first_layer()
    run_layer(1, False, 6, 0)
    run_layer(2, True, 7, 6)

    def layer_pair(i, carry):
        run_layer(2 * i + 3, False, 7, 7)
        run_layer(2 * i + 4, True, 7, 7)
        return carry

    lax.fori_loop(0, LAYERS // 2 - 2, layer_pair, 0)
    run_layer(LAYERS - 1, False, 7, 7)

    cos_half, sin_half = half_angle(LAYERS - 1)
    energy_part[...] = jnp.zeros((8, LANES), jnp.float32)

    def slot_gates(a, b, sub, i):
        return rotate(*[[recv[0, a, b, sub, o, c, rows_of(i), :] for o in range(8)] for c in range(2)],
                      cos_half, sin_half)

    def early_half(a, carry):
        def early_sub(sub, carry):
            wait_all(recv, recv_sem, (0, a, 0, sub), 7)

            def slots(i, carry):
                for c, values in enumerate(slot_gates(a, 0, sub, i)):
                    for o in range(8):
                        recv[0, a, 0, sub, o, c, rows_of(i), :] = values[o]
                return carry

            lax.fori_loop(0, PER_SUB, slots, 0)
            return carry

        lax.fori_loop(0, SUB, early_sub, 0)
        return carry

    lax.fori_loop(0, 2, early_half, 0)

    def final_half(a, carry):
        def final_sub(sub, carry):
            wait_all(recv, recv_sem, (0, a, 1, sub), 7)

            def slots(i, carry):
                r = sub * PER_SUB + i
                re, im = slot_gates(a, 1, sub, i)
                total = energy_part[...]
                for o in range(8):
                    early = [recv[0, a, 0, sub, o, c, rows_of(i), :] for c in range(2)]
                    pair_re, pair_im = rotate([early[0], re[o]], [early[1], im[o]], cos_half, sin_half)
                    for b in range(2):
                        at = (block(o), a, b, rows_of(r))
                        x, y = pair_re[b], pair_im[b]
                        out_re[at] = x
                        out_im[at] = y
                        total = total + cost[at] * (x * x + y * y)
                energy_part[...] = total
                return carry

            lax.fori_loop(0, PER_SUB, slots, 0, unroll=True)
            return carry

        lax.fori_loop(0, SUB, final_sub, 0)
        return carry

    lax.fori_loop(0, 2, final_half, 0)

    me = block(0)
    energy_row[...] = jnp.sum(energy_part[...], axis=0, keepdims=True)
    energy_all[me] = energy_row[...]

    def drain(par):
        for a in range(2):
            for b in range(2):
                for sub in range(SUB):
                    wait_all(send, send_sem, (par, a, b, sub), 7)

    for a in range(2):
        for sub in range(SUB):
            wait_bytes(cost.at[:, a, :, pl.ds(sub * 8 * PER_SUB, 8 * PER_SUB)], near_send.at[a, sub])
    wait_bytes(cost_swap.at[pl.ds(0, 6)], cost_send)
    for offset in (7, 5, 6, 4, 3, 1, 2):
        remote(energy_row, energy_all.at[me], e_send.at[offset], e_recv.at[offset], offset)
    drain(0)
    drain(1)
    for offset in range(1, 8):
        wait_bytes(energy_row, e_send.at[offset])
        wait_bytes(energy_row, e_recv.at[offset])


def write_out(energy_all, in_re, in_im, energy, out_re, out_im, value, sem):
    copies = [pltpu.make_async_copy(in_re, out_re, sem.at[0]), pltpu.make_async_copy(in_im, out_im, sem.at[1])]
    for copy in copies:
        copy.start()
    total = energy_all[0]
    for i in range(1, 8):
        total = total + energy_all[i]
    value[0] = jnp.sum(total) * (1.0 / (1 << 21))
    copies.append(pltpu.make_async_copy(value, energy, sem.at[2]))
    copies[2].start()
    for copy in copies:
        copy.wait()


def solution(mesh):
    state_spec = P(('inst', 'qx', 'qy'))

    def device_body(cost_local, gammas, betas):
        local_len = cost_local.shape[0]
        shape = (8, 2, 2, local_len // (32 * LANES), LANES)
        f32 = jnp.float32
        vmem = pl.BlockSpec(memory_space=pltpu.VMEM)
        dma = pltpu.SemaphoreType.DMA
        parts = (2, 2, 2, SUB, 8, 2, 8 * PER_SUB, LANES)
        hbm = pl.BlockSpec(memory_space=pl.ANY)
        results = pl.pallas_call(
            kernel,
            out_shape=(pltpu.VMEM((8, 1, LANES), f32), pltpu.VMEM(shape, f32), pltpu.VMEM(shape, f32)),
            in_specs=[hbm, hbm, hbm],
            out_specs=(vmem, vmem, vmem),
            scratch_shapes=[
                pltpu.VMEM(shape, f32), pltpu.VMEM(shape, f32), pltpu.VMEM(shape, f32),
                pltpu.VMEM(parts, f32), pltpu.VMEM(parts, f32),
                pltpu.VMEM((2, 4, 2 * LANES, 2 * LANES), f32),
                pltpu.VMEM((2, 16, 64, LANES), f32), pltpu.VMEM((2, 16, 64, LANES), f32),
                pltpu.VMEM((16, 8, LANES), f32), pltpu.VMEM((16, 8, LANES), f32),
                pltpu.VMEM((4 * LANES, 2 * LANES), f32), pltpu.VMEM((2 * LANES, 2 * LANES), f32),
                pltpu.VMEM((8, LANES), f32), pltpu.VMEM((1, LANES), f32),
                pltpu.SMEM((LAYERS,), f32), pltpu.SMEM((LAYERS,), f32), dma((2,)), pltpu.SemaphoreType.REGULAR((2,)),
                dma((SUB,)), dma((2, SUB)), dma((2, SUB)), dma, dma,
                dma((2, 2, 2, SUB)), dma((2, 2, 2, SUB)),
                dma((8,)), dma((8,)),
            ],
            compiler_params=pltpu.CompilerParams(collective_id=0, has_side_effects=True),
            name='qaoa',
        )(cost_local.reshape(shape), gammas, betas)
        energy, state_re, state_im = pl.pallas_call(
            write_out,
            out_shape=(jax.ShapeDtypeStruct((1,), f32),
                       jax.ShapeDtypeStruct(shape, f32), jax.ShapeDtypeStruct(shape, f32)),
            in_specs=[vmem, vmem, vmem],
            out_specs=(hbm, hbm, hbm),
            scratch_shapes=[pltpu.SMEM((1,), f32), dma((3,))],
            name='write_out',
        )(*[pltpu.with_memory_space_constraint(value, pltpu.VMEM) for value in results])
        return energy, state_re.reshape(local_len), state_im.reshape(local_len)

    return jax.shard_map(device_body, mesh=mesh, in_specs=(state_spec, P(), P()),
                         out_specs=(P('inst'), state_spec, state_spec), check_vma=False)
```

```python
import jax
import jax.numpy as jnp
from jax import lax
from jax.experimental import pallas as pl
from jax.experimental.pallas import tpu as pltpu
from jax.sharding import PartitionSpec as P

LANES = 128
LAYERS = 8
SUB = 4
PER_SUB = 8 // SUB
SEND_ORDER = (5, 7, 4, 6, 1, 3, 2)
NEAR = (4, 1)


def rotate(re, im, cos_half, sin_half, steps=None):
    count = len(re)
    for step in steps or [1 << i for i in range(count.bit_length() - 1)]:
        new_re = [cos_half * re[i] + sin_half * im[i ^ step] for i in range(count)]
        new_im = [cos_half * im[i] - sin_half * re[i ^ step] for i in range(count)]
        re, im = new_re, new_im
    return re, im


def sublane_rotate(re, im, cos_half, sin_half):
    row = lax.broadcasted_iota(jnp.int32, (8, LANES), 0)
    for step in (1, 2, 4):
        bit_set = (row & step) != 0

        def flip(value):
            down = pltpu.roll(value, step, 0)
            if step == 4:
                return down
            return jnp.where(bit_set, down, pltpu.roll(value, 8 - step, 0))

        flip_re = [flip(value) for value in re]
        flip_im = [flip(value) for value in im]
        re, im = ([cos_half * r + sin_half * fi for r, fi in zip(re, flip_im)],
                  [cos_half * i - sin_half * fr for i, fr in zip(im, flip_re)])
    return re, im


def lane_matrix(cos_half, sin_half):
    row = lax.broadcasted_iota(jnp.int32, (LANES, LANES), 0)
    col = lax.broadcasted_iota(jnp.int32, (LANES, LANES), 1)
    diff = row ^ col
    cos_full = jnp.broadcast_to(cos_half[0:1], (LANES, LANES))
    sin_full = jnp.broadcast_to(sin_half[0:1], (LANES, LANES))
    mag = jnp.ones((LANES, LANES), jnp.float32)
    weight = jnp.zeros((LANES, LANES), jnp.int32)
    for bit in range(7):
        on = (diff >> bit) & 1
        mag = mag * jnp.where(on == 1, sin_full, cos_full)
        weight = weight + on
    quarter = weight & 3
    zero = jnp.zeros_like(mag)
    real = jnp.where(quarter == 0, mag, jnp.where(quarter == 2, -mag, zero))
    imag = jnp.where(quarter == 1, -mag, jnp.where(quarter == 3, mag, zero))
    return real, imag


def kernel(cost_hbm, gammas_hbm, betas_hbm, energy_all, out_re, out_im,
           cost, cost_near, cost_swap, recv, send, work, cos_buf, sin_buf, cos_near, sin_near,
           rows_in, matrix, energy_part, energy_row, gammas, betas, angle_in, near_in, cost_in, near_send, near_recv, cost_send, cost_recv,
           send_sem, recv_sem, e_send, e_recv):
    qx = lax.axis_index('qx')
    qy = lax.axis_index('qy')
    bits = (qy, qx % 2, qx // 2)

    def flipped(offset):
        return [1 - bit if (offset >> i) & 1 else bit for i, bit in enumerate(bits)]

    def block(offset):
        y, core, x = flipped(offset)
        return (x * 2 + core) * 2 + y

    def peer(offset):
        y, core, x = flipped(offset)
        return {'qy': y, 'qx': x * 2 + core}

    def remote(source, target, send_at, recv_at, offset):
        pltpu.make_async_remote_copy(
            src_ref=source, dst_ref=target, send_sem=send_at, recv_sem=recv_at,
            device_id=peer(offset), device_id_type=pl.DeviceIdType.MESH).start()

    barrier = pltpu.get_barrier_semaphore()

    def signal_next(sem):
        for offset in (4, 1, 2):
            pl.semaphore_signal(sem, inc=1, device_id=peer(offset), device_id_type=pl.DeviceIdType.MESH)

    signal_next(barrier)
    loads = [pltpu.make_async_copy(cost_hbm.at[:, :, :, pl.ds(sub * 8 * PER_SUB, 8 * PER_SUB)],
                                   cost.at[:, :, :, pl.ds(sub * 8 * PER_SUB, 8 * PER_SUB)], cost_in.at[sub])
             for sub in range(SUB)]
    for load in loads:
        load.start()
    angle_loads = [pltpu.make_async_copy(gammas_hbm, gammas, angle_in.at[0]),
                   pltpu.make_async_copy(betas_hbm, betas, angle_in.at[1])]
    for load in angle_loads:
        load.start()
    pl.semaphore_wait(barrier, 3)

    def half_angle(layer):
        angle = jnp.full((8, LANES), 0.5 * betas[layer], jnp.float32)
        return jnp.cos(angle), jnp.sin(angle)

    def wait_bytes(part, sem):
        pltpu.make_async_copy(part, part, sem).wait()

    def wait_all(buffer, sem, at, count):
        wait_bytes(buffer.at[(*at, pl.ds(0, count))], sem.at[at])

    def rows_of(r):
        return pl.ds(pl.multiple_of(r * 8, 8), 8)

    def set_matrix(cos_half, sin_half):
        real, imag = lane_matrix(cos_half, sin_half)
        matrix[0:LANES, 0:LANES] = real
        matrix[0:LANES, LANES:] = imag
        matrix[LANES:, 0:LANES] = -imag
        matrix[LANES:, LANES:] = real

    def put_rows(i, re, im, base=0):
        for o in range(16):
            at = pl.multiple_of(base + o * 16 + i * 8, 8)
            rows_in[pl.ds(at, 8), 0:LANES] = re[o]
            rows_in[pl.ds(at, 8), LANES:] = im[o]

    def lanes(count):
        return lax.dot(rows_in[0:count, :], matrix[...],
                       precision=lax.Precision.HIGHEST, preferred_element_type=jnp.float32)

    def emit(held, mixed, target, a, b, cos_half, sin_half, order, route, local):
        def across(o, buffer):
            def part(r, c):
                at = pl.multiple_of((mixed * 8 + o) * 16 + (r % 2) * 8, 8)
                return work[held, r // 2, pl.ds(at, 8), c * LANES:(c + 1) * LANES]

            re = [part(r, 0) for r in range(8)]
            im = [part(r, 1) for r in range(8)]
            re, im = rotate(re, im, cos_half, sin_half)
            for r in range(8):
                row = (r % PER_SUB) * 8
                buffer[target, a, b, r // PER_SUB, o, 0, row:row + 8, :] = re[r]
                buffer[target, a, b, r // PER_SUB, o, 1, row:row + 8, :] = im[r]

        def body(o, carry):
            across(o, send)
            return carry

        lax.fori_loop(1, 8, body, 0)
        for o in local:
            across(o, recv)
        for sub in range(SUB):
            at = (target, a, b, sub)
            for o in order:
                remote(send.at[(*at, o)], recv.at[(*at, o)], send_sem.at[at], recv_sem.at[at], route(o))

    def first_layer():
        def sub_rows(sub):
            return pl.ds(pl.multiple_of(sub * 8 * PER_SUB, 8), 8 * PER_SUB)

        for sub in range(SUB):
            loads[sub].wait()
            for a in range(2):
                remote(cost.at[:, a, :, sub_rows(sub)], cost_near.at[:, a, :, sub_rows(sub)],
                       near_send.at[a, sub], near_recv.at[a, sub], NEAR[a])
        signal_next(near_in.at[0])
        for load in angle_loads:
            load.wait()
        gamma = gammas[0]
        cos_half, sin_half = half_angle(0)
        set_matrix(cos_half, sin_half)

        def own_trig(r, carry):
            for a in range(2):
                for b in range(2):
                    for o in range(8):
                        angle = gamma * cost[block(o), a, b, rows_of(r), :]
                        cos_buf[a, b * 8 + o, rows_of(r), :] = jnp.cos(angle)
                        sin_buf[a, b * 8 + o, rows_of(r), :] = jnp.sin(angle)
            return carry

        for round_id in range(2):
            lax.fori_loop(4 * round_id, 4 * round_id + 4, own_trig, 0)
            pl.semaphore_wait(near_in.at[round_id], 3)
            if round_id == 0:
                signal_next(near_in.at[1])
        for a in range(2):
            for o in range(1, 8):
                if not o & NEAR[a]:
                    remote(cost.at[block(o), a], cost_swap.at[o, a], cost_send, cost_recv, o)

        def sub_step(sub, carry):
            for a in range(2):
                bit = NEAR[a]
                part = cost_near.at[:, a, :, sub_rows(sub)]
                wait_bytes(part, near_recv.at[a, sub])
                for o in range(1, 8):
                    if not o & bit:
                        remote(cost_near.at[block(o), a, :, sub_rows(sub)],
                               cost_swap.at[o | bit, a, :, sub_rows(sub)], cost_send, cost_recv, o)

                def slots(i, carry):
                    r = sub * PER_SUB + i
                    for b in range(2):
                        for o in range(8):
                            angle = gamma * cost_near[block(o), a, b, rows_of(r), :]
                            cos_near[b * 8 + o] = jnp.cos(angle)
                            sin_near[b * 8 + o] = jnp.sin(angle)
                    re, im = [None] * 16, [None] * 16
                    for b in range(2):
                        for o in range(8):
                            if o & bit:
                                continue
                            here, there = b * 8 + o, b * 8 + (o | bit)
                            for slot, cos_at, sin_at in (
                                    (here, lambda k: cos_buf[a, k, rows_of(r), :], lambda k: sin_buf[a, k, rows_of(r), :]),
                                    (there, lambda k: cos_near[k], lambda k: sin_near[k])):
                                re[slot] = cos_half * cos_at(here) - sin_half * sin_at(there)
                                im[slot] = -(cos_half * sin_at(here)) - sin_half * cos_at(there)
                    re, im = rotate(re, im, cos_half, sin_half, [step for step in (1, 2, 4, 8) if step != bit])
                    re, im = sublane_rotate(re, im, cos_half, sin_half)
                    put_rows(i, re, im, a * 2 * LANES)
                    return carry

                lax.fori_loop(0, PER_SUB, slots, 0)
            rows = lanes(4 * LANES)
            for a in range(2):
                work[a, sub] = rows[a * 2 * LANES:(a + 1) * 2 * LANES]
            return carry

        lax.fori_loop(0, SUB, sub_step, 0)

        def quarters(b, carry):
            for a in range(2):
                bit = NEAR[a]
                emit(a, b, 1, a, b, cos_half, sin_half,
                     [o for o in (3, 6, 7, 1, 4, 5, 2) if o & ~bit], lambda o: o & ~bit, (0, bit))
            return carry

        lax.fori_loop(0, 2, quarters, 0)
        cost_swap[0] = cost[block(0)]
        for a in range(2):
            cost_swap[NEAR[a], a] = cost_near[block(0), a]
        wait_bytes(cost_swap.at[pl.ds(0, 6)], cost_recv)

    def run_layer(layer, odd, arrived, drained):
        source, target = (0, 1) if odd else (1, 0)

        def quarter(held, mixed):
            return (held, mixed) if odd else (mixed, held)

        cos_half, sin_half = half_angle(layer)
        cos_prev, sin_prev = half_angle(layer - 1)
        gamma = gammas[layer]
        set_matrix(cos_half, sin_half)

        def half(held, carry):
            def trig(r, carry):
                for mixed in range(2):
                    for o in range(8):
                        at = (block(o) if odd else o, *quarter(held, mixed), rows_of(r))
                        angle = gamma * (cost if odd else cost_swap)[at]
                        cos_buf[held, mixed * 8 + o, rows_of(r), :] = jnp.cos(angle)
                        sin_buf[held, mixed * 8 + o, rows_of(r), :] = jnp.sin(angle)
                return carry

            lax.fori_loop(0, 8, trig, 0)

            def sub_step(sub, carry):
                for mixed in range(2):
                    wait_all(recv, recv_sem, (source, *quarter(held, mixed), sub), arrived)

                def slots(i, carry):
                    r = sub * PER_SUB + i
                    cos_phase = [cos_buf[held, o, rows_of(r), :] for o in range(16)]
                    sin_phase = [sin_buf[held, o, rows_of(r), :] for o in range(16)]
                    old = [[recv[(source, *quarter(held, mixed), sub, o, c, rows_of(i))]
                            for mixed in range(2) for o in range(8)] for c in range(2)]
                    old_re, old_im = rotate(*old, cos_prev, sin_prev)
                    re = [r * c + i * s for r, i, c, s in zip(old_re, old_im, cos_phase, sin_phase)]
                    im = [i * c - r * s for r, i, c, s in zip(old_re, old_im, cos_phase, sin_phase)]
                    re, im = rotate(re, im, cos_half, sin_half)
                    re, im = sublane_rotate(re, im, cos_half, sin_half)
                    put_rows(i, re, im)
                    return carry

                lax.fori_loop(0, PER_SUB, slots, 0)
                work[held, sub] = lanes(2 * LANES)
                return carry

            lax.fori_loop(0, SUB, sub_step, 0)

            if drained:
                for mixed in range(2):
                    for sub in range(SUB):
                        wait_all(send, send_sem, (target, *quarter(held, mixed), sub), drained)

            def quarters(mixed, carry):
                emit(held, mixed, target, *quarter(held, mixed), cos_half, sin_half, SEND_ORDER, lambda o: o, (0,))
                return carry

            lax.fori_loop(0, 2, quarters, 0)
            return carry

        lax.fori_loop(0, 2, half, 0)

    first_layer()
    run_layer(1, False, 6, 0)
    run_layer(2, True, 7, 6)

    def layer_pair(i, carry):
        run_layer(2 * i + 3, False, 7, 7)
        run_layer(2 * i + 4, True, 7, 7)
        return carry

    lax.fori_loop(0, LAYERS // 2 - 2, layer_pair, 0)
    run_layer(LAYERS - 1, False, 7, 7)

    cos_half, sin_half = half_angle(LAYERS - 1)
    energy_part[...] = jnp.zeros((8, LANES), jnp.float32)

    def slot_gates(a, b, sub, i):
        return rotate(*[[recv[0, a, b, sub, o, c, rows_of(i), :] for o in range(8)] for c in range(2)],
                      cos_half, sin_half)

    def early_half(a, carry):
        def early_sub(sub, carry):
            wait_all(recv, recv_sem, (0, a, 0, sub), 7)

            def slots(i, carry):
                for c, values in enumerate(slot_gates(a, 0, sub, i)):
                    for o in range(8):
                        recv[0, a, 0, sub, o, c, rows_of(i), :] = values[o]
                return carry

            lax.fori_loop(0, PER_SUB, slots, 0)
            return carry

        lax.fori_loop(0, SUB, early_sub, 0)
        return carry

    lax.fori_loop(0, 2, early_half, 0)

    def final_half(a, carry):
        def final_sub(sub, carry):
            wait_all(recv, recv_sem, (0, a, 1, sub), 7)

            def slots(i, carry):
                r = sub * PER_SUB + i
                re, im = slot_gates(a, 1, sub, i)
                total = energy_part[...]
                for o in range(8):
                    early = [recv[0, a, 0, sub, o, c, rows_of(i), :] for c in range(2)]
                    pair_re, pair_im = rotate([early[0], re[o]], [early[1], im[o]], cos_half, sin_half)
                    for b in range(2):
                        at = (block(o), a, b, rows_of(r))
                        x, y = pair_re[b], pair_im[b]
                        out_re[at] = x
                        out_im[at] = y
                        total = total + cost[at] * (x * x + y * y)
                energy_part[...] = total
                return carry

            lax.fori_loop(0, PER_SUB, slots, 0, unroll=True)
            return carry

        lax.fori_loop(0, SUB, final_sub, 0)
        return carry

    lax.fori_loop(0, 2, final_half, 0)

    me = block(0)
    energy_row[...] = jnp.sum(energy_part[...], axis=0, keepdims=True)
    energy_all[me] = energy_row[...]

    def drain(par):
        for a in range(2):
            for b in range(2):
                for sub in range(SUB):
                    wait_all(send, send_sem, (par, a, b, sub), 7)

    for a in range(2):
        for sub in range(SUB):
            wait_bytes(cost.at[:, a, :, pl.ds(sub * 8 * PER_SUB, 8 * PER_SUB)], near_send.at[a, sub])
    wait_bytes(cost_swap.at[pl.ds(0, 6)], cost_send)
    for offset in (7, 5, 6, 4, 3, 1, 2):
        remote(energy_row, energy_all.at[me], e_send, e_recv, offset)
    drain(0)
    drain(1)
    wait_bytes(energy_all.at[pl.ds(0, 7)], e_send)
    wait_bytes(energy_all.at[pl.ds(0, 7)], e_recv)


def write_out(energy_all, in_re, in_im, energy, out_re, out_im, value, sem):
    copies = [pltpu.make_async_copy(in_re, out_re, sem.at[0]), pltpu.make_async_copy(in_im, out_im, sem.at[1])]
    for copy in copies:
        copy.start()
    total = energy_all[0]
    for i in range(1, 8):
        total = total + energy_all[i]
    value[0] = jnp.sum(total) * (1.0 / (1 << 21))
    copies.append(pltpu.make_async_copy(value, energy, sem.at[2]))
    copies[2].start()
    for copy in copies:
        copy.wait()


def solution(mesh):
    state_spec = P(('inst', 'qx', 'qy'))

    def device_body(cost_local, gammas, betas):
        local_len = cost_local.shape[0]
        shape = (8, 2, 2, local_len // (32 * LANES), LANES)
        f32 = jnp.float32
        vmem = pl.BlockSpec(memory_space=pltpu.VMEM)
        dma = pltpu.SemaphoreType.DMA
        parts = (2, 2, 2, SUB, 8, 2, 8 * PER_SUB, LANES)
        hbm = pl.BlockSpec(memory_space=pl.ANY)
        results = pl.pallas_call(
            kernel,
            out_shape=(pltpu.VMEM((8, 1, LANES), f32), pltpu.VMEM(shape, f32), pltpu.VMEM(shape, f32)),
            in_specs=[hbm, hbm, hbm],
            out_specs=(vmem, vmem, vmem),
            scratch_shapes=[
                pltpu.VMEM(shape, f32), pltpu.VMEM(shape, f32), pltpu.VMEM(shape, f32),
                pltpu.VMEM(parts, f32), pltpu.VMEM(parts, f32),
                pltpu.VMEM((2, 4, 2 * LANES, 2 * LANES), f32),
                pltpu.VMEM((2, 16, 64, LANES), f32), pltpu.VMEM((2, 16, 64, LANES), f32),
                pltpu.VMEM((16, 8, LANES), f32), pltpu.VMEM((16, 8, LANES), f32),
                pltpu.VMEM((4 * LANES, 2 * LANES), f32), pltpu.VMEM((2 * LANES, 2 * LANES), f32),
                pltpu.VMEM((8, LANES), f32), pltpu.VMEM((1, LANES), f32),
                pltpu.SMEM((LAYERS,), f32), pltpu.SMEM((LAYERS,), f32), dma((2,)), pltpu.SemaphoreType.REGULAR((2,)),
                dma((SUB,)), dma((2, SUB)), dma((2, SUB)), dma, dma,
                dma((2, 2, 2, SUB)), dma((2, 2, 2, SUB)),
                dma, dma,
            ],
            compiler_params=pltpu.CompilerParams(collective_id=0, has_side_effects=True),
            name='qaoa',
        )(cost_local.reshape(shape), gammas, betas)
        energy, state_re, state_im = pl.pallas_call(
            write_out,
            out_shape=(jax.ShapeDtypeStruct((1,), f32),
                       jax.ShapeDtypeStruct(shape, f32), jax.ShapeDtypeStruct(shape, f32)),
            in_specs=[vmem, vmem, vmem],
            out_specs=(hbm, hbm, hbm),
            scratch_shapes=[pltpu.SMEM((1,), f32), dma((3,))],
            name='write_out',
        )(*[pltpu.with_memory_space_constraint(value, pltpu.VMEM) for value in results])
        return energy, state_re.reshape(local_len), state_im.reshape(local_len)

    return jax.shard_map(device_body, mesh=mesh, in_specs=(state_spec, P(), P()),
                         out_specs=(P('inst'), state_spec, state_spec), check_vma=False)
```

```python
import jax
import jax.numpy as jnp
from jax import lax
from jax.experimental import pallas as pl
from jax.experimental.pallas import tpu as pltpu
from jax.sharding import PartitionSpec as P

LANES = 128
LAYERS = 8
SUB = 4
PER_SUB = 8 // SUB
SEND_ORDER = (5, 7, 4, 6, 1, 3, 2)
NEAR = (4, 1)


def rotate(re, im, cos_half, sin_half, steps=None):
    count = len(re)
    for step in steps or [1 << i for i in range(count.bit_length() - 1)]:
        new_re = [cos_half * re[i] + sin_half * im[i ^ step] for i in range(count)]
        new_im = [cos_half * im[i] - sin_half * re[i ^ step] for i in range(count)]
        re, im = new_re, new_im
    return re, im


def sublane_rotate(re, im, cos_half, sin_half):
    row = lax.broadcasted_iota(jnp.int32, (8, LANES), 0)
    for step in (1, 2, 4):
        bit_set = (row & step) != 0

        def flip(value):
            down = pltpu.roll(value, step, 0)
            if step == 4:
                return down
            return jnp.where(bit_set, down, pltpu.roll(value, 8 - step, 0))

        flip_re = [flip(value) for value in re]
        flip_im = [flip(value) for value in im]
        re, im = ([cos_half * r + sin_half * fi for r, fi in zip(re, flip_im)],
                  [cos_half * i - sin_half * fr for i, fr in zip(im, flip_re)])
    return re, im


def lane_matrix(cos_half, sin_half):
    row = lax.broadcasted_iota(jnp.int32, (LANES, LANES), 0)
    col = lax.broadcasted_iota(jnp.int32, (LANES, LANES), 1)
    diff = row ^ col
    cos_full = jnp.broadcast_to(cos_half[0:1], (LANES, LANES))
    sin_full = jnp.broadcast_to(sin_half[0:1], (LANES, LANES))
    mag = jnp.ones((LANES, LANES), jnp.float32)
    weight = jnp.zeros((LANES, LANES), jnp.int32)
    for bit in range(7):
        on = (diff >> bit) & 1
        mag = mag * jnp.where(on == 1, sin_full, cos_full)
        weight = weight + on
    quarter = weight & 3
    zero = jnp.zeros_like(mag)
    real = jnp.where(quarter == 0, mag, jnp.where(quarter == 2, -mag, zero))
    imag = jnp.where(quarter == 1, -mag, jnp.where(quarter == 3, mag, zero))
    return real, imag


def kernel(cost_hbm, gammas_hbm, betas_hbm, energy_all, out_re, out_im,
           cost, cost_near, cost_swap, recv, send, work, cos_buf, sin_buf, cos_near, sin_near,
           rows_in, matrix, energy_part, energy_row, gammas, betas, angle_in, near_in, cost_in, near_send, near_recv, cost_send, cost_recv,
           send_sem, recv_sem, e_send, e_recv):
    qx = lax.axis_index('qx')
    qy = lax.axis_index('qy')
    bits = (qy, qx % 2, qx // 2)

    def flipped(offset):
        return [1 - bit if (offset >> i) & 1 else bit for i, bit in enumerate(bits)]

    def block(offset):
        y, core, x = flipped(offset)
        return (x * 2 + core) * 2 + y

    def peer(offset):
        y, core, x = flipped(offset)
        return {'qy': y, 'qx': x * 2 + core}

    def remote(source, target, send_at, recv_at, offset):
        pltpu.make_async_remote_copy(
            src_ref=source, dst_ref=target, send_sem=send_at, recv_sem=recv_at,
            device_id=peer(offset), device_id_type=pl.DeviceIdType.MESH).start()

    barrier = pltpu.get_barrier_semaphore()

    def signal_next(sem):
        for offset in (4, 1, 2):
            pl.semaphore_signal(sem, inc=1, device_id=peer(offset), device_id_type=pl.DeviceIdType.MESH)

    signal_next(barrier)
    loads = [pltpu.make_async_copy(cost_hbm.at[:, :, :, pl.ds(sub * 8 * PER_SUB, 8 * PER_SUB)],
                                   cost.at[:, :, :, pl.ds(sub * 8 * PER_SUB, 8 * PER_SUB)], cost_in.at[sub])
             for sub in range(SUB)]
    for load in loads:
        load.start()
    angle_loads = [pltpu.make_async_copy(gammas_hbm, gammas, angle_in.at[0]),
                   pltpu.make_async_copy(betas_hbm, betas, angle_in.at[1])]
    for load in angle_loads:
        load.start()
    pl.semaphore_wait(barrier, 3)

    def half_angle(layer):
        angle = jnp.full((8, LANES), 0.5 * betas[layer], jnp.float32)
        return jnp.cos(angle), jnp.sin(angle)

    def wait_bytes(part, sem):
        pltpu.make_async_copy(part, part, sem).wait()

    def wait_all(buffer, sem, at, count):
        wait_bytes(buffer.at[(*at, pl.ds(0, count))], sem.at[at])

    def rows_of(r):
        return pl.ds(pl.multiple_of(r * 8, 8), 8)

    def set_matrix(cos_half, sin_half):
        real, imag = lane_matrix(cos_half, sin_half)
        matrix[0:LANES, 0:LANES] = real
        matrix[0:LANES, LANES:] = imag
        matrix[LANES:, 0:LANES] = -imag
        matrix[LANES:, LANES:] = real

    def put_rows(i, re, im, base=0):
        for o in range(16):
            at = pl.multiple_of(base + o * 16 + i * 8, 8)
            rows_in[pl.ds(at, 8), 0:LANES] = re[o]
            rows_in[pl.ds(at, 8), LANES:] = im[o]

    def lanes(count):
        return lax.dot(rows_in[0:count, :], matrix[...],
                       precision=lax.Precision.HIGHEST, preferred_element_type=jnp.float32)

    def emit(held, mixed, target, a, b, cos_half, sin_half, order, route, local):
        def across(o, buffer):
            def part(r, c):
                at = pl.multiple_of((mixed * 8 + o) * 16 + (r % 2) * 8, 8)
                return work[held, r // 2, pl.ds(at, 8), c * LANES:(c + 1) * LANES]

            re = [part(r, 0) for r in range(8)]
            im = [part(r, 1) for r in range(8)]
            re, im = rotate(re, im, cos_half, sin_half)
            for r in range(8):
                row = (r % PER_SUB) * 8
                buffer[target, a, b, r // PER_SUB, o, 0, row:row + 8, :] = re[r]
                buffer[target, a, b, r // PER_SUB, o, 1, row:row + 8, :] = im[r]

        def body(o, carry):
            across(o, send)
            return carry

        lax.fori_loop(1, 8, body, 0)
        for o in local:
            across(o, recv)
        for sub in range(SUB):
            at = (target, a, b, sub)
            for o in order:
                remote(send.at[(*at, o)], recv.at[(*at, o)], send_sem.at[at], recv_sem.at[at], route(o))

    def first_layer():
        def sub_rows(sub):
            return pl.ds(pl.multiple_of(sub * 8 * PER_SUB, 8), 8 * PER_SUB)

        for sub in range(SUB):
            loads[sub].wait()
            for a in range(2):
                remote(cost.at[:, a, :, sub_rows(sub)], cost_near.at[:, a, :, sub_rows(sub)],
                       near_send, near_recv.at[a, sub], NEAR[a])
        signal_next(near_in.at[0])
        for load in angle_loads:
            load.wait()
        gamma = gammas[0]
        cos_half, sin_half = half_angle(0)
        set_matrix(cos_half, sin_half)

        def own_trig(r, carry):
            for a in range(2):
                for b in range(2):
                    for o in range(8):
                        angle = gamma * cost[block(o), a, b, rows_of(r), :]
                        cos_buf[a, b * 8 + o, rows_of(r), :] = jnp.cos(angle)
                        sin_buf[a, b * 8 + o, rows_of(r), :] = jnp.sin(angle)
            return carry

        for round_id in range(2):
            lax.fori_loop(4 * round_id, 4 * round_id + 4, own_trig, 0)
            pl.semaphore_wait(near_in.at[round_id], 3)
            if round_id == 0:
                signal_next(near_in.at[1])
        for a in range(2):
            for o in range(1, 8):
                if not o & NEAR[a]:
                    remote(cost.at[block(o), a], cost_swap.at[o, a], cost_send, cost_recv, o)

        def sub_step(sub, carry):
            for a in range(2):
                bit = NEAR[a]
                part = cost_near.at[:, a, :, sub_rows(sub)]
                wait_bytes(part, near_recv.at[a, sub])
                for o in range(1, 8):
                    if not o & bit:
                        remote(cost_near.at[block(o), a, :, sub_rows(sub)],
                               cost_swap.at[o | bit, a, :, sub_rows(sub)], cost_send, cost_recv, o)

                def slots(i, carry):
                    r = sub * PER_SUB + i
                    for b in range(2):
                        for o in range(8):
                            angle = gamma * cost_near[block(o), a, b, rows_of(r), :]
                            cos_near[b * 8 + o] = jnp.cos(angle)
                            sin_near[b * 8 + o] = jnp.sin(angle)
                    re, im = [None] * 16, [None] * 16
                    for b in range(2):
                        for o in range(8):
                            if o & bit:
                                continue
                            here, there = b * 8 + o, b * 8 + (o | bit)
                            for slot, cos_at, sin_at in (
                                    (here, lambda k: cos_buf[a, k, rows_of(r), :], lambda k: sin_buf[a, k, rows_of(r), :]),
                                    (there, lambda k: cos_near[k], lambda k: sin_near[k])):
                                re[slot] = cos_half * cos_at(here) - sin_half * sin_at(there)
                                im[slot] = -(cos_half * sin_at(here)) - sin_half * cos_at(there)
                    re, im = rotate(re, im, cos_half, sin_half, [step for step in (1, 2, 4, 8) if step != bit])
                    re, im = sublane_rotate(re, im, cos_half, sin_half)
                    put_rows(i, re, im, a * 2 * LANES)
                    return carry

                lax.fori_loop(0, PER_SUB, slots, 0)
            rows = lanes(4 * LANES)
            for a in range(2):
                work[a, sub] = rows[a * 2 * LANES:(a + 1) * 2 * LANES]
            return carry

        lax.fori_loop(0, SUB, sub_step, 0)

        def quarters(b, carry):
            for a in range(2):
                bit = NEAR[a]
                emit(a, b, 1, a, b, cos_half, sin_half,
                     [o for o in (3, 6, 7, 1, 4, 5, 2) if o & ~bit], lambda o: o & ~bit, (0, bit))
            return carry

        lax.fori_loop(0, 2, quarters, 0)
        cost_swap[0] = cost[block(0)]
        for a in range(2):
            cost_swap[NEAR[a], a] = cost_near[block(0), a]
        wait_bytes(cost_swap.at[pl.ds(0, 6)], cost_recv)

    def run_layer(layer, odd, arrived, drained):
        source, target = (0, 1) if odd else (1, 0)

        def quarter(held, mixed):
            return (held, mixed) if odd else (mixed, held)

        cos_half, sin_half = half_angle(layer)
        cos_prev, sin_prev = half_angle(layer - 1)
        gamma = gammas[layer]
        set_matrix(cos_half, sin_half)

        def half(held, carry):
            def trig(r, carry):
                for mixed in range(2):
                    for o in range(8):
                        at = (block(o) if odd else o, *quarter(held, mixed), rows_of(r))
                        angle = gamma * (cost if odd else cost_swap)[at]
                        cos_buf[held, mixed * 8 + o, rows_of(r), :] = jnp.cos(angle)
                        sin_buf[held, mixed * 8 + o, rows_of(r), :] = jnp.sin(angle)
                return carry

            lax.fori_loop(0, 8, trig, 0)

            def sub_step(sub, carry):
                for mixed in range(2):
                    wait_all(recv, recv_sem, (source, *quarter(held, mixed), sub), arrived)

                def slots(i, carry):
                    r = sub * PER_SUB + i
                    cos_phase = [cos_buf[held, o, rows_of(r), :] for o in range(16)]
                    sin_phase = [sin_buf[held, o, rows_of(r), :] for o in range(16)]
                    old = [[recv[(source, *quarter(held, mixed), sub, o, c, rows_of(i))]
                            for mixed in range(2) for o in range(8)] for c in range(2)]
                    old_re, old_im = rotate(*old, cos_prev, sin_prev)
                    re = [r * c + i * s for r, i, c, s in zip(old_re, old_im, cos_phase, sin_phase)]
                    im = [i * c - r * s for r, i, c, s in zip(old_re, old_im, cos_phase, sin_phase)]
                    re, im = rotate(re, im, cos_half, sin_half)
                    re, im = sublane_rotate(re, im, cos_half, sin_half)
                    put_rows(i, re, im)
                    return carry

                lax.fori_loop(0, PER_SUB, slots, 0)
                work[held, sub] = lanes(2 * LANES)
                return carry

            lax.fori_loop(0, SUB, sub_step, 0)

            if drained:
                for mixed in range(2):
                    for sub in range(SUB):
                        wait_all(send, send_sem, (target, *quarter(held, mixed), sub), drained)

            def quarters(mixed, carry):
                emit(held, mixed, target, *quarter(held, mixed), cos_half, sin_half, SEND_ORDER, lambda o: o, (0,))
                return carry

            lax.fori_loop(0, 2, quarters, 0)
            return carry

        lax.fori_loop(0, 2, half, 0)

    first_layer()
    run_layer(1, False, 6, 0)
    run_layer(2, True, 7, 6)

    def layer_pair(i, carry):
        run_layer(2 * i + 3, False, 7, 7)
        run_layer(2 * i + 4, True, 7, 7)
        return carry

    lax.fori_loop(0, LAYERS // 2 - 2, layer_pair, 0)
    run_layer(LAYERS - 1, False, 7, 7)

    cos_half, sin_half = half_angle(LAYERS - 1)
    energy_part[...] = jnp.zeros((8, LANES), jnp.float32)

    def slot_gates(a, b, sub, i):
        return rotate(*[[recv[0, a, b, sub, o, c, rows_of(i), :] for o in range(8)] for c in range(2)],
                      cos_half, sin_half)

    def early_half(a, carry):
        def early_sub(sub, carry):
            wait_all(recv, recv_sem, (0, a, 0, sub), 7)

            def slots(i, carry):
                for c, values in enumerate(slot_gates(a, 0, sub, i)):
                    for o in range(8):
                        recv[0, a, 0, sub, o, c, rows_of(i), :] = values[o]
                return carry

            lax.fori_loop(0, PER_SUB, slots, 0)
            return carry

        lax.fori_loop(0, SUB, early_sub, 0)
        return carry

    lax.fori_loop(0, 2, early_half, 0)

    def final_half(a, carry):
        def final_sub(sub, carry):
            wait_all(recv, recv_sem, (0, a, 1, sub), 7)

            def slots(i, carry):
                r = sub * PER_SUB + i
                re, im = slot_gates(a, 1, sub, i)
                total = energy_part[...]
                for o in range(8):
                    early = [recv[0, a, 0, sub, o, c, rows_of(i), :] for c in range(2)]
                    pair_re, pair_im = rotate([early[0], re[o]], [early[1], im[o]], cos_half, sin_half)
                    for b in range(2):
                        at = (block(o), a, b, rows_of(r))
                        x, y = pair_re[b], pair_im[b]
                        out_re[at] = x
                        out_im[at] = y
                        total = total + cost[at] * (x * x + y * y)
                energy_part[...] = total
                return carry

            lax.fori_loop(0, PER_SUB, slots, 0, unroll=True)
            return carry

        lax.fori_loop(0, SUB, final_sub, 0)
        return carry

    lax.fori_loop(0, 2, final_half, 0)

    me = block(0)
    energy_row[...] = jnp.sum(energy_part[...], axis=0, keepdims=True)
    energy_all[me] = energy_row[...]

    def drain(par):
        for a in range(2):
            for b in range(2):
                for sub in range(SUB):
                    wait_all(send, send_sem, (par, a, b, sub), 7)

    wait_bytes(cost, near_send)
    wait_bytes(cost_swap.at[pl.ds(0, 6)], cost_send)
    for offset in (7, 5, 6, 4, 3, 1, 2):
        remote(energy_row, energy_all.at[me], e_send, e_recv, offset)
    drain(0)
    drain(1)
    wait_bytes(energy_all.at[pl.ds(0, 7)], e_send)
    wait_bytes(energy_all.at[pl.ds(0, 7)], e_recv)


def write_out(energy_all, in_re, in_im, energy, out_re, out_im, value, sem):
    copies = [pltpu.make_async_copy(in_re, out_re, sem.at[0]), pltpu.make_async_copy(in_im, out_im, sem.at[1])]
    for copy in copies:
        copy.start()
    total = energy_all[0]
    for i in range(1, 8):
        total = total + energy_all[i]
    value[0] = jnp.sum(total) * (1.0 / (1 << 21))
    copies.append(pltpu.make_async_copy(value, energy, sem.at[2]))
    copies[2].start()
    for copy in copies:
        copy.wait()


def solution(mesh):
    state_spec = P(('inst', 'qx', 'qy'))

    def device_body(cost_local, gammas, betas):
        local_len = cost_local.shape[0]
        shape = (8, 2, 2, local_len // (32 * LANES), LANES)
        f32 = jnp.float32
        vmem = pl.BlockSpec(memory_space=pltpu.VMEM)
        dma = pltpu.SemaphoreType.DMA
        parts = (2, 2, 2, SUB, 8, 2, 8 * PER_SUB, LANES)
        hbm = pl.BlockSpec(memory_space=pl.ANY)
        results = pl.pallas_call(
            kernel,
            out_shape=(pltpu.VMEM((8, 1, LANES), f32), pltpu.VMEM(shape, f32), pltpu.VMEM(shape, f32)),
            in_specs=[hbm, hbm, hbm],
            out_specs=(vmem, vmem, vmem),
            scratch_shapes=[
                pltpu.VMEM(shape, f32), pltpu.VMEM(shape, f32), pltpu.VMEM(shape, f32),
                pltpu.VMEM(parts, f32), pltpu.VMEM(parts, f32),
                pltpu.VMEM((2, 4, 2 * LANES, 2 * LANES), f32),
                pltpu.VMEM((2, 16, 64, LANES), f32), pltpu.VMEM((2, 16, 64, LANES), f32),
                pltpu.VMEM((16, 8, LANES), f32), pltpu.VMEM((16, 8, LANES), f32),
                pltpu.VMEM((4 * LANES, 2 * LANES), f32), pltpu.VMEM((2 * LANES, 2 * LANES), f32),
                pltpu.VMEM((8, LANES), f32), pltpu.VMEM((1, LANES), f32),
                pltpu.SMEM((LAYERS,), f32), pltpu.SMEM((LAYERS,), f32), dma((2,)), pltpu.SemaphoreType.REGULAR((2,)),
                dma((SUB,)), dma, dma((2, SUB)), dma, dma,
                dma((2, 2, 2, SUB)), dma((2, 2, 2, SUB)),
                dma, dma,
            ],
            compiler_params=pltpu.CompilerParams(collective_id=0, has_side_effects=True),
            name='qaoa',
        )(cost_local.reshape(shape), gammas, betas)
        energy, state_re, state_im = pl.pallas_call(
            write_out,
            out_shape=(jax.ShapeDtypeStruct((1,), f32),
                       jax.ShapeDtypeStruct(shape, f32), jax.ShapeDtypeStruct(shape, f32)),
            in_specs=[vmem, vmem, vmem],
            out_specs=(hbm, hbm, hbm),
            scratch_shapes=[pltpu.SMEM((1,), f32), dma((3,))],
            name='write_out',
        )(*[pltpu.with_memory_space_constraint(value, pltpu.VMEM) for value in results])
        return energy, state_re.reshape(local_len), state_im.reshape(local_len)

    return jax.shard_map(device_body, mesh=mesh, in_specs=(state_spec, P(), P()),
                         out_specs=(P('inst'), state_spec, state_spec), check_vma=False)
```

```python
import jax
import jax.numpy as jnp
from jax import lax
from jax.experimental import pallas as pl
from jax.experimental.pallas import tpu as pltpu
from jax.sharding import PartitionSpec as P

LANES = 128
LAYERS = 8
SUB = 4
PER_SUB = 8 // SUB
SEND_ORDER = (5, 7, 4, 6, 1, 3, 2)
NEAR = (4, 1)


def rotate(re, im, cos_half, sin_half, steps=None):
    count = len(re)
    for step in steps or [1 << i for i in range(count.bit_length() - 1)]:
        new_re = [cos_half * re[i] + sin_half * im[i ^ step] for i in range(count)]
        new_im = [cos_half * im[i] - sin_half * re[i ^ step] for i in range(count)]
        re, im = new_re, new_im
    return re, im


def sublane_rotate(re, im, cos_half, sin_half):
    row = lax.broadcasted_iota(jnp.int32, (8, LANES), 0)
    for step in (1, 2, 4):
        bit_set = (row & step) != 0

        def flip(value):
            down = pltpu.roll(value, step, 0)
            if step == 4:
                return down
            return jnp.where(bit_set, down, pltpu.roll(value, 8 - step, 0))

        flip_re = [flip(value) for value in re]
        flip_im = [flip(value) for value in im]
        re, im = ([cos_half * r + sin_half * fi for r, fi in zip(re, flip_im)],
                  [cos_half * i - sin_half * fr for i, fr in zip(im, flip_re)])
    return re, im


def lane_matrix(cos_half, sin_half):
    row = lax.broadcasted_iota(jnp.int32, (LANES, LANES), 0)
    col = lax.broadcasted_iota(jnp.int32, (LANES, LANES), 1)
    diff = row ^ col
    cos_full = jnp.broadcast_to(cos_half[0:1], (LANES, LANES))
    sin_full = jnp.broadcast_to(sin_half[0:1], (LANES, LANES))
    mag = jnp.ones((LANES, LANES), jnp.float32)
    weight = jnp.zeros((LANES, LANES), jnp.int32)
    for bit in range(7):
        on = (diff >> bit) & 1
        mag = mag * jnp.where(on == 1, sin_full, cos_full)
        weight = weight + on
    quarter = weight & 3
    zero = jnp.zeros_like(mag)
    real = jnp.where(quarter == 0, mag, jnp.where(quarter == 2, -mag, zero))
    imag = jnp.where(quarter == 1, -mag, jnp.where(quarter == 3, mag, zero))
    return real, imag


def kernel(cost_hbm, gammas_hbm, betas_hbm, energy_all, out_re, out_im,
           cost, cost_near, cost_swap, recv, send, work, cos_buf, sin_buf, cos_near, sin_near,
           rows_in, matrix, energy_part, energy_row, gammas, betas, angle_in, near_in, cost_in, near_send, near_recv, cost_send, cost_recv,
           send_sem, recv_sem, e_send, e_recv):
    qx = lax.axis_index('qx')
    qy = lax.axis_index('qy')
    bits = (qy, qx % 2, qx // 2)

    def flipped(offset):
        return [1 - bit if (offset >> i) & 1 else bit for i, bit in enumerate(bits)]

    def block(offset):
        y, core, x = flipped(offset)
        return (x * 2 + core) * 2 + y

    def peer(offset):
        y, core, x = flipped(offset)
        return {'qy': y, 'qx': x * 2 + core}

    def remote(source, target, send_at, recv_at, offset):
        pltpu.make_async_remote_copy(
            src_ref=source, dst_ref=target, send_sem=send_at, recv_sem=recv_at,
            device_id=peer(offset), device_id_type=pl.DeviceIdType.MESH).start()

    barrier = pltpu.get_barrier_semaphore()

    def signal_next(sem):
        for offset in (4, 1, 2):
            pl.semaphore_signal(sem, inc=1, device_id=peer(offset), device_id_type=pl.DeviceIdType.MESH)

    signal_next(barrier)
    loads = [pltpu.make_async_copy(cost_hbm.at[:, :, :, pl.ds(sub * 8 * PER_SUB, 8 * PER_SUB)],
                                   cost.at[:, :, :, pl.ds(sub * 8 * PER_SUB, 8 * PER_SUB)], cost_in.at[sub])
             for sub in range(SUB)]
    for load in loads:
        load.start()
    angle_loads = [pltpu.make_async_copy(gammas_hbm, gammas, angle_in.at[0]),
                   pltpu.make_async_copy(betas_hbm, betas, angle_in.at[1])]
    for load in angle_loads:
        load.start()
    pl.semaphore_wait(barrier, 3)

    def half_angle(layer):
        angle = jnp.full((8, LANES), 0.5 * betas[layer], jnp.float32)
        return jnp.cos(angle), jnp.sin(angle)

    def wait_bytes(part, sem):
        pltpu.make_async_copy(part, part, sem).wait()

    def wait_all(buffer, sem, at, count):
        wait_bytes(buffer.at[(*at, pl.ds(0, count))], sem.at[at])

    def rows_of(r):
        return pl.ds(pl.multiple_of(r * 8, 8), 8)

    def set_matrix(cos_half, sin_half):
        real, imag = lane_matrix(cos_half, sin_half)
        matrix[0:LANES, 0:LANES] = real
        matrix[0:LANES, LANES:] = imag
        matrix[LANES:, 0:LANES] = -imag
        matrix[LANES:, LANES:] = real

    def put_rows(i, re, im, base=0):
        for o in range(16):
            at = pl.multiple_of(base + o * 16 + i * 8, 8)
            rows_in[pl.ds(at, 8), 0:LANES] = re[o]
            rows_in[pl.ds(at, 8), LANES:] = im[o]

    def lanes(count):
        return lax.dot(rows_in[0:count, :], matrix[...],
                       precision=lax.Precision.HIGHEST, preferred_element_type=jnp.float32)

    def emit(held, mixed, target, a, b, cos_half, sin_half, order, route, local):
        def across(o, buffer):
            def part(r, c):
                at = pl.multiple_of((mixed * 8 + o) * 16 + (r % 2) * 8, 8)
                return work[held, r // 2, pl.ds(at, 8), c * LANES:(c + 1) * LANES]

            re = [part(r, 0) for r in range(8)]
            im = [part(r, 1) for r in range(8)]
            re, im = rotate(re, im, cos_half, sin_half)
            for r in range(8):
                row = (r % PER_SUB) * 8
                buffer[target, a, b, r // PER_SUB, o, 0, row:row + 8, :] = re[r]
                buffer[target, a, b, r // PER_SUB, o, 1, row:row + 8, :] = im[r]

        def body(o, carry):
            across(o, send)
            return carry

        lax.fori_loop(1, 8, body, 0)
        for o in local:
            across(o, recv)
        for sub in range(SUB):
            at = (target, a, b, sub)
            for o in order:
                remote(send.at[(*at, o)], recv.at[(*at, o)], send_sem.at[at], recv_sem.at[at], route(o))

    def first_layer():
        def sub_rows(sub):
            return pl.ds(pl.multiple_of(sub * 8 * PER_SUB, 8), 8 * PER_SUB)

        for sub in range(SUB):
            loads[sub].wait()
            for a in range(2):
                remote(cost.at[:, a, :, sub_rows(sub)], cost_near.at[:, a, :, sub_rows(sub)],
                       near_send, near_recv.at[a, sub], NEAR[a])
        signal_next(near_in.at[0])
        for load in angle_loads:
            load.wait()
        gamma = gammas[0]
        cos_half, sin_half = half_angle(0)
        set_matrix(cos_half, sin_half)

        def own_trig(r, carry):
            for a in range(2):
                for b in range(2):
                    for o in range(8):
                        angle = gamma * cost[block(o), a, b, rows_of(r), :]
                        cos_buf[a, b * 8 + o, rows_of(r), :] = jnp.cos(angle)
                        sin_buf[a, b * 8 + o, rows_of(r), :] = jnp.sin(angle)
            return carry

        for round_id in range(2):
            lax.fori_loop(4 * round_id, 4 * round_id + 4, own_trig, 0)
            pl.semaphore_wait(near_in.at[round_id], 3)
            if round_id == 0:
                signal_next(near_in.at[1])
        for a in range(2):
            for o in range(1, 8):
                if not o & NEAR[a]:
                    remote(cost.at[block(o), a], cost_swap.at[o, a], cost_send, cost_recv, o)

        def sub_step(sub, carry):
            for a in range(2):
                bit = NEAR[a]
                part = cost_near.at[:, a, :, sub_rows(sub)]
                wait_bytes(part, near_recv.at[a, sub])
                for o in range(1, 8):
                    if not o & bit:
                        remote(cost_near.at[block(o), a, :, sub_rows(sub)],
                               cost_swap.at[o | bit, a, :, sub_rows(sub)], cost_send, cost_recv, o)

                def slots(i, carry):
                    r = sub * PER_SUB + i
                    for b in range(2):
                        for o in range(8):
                            angle = gamma * cost_near[block(o), a, b, rows_of(r), :]
                            cos_near[b * 8 + o] = jnp.cos(angle)
                            sin_near[b * 8 + o] = jnp.sin(angle)
                    re, im = [None] * 16, [None] * 16
                    for b in range(2):
                        for o in range(8):
                            if o & bit:
                                continue
                            here, there = b * 8 + o, b * 8 + (o | bit)
                            for slot, cos_at, sin_at in (
                                    (here, lambda k: cos_buf[a, k, rows_of(r), :], lambda k: sin_buf[a, k, rows_of(r), :]),
                                    (there, lambda k: cos_near[k], lambda k: sin_near[k])):
                                re[slot] = cos_half * cos_at(here) - sin_half * sin_at(there)
                                im[slot] = -(cos_half * sin_at(here)) - sin_half * cos_at(there)
                    re, im = rotate(re, im, cos_half, sin_half, [step for step in (1, 2, 4, 8) if step != bit])
                    re, im = sublane_rotate(re, im, cos_half, sin_half)
                    put_rows(i, re, im, a * 2 * LANES)
                    return carry

                lax.fori_loop(0, PER_SUB, slots, 0)
            rows = lanes(4 * LANES)
            for a in range(2):
                work[a, sub] = rows[a * 2 * LANES:(a + 1) * 2 * LANES]
            return carry

        lax.fori_loop(0, SUB, sub_step, 0)

        def quarters(b, carry):
            for a in range(2):
                bit = NEAR[a]
                emit(a, b, 1, a, b, cos_half, sin_half,
                     [o for o in (3, 6, 7, 1, 4, 5, 2) if o & ~bit], lambda o: o & ~bit, (0, bit))
            return carry

        lax.fori_loop(0, 2, quarters, 0)
        cost_swap[0] = cost[block(0)]
        for a in range(2):
            cost_swap[NEAR[a], a] = cost_near[block(0), a]
        wait_bytes(cost_swap.at[pl.ds(0, 6)], cost_recv)

    def run_layer(layer, odd, arrived, drained):
        source, target = (0, 1) if odd else (1, 0)

        def quarter(held, mixed):
            return (held, mixed) if odd else (mixed, held)

        cos_half, sin_half = half_angle(layer)
        cos_prev, sin_prev = half_angle(layer - 1)
        gamma = gammas[layer]
        set_matrix(cos_half, sin_half)

        def half(held, carry):
            def trig(r, carry):
                for mixed in range(2):
                    for o in range(8):
                        at = (block(o) if odd else o, *quarter(held, mixed), rows_of(r))
                        angle = gamma * (cost if odd else cost_swap)[at]
                        cos_buf[held, mixed * 8 + o, rows_of(r), :] = jnp.cos(angle)
                        sin_buf[held, mixed * 8 + o, rows_of(r), :] = jnp.sin(angle)
                return carry

            lax.fori_loop(0, 8, trig, 0)

            def sub_step(sub, carry):
                for mixed in range(2):
                    wait_all(recv, recv_sem, (source, *quarter(held, mixed), sub), arrived)

                def slots(i, carry):
                    r = sub * PER_SUB + i
                    cos_phase = [cos_buf[held, o, rows_of(r), :] for o in range(16)]
                    sin_phase = [sin_buf[held, o, rows_of(r), :] for o in range(16)]
                    old = [[recv[(source, *quarter(held, mixed), sub, o, c, rows_of(i))]
                            for mixed in range(2) for o in range(8)] for c in range(2)]
                    old_re, old_im = rotate(*old, cos_prev, sin_prev)
                    re = [r * c + i * s for r, i, c, s in zip(old_re, old_im, cos_phase, sin_phase)]
                    im = [i * c - r * s for r, i, c, s in zip(old_re, old_im, cos_phase, sin_phase)]
                    re, im = rotate(re, im, cos_half, sin_half)
                    re, im = sublane_rotate(re, im, cos_half, sin_half)
                    put_rows(i, re, im)
                    return carry

                lax.fori_loop(0, PER_SUB, slots, 0)
                work[held, sub] = lanes(2 * LANES)
                return carry

            lax.fori_loop(0, SUB, sub_step, 0)

            if drained:
                for mixed in range(2):
                    for sub in range(SUB):
                        wait_all(send, send_sem, (target, *quarter(held, mixed), sub), drained)

            def quarters(mixed, carry):
                emit(held, mixed, target, *quarter(held, mixed), cos_half, sin_half, SEND_ORDER, lambda o: o, (0,))
                return carry

            lax.fori_loop(0, 2, quarters, 0)
            return carry

        lax.fori_loop(0, 2, half, 0)

    first_layer()
    run_layer(1, False, 6, 0)
    run_layer(2, True, 7, 6)

    def layer_pair(i, carry):
        run_layer(2 * i + 3, False, 7, 7)
        run_layer(2 * i + 4, True, 7, 7)
        return carry

    lax.fori_loop(0, LAYERS // 2 - 2, layer_pair, 0)
    run_layer(LAYERS - 1, False, 7, 7)

    cos_half, sin_half = half_angle(LAYERS - 1)
    energy_part[...] = jnp.zeros((8, LANES), jnp.float32)

    def slot_gates(a, b, sub, i):
        return rotate(*[[recv[0, a, b, sub, o, c, rows_of(i), :] for o in range(8)] for c in range(2)],
                      cos_half, sin_half)

    def early_half(a, carry):
        def early_sub(sub, carry):
            wait_all(recv, recv_sem, (0, a, 0, sub), 7)

            def slots(i, carry):
                for c, values in enumerate(slot_gates(a, 0, sub, i)):
                    for o in range(8):
                        recv[0, a, 0, sub, o, c, rows_of(i), :] = values[o]
                return carry

            lax.fori_loop(0, PER_SUB, slots, 0)
            return carry

        lax.fori_loop(0, SUB, early_sub, 0)
        return carry

    lax.fori_loop(0, 2, early_half, 0)

    def final_half(a, carry):
        def final_sub(sub, carry):
            wait_all(recv, recv_sem, (0, a, 1, sub), 7)

            def slots(i, carry):
                r = sub * PER_SUB + i
                re, im = slot_gates(a, 1, sub, i)
                total = energy_part[...]
                for o in range(8):
                    early = [recv[0, a, 0, sub, o, c, rows_of(i), :] for c in range(2)]
                    pair_re, pair_im = rotate([early[0], re[o]], [early[1], im[o]], cos_half, sin_half)
                    for b in range(2):
                        at = (block(o), a, b, rows_of(r))
                        x, y = pair_re[b], pair_im[b]
                        out_re[at] = x
                        out_im[at] = y
                        total = total + cost[at] * (x * x + y * y)
                energy_part[...] = total
                return carry

            lax.fori_loop(0, PER_SUB, slots, 0, unroll=True)
            return carry

        lax.fori_loop(0, SUB, final_sub, 0)
        return carry

    lax.fori_loop(0, 2, final_half, 0)

    me = block(0)
    energy_row[...] = jnp.sum(energy_part[...], axis=0, keepdims=True)
    energy_all[me] = energy_row[...]

    def drain(par):
        for a in range(2):
            for b in range(2):
                for sub in range(SUB):
                    wait_all(send, send_sem, (par, a, b, sub), 7)

    wait_bytes(cost, near_send)
    for offset in (7, 5, 6, 4, 3, 1, 2):
        remote(energy_row, energy_all.at[me], e_send, e_recv, offset)
    drain(0)
    drain(1)
    wait_bytes(cost_swap.at[pl.ds(0, 6)], cost_send)
    wait_bytes(energy_all.at[pl.ds(0, 7)], e_send)
    wait_bytes(energy_all.at[pl.ds(0, 7)], e_recv)


def write_out(energy_all, in_re, in_im, energy, out_re, out_im, value, sem):
    copies = [pltpu.make_async_copy(in_re, out_re, sem.at[0]), pltpu.make_async_copy(in_im, out_im, sem.at[1])]
    for copy in copies:
        copy.start()
    total = energy_all[0]
    for i in range(1, 8):
        total = total + energy_all[i]
    value[0] = jnp.sum(total) * (1.0 / (1 << 21))
    copies.append(pltpu.make_async_copy(value, energy, sem.at[2]))
    copies[2].start()
    for copy in copies:
        copy.wait()


def solution(mesh):
    state_spec = P(('inst', 'qx', 'qy'))

    def device_body(cost_local, gammas, betas):
        local_len = cost_local.shape[0]
        shape = (8, 2, 2, local_len // (32 * LANES), LANES)
        f32 = jnp.float32
        vmem = pl.BlockSpec(memory_space=pltpu.VMEM)
        dma = pltpu.SemaphoreType.DMA
        parts = (2, 2, 2, SUB, 8, 2, 8 * PER_SUB, LANES)
        hbm = pl.BlockSpec(memory_space=pl.ANY)
        results = pl.pallas_call(
            kernel,
            out_shape=(pltpu.VMEM((8, 1, LANES), f32), pltpu.VMEM(shape, f32), pltpu.VMEM(shape, f32)),
            in_specs=[hbm, hbm, hbm],
            out_specs=(vmem, vmem, vmem),
            scratch_shapes=[
                pltpu.VMEM(shape, f32), pltpu.VMEM(shape, f32), pltpu.VMEM(shape, f32),
                pltpu.VMEM(parts, f32), pltpu.VMEM(parts, f32),
                pltpu.VMEM((2, 4, 2 * LANES, 2 * LANES), f32),
                pltpu.VMEM((2, 16, 64, LANES), f32), pltpu.VMEM((2, 16, 64, LANES), f32),
                pltpu.VMEM((16, 8, LANES), f32), pltpu.VMEM((16, 8, LANES), f32),
                pltpu.VMEM((4 * LANES, 2 * LANES), f32), pltpu.VMEM((2 * LANES, 2 * LANES), f32),
                pltpu.VMEM((8, LANES), f32), pltpu.VMEM((1, LANES), f32),
                pltpu.SMEM((LAYERS,), f32), pltpu.SMEM((LAYERS,), f32), dma((2,)), pltpu.SemaphoreType.REGULAR((2,)),
                dma((SUB,)), dma, dma((2, SUB)), dma, dma,
                dma((2, 2, 2, SUB)), dma((2, 2, 2, SUB)),
                dma, dma,
            ],
            compiler_params=pltpu.CompilerParams(collective_id=0, has_side_effects=True),
            name='qaoa',
        )(cost_local.reshape(shape), gammas, betas)
        energy, state_re, state_im = pl.pallas_call(
            write_out,
            out_shape=(jax.ShapeDtypeStruct((1,), f32),
                       jax.ShapeDtypeStruct(shape, f32), jax.ShapeDtypeStruct(shape, f32)),
            in_specs=[vmem, vmem, vmem],
            out_specs=(hbm, hbm, hbm),
            scratch_shapes=[pltpu.SMEM((1,), f32), dma((3,))],
            name='write_out',
        )(*[pltpu.with_memory_space_constraint(value, pltpu.VMEM) for value in results])
        return energy, state_re.reshape(local_len), state_im.reshape(local_len)

    return jax.shard_map(device_body, mesh=mesh, in_specs=(state_spec, P(), P()),
                         out_specs=(P('inst'), state_spec, state_spec), check_vma=False)
```
